8 devices in a mesh: dp: 1 (over z), depth: 2 (over y), col: 2 (over x), row: 2 (over core).
Axes of the slice: x: 2, y: 2, z: 1, core: 2. Of those that a mesh axis runs over, the one named last changes fastest.
Arguments:
- x_in: bfloat16 [32768, 1024], P(('dp', 'depth', 'row'), 'col')
- ln_gamma: float32 [1024], P('col')
- ln_beta: float32 [1024], P('col')
- w_up: bfloat16 [1024, 4096], P('row', 'col')
- b_up: bfloat16 [4096], P('col')
- w_down: bfloat16 [4096, 1024], P('row', 'col')
- b_down: bfloat16 [1024], P('col')
- grad_out: bfloat16 [32768, 1024], P(('dp', 'depth', 'row'), 'col')
Outputs:
- output 1: bfloat16 [32768, 1024], P(('dp', 'depth', 'row'), 'col')
- output 2: bfloat16 [32768, 1024], P(('dp', 'depth', 'row'), 'col')
- output 3: float32 [1024], P(('dp', 'col'))
- output 4: float32 [1024], P(('dp', 'col'))
- output 5: bfloat16 [1024, 4096], P(('dp', 'row'), 'col')
- output 6: float32 [4096], P(('dp', 'col'))
- output 7: bfloat16 [4096, 1024], P(('dp', 'row'), 'col')
- output 8: float32 [1024], P(('dp', 'col'))
All inputs are finite; a program needn't handle non-finite values.
Results may differ from the reference program's by a relative error of at most 0.0111409.
Values are sent between devices in bfloat16 or wider.
A program may use at most 1 GiB of HBM per device.

```python
import jax
import jax.numpy as jnp
from jax import lax

ROWS = 8192
WIDTH = 1024
FFN = 4096
TOKENS = 32768
SEGMENTS = 64
NUM_BLOCKS = TOKENS // ROWS
SEG_WIDTH = WIDTH // SEGMENTS
LN_EPS = 1e-5


def gelu_tanh(values):
    return jax.nn.gelu(values, approximate=True)


def setup_inputs(seed: int = 0, part: int = 0) -> dict:
    base_key = jax.random.key(seed)
    part_key = jax.random.fold_in(base_key, part)
    key_mean, key_scale, key_noise, key_grad = jax.random.split(part_key, 4)
    shared_key = jax.random.key(seed + 1)
    key_gamma, key_beta, key_wup, key_bup, key_wdown, key_bdown = jax.random.split(shared_key, 6)
    seg_mean = jax.random.normal(key_mean, (TOKENS, SEGMENTS), jnp.float32)
    seg_scale = jax.random.uniform(key_scale, (TOKENS, SEGMENTS), jnp.float32, 0.5, 2.0)
    white_noise = jax.random.normal(key_noise, (TOKENS, WIDTH), jnp.float32)
    x_in = jnp.repeat(seg_mean, SEG_WIDTH, axis=1) + jnp.repeat(seg_scale, SEG_WIDTH, axis=1) * white_noise
    grad_out = jax.random.normal(key_grad, (TOKENS, WIDTH), jnp.float32)
    ln_gamma = jax.random.uniform(key_gamma, (WIDTH,), jnp.float32, 0.5, 1.5)
    ln_beta = 0.5 * jax.random.normal(key_beta, (WIDTH,), jnp.float32)
    w_up = jax.random.normal(key_wup, (WIDTH, FFN), jnp.float32) * WIDTH ** -0.5
    b_up = 0.5 * jax.random.normal(key_bup, (FFN,), jnp.float32)
    w_down = jax.random.normal(key_wdown, (FFN, WIDTH), jnp.float32) * FFN ** -0.5
    b_down = 0.5 * jax.random.normal(key_bdown, (WIDTH,), jnp.float32)
    return {
        'x_in': x_in.astype(jnp.bfloat16),
        'ln_gamma': ln_gamma,
        'ln_beta': ln_beta,
        'w_up': w_up.astype(jnp.bfloat16),
        'b_up': b_up.astype(jnp.bfloat16),
        'w_down': w_down.astype(jnp.bfloat16),
        'b_down': b_down.astype(jnp.bfloat16),
        'grad_out': grad_out.astype(jnp.bfloat16),
    }


def block_pass(x_blk, dy_blk, ln_gamma, ln_beta, w_up, b_up, w_down, b_down):
    x_f32 = x_blk.astype(jnp.float32)
    row_mean = jnp.mean(x_f32, axis=1, keepdims=True)
    centered = x_f32 - row_mean
    row_var = jnp.mean(centered * centered, axis=1, keepdims=True)
    inv_std = lax.rsqrt(row_var + LN_EPS)
    x_hat = centered * inv_std
    x_norm = (x_hat * ln_gamma + ln_beta).astype(jnp.bfloat16)
    pre_act = (jnp.dot(x_norm, w_up, preferred_element_type=jnp.float32) + b_up.astype(jnp.float32)).astype(jnp.bfloat16)
    act_f32, gelu_vjp = jax.vjp(gelu_tanh, pre_act.astype(jnp.float32))
    hidden = act_f32.astype(jnp.bfloat16)
    y_blk = (x_f32 + jnp.dot(hidden, w_down, preferred_element_type=jnp.float32) + b_down.astype(jnp.float32)).astype(jnp.bfloat16)
    dy_f32 = dy_blk.astype(jnp.float32)
    sum_w_down = jnp.dot(hidden.T, dy_blk, preferred_element_type=jnp.float32)
    grad_hidden = jnp.dot(dy_blk, w_down.T, preferred_element_type=jnp.float32)
    grad_pre = gelu_vjp(grad_hidden)[0].astype(jnp.bfloat16)
    sum_w_up = jnp.dot(x_norm.T, grad_pre, preferred_element_type=jnp.float32)
    grad_norm = jnp.dot(grad_pre, w_up.T, preferred_element_type=jnp.float32)
    grad_hat = grad_norm * ln_gamma
    mean_plain = jnp.mean(grad_hat, axis=1, keepdims=True)
    mean_proj = jnp.mean(grad_hat * x_hat, axis=1, keepdims=True)
    dx_blk = (dy_f32 + inv_std * (grad_hat - mean_plain - x_hat * mean_proj)).astype(jnp.bfloat16)
    block_sums = (
        jnp.sum(grad_norm * x_hat, axis=0),
        jnp.sum(grad_norm, axis=0),
        sum_w_up,
        jnp.sum(grad_pre.astype(jnp.float32), axis=0),
        sum_w_down,
        jnp.sum(dy_f32, axis=0),
    )
    return y_blk, dx_blk, block_sums


def reference(x_in, ln_gamma, ln_beta, w_up, b_up, w_down, b_down, grad_out):
    x_blocks = x_in.reshape(NUM_BLOCKS, ROWS, WIDTH)
    dy_blocks = grad_out.reshape(NUM_BLOCKS, ROWS, WIDTH)

    def scan_body(run_sums, blocks):
        y_blk, dx_blk, block_sums = block_pass(blocks[0], blocks[1], ln_gamma, ln_beta, w_up, b_up, w_down, b_down)
        new_sums = jax.tree.map(lambda total, update: total + update, run_sums, block_sums)
        return new_sums, (y_blk, dx_blk)

    init_sums = (
        jnp.zeros((WIDTH,), jnp.float32),
        jnp.zeros((WIDTH,), jnp.float32),
        jnp.zeros((WIDTH, FFN), jnp.float32),
        jnp.zeros((FFN,), jnp.float32),
        jnp.zeros((FFN, WIDTH), jnp.float32),
        jnp.zeros((WIDTH,), jnp.float32),
    )
    final_sums, outputs = lax.scan(scan_body, init_sums, (x_blocks, dy_blocks))
    y_blocks, dx_blocks = outputs
    grad_gamma, grad_beta, sum_w_up, grad_b_up, sum_w_down, grad_b_down = final_sums
    return (
        y_blocks.reshape(TOKENS, WIDTH),
        dx_blocks.reshape(TOKENS, WIDTH),
        grad_gamma,
        grad_beta,
        sum_w_up.astype(jnp.bfloat16),
        grad_b_up,
        sum_w_down.astype(jnp.bfloat16),
        grad_b_down,
    )
```

```python
import jax
import jax.numpy as jnp
from jax import lax
from jax.sharding import PartitionSpec as P

LN_EPS = 1e-5
CHUNKS = 4
SWAP = ((0, 1), (1, 0))


def gelu_tanh(values):
    return jax.nn.gelu(values, approximate=True)


def mm(lhs, rhs, dims):
    return lax.dot_general(lhs, rhs, (dims, ((), ())), preferred_element_type=jnp.float32)


def solution(mesh):
    tok_spec = P(('dp', 'depth', 'row'), 'col')
    vec_spec = P('col')
    mat_spec = P('row', 'col')
    grad_vec = P(('dp', 'col'))
    grad_mat = P(('dp', 'row'), 'col')

    def swap(v, axis):
        return lax.ppermute(v, axis, SWAP)

    def local_pass(x, gamma, beta, w_up, b_up, w_down, b_down, dy):
        rows, width = x.shape
        full = 2 * width
        col, row, depth = lax.axis_index('col'), lax.axis_index('row'), lax.axis_index('depth')
        step = rows // CHUNKS
        cut = [slice(i * step, (i + 1) * step) for i in range(CHUNKS)]

        def other_cols(w):
            half = w.shape[0] // 2
            part = swap(lax.dynamic_slice_in_dim(w, depth * half, half, 0), 'col')
            return lax.all_gather(part, 'depth', axis=0, tiled=True)

        def local_rows(w):
            peer = swap(w, 'row')
            first = jnp.where(row == col, w, peer)
            second = jnp.where(row == col, peer, w)
            return jnp.concatenate([first, second], axis=0)

        small = jnp.concatenate([gamma, beta, b_up.astype(jnp.float32)])
        small_o = swap(small, 'col')
        gam = jnp.concatenate([gamma, small_o[:width]])
        bet = jnp.concatenate([beta, small_o[width:full]])
        bup = jnp.concatenate([small[full:], small_o[full:]])

        wu_o = other_cols(w_up)
        x_o = [swap(x[c], 'col') for c in cut]
        wd_o = other_cols(w_down)
        dy_o = [swap(dy[c], 'col') for c in cut]

        wu = jnp.concatenate([local_rows(w_up), local_rows(wu_o)], axis=1)
        wd_own = local_rows(w_down)
        wd = jnp.concatenate([wd_own, local_rows(wd_o)], axis=1)

        inv = 1.0 / full
        pre, stats, xns = [], [], []
        sum_down = 0.0
        ys = []
        for i, c in enumerate(cut):
            xf = jnp.concatenate([x[c], x_o[i]], axis=1).astype(jnp.float32)
            mean = jnp.sum(xf, axis=1, keepdims=True) * inv
            cen = xf - mean
            istd = lax.rsqrt(jnp.sum(cen * cen, axis=1, keepdims=True) * inv + LN_EPS)
            xn = (cen * istd * gam + bet).astype(jnp.bfloat16)
            u = (mm(xn, wu, ((1,), (0,))) + bup).astype(jnp.bfloat16)
            a = gelu_tanh(u.astype(jnp.float32)).astype(jnp.bfloat16)
            ys.append((xf[:, :width] + mm(a, wd_own, ((1,), (0,))) + b_down.astype(jnp.float32)).astype(jnp.bfloat16))
            sum_down = sum_down + mm(a, dy[c], ((0,), (0,)))
            pre.append(u)
            xns.append(xn)
            stats.append((mean, istd))

        def reduce(total):
            half = total.shape[0] // 2
            keep_at = jnp.where(row == col, 0, half)
            keep = lax.dynamic_slice_in_dim(total, keep_at, half, 0)
            send = lax.dynamic_slice_in_dim(total, half - keep_at, half, 0)
            mine = keep + swap(send, 'row')
            quarter = half // 2
            keep = lax.dynamic_slice_in_dim(mine, depth * quarter, quarter, 0)
            send = lax.dynamic_slice_in_dim(mine, quarter - depth * quarter, quarter, 0)
            part = (keep + swap(send, 'depth')).astype(jnp.bfloat16)
            peer = swap(part, 'depth')
            lo = jnp.where(depth == 0, part, peer)
            hi = jnp.where(depth == 0, peer, part)
            return jnp.concatenate([lo, hi], axis=0)

        grad_w_down = reduce(sum_down)

        sum_up = 0.0
        sum_bup = 0.0
        sum_gam = 0.0
        sum_bet = 0.0
        dxs = []
        for i, c in enumerate(cut):
            dyc = jnp.concatenate([dy[c], dy_o[i]], axis=1)
            da = mm(dyc, wd, ((1,), (1,)))
            _, vjp = jax.vjp(gelu_tanh, pre[i].astype(jnp.float32))
            du = vjp(da)[0].astype(jnp.bfloat16)
            half = du.shape[1] // 2
            sum_bup = sum_bup + jnp.sum(du[:, :half].astype(jnp.float32), axis=0)
            sum_up = sum_up + mm(xns[i], du[:, :half], ((0,), (0,)))
            dxn = mm(du, wu[:width], ((1,), (1,)))
            mean, istd = stats[i]
            xh = (x[c].astype(jnp.float32) - mean) * istd
            sum_gam = sum_gam + jnp.sum(dxn * xh, axis=0)
            sum_bet = sum_bet + jnp.sum(dxn, axis=0)
            g = dxn * gamma
            sums = jnp.stack([jnp.sum(g, axis=1), jnp.sum(g * xh, axis=1)])
            sums = (sums + swap(sums, 'col')) * inv
            dxs.append((dy[c].astype(jnp.float32) + istd * (g - sums[0][:, None] - xh * sums[1][:, None])).astype(jnp.bfloat16))

        grad_w_up = reduce(sum_up)
        vec = jnp.concatenate([sum_gam, sum_bet, sum_bup, jnp.sum(dy.astype(jnp.float32), axis=0)])
        vec = lax.psum(vec, ('depth', 'row'))
        g_gam, g_bet = vec[:width], vec[width:full]
        g_bup, g_bdown = vec[full:full + b_up.shape[0]], vec[full + b_up.shape[0]:]
        return (jnp.concatenate(ys, axis=0), jnp.concatenate(dxs, axis=0), g_gam, g_bet, grad_w_up, g_bup, grad_w_down, g_bdown)

    return jax.shard_map(
        local_pass,
        mesh=mesh,
        in_specs=(tok_spec, vec_spec, vec_spec, mat_spec, vec_spec, mat_spec, vec_spec, tok_spec),
        out_specs=(tok_spec, tok_spec, grad_vec, grad_vec, grad_mat, grad_vec, grad_mat, grad_vec),
        check_vma=False,
    )
```

```python
import functools

import jax
import jax.numpy as jnp
from jax import lax
from jax.experimental import pallas as pl
from jax.experimental.pallas import tpu as pltpu
from jax.sharding import PartitionSpec as P

LN_EPS = 1e-5
C0 = 0.7978845608
C1 = C0 * 0.044715
M = 512
FT = 512
SUBS = 4
BF16, F32 = jnp.bfloat16, jnp.float32
MESH = pl.DeviceIdType.MESH


def dot(lhs, rhs, lhs_dim, rhs_dim):
    return lax.dot_general(lhs, rhs, (((lhs_dim,), (rhs_dim,)), ((), ())), preferred_element_type=F32)


def gelu(v):
    t = jnp.tanh(v * (C1 * (v * v) + C0))
    h = 0.5 * v
    return h * t + h


def gelu_slope(v):
    v2 = v * v
    t = jnp.tanh(v * (C1 * v2 + C0))
    return (v * (1.0 - t * t)) * (1.5 * C1 * v2 + 0.5 * C0) + (0.5 * t + 0.5)


def fold8(v):
    return jnp.sum(v.reshape(v.shape[0] // 8, 8, v.shape[1]), axis=0)


def kernel(x_h, dy_h, wu_h, wd_h, sm_h,
           y_h, dx_h, gwu_h, gwd_h, gs_h, u_h, xn_h, st_h, dxn_h, rdown_h, ydown_h,
           wu, wd, acc_d, acc_u, own, land, aux, xn2, tr, ub, st, da_s, act, acc, yo,
           bup8, gb8, smv, s12, s12o, gd_s, gu_s, gsp, gsl,
           w_sem, wrow_s, wrow_r, wx_s, wx_r, wy_s, wy_r, wa_s, wa_r, wb_s, wb_r,
           sm_sem, land_s, land_r, ld_sem, out_sem, rd_sem, yd_sem, dl_sem, gd_sem,
           ru_s, ru_r, yu_s, yu_r, gu_s_sem, gu_r_sem, s12_sem, gs_sem, credit, free_row, free_dep):
    chunks = x_h.shape[0] // M
    half_f = wu_h.shape[1]
    hw = x_h.shape[1]
    full = 2 * hw
    tiles = 2 * half_f // FT
    c, r, d = lax.axis_index('col'), lax.axis_index('row'), lax.axis_index('depth')
    b = lax.rem(r + c, 2)
    peer = {'col': 1 - c, 'row': 1 - r, 'depth': 1 - d}

    def send(src, dst, s_sem, r_sem, axis):
        return pltpu.make_async_remote_copy(src_ref=src, dst_ref=dst, send_sem=s_sem, recv_sem=r_sem,
                                            device_id={axis: peer[axis]}, device_id_type=MESH)

    def local(src, dst, sem):
        return pltpu.make_async_copy(src, dst, sem)

    def rows_of(k):
        return pl.ds(pl.multiple_of(k * M, M), M)

    bar = pltpu.get_barrier_semaphore()
    for axis in ('col', 'row', 'depth'):
        pl.semaphore_signal(bar, inc=1, device_id={axis: peer[axis]}, device_id_type=MESH)
    pl.semaphore_wait(bar, 3)

    def w_cols(kind, blk, dep, s):
        if kind == 0:
            n = half_rows_u // SUBS
            return wu.at[pl.ds(pl.multiple_of(blk * hw + dep * half_rows_u + s * n, n), n), pl.ds(half_f, half_f)]
        n = half_rows_d // SUBS
        return wd.at[pl.ds(pl.multiple_of(blk * half_f + dep * half_rows_d + s * n, n), n), pl.ds(hw, hw)]

    half_rows_u, half_rows_d = hw // 2, half_f // 2
    w_srcs = (wu_h, wd_h)

    def w_src(kind, s):
        half = (half_rows_u, half_rows_d)[kind]
        n = half // SUBS
        return w_srcs[kind].at[pl.ds(pl.multiple_of(d * half + s * n, n), n), :]

    def w_own(kind):
        if kind == 0:
            return wu.at[pl.ds(pl.multiple_of(b * hw, hw), hw), pl.ds(0, half_f)]
        return wd.at[pl.ds(pl.multiple_of(b * half_f, half_f), half_f), pl.ds(0, hw)]

    def w_x(kind, s):
        return send(w_src(kind, s), w_cols(kind, 1 - b, d, s), wx_s.at[kind, s], wx_r.at[kind, s], 'col')

    def w_y(kind, s):
        return send(w_cols(kind, b, d, s), w_cols(kind, b, d, s), wy_s.at[kind, s], wy_r.at[kind, s], 'depth')

    def w_a(kind, s):
        return send(w_cols(kind, b, d, s), w_cols(kind, b, d, s), wa_s.at[kind, s], wa_r.at[kind, s], 'row')

    def w_b(kind, s):
        return send(w_cols(kind, b, 1 - d, s), w_cols(kind, b, 1 - d, s), wb_s.at[kind, s], wb_r.at[kind, s], 'row')

    def w_row(kind):
        return send(w_srcs[kind], w_own(kind), wrow_s.at[kind], wrow_r.at[kind], 'row')

    def w_load(kind):
        return local(w_srcs[kind], w_own(kind), w_sem.at[kind])

    def w_forward(kind):
        for s in range(SUBS):
            w_x(kind, s).wait_recv()
            w_y(kind, s).start()
            w_a(kind, s).start()
        for s in range(SUBS):
            w_y(kind, s).wait_recv()
            w_b(kind, s).start()
        for s in range(SUBS):
            w_a(kind, s).wait_recv()
            w_b(kind, s).wait_recv()
        for s in range(SUBS):
            w_x(kind, s).wait_send()
            w_y(kind, s).wait_send()
            w_a(kind, s).wait_send()
            w_b(kind, s).wait_send()

    def stream(src, k, q):
        slot = lax.rem(q, 4)
        return send(src.at[rows_of(k), :], land.at[slot], land_s.at[slot], land_r.at[slot], 'col')

    def stream_next(src, k, q):
        @pl.when(q >= 4)
        def _():
            stream(src, k, q).wait_send()
            pl.semaphore_wait(credit, 1)
        stream(src, k, q).start()

    for s in range(SUBS):
        w_x(0, s).start()
    sm_out = send(sm_h, smv.at[1], sm_sem.at[0], sm_sem.at[1], 'col')
    sm_own = local(sm_h, smv.at[0], sm_sem.at[2])
    sm_out.start()
    sm_own.start()
    for kind in range(2):
        w_load(kind).start()
        w_row(kind).start()
    stream(x_h, 0, 0).start()
    stream(x_h, 1, 1).start()

    def load_f(k):
        s = lax.rem(k, 2)
        return (local(x_h.at[rows_of(k), :], own.at[s], ld_sem.at[0, s]),
                local(dy_h.at[rows_of(k), :], aux.at[s], ld_sem.at[1, s]))

    for cp in load_f(0):
        cp.start()

    acc_d[...] = jnp.zeros_like(acc_d)
    acc_u[...] = jnp.zeros_like(acc_u)
    bup8[...] = jnp.zeros_like(bup8)
    gb8[...] = jnp.zeros_like(gb8)

    for kind in range(2):
        w_load(kind).wait()
        w_row(kind).wait()
    sm_own.wait()
    sm_out.wait()
    w_forward(0)

    def out_f(k):
        s = lax.rem(k, 2)
        return (local(ub.at[s], u_h.at[rows_of(k), :], out_sem.at[0, s]),
                local(xn2.at[s], xn_h.at[rows_of(k), :], out_sem.at[1, s]),
                local(st.at[s], st_h.at[rows_of(k), :], out_sem.at[2, s]),
                local(yo.at[s], y_h.at[rows_of(k), :], out_sem.at[3, s]))

    def chunk_f(k, carry):
        s = lax.rem(k, 2)
        slot = lax.rem(k, 4)

        @pl.when(k < chunks - 2)
        def _():
            stream_next(x_h, k + 2, k + 2)

        @pl.when(k == chunks - 2)
        def _():
            for p in range(SUBS):
                w_x(1, p).start()

        @pl.when(k == chunks - 1)
        def _():
            stream_next(dy_h, k - (chunks - 1), k + 1)

        for cp in load_f(k):
            cp.wait()

        @pl.when(k < chunks - 1)
        def _():
            for cp in load_f(k + 1):
                cp.start()

        @pl.when(k >= 2)
        def _():
            for cp in out_f(k):
                cp.wait()

        stream(x_h, k, k).wait_recv()

        gam = jnp.concatenate([smv[0, 1:2, :hw], smv[1, 1:2, :hw]], axis=1)
        bet = jnp.concatenate([smv[0, 1:2, hw:full], smv[1, 1:2, hw:full]], axis=1)
        step = 32
        for i in range(M // step):
            rs = slice(i * step, (i + 1) * step)
            xv = jnp.concatenate([own[s, rs, :], land[slot, rs, :]], axis=1).astype(F32)
            mean = jnp.sum(xv, axis=1, keepdims=True) * (1.0 / full)
            cen = xv - mean
            istd = lax.rsqrt(jnp.sum(cen * cen, axis=1, keepdims=True) * (1.0 / full) + LN_EPS)
            xn2[s, rs, :] = (cen * istd * gam + bet).astype(BF16)
            st[s, rs, :] = jnp.concatenate([jnp.broadcast_to(mean, (step, 64)), jnp.broadcast_to(istd, (step, 64))], axis=1)
        dyv = aux[s]
        tr[:hw, :] = dyv.T
        gb8[:, full:full + hw] += fold8(dyv.astype(F32))

        def up(j):
            js = slice(j * FT, (j + 1) * FT)
            side, at = divmod(j * FT, half_f)
            u = dot(xn2[s], wu[:, js], 1, 0) + smv[side, 0:1, at:at + FT]
            ub[s, :, js] = u.astype(BF16)

        def down(j):
            js = slice(j * FT, (j + 1) * FT)
            act[j % 2] = gelu(ub[s, :, js].astype(F32)).astype(BF16)
            part = dot(act[j % 2], wd[js, :hw], 1, 0)
            acc[...] = part if j == 0 else acc[...] + part
            blk, rest = divmod(j * FT, half_f)
            qt, at = divmod(rest, half_f // 2)
            acc_d[blk, qt, :, at:at + FT] += dot(tr[:hw, :], act[j % 2], 1, 0)

        up(0)
        for j in range(tiles):
            if j + 1 < tiles:
                up(j + 1)
            down(j)
        bdn = smv[0, 1:2, full:full + hw]
        yo[s] = (own[s].astype(F32) + acc[...] + bdn).astype(BF16)
        for cp in out_f(k):
            cp.start()
        pl.semaphore_signal(credit, inc=1, device_id={'col': peer['col']}, device_id_type=MESH)
        return carry

    lax.fori_loop(0, chunks, chunk_f, 0)

    rdown = send(acc_d.at[1 - b], rdown_h, rd_sem.at[0], rd_sem.at[1], 'row')
    rdown.start()
    stream_next(dy_h, 1, chunks + 1)
    for k in (chunks - 2, chunks - 1):
        for cp in out_f(k):
            cp.wait()

    def load_b(k):
        s = lax.rem(k, 2)
        rs = rows_of(k)
        return (local(dy_h.at[rs, :], own.at[s], ld_sem.at[0, s]),
                local(x_h.at[rs, :], aux.at[s], ld_sem.at[1, s]),
                local(u_h.at[rs, :], ub.at[s], ld_sem.at[2, s]),
                local(xn_h.at[rs, :], xn2.at[s], ld_sem.at[3, s]),
                local(st_h.at[rs, :], st.at[s], ld_sem.at[4, s]))

    for cp in load_b(0):
        cp.start()
    w_forward(1)

    rd_load = local(rdown_h, acc_d.at[1 - b], dl_sem.at[0])
    ydown = send(acc_d.at[b, 1 - d], ydown_h, yd_sem.at[0], yd_sem.at[1], 'depth')
    yd_load = local(ydown_h, acc_d.at[1 - b, 0], dl_sem.at[1])
    half_d = half_f // 2
    gd_rows = pl.ds(pl.multiple_of(d * half_d, half_d), half_d)
    gd_own = local(gd_s, gwd_h.at[gd_rows, :], gd_sem.at[0])
    gd_far = send(gd_s, gwd_h.at[gd_rows, :], gd_sem.at[1], gd_sem.at[2], 'depth')
    dxn_out = lambda k: local(acc, dxn_h.at[rows_of(k), :], out_sem.at[0, 0])

    def reduce_down(k):
        @pl.when(k == 1)
        def _():
            rdown.wait()
            rd_load.start()

        @pl.when(k == 2)
        def _():
            rd_load.wait()
            for q in range(2):
                for i in range(hw // 64):
                    rs = slice(i * 64, (i + 1) * 64)
                    acc_d[b, q, rs, :] += acc_d[1 - b, q, rs, :]

        @pl.when(k == 3)
        def _():
            ydown.start()

        @pl.when(k == 9)
        def _():
            ydown.wait()
            yd_load.start()

        @pl.when(k == 10)
        def _():
            yd_load.wait()
            for i in range(half_d // 128):
                cs = slice(i * 128, (i + 1) * 128)
                total = acc_d[b, d, :, cs] + acc_d[1 - b, 0, :, cs]
                gd_s[cs, :] = total.T.astype(BF16)

        @pl.when(k == 11)
        def _():
            gd_own.start()
            gd_far.start()
            pl.semaphore_signal(free_row, inc=1, device_id={'row': peer['row']}, device_id_type=MESH)
            pl.semaphore_signal(free_dep, inc=1, device_id={'depth': peer['depth']}, device_id_type=MESH)

    gam_own = lambda: smv[0, 1:2, :hw]

    def chunk_b(k, carry):
        s = lax.rem(k, 2)
        q = k + chunks
        slot = lax.rem(q, 4)

        @pl.when(k < chunks - 2)
        def _():
            stream_next(dy_h, k + 2, q + 2)

        reduce_down(k)
        for cp in load_b(k):
            cp.wait()

        @pl.when(k < chunks - 1)
        def _():
            for cp in load_b(k + 1):
                cp.start()

        @pl.when(k >= 1)
        def _():
            dxn_out(k).wait()

        stream(dy_h, k, q).wait_recv()
        tr[...] = xn2[s].T

        def grad(j):
            js = slice(j * FT, (j + 1) * FT)
            dyv = jnp.concatenate([own[s], land[slot]], axis=1)
            da_s[j % 2] = dot(dyv, wd[js, :], 1, 1)

        def back(j):
            js = slice(j * FT, (j + 1) * FT)
            du = (da_s[j % 2] * gelu_slope(ub[s, :, js].astype(F32))).astype(BF16)
            act[j % 2] = du
            if j * FT < half_f:
                bup8[:, js] += fold8(du.astype(F32))
            part = dot(act[j % 2], wu[:hw, js], 1, 1)
            acc[...] = part if j == 0 else acc[...] + part
            if j * FT < half_f:
                up = dot(tr[...], act[j % 2], 1, 0)
                for i in range(4):
                    acc_u[i // 2, i % 2, :, js] += up[i * (hw // 2):(i + 1) * (hw // 2)]

        grad(0)
        for j in range(tiles):
            if j + 1 < tiles:
                grad(j + 1)
            back(j)
        gam = gam_own()
        step = 128
        for i in range(M // step):
            rs = slice(i * step, (i + 1) * step)
            dxn = acc[rs, :]
            xh = (aux[s, rs, :].astype(F32) - st[s, rs, 0:1]) * st[s, rs, 64:65]
            px = dxn * xh
            gb8[:, :hw] += fold8(px)
            gb8[:, hw:full] += fold8(dxn)
            s1 = jnp.sum(dxn * gam, axis=1, keepdims=True)
            s2 = jnp.sum(px * gam, axis=1, keepdims=True)
            both = jnp.concatenate([jnp.broadcast_to(s1, (step, 64)), jnp.broadcast_to(s2, (step, 64))], axis=1).T
            s12[k, 0:4, rs] = both[0:4]
            s12[k, 4:8, rs] = both[64:68]
        dxn_out(k).start()

        @pl.when(k < chunks - 4)
        def _():
            pl.semaphore_signal(credit, inc=1, device_id={'col': peer['col']}, device_id_type=MESH)
        return carry

    lax.fori_loop(0, chunks, chunk_b, 0)

    pl.semaphore_wait(free_row, 1)
    pl.semaphore_wait(free_dep, 1)
    parts = half_f // FT
    hq = hw // 2

    def ru(p):
        dst = acc_d.at[0, :, pl.ds((p // 2) * hq, hq), pl.ds((p % 2) * FT, FT)]
        return send(acc_u.at[1 - b, :, :, pl.ds(p * FT, FT)], dst, ru_s.at[p], ru_r.at[p], 'row')

    def yu(p):
        dst = acc_d.at[1, p // 2, pl.ds(0, hq), pl.ds((p % 2) * FT, FT)]
        return send(acc_u.at[b, 1 - d, :, pl.ds(p * FT, FT)], dst, yu_s.at[p], yu_r.at[p], 'depth')

    gu_rows = pl.ds(pl.multiple_of(d * hq, hq), hq)

    def gu_far(p):
        ps = pl.ds(p * FT, FT)
        return send(gu_s.at[:, ps], gwu_h.at[gu_rows, ps], gu_s_sem.at[p], gu_r_sem.at[p], 'depth')

    gu_own = local(gu_s, gwu_h.at[gu_rows, :], gd_sem.at[3])
    for p in range(parts):
        ru(p).start()
    s12_x = send(s12, s12o, s12_sem.at[0], s12_sem.at[1], 'col')
    s12_x.start()
    gsp[0] = jnp.concatenate([jnp.sum(bup8[...], axis=0, keepdims=True), jnp.sum(gb8[...], axis=0, keepdims=True),
                              jnp.zeros((6, half_f), F32)], axis=0)
    gs_row = send(gsp.at[0], gsl.at[0], gs_sem.at[0], gs_sem.at[1], 'row')
    gs_row.start()
    dxn_out(chunks - 1).wait()

    def load_t(k):
        s = lax.rem(k, 2)
        rs = rows_of(k)
        return (local(dy_h.at[rs, :], own.at[s], ld_sem.at[0, s]),
                local(x_h.at[rs, :], aux.at[s], ld_sem.at[1, s]),
                local(dxn_h.at[rs, :], da_s.at[s], ld_sem.at[2, s]),
                local(st_h.at[rs, :], st.at[s], ld_sem.at[3, s]))

    for cp in load_t(0):
        cp.start()
    for p in range(parts):
        ru(p).wait_recv()
        for i in range(2):
            rs = slice((p // 2) * hq, (p // 2) * hq + hq)
            cs = slice((p % 2) * FT, (p % 2) * FT + FT)
            acc_u[b, i, :, p * FT:(p + 1) * FT] += acc_d[0, i, rs, cs]
        yu(p).start()
    gs_row.wait()
    gsp[1] = gsp[0] + gsl[0]
    gs_dep = send(gsp.at[1], gsl.at[1], gs_sem.at[2], gs_sem.at[3], 'depth')
    gs_dep.start()
    s12_x.wait()

    def out_t(k):
        s = lax.rem(k, 2)
        return local(yo.at[s], dx_h.at[rows_of(k), :], out_sem.at[3, s])

    def chunk_t(k, carry):
        s = lax.rem(k, 2)
        for cp in load_t(k):
            cp.wait()

        @pl.when(k < chunks - 1)
        def _():
            for cp in load_t(k + 1):
                cp.start()

        @pl.when(k >= 2)
        def _():
            out_t(k).wait()

        gam = gam_own()
        step = 128
        for i in range(M // step):
            rs = slice(i * step, (i + 1) * step)
            sums = (s12[k, :, rs] + s12o[k, :, rs]) * (1.0 / full)
            cols = jnp.concatenate([sums] * (step // 8), axis=0).T
            istd = st[s, rs, 64:65]
            xh = (aux[s, rs, :].astype(F32) - st[s, rs, 0:1]) * istd
            g = da_s[s, rs, :] * gam
            yo[s, rs, :] = (own[s, rs, :].astype(F32) + istd * (g - cols[:, 0:1] - xh * cols[:, 4:5])).astype(BF16)
        out_t(k).start()
        return carry

    lax.fori_loop(0, chunks, chunk_t, 0)
    gs_dep.wait()
    gsp[0] = gsp[1] + gsl[1]
    gs_out = local(gsp.at[0], gs_h, gs_sem.at[4])
    gs_out.start()
    for p in range(parts):
        yu(p).wait_recv()
        cs = slice((p % 2) * FT, (p % 2) * FT + FT)
        gu_s[:, p * FT:(p + 1) * FT] = (acc_u[b, d, :, p * FT:(p + 1) * FT] + acc_d[1, p // 2, 0:hq, cs]).astype(BF16)
        gu_far(p).start()
    gu_own.start()
    for k in (chunks - 2, chunks - 1):
        out_t(k).wait()
    gs_out.wait()
    gd_own.wait()
    gd_far.wait()
    for k in range(4):
        stream(dy_h, k, chunks + k).wait_send()
    for p in range(parts):
        ru(p).wait_send()
        yu(p).wait_send()
        gu_far(p).wait()
    gu_own.wait()


def solution(mesh):
    tok_spec = P(('dp', 'depth', 'row'), 'col')
    vec_spec = P('col')
    mat_spec = P('row', 'col')
    grad_vec = P(('dp', 'col'))
    grad_mat = P(('dp', 'row'), 'col')

    def local_pass(x, gamma, beta, w_up, b_up, w_down, b_down, dy):
        rows, hw = x.shape
        half_f = b_up.shape[0]
        full_f, full = 2 * half_f, 2 * hw
        chunks = rows // M
        small = jnp.zeros((8, half_f), F32)
        small = small.at[0, :].set(b_up.astype(F32))
        small = small.at[1, :].set(jnp.concatenate([gamma, beta, b_down.astype(F32), jnp.zeros((half_f - 3 * hw,), F32)]))
        hbm = pl.BlockSpec(memory_space=pltpu.HBM)
        sds = jax.ShapeDtypeStruct
        V, D = pltpu.VMEM, pltpu.SemaphoreType.DMA
        outs = [
            sds((rows, hw), BF16), sds((rows, hw), BF16), sds((hw, half_f), BF16), sds((half_f, hw), BF16), sds((8, half_f), F32),
            sds((rows, full_f), BF16), sds((rows, full), BF16), sds((rows, 128), F32), sds((rows, hw), F32),
            sds((2, hw, half_f // 2), F32), sds((hw, half_f // 2), F32),
        ]
        scratch = [
            V((full, full_f), BF16), V((full_f, full), BF16), V((2, 2, hw, half_f // 2), F32), V((2, 2, hw // 2, half_f), F32),
            V((2, M, hw), BF16), V((4, M, hw), BF16), V((2, M, hw), BF16), V((2, M, full), BF16), V((full, M), BF16),
            V((2, M, full_f), BF16), V((2, M, 128), F32), V((2, M, FT), F32), V((2, M, FT), BF16), V((M, hw), F32), V((2, M, hw), BF16),
            V((8, half_f), F32), V((8, half_f), F32), V((2, 8, half_f), F32), V((chunks, 8, M), F32), V((chunks, 8, M), F32),
            V((half_f // 2, hw), BF16), V((hw // 2, half_f), BF16), V((2, 8, half_f), F32), V((2, 8, half_f), F32),
            D((2,)), D((2,)), D((2,)), D((2, SUBS)), D((2, SUBS)), D((2, SUBS)), D((2, SUBS)), D((2, SUBS)), D((2, SUBS)), D((2, SUBS)), D((2, SUBS)),
            D((3,)), D((4,)), D((4,)), D((5, 2)), D((4, 2)), D((2,)), D((2,)), D((2,)), D((4,)),
            D((half_f // FT,)), D((half_f // FT,)), D((half_f // FT,)), D((half_f // FT,)), D((half_f // FT,)), D((half_f // FT,)), D((2,)), D((5,)),
            pltpu.SemaphoreType.REGULAR, pltpu.SemaphoreType.REGULAR, pltpu.SemaphoreType.REGULAR,
        ]
        res = pl.pallas_call(
            kernel,
            out_shape=outs,
            in_specs=[hbm] * 5,
            out_specs=[hbm] * len(outs),
            scratch_shapes=scratch,
            compiler_params=pltpu.CompilerParams(collective_id=0, has_side_effects=True, vmem_limit_bytes=67043328),
            cost_estimate=pl.CostEstimate(flops=16 * rows * full * full_f, bytes_accessed=2 ** 28, transcendentals=2 * rows * full_f),
            name='mlp_block',
        )(x, dy, w_up, w_down, small)
        y, dx, gwu, gwd, gs = res[:5]
        return (y, dx, gs[1, :hw], gs[1, hw:full], gwu, gs[0], gwd, gs[1, full:full + hw])

    return jax.shard_map(
        local_pass,
        mesh=mesh,
        in_specs=(tok_spec, vec_spec, vec_spec, mat_spec, vec_spec, mat_spec, vec_spec, tok_spec),
        out_specs=(tok_spec, tok_spec, grad_vec, grad_vec, grad_mat, grad_vec, grad_mat, grad_vec),
        check_vma=False,
    )
```

```python
import functools

import jax
import jax.numpy as jnp
from jax import lax
from jax.experimental import pallas as pl
from jax.experimental.pallas import tpu as pltpu
from jax.sharding import PartitionSpec as P

LN_EPS = 1e-5
C0 = 0.7978845608
C1 = C0 * 0.044715
M = 512
FT = 512
SUBS = 4
BF16, F32 = jnp.bfloat16, jnp.float32
MESH = pl.DeviceIdType.MESH


def dot(lhs, rhs, lhs_dim, rhs_dim):
    return lax.dot_general(lhs, rhs, (((lhs_dim,), (rhs_dim,)), ((), ())), preferred_element_type=F32)


def gelu(v):
    t = jnp.tanh(v * (C1 * (v * v) + C0))
    h = 0.5 * v
    return h * t + h


def gelu_slope(v):
    v2 = v * v
    t = jnp.tanh(v * (C1 * v2 + C0))
    return (v * (1.0 - t * t)) * (1.5 * C1 * v2 + 0.5 * C0) + (0.5 * t + 0.5)


def fold8(v):
    return jnp.sum(v.reshape(v.shape[0] // 8, 8, v.shape[1]), axis=0)


def kernel(x_h, dy_h, wu_h, wd_h, sm_h,
           y_h, gu_h, gwd_h, gs_h, st_h, dxn_h, s12_h, s12o_h, u_h, xn_h, rdown_h, ydown_h,
           wu, wd, acc_d, acc_u, own, land, aux, xn2, tr, ub, st, da_s, act, acc, yo,
           bup8, gb8, smv, s12, gd_s, gu_s, gsp, gsl,
           w_sem, wrow_s, wrow_r, wx_s, wx_r, wy_s, wy_r, wa_s, wa_r, wb_s, wb_r,
           sm_sem, land_s, land_r, ld_sem, out_sem, rd_sem, yd_sem, dl_sem, gd_sem,
           ru_s, ru_r, yu_s, yu_r, gu_sem, s12_sem, gs_sem, credit, free_row, free_dep):
    chunks = x_h.shape[0] // M
    half_f = wu_h.shape[1]
    hw = x_h.shape[1]
    full = 2 * hw
    tiles = 2 * half_f // FT
    c, r, d = lax.axis_index('col'), lax.axis_index('row'), lax.axis_index('depth')
    b = lax.rem(r + c, 2)
    peer = {'col': 1 - c, 'row': 1 - r, 'depth': 1 - d}

    def send(src, dst, s_sem, r_sem, axis):
        return pltpu.make_async_remote_copy(src_ref=src, dst_ref=dst, send_sem=s_sem, recv_sem=r_sem,
                                            device_id={axis: peer[axis]}, device_id_type=MESH)

    def local(src, dst, sem):
        return pltpu.make_async_copy(src, dst, sem)

    def rows_of(k):
        return pl.ds(pl.multiple_of(k * M, M), M)

    def pipelined(lo, hi, first, mid, last):
        first(lo)
        first(lo + 1)
        mid(lo)
        for j in range(lo, hi):
            if j + 2 < hi:
                first(j + 2)
            last(j)
            if j + 1 < hi:
                mid(j + 1)

    bar = pltpu.get_barrier_semaphore()
    for axis in ('col', 'row', 'depth'):
        pl.semaphore_signal(bar, inc=1, device_id={axis: peer[axis]}, device_id_type=MESH)
    pl.semaphore_wait(bar, 3)

    def w_cols(kind, blk, dep, s):
        if kind == 0:
            n = half_rows_u // SUBS
            return wu.at[pl.ds(pl.multiple_of(blk * hw + dep * half_rows_u + s * n, n), n), pl.ds(half_f, half_f)]
        n = half_rows_d // SUBS
        return wd.at[pl.ds(pl.multiple_of(blk * half_f + dep * half_rows_d + s * n, n), n), pl.ds(hw, hw)]

    half_rows_u, half_rows_d = hw // 2, half_f // 2
    w_srcs = (wu_h, wd_h)

    def w_src(kind, s):
        half = (half_rows_u, half_rows_d)[kind]
        n = half // SUBS
        return w_srcs[kind].at[pl.ds(pl.multiple_of(d * half + s * n, n), n), :]

    def w_own(kind):
        if kind == 0:
            return wu.at[pl.ds(pl.multiple_of(b * hw, hw), hw), pl.ds(0, half_f)]
        return wd.at[pl.ds(pl.multiple_of(b * half_f, half_f), half_f), pl.ds(0, hw)]

    def w_x(kind, s):
        return send(w_src(kind, s), w_cols(kind, 1 - b, d, s), wx_s.at[kind, s], wx_r.at[kind, s], 'col')

    def w_y(kind, s):
        return send(w_cols(kind, b, d, s), w_cols(kind, b, d, s), wy_s.at[kind, s], wy_r.at[kind, s], 'depth')

    def w_a(kind, s):
        return send(w_cols(kind, b, d, s), w_cols(kind, b, d, s), wa_s.at[kind, s], wa_r.at[kind, s], 'row')

    def w_b(kind, s):
        return send(w_cols(kind, b, 1 - d, s), w_cols(kind, b, 1 - d, s), wb_s.at[kind, s], wb_r.at[kind, s], 'row')

    def w_row(kind):
        return send(w_srcs[kind], w_own(kind), wrow_s.at[kind], wrow_r.at[kind], 'row')

    def w_load(kind):
        return local(w_srcs[kind], w_own(kind), w_sem.at[kind])

    def w_forward_x(kind):
        for s in range(SUBS):
            w_x(kind, s).wait_recv()
            w_y(kind, s).start()
            w_a(kind, s).start()

    def w_forward_y(kind):
        for s in range(SUBS):
            w_y(kind, s).wait_recv()
            w_b(kind, s).start()

    def w_finish(kind):
        for s in range(SUBS):
            w_a(kind, s).wait_recv()
            w_b(kind, s).wait_recv()
        for s in range(SUBS):
            w_x(kind, s).wait_send()
            w_y(kind, s).wait_send()
            w_a(kind, s).wait_send()
            w_b(kind, s).wait_send()

    def stream(src, k, q):
        slot = lax.rem(q, 4)
        return send(src.at[rows_of(k), :], land.at[slot], land_s.at[slot], land_r.at[slot], 'col')

    def stream_next(src, k, q):
        @pl.when(q >= 4)
        def _():
            stream(src, k, q).wait_send()
            pl.semaphore_wait(credit, 1)
        stream(src, k, q).start()

    sm_out = send(sm_h, smv.at[1], sm_sem.at[0], sm_sem.at[1], 'col')
    sm_own = local(sm_h, smv.at[0], sm_sem.at[2])
    sm_out.start()
    sm_own.start()
    for s in range(SUBS):
        w_x(0, s).start()
    for kind in range(2):
        w_load(kind).start()
        w_row(kind).start()
    stream(x_h, 0, 0).start()
    stream(x_h, 1, 1).start()

    def load_f(k):
        s = lax.rem(k, 2)
        return (local(x_h.at[rows_of(k), :], own.at[s], ld_sem.at[0, s]),
                local(dy_h.at[rows_of(k), :], aux.at[s], ld_sem.at[1, s]))

    for cp in load_f(0):
        cp.start()

    acc_d[...] = jnp.zeros_like(acc_d)
    acc_u[...] = jnp.zeros_like(acc_u)
    bup8[...] = jnp.zeros_like(bup8)
    gb8[...] = jnp.zeros_like(gb8)

    w_forward_x(0)
    w_forward_y(0)
    for kind in range(2):
        w_load(kind).wait()
        w_row(kind).wait()
    sm_own.wait()
    sm_out.wait()
    w_finish(0)

    def out_f(k):
        s = lax.rem(k, 2)
        return (local(ub.at[s], u_h.at[rows_of(k), :], out_sem.at[0, s]),
                local(xn2.at[s], xn_h.at[rows_of(k), :], out_sem.at[1, s]),
                local(st.at[s], st_h.at[rows_of(k), :], out_sem.at[2, s]),
                local(yo.at[s], y_h.at[rows_of(k), :], out_sem.at[3, s]))

    def chunk_f(k, carry):
        s = lax.rem(k, 2)
        slot = lax.rem(k, 4)

        @pl.when(k < chunks - 2)
        def _():
            stream_next(x_h, k + 2, k + 2)

        @pl.when(k == chunks - 7)
        def _():
            for p in range(SUBS):
                w_x(1, p).start()

        @pl.when(k == chunks - 3)
        def _():
            w_forward_x(1)

        @pl.when(k == chunks - 1)
        def _():
            w_forward_y(1)

        @pl.when(k >= chunks - 2)
        def _():
            stream_next(dy_h, k - (chunks - 2), k + 2)

        for cp in load_f(k):
            cp.wait()

        @pl.when(k < chunks - 1)
        def _():
            for cp in load_f(k + 1):
                cp.start()

        @pl.when(k >= 2)
        def _():
            for cp in out_f(k):
                cp.wait()

        stream(x_h, k, k).wait_recv()

        gam = jnp.concatenate([smv[0, :, half_f:half_f + hw], smv[1, :, half_f:half_f + hw]], axis=1)
        bet = jnp.concatenate([smv[0, :, half_f + hw:half_f + full], smv[1, :, half_f + hw:half_f + full]], axis=1)
        step = 32
        for i in range(M // step):
            rs = slice(i * step, (i + 1) * step)
            xv = jnp.concatenate([own[s, rs, :], land[slot, rs, :]], axis=1).astype(F32)
            mean = jnp.sum(xv, axis=1, keepdims=True) * (1.0 / full)
            cen = xv - mean
            istd = lax.rsqrt(jnp.sum(cen * cen, axis=1, keepdims=True) * (1.0 / full) + LN_EPS)
            xn2[s, rs, :] = (cen * istd * gam + bet).astype(BF16)
            st[s, rs, :] = jnp.concatenate([jnp.broadcast_to(mean, (step, 64)), jnp.broadcast_to(istd, (step, 64))], axis=1)
        dyv = aux[s]
        tr[:hw, :] = dyv.T
        gb8[:, full:full + hw] += fold8(dyv.astype(F32))

        def up(j):
            js = slice(j * FT, (j + 1) * FT)
            side, at = divmod(j * FT, half_f)
            u = dot(xn2[s], wu[:, js], 1, 0) + smv[side, :, at:at + FT]
            ub[s, :, js] = u.astype(BF16)

        def mid(j):
            js = slice(j * FT, (j + 1) * FT)
            act[j % 2] = gelu(ub[s, :, js].astype(F32)).astype(BF16)

        def down(j):
            js = slice(j * FT, (j + 1) * FT)
            part = dot(act[j % 2], wd[js, :hw], 1, 0)
            acc[0] = part if j == 0 else acc[0] + part
            blk, rest = divmod(j * FT, half_f)
            qt, at = divmod(rest, half_f // 2)
            acc_d[blk, qt, :, at:at + FT] += dot(tr[:hw, :], act[j % 2], 1, 0)

        pipelined(0, tiles, up, mid, down)
        bdn = smv[0, :, half_f + full:half_f + full + hw]
        yo[s] = (own[s].astype(F32) + acc[0] + bdn).astype(BF16)
        for cp in out_f(k):
            cp.start()
        pl.semaphore_signal(credit, inc=1, device_id={'col': peer['col']}, device_id_type=MESH)
        return carry

    lax.fori_loop(0, chunks, chunk_f, 0)

    rdown = send(acc_d.at[1 - b], rdown_h, rd_sem.at[0], rd_sem.at[1], 'row')
    rdown.start()
    for k in (chunks - 2, chunks - 1):
        for cp in out_f(k):
            cp.wait()

    def load_b(k):
        s = lax.rem(k, 2)
        rs = rows_of(k)
        return (local(dy_h.at[rs, :], own.at[s], ld_sem.at[0, s]),
                local(x_h.at[rs, :], aux.at[s], ld_sem.at[1, s]),
                local(u_h.at[rs, :], ub.at[s], ld_sem.at[2, s]),
                local(xn_h.at[rs, :], xn2.at[s], ld_sem.at[3, s]),
                local(st_h.at[rs, :], st.at[s], ld_sem.at[4, s]))

    for cp in load_b(0):
        cp.start()
    w_finish(1)

    rd_load = local(rdown_h, acc_d.at[1 - b], dl_sem.at[0])
    ydown = send(acc_d.at[b, 1 - d], ydown_h, yd_sem.at[0], yd_sem.at[1], 'depth')
    yd_load = local(ydown_h, acc_d.at[1 - b, 0], dl_sem.at[1])
    half_d = half_f // 2
    gd_rows = pl.ds(pl.multiple_of(d * half_d, half_d), half_d)
    gd_own = local(gd_s, gwd_h.at[gd_rows, :], gd_sem.at[0])
    gd_far = send(gd_s, gwd_h.at[gd_rows, :], gd_sem.at[1], gd_sem.at[2], 'depth')

    def dxn_out(k):
        s = lax.rem(k, 2)
        return local(acc.at[s], dxn_h.at[rows_of(k), :], out_sem.at[0, s])

    def reduce_down(k):
        @pl.when(k == 1)
        def _():
            rdown.wait()
            rd_load.start()

        @pl.when(k == 2)
        def _():
            rd_load.wait()
            for q in range(2):
                for i in range(hw // 64):
                    rs = slice(i * 64, (i + 1) * 64)
                    acc_d[b, q, rs, :] += acc_d[1 - b, q, rs, :]

        @pl.when(k == 3)
        def _():
            ydown.start()

        @pl.when(k == 9)
        def _():
            ydown.wait()
            yd_load.start()

        @pl.when(k == 10)
        def _():
            yd_load.wait()
            for i in range(half_d // 128):
                cs = slice(i * 128, (i + 1) * 128)
                total = acc_d[b, d, :, cs] + acc_d[1 - b, 0, :, cs]
                gd_s[cs, :] = total.T.astype(BF16)

        @pl.when(k == 11)
        def _():
            gd_own.start()
            gd_far.start()
            pl.semaphore_signal(free_row, inc=1, device_id={'row': peer['row']}, device_id_type=MESH)
            pl.semaphore_signal(free_dep, inc=1, device_id={'depth': peer['depth']}, device_id_type=MESH)

    own_tiles = half_f // FT

    def grads(k, s, slot, lo, hi):
        def grad(j):
            js = slice(j * FT, (j + 1) * FT)
            dyv = jnp.concatenate([own[s], land[slot]], axis=1)
            da_s[j % 2] = dot(dyv, wd[js, :], 1, 1)

        def mid(j):
            js = slice(j * FT, (j + 1) * FT)
            du = (da_s[j % 2] * gelu_slope(ub[s, :, js].astype(F32))).astype(BF16)
            act[j % 2] = du
            if j < own_tiles:
                bup8[:, js] += fold8(du.astype(F32))

        def back(j):
            js = slice(j * FT, (j + 1) * FT)
            part = dot(act[j % 2], wu[:hw, js], 1, 1)
            acc[s] = part if j == 0 else acc[s] + part
            if j < own_tiles:
                up = dot(tr[...], act[j % 2], 1, 0)
                for i in range(4):
                    acc_u[i // 2, i % 2, :, js] += up[i * (hw // 2):(i + 1) * (hw // 2)]

        pipelined(lo, hi, grad, mid, back)

    def other_half(k, s, slot):
        grads(k, s, slot, own_tiles, tiles)
        gam = smv[0, :, half_f:half_f + hw]
        step = 128
        for i in range(M // step):
            rs = slice(i * step, (i + 1) * step)
            dxn = acc[s, rs, :]
            xh = (aux[s, rs, :].astype(F32) - st[s, rs, 0:1]) * st[s, rs, 64:65]
            px = dxn * xh
            gb8[:, :hw] += fold8(px)
            gb8[:, hw:full] += fold8(dxn)
            s1 = jnp.sum(dxn * gam, axis=1, keepdims=True)
            s2 = jnp.sum(px * gam, axis=1, keepdims=True)
            both = jnp.concatenate([jnp.broadcast_to(s1, (step, 64)), jnp.broadcast_to(s2, (step, 64))], axis=1).T
            s12[k, 0:4, rs] = both[0:4]
            s12[k, 4:8, rs] = both[64:68]
        dxn_out(k).start()

    def chunk_b(k, carry):
        s = lax.rem(k, 2)
        q = k + chunks
        slot = lax.rem(q, 4)

        @pl.when(k < chunks - 2)
        def _():
            stream_next(dy_h, k + 2, q + 2)

        reduce_down(k)
        for cp in load_b(k):
            cp.wait()

        @pl.when(k < chunks - 1)
        def _():
            for cp in load_b(k + 1):
                cp.start()

        @pl.when(k >= 2)
        def _():
            dxn_out(k).wait()

        stream(dy_h, k, q).wait_recv()
        tr[...] = xn2[s].T
        grads(k, s, slot, 0, own_tiles)

        @pl.when(k < chunks - 1)
        def _():
            other_half(k, s, slot)

        @pl.when(k < chunks - 4)
        def _():
            pl.semaphore_signal(credit, inc=1, device_id={'col': peer['col']}, device_id_type=MESH)
        return carry

    lax.fori_loop(0, chunks, chunk_b, 0)

    pl.semaphore_wait(free_row, 1)
    pl.semaphore_wait(free_dep, 1)
    parts = half_f // FT
    hq = hw // 2

    def ru(p):
        dst = acc_d.at[0, :, pl.ds((p // 2) * hq, hq), pl.ds((p % 2) * FT, FT)]
        return send(acc_u.at[1 - b, :, :, pl.ds(p * FT, FT)], dst, ru_s.at[p], ru_r.at[p], 'row')

    def yu(p):
        dst = acc_d.at[1, p // 2, pl.ds(0, hq), pl.ds((p % 2) * FT, FT)]
        return send(acc_u.at[b, 1 - d, :, pl.ds(p * FT, FT)], dst, yu_s.at[p], yu_r.at[p], 'depth')

    def gu_out(p):
        ps = pl.ds(p * FT, FT)
        return local(gu_s.at[:, ps], gu_h.at[:, ps], gu_sem.at[p])

    for p in range(parts):
        ru(p).start()
    for p in range(parts):
        ru(p).wait_recv()
        for i in range(2):
            rs = slice((p // 2) * hq, (p // 2) * hq + hq)
            cs = slice((p % 2) * FT, (p % 2) * FT + FT)
            acc_u[b, i, :, p * FT:(p + 1) * FT] += acc_d[0, i, rs, cs]
        yu(p).start()

    last = chunks - 1
    other_half(last, last % 2, (chunks + last) % 4)
    s12_x = send(s12, s12o_h, s12_sem.at[0], s12_sem.at[1], 'col')
    s12_x.start()
    s12_out = local(s12, s12_h, s12_sem.at[2])
    s12_out.start()
    gsp[0] = jnp.concatenate([jnp.sum(bup8[...], axis=0, keepdims=True), jnp.sum(gb8[...], axis=0, keepdims=True)], axis=1)
    gs_row = send(gsp.at[0], gsl.at[0], gs_sem.at[0], gs_sem.at[1], 'row')
    gs_row.start()
    gs_row.wait()
    gsp[1] = gsp[0] + gsl[0]
    gs_dep = send(gsp.at[1], gsl.at[1], gs_sem.at[2], gs_sem.at[3], 'depth')
    gs_dep.start()
    for k in range(4):
        stream(dy_h, k, chunks + k).wait_send()
    for k in (chunks - 2, chunks - 1):
        dxn_out(k).wait()
    gd_own.wait()
    gd_far.wait()
    for p in range(parts):
        ru(p).wait_send()
    for p in range(parts):
        yu(p).wait_recv()
        cs = slice((p % 2) * FT, (p % 2) * FT + FT)
        gu_s[:, p * FT:(p + 1) * FT] = (acc_u[b, d, :, p * FT:(p + 1) * FT] + acc_d[1, p // 2, 0:hq, cs]).astype(BF16)
        gu_out(p).start()
    gs_dep.wait()
    gsp[0] = gsp[1] + gsl[1]
    gs_out = local(gsp.at[0], gs_h, gs_sem.at[4])
    gs_out.start()
    s12_x.wait()
    s12_out.wait()
    for p in range(parts):
        yu(p).wait_send()
        gu_out(p).wait()
    gs_out.wait()


def dx_kernel(x, dy, dxn, st, s12, s12o, gam, dx):
    full = 2 * x.shape[1]
    step = 128
    for i in range(x.shape[0] // step):
        rs = slice(i * step, (i + 1) * step)
        sums = (s12[0, :, rs] + s12o[0, :, rs]) * (1.0 / full)
        cols = jnp.concatenate([sums] * (step // 8), axis=0).T
        istd = st[rs, 64:65]
        xh = (x[rs, :].astype(F32) - st[rs, 0:1]) * istd
        g = dxn[rs, :] * gam[...]
        dx[rs, :] = (dy[rs, :].astype(F32) + istd * (g - cols[:, 0:1] - xh * cols[:, 4:5])).astype(BF16)


def solution(mesh):
    tok_spec = P(('dp', 'depth', 'row'), 'col')
    vec_spec = P('col')
    mat_spec = P('row', 'col')
    grad_vec = P(('dp', 'col'))
    grad_mat = P(('dp', 'row'), 'col')

    def local_pass(x, gamma, beta, w_up, b_up, w_down, b_down, dy):
        rows, hw = x.shape
        half_f = b_up.shape[0]
        full_f, full = 2 * half_f, 2 * hw
        chunks = rows // M
        small = jnp.concatenate([b_up.astype(F32), gamma, beta, b_down.astype(F32), jnp.zeros((half_f - 3 * hw,), F32)])
        small = small.reshape(1, full_f)
        hbm = pl.BlockSpec(memory_space=pltpu.HBM)
        sds = jax.ShapeDtypeStruct
        V, D, R = pltpu.VMEM, pltpu.SemaphoreType.DMA, pltpu.SemaphoreType.REGULAR
        outs = [
            sds((rows, hw), BF16), sds((hw // 2, half_f), BF16), sds((half_f, hw), BF16), sds((1, full_f), F32),
            sds((rows, 128), F32), sds((rows, hw), F32), sds((chunks, 8, M), F32), sds((chunks, 8, M), F32),
            sds((rows, full_f), BF16), sds((rows, full), BF16), sds((2, hw, half_f // 2), F32), sds((hw, half_f // 2), F32),
        ]
        parts = half_f // FT
        scratch = [
            V((full, full_f), BF16), V((full_f, full), BF16), V((2, 2, hw, half_f // 2), F32), V((2, 2, hw // 2, half_f), F32),
            V((2, M, hw), BF16), V((4, M, hw), BF16), V((2, M, hw), BF16), V((2, M, full), BF16), V((full, M), BF16),
            V((2, M, full_f), BF16), V((2, M, 128), F32), V((2, M, FT), F32), V((2, M, FT), BF16), V((2, M, hw), F32), V((2, M, hw), BF16),
            V((8, half_f), F32), V((8, half_f), F32), V((2, 1, full_f), F32), V((chunks, 8, M), F32),
            V((half_f // 2, hw), BF16), V((hw // 2, half_f), BF16), V((2, 1, full_f), F32), V((2, 1, full_f), F32),
            D((2,)), D((2,)), D((2,)), D((2, SUBS)), D((2, SUBS)), D((2, SUBS)), D((2, SUBS)), D((2, SUBS)), D((2, SUBS)), D((2, SUBS)), D((2, SUBS)),
            D((3,)), D((4,)), D((4,)), D((5, 2)), D((4, 2)), D((2,)), D((2,)), D((2,)), D((3,)),
            D((parts,)), D((parts,)), D((parts,)), D((parts,)), D((parts,)), D((3,)), D((5,)), R, R, R,
        ]
        res = pl.pallas_call(
            kernel,
            out_shape=outs,
            in_specs=[hbm] * 5,
            out_specs=[hbm] * len(outs),
            scratch_shapes=scratch,
            compiler_params=pltpu.CompilerParams(
                collective_id=0, has_side_effects=True, vmem_limit_bytes=67043328),
            cost_estimate=pl.CostEstimate(flops=16 * rows * full * full_f, bytes_accessed=2 ** 28, transcendentals=2 * rows * full_f),
            name='mlp_block',
        )(x, dy, w_up, w_down, small)
        y, gu, gwd, gs, st, dxn, s12, s12o = res[:8]
        gu_peer = lax.ppermute(gu, 'depth', ((0, 1), (1, 0)))
        blk = lambda w: pl.BlockSpec((M, w), lambda i: (i, 0))
        sums = pl.BlockSpec((1, 8, M), lambda i: (i, 0, 0))
        dx = pl.pallas_call(
            dx_kernel,
            grid=(chunks,),
            out_shape=sds((rows, hw), BF16),
            in_specs=[blk(hw), blk(hw), blk(hw), blk(128), sums, sums, pl.BlockSpec((1, hw), lambda i: (0, 0))],
            out_specs=blk(hw),
            compiler_params=pltpu.CompilerParams(dimension_semantics=('arbitrary',)),
            cost_estimate=pl.CostEstimate(flops=2 ** 33, bytes_accessed=44 * 2 ** 20, transcendentals=0),
            name='dx',
        )(x, dy, dxn, st, s12, s12o, gamma.reshape(1, hw))
        first = lax.axis_index('depth') == 0
        gwu = jnp.concatenate([jnp.where(first, gu, gu_peer), jnp.where(first, gu_peer, gu)], axis=0)
        gs = gs.reshape(-1)
        return (y, dx, gs[half_f:half_f + hw], gs[half_f + hw:half_f + full], gwu, gs[:half_f], gwd,
                gs[half_f + full:half_f + full + hw])

    return jax.shard_map(
        local_pass,
        mesh=mesh,
        in_specs=(tok_spec, vec_spec, vec_spec, mat_spec, vec_spec, mat_spec, vec_spec, tok_spec),
        out_specs=(tok_spec, tok_spec, grad_vec, grad_vec, grad_mat, grad_vec, grad_mat, grad_vec),
        check_vma=False,
    )
```

```python
import functools

import jax
import jax.numpy as jnp
from jax import lax
from jax.experimental import pallas as pl
from jax.experimental.pallas import tpu as pltpu
from jax.sharding import PartitionSpec as P

LN_EPS = 1e-5
C0 = 0.7978845608
C1 = C0 * 0.044715
M = 512
FT = 512
SUBS = 4
BF16, F32 = jnp.bfloat16, jnp.float32
MESH = pl.DeviceIdType.MESH


def dot(lhs, rhs, lhs_dim, rhs_dim):
    return lax.dot_general(lhs, rhs, (((lhs_dim,), (rhs_dim,)), ((), ())), preferred_element_type=F32)


def gelu(v):
    t = jnp.tanh(v * (C1 * (v * v) + C0))
    h = 0.5 * v
    return h * t + h


def gelu_slope(v):
    v2 = v * v
    t = jnp.tanh(v * (C1 * v2 + C0))
    return (v * (1.0 - t * t)) * (1.5 * C1 * v2 + 0.5 * C0) + (0.5 * t + 0.5)


def fold8(v):
    return jnp.sum(v.reshape(v.shape[0] // 8, 8, v.shape[1]), axis=0)


def kernel(x_h, dy_h, wu_h, wd_h, bup_h, gam_h, bet_h, bdn_h,
           y_h, gu_h, gwd_h, gs_h, st_h, dxn_h, s12_h, s12o_h, u_h, xn_h, rdown_h, ydown_h,
           wu, wd, acc_d, acc_u, own, land, aux, xn2, tr, ub, st, da_s, act, acc, yo,
           bup8, gb8, smv, s12, gd_s, gu_s, gsp, gsl,
           w_sem, wrow_s, wrow_r, wx_s, wx_r, wy_s, wy_r, wa_s, wa_r, wb_s, wb_r,
           sm_sem, land_s, land_r, ld_sem, out_sem, rd_sem, yd_sem, dl_sem, gd_sem,
           ru_s, ru_r, yu_s, yu_r, gu_sem, s12_sem, gs_sem, credit, free_row, free_dep):
    chunks = x_h.shape[0] // M
    half_f = wu_h.shape[1]
    hw = x_h.shape[1]
    full = 2 * hw
    tiles = 2 * half_f // FT
    c, r, d = lax.axis_index('col'), lax.axis_index('row'), lax.axis_index('depth')
    b = lax.rem(r + c, 2)
    peer = {'col': 1 - c, 'row': 1 - r, 'depth': 1 - d}

    def send(src, dst, s_sem, r_sem, axis):
        return pltpu.make_async_remote_copy(src_ref=src, dst_ref=dst, send_sem=s_sem, recv_sem=r_sem,
                                            device_id={axis: peer[axis]}, device_id_type=MESH)

    def local(src, dst, sem):
        return pltpu.make_async_copy(src, dst, sem)

    def rows_of(k):
        return pl.ds(pl.multiple_of(k * M, M), M)

    def pipelined(lo, hi, first, mid, last):
        first(lo)
        first(lo + 1)
        mid(lo)
        for j in range(lo, hi):
            if j + 2 < hi:
                first(j + 2)
            last(j)
            if j + 1 < hi:
                mid(j + 1)

    bar = pltpu.get_barrier_semaphore()
    for axis in ('col', 'row', 'depth'):
        pl.semaphore_signal(bar, inc=1, device_id={axis: peer[axis]}, device_id_type=MESH)
    pl.semaphore_wait(bar, 3)

    def w_cols(kind, blk, dep, s):
        if kind == 0:
            n = half_rows_u // SUBS
            return wu.at[pl.ds(pl.multiple_of(blk * hw + dep * half_rows_u + s * n, n), n), pl.ds(half_f, half_f)]
        n = half_rows_d // SUBS
        return wd.at[pl.ds(pl.multiple_of(blk * half_f + dep * half_rows_d + s * n, n), n), pl.ds(hw, hw)]

    half_rows_u, half_rows_d = hw // 2, half_f // 2
    w_srcs = (wu_h, wd_h)

    def w_src(kind, s):
        half = (half_rows_u, half_rows_d)[kind]
        n = half // SUBS
        return w_srcs[kind].at[pl.ds(pl.multiple_of(d * half + s * n, n), n), :]

    def w_own(kind):
        if kind == 0:
            return wu.at[pl.ds(pl.multiple_of(b * hw, hw), hw), pl.ds(0, half_f)]
        return wd.at[pl.ds(pl.multiple_of(b * half_f, half_f), half_f), pl.ds(0, hw)]

    def w_x(kind, s):
        return send(w_src(kind, s), w_cols(kind, 1 - b, d, s), wx_s.at[kind, s], wx_r.at[kind, s], 'col')

    def w_y(kind, s):
        return send(w_cols(kind, b, d, s), w_cols(kind, b, d, s), wy_s.at[kind, s], wy_r.at[kind, s], 'depth')

    def w_a(kind, s):
        return send(w_cols(kind, b, d, s), w_cols(kind, b, d, s), wa_s.at[kind, s], wa_r.at[kind, s], 'row')

    def w_b(kind, s):
        return send(w_cols(kind, b, 1 - d, s), w_cols(kind, b, 1 - d, s), wb_s.at[kind, s], wb_r.at[kind, s], 'row')

    def w_row(kind):
        return send(w_srcs[kind], w_own(kind), wrow_s.at[kind], wrow_r.at[kind], 'row')

    def w_load(kind):
        return local(w_srcs[kind], w_own(kind), w_sem.at[kind])

    def w_forward_x(kind):
        for s in range(SUBS):
            w_x(kind, s).wait_recv()
            w_y(kind, s).start()
            w_a(kind, s).start()

    def w_forward_y(kind):
        for s in range(SUBS):
            w_y(kind, s).wait_recv()
            w_b(kind, s).start()

    def w_finish(kind):
        for s in range(SUBS):
            w_a(kind, s).wait_recv()
            w_b(kind, s).wait_recv()
        for s in range(SUBS):
            w_x(kind, s).wait_send()
            w_y(kind, s).wait_send()
            w_a(kind, s).wait_send()
            w_b(kind, s).wait_send()

    def stream(src, k, q):
        slot = lax.rem(q, 4)
        return send(src.at[rows_of(k), :], land.at[slot], land_s.at[slot], land_r.at[slot], 'col')

    def stream_next(src, k, q):
        @pl.when(q >= 4)
        def _():
            stream(src, k, q).wait_send()
            pl.semaphore_wait(credit, 1)
        stream(src, k, q).start()

    smalls = ((bup_h, 0, half_f), (gam_h, half_f, hw), (bet_h, half_f + hw, hw), (bdn_h, half_f + full, hw))
    sm_own = [local(ref, smv.at[0, :, pl.ds(at, n)], sm_sem.at[2, i]) for i, (ref, at, n) in enumerate(smalls)]
    sm_out = [send(ref, smv.at[1, :, pl.ds(at, n)], sm_sem.at[0, i], sm_sem.at[1, i], 'col')
              for i, (ref, at, n) in enumerate(smalls[:3])]
    for cp in sm_own + sm_out:
        cp.start()
    for s in range(SUBS):
        w_x(0, s).start()
    for kind in range(2):
        w_load(kind).start()
        w_row(kind).start()
    stream(x_h, 0, 0).start()
    stream(x_h, 1, 1).start()

    def load_f(k):
        s = lax.rem(k, 2)
        return (local(x_h.at[rows_of(k), :], own.at[s], ld_sem.at[0, s]),
                local(dy_h.at[rows_of(k), :], aux.at[s], ld_sem.at[1, s]))

    for cp in load_f(0):
        cp.start()

    acc_d[...] = jnp.zeros_like(acc_d)
    acc_u[...] = jnp.zeros_like(acc_u)
    bup8[...] = jnp.zeros_like(bup8)
    gb8[...] = jnp.zeros_like(gb8)

    w_forward_x(0)
    w_forward_y(0)
    for kind in range(2):
        w_load(kind).wait()
        w_row(kind).wait()
    for cp in sm_own + sm_out:
        cp.wait()
    w_finish(0)

    def out_f(k):
        s = lax.rem(k, 2)
        return (local(ub.at[s], u_h.at[rows_of(k), :], out_sem.at[0, s]),
                local(xn2.at[s], xn_h.at[rows_of(k), :], out_sem.at[1, s]),
                local(st.at[s], st_h.at[rows_of(k), :], out_sem.at[2, s]),
                local(yo.at[s], y_h.at[rows_of(k), :], out_sem.at[3, s]))

    def chunk_f(k, carry):
        s = lax.rem(k, 2)
        slot = lax.rem(k, 4)

        @pl.when(k < chunks - 2)
        def _():
            stream_next(x_h, k + 2, k + 2)

        @pl.when(k == chunks - 7)
        def _():
            for p in range(SUBS):
                w_x(1, p).start()

        @pl.when(k == chunks - 3)
        def _():
            w_forward_x(1)

        @pl.when(k == chunks - 1)
        def _():
            w_forward_y(1)

        @pl.when(k >= chunks - 2)
        def _():
            stream_next(dy_h, k - (chunks - 2), k + 2)

        for cp in load_f(k):
            cp.wait()

        @pl.when(k < chunks - 1)
        def _():
            for cp in load_f(k + 1):
                cp.start()

        @pl.when(k >= 2)
        def _():
            for cp in out_f(k):
                cp.wait()

        stream(x_h, k, k).wait_recv()

        gam = jnp.concatenate([smv[0, :, half_f:half_f + hw], smv[1, :, half_f:half_f + hw]], axis=1)
        bet = jnp.concatenate([smv[0, :, half_f + hw:half_f + full], smv[1, :, half_f + hw:half_f + full]], axis=1)
        step = 32
        for i in range(M // step):
            rs = slice(i * step, (i + 1) * step)
            xv = jnp.concatenate([own[s, rs, :], land[slot, rs, :]], axis=1).astype(F32)
            mean = jnp.sum(xv, axis=1, keepdims=True) * (1.0 / full)
            cen = xv - mean
            istd = lax.rsqrt(jnp.sum(cen * cen, axis=1, keepdims=True) * (1.0 / full) + LN_EPS)
            xn2[s, rs, :] = (cen * istd * gam + bet).astype(BF16)
            st[s, rs, :] = jnp.concatenate([jnp.broadcast_to(mean, (step, 64)), jnp.broadcast_to(istd, (step, 64))], axis=1)
        dyv = aux[s]
        tr[:hw, :] = dyv.T
        gb8[:, full:full + hw] += fold8(dyv.astype(F32))

        def up(j):
            js = slice(j * FT, (j + 1) * FT)
            side, at = divmod(j * FT, half_f)
            u = dot(xn2[s], wu[:, js], 1, 0) + smv[side, :, at:at + FT]
            ub[s, :, js] = u.astype(BF16)

        def mid(j):
            js = slice(j * FT, (j + 1) * FT)
            act[j % 2] = gelu(ub[s, :, js].astype(F32)).astype(BF16)

        def down(j):
            js = slice(j * FT, (j + 1) * FT)
            part = dot(act[j % 2], wd[js, :hw], 1, 0)
            acc[0] = part if j == 0 else acc[0] + part
            blk, rest = divmod(j * FT, half_f)
            qt, at = divmod(rest, half_f // 2)
            acc_d[blk, qt, :, at:at + FT] += dot(tr[:hw, :], act[j % 2], 1, 0)

        pipelined(0, tiles, up, mid, down)
        bdn = smv[0, :, half_f + full:half_f + full + hw]
        yo[s] = (own[s].astype(F32) + acc[0] + bdn).astype(BF16)
        for cp in out_f(k):
            cp.start()
        pl.semaphore_signal(credit, inc=1, device_id={'col': peer['col']}, device_id_type=MESH)
        return carry

    lax.fori_loop(0, chunks, chunk_f, 0)

    rdown = send(acc_d.at[1 - b], rdown_h, rd_sem.at[0], rd_sem.at[1], 'row')
    rdown.start()
    for k in (chunks - 2, chunks - 1):
        for cp in out_f(k):
            cp.wait()

    def load_b(k):
        s = lax.rem(k, 2)
        rs = rows_of(k)
        return (local(dy_h.at[rs, :], own.at[s], ld_sem.at[0, s]),
                local(x_h.at[rs, :], aux.at[s], ld_sem.at[1, s]),
                local(u_h.at[rs, :], ub.at[s], ld_sem.at[2, s]),
                local(xn_h.at[rs, :], xn2.at[s], ld_sem.at[3, s]),
                local(st_h.at[rs, :], st.at[s], ld_sem.at[4, s]))

    for cp in load_b(0):
        cp.start()
    w_finish(1)

    rd_load = local(rdown_h, acc_d.at[1 - b], dl_sem.at[0])
    ydown = send(acc_d.at[b, 1 - d], ydown_h, yd_sem.at[0], yd_sem.at[1], 'depth')
    yd_load = local(ydown_h, acc_d.at[1 - b, 0], dl_sem.at[1])
    half_d = half_f // 2
    gd_rows = pl.ds(pl.multiple_of(d * half_d, half_d), half_d)
    gd_own = local(gd_s, gwd_h.at[gd_rows, :], gd_sem.at[0])
    gd_far = send(gd_s, gwd_h.at[gd_rows, :], gd_sem.at[1], gd_sem.at[2], 'depth')

    def dxn_out(k):
        s = lax.rem(k, 2)
        return local(acc.at[s], dxn_h.at[rows_of(k), :], out_sem.at[0, s])

    def reduce_down(k):
        @pl.when(k == 1)
        def _():
            rdown.wait()
            rd_load.start()

        @pl.when(k == 2)
        def _():
            rd_load.wait()
            for q in range(2):
                for i in range(hw // 64):
                    rs = slice(i * 64, (i + 1) * 64)
                    acc_d[b, q, rs, :] += acc_d[1 - b, q, rs, :]

        @pl.when(k == 3)
        def _():
            ydown.start()

        @pl.when(k == 9)
        def _():
            ydown.wait()
            yd_load.start()

        @pl.when(k == 10)
        def _():
            yd_load.wait()
            for i in range(half_d // 128):
                cs = slice(i * 128, (i + 1) * 128)
                total = acc_d[b, d, :, cs] + acc_d[1 - b, 0, :, cs]
                gd_s[cs, :] = total.T.astype(BF16)

        @pl.when(k == 11)
        def _():
            gd_own.start()
            gd_far.start()
            pl.semaphore_signal(free_row, inc=1, device_id={'row': peer['row']}, device_id_type=MESH)
            pl.semaphore_signal(free_dep, inc=1, device_id={'depth': peer['depth']}, device_id_type=MESH)

    own_tiles = half_f // FT

    def grads(k, s, slot, lo, hi, peeled=None):
        def grad(j):
            js = slice(j * FT, (j + 1) * FT)
            dyv = jnp.concatenate([own[s], land[slot]], axis=1)
            da_s[j % 2] = dot(dyv, wd[js, :], 1, 1)

        def mid(j):
            js = slice(j * FT, (j + 1) * FT)
            du = (da_s[j % 2] * gelu_slope(ub[s, :, js].astype(F32))).astype(BF16)
            act[j % 2] = du
            if j < own_tiles:
                bup8[:, js] += fold8(du.astype(F32))

        def back(j):
            js = slice(j * FT, (j + 1) * FT)
            part = dot(act[j % 2], wu[:hw, js], 1, 1)
            acc[s] = part if j == 0 else acc[s] + part
            if j < own_tiles:
                up = dot(tr[...], act[j % 2], 1, 0)
                for i in range(4):
                    acc_u[i // 2, i % 2, :, js] += up[i * (hw // 2):(i + 1) * (hw // 2)]

        def back_peeled(j):
            js = slice(j * FT, (j + 1) * FT)
            ub[s, :, js] = act[j % 2]
            up = dot(tr[...], act[j % 2], 1, 0)
            for i in range(4):
                acc_u[i // 2, i % 2, :, js] += up[i * (hw // 2):(i + 1) * (hw // 2)]
            peeled(j)

        pipelined(lo, hi, grad, mid, back if peeled is None else back_peeled)

    def other_half(k, s, slot, peeled=False):
        if peeled:
            for j in range(own_tiles):
                js = slice(j * FT, (j + 1) * FT)
                part = dot(ub[s, :, js], wu[:hw, js], 1, 1)
                acc[s] = part if j == 0 else acc[s] + part
        grads(k, s, slot, own_tiles, tiles)
        gam = smv[0, :, half_f:half_f + hw]
        step = 128
        for i in range(M // step):
            rs = slice(i * step, (i + 1) * step)
            dxn = acc[s, rs, :]
            xh = (aux[s, rs, :].astype(F32) - st[s, rs, 0:1]) * st[s, rs, 64:65]
            px = dxn * xh
            gb8[:, :hw] += fold8(px)
            gb8[:, hw:full] += fold8(dxn)
            s1 = jnp.sum(dxn * gam, axis=1, keepdims=True)
            s2 = jnp.sum(px * gam, axis=1, keepdims=True)
            both = jnp.concatenate([jnp.broadcast_to(s1, (step, 64)), jnp.broadcast_to(s2, (step, 64))], axis=1).T
            s12[k, 0:4, rs] = both[0:4]
            s12[k, 4:8, rs] = both[64:68]
        dxn_out(k).start()

    last = chunks - 1

    def chunk_b(k, carry):
        s = lax.rem(k, 2)
        q = k + chunks
        slot = lax.rem(q, 4)

        @pl.when(k < chunks - 2)
        def _():
            stream_next(dy_h, k + 2, q + 2)

        reduce_down(k)
        for cp in load_b(k):
            cp.wait()
        for cp in load_b(k + 1):
            cp.start()

        @pl.when(k >= 2)
        def _():
            dxn_out(k).wait()

        stream(dy_h, k, q).wait_recv()
        tr[...] = xn2[s].T
        grads(k, s, slot, 0, own_tiles)
        other_half(k, s, slot)

        @pl.when(k < chunks - 4)
        def _():
            pl.semaphore_signal(credit, inc=1, device_id={'col': peer['col']}, device_id_type=MESH)
        return carry

    lax.fori_loop(0, last, chunk_b, 0)

    pl.semaphore_wait(free_row, 1)
    pl.semaphore_wait(free_dep, 1)
    parts = half_f // FT
    hq = hw // 2

    def ru(p):
        dst = acc_d.at[0, :, pl.ds((p // 2) * hq, hq), pl.ds((p % 2) * FT, FT)]
        return send(acc_u.at[1 - b, :, :, pl.ds(p * FT, FT)], dst, ru_s.at[p], ru_r.at[p], 'row')

    def yu(p):
        dst = acc_d.at[1, p // 2, pl.ds(0, hq), pl.ds((p % 2) * FT, FT)]
        return send(acc_u.at[b, 1 - d, :, pl.ds(p * FT, FT)], dst, yu_s.at[p], yu_r.at[p], 'depth')

    def gu_out(p):
        ps = pl.ds(p * FT, FT)
        return local(gu_s.at[:, ps], gu_h.at[:, ps], gu_sem.at[p])

    def to_depth(p):
        ru(p).wait_recv()
        for i in range(2):
            rs = slice((p // 2) * hq, (p // 2) * hq + hq)
            cs = slice((p % 2) * FT, (p % 2) * FT + FT)
            acc_u[b, i, :, p * FT:(p + 1) * FT] += acc_d[0, i, rs, cs]
        yu(p).start()

    def tile_done(p):
        ru(p).start()
        if p >= 1:
            to_depth(p - 1)

    slot_l, s_l = (chunks + last) % 4, last % 2
    for cp in load_b(last):
        cp.wait()
    dxn_out(last).wait()
    tr[...] = xn2[s_l].T
    stream(dy_h, last, chunks + last).wait_recv()
    grads(last, s_l, slot_l, 0, own_tiles, tile_done)
    to_depth(parts - 1)

    other_half(last, s_l, slot_l, True)
    s12_x = send(s12, s12o_h, s12_sem.at[0], s12_sem.at[1], 'col')
    s12_x.start()
    s12_out = local(s12, s12_h, s12_sem.at[2])
    s12_out.start()
    gsp[0] = jnp.concatenate([jnp.sum(bup8[...], axis=0, keepdims=True), jnp.sum(gb8[...], axis=0, keepdims=True)], axis=1)
    gs_row = send(gsp.at[0], gsl.at[0], gs_sem.at[0], gs_sem.at[1], 'row')
    gs_row.start()
    gs_row.wait()
    gsp[1] = gsp[0] + gsl[0]
    gs_dep = send(gsp.at[1], gsl.at[1], gs_sem.at[2], gs_sem.at[3], 'depth')
    gs_dep.start()
    for k in range(4):
        stream(dy_h, k, chunks + k).wait_send()
    for k in (chunks - 2, chunks - 1):
        dxn_out(k).wait()
    gd_own.wait()
    gd_far.wait()
    for p in range(parts):
        ru(p).wait_send()
    for p in range(parts):
        yu(p).wait_recv()
        cs = slice((p % 2) * FT, (p % 2) * FT + FT)
        gu_s[:, p * FT:(p + 1) * FT] = (acc_u[b, d, :, p * FT:(p + 1) * FT] + acc_d[1, p // 2, 0:hq, cs]).astype(BF16)
        gu_out(p).start()
    gs_dep.wait()
    gsp[0] = gsp[1] + gsl[1]
    gs_out = local(gsp.at[0], gs_h, gs_sem.at[4])
    gs_out.start()
    s12_x.wait()
    s12_out.wait()
    for p in range(parts):
        yu(p).wait_send()
        gu_out(p).wait()
    gs_out.wait()


def finish_kernel(x, dy, dxn, st, s12, s12o, gam, y_in, gwd_in, gs, dx, y, gwd, gbup, ggam, gbet, gbdn):
    hw = x.shape[1]
    half_f = gbup.shape[1]
    y[...] = y_in[...]
    gwd[...] = gwd_in[...]
    gbup[...] = gs[:, :half_f]
    ggam[...] = gs[:, half_f:half_f + hw]
    gbet[...] = gs[:, half_f + hw:half_f + 2 * hw]
    gbdn[...] = gs[:, half_f + 2 * hw:half_f + 3 * hw]
    step = 128
    for i in range(x.shape[0] // step):
        rs = slice(i * step, (i + 1) * step)
        at = slice((i * step) % M, (i * step) % M + step)
        sums = (s12[i * step // M, :, at] + s12o[i * step // M, :, at]) * (0.5 / hw)
        cols = jnp.concatenate([sums] * (step // 8), axis=0).T
        istd = st[rs, 64:65]
        xh = (x[rs, :].astype(F32) - st[rs, 0:1]) * istd
        g = dxn[rs, :] * gam[...]
        dx[rs, :] = (dy[rs, :].astype(F32) + istd * (g - cols[:, 0:1] - xh * cols[:, 4:5])).astype(BF16)


def solution(mesh):
    tok_spec = P(('dp', 'depth', 'row'), 'col')
    vec_spec = P('col')
    mat_spec = P('row', 'col')
    grad_vec = P(('dp', 'col'))
    grad_mat = P(('dp', 'row'), 'col')

    def local_pass(x, gamma, beta, w_up, b_up, w_down, b_down, dy):
        rows, hw = x.shape
        half_f = b_up.shape[0]
        full_f, full = 2 * half_f, 2 * hw
        chunks = rows // M
        smalls = [v.astype(F32).reshape(1, -1) for v in (b_up, gamma, beta, b_down)]
        hbm = pl.BlockSpec(memory_space=pltpu.HBM)
        sds = jax.ShapeDtypeStruct
        V, D, R = pltpu.VMEM, pltpu.SemaphoreType.DMA, pltpu.SemaphoreType.REGULAR
        outs = [
            sds((rows, hw), BF16), sds((hw // 2, half_f), BF16), sds((half_f, hw), BF16), sds((1, full_f), F32),
            sds((rows, 128), F32), sds((rows, hw), F32), sds((chunks, 8, M), F32), sds((chunks, 8, M), F32),
            sds((rows, full_f), BF16), sds((rows, full), BF16), sds((2, hw, half_f // 2), F32), sds((hw, half_f // 2), F32),
        ]
        parts = half_f // FT
        scratch = [
            V((full, full_f), BF16), V((full_f, full), BF16), V((2, 2, hw, half_f // 2), F32), V((2, 2, hw // 2, half_f), F32),
            V((2, M, hw), BF16), V((4, M, hw), BF16), V((2, M, hw), BF16), V((2, M, full), BF16), V((full, M), BF16),
            V((2, M, full_f), BF16), V((2, M, 128), F32), V((2, M, FT), F32), V((2, M, FT), BF16), V((2, M, hw), F32), V((2, M, hw), BF16),
            V((8, half_f), F32), V((8, half_f), F32), V((2, 1, full_f), F32), V((chunks, 8, M), F32),
            V((half_f // 2, hw), BF16), V((hw // 2, half_f), BF16), V((2, 1, full_f), F32), V((2, 1, full_f), F32),
            D((2,)), D((2,)), D((2,)), D((2, SUBS)), D((2, SUBS)), D((2, SUBS)), D((2, SUBS)), D((2, SUBS)), D((2, SUBS)), D((2, SUBS)), D((2, SUBS)),
            D((3, 4)), D((4,)), D((4,)), D((5, 2)), D((4, 2)), D((2,)), D((2,)), D((2,)), D((3,)),
            D((parts,)), D((parts,)), D((parts,)), D((parts,)), D((parts,)), D((3,)), D((5,)), R, R, R,
        ]
        res = pl.pallas_call(
            kernel,
            out_shape=outs,
            in_specs=[hbm] * 8,
            out_specs=[hbm] * len(outs),
            scratch_shapes=scratch,
            compiler_params=pltpu.CompilerParams(
                collective_id=0, has_side_effects=True, vmem_limit_bytes=67043328),
            cost_estimate=pl.CostEstimate(flops=16 * rows * full * full_f, bytes_accessed=2 ** 28, transcendentals=2 * rows * full_f),
            name='mlp_block',
        )(x, dy, w_up, w_down, *smalls)
        y, gu, gwd, gs, st, dxn, s12, s12o = res[:8]
        gu_peer = lax.ppermute(gu, 'depth', ((0, 1), (1, 0)))
        group = 2
        block = lambda n, w: pl.BlockSpec((n, w), lambda i: (i, 0))
        tok = block(group * M, hw)
        sums = pl.BlockSpec((group, 8, M), lambda i: (i, 0, 0))
        vec = lambda n: pl.BlockSpec((1, n), lambda i: (0, 0))
        steps = chunks // group
        dx, y, gwd, gbup, ggam, gbet, gbdn = pl.pallas_call(
            finish_kernel,
            grid=(steps,),
            out_shape=[sds((rows, hw), BF16), sds((rows, hw), BF16), sds((half_f, hw), BF16), sds((1, half_f), F32),
                       sds((1, hw), F32), sds((1, hw), F32), sds((1, hw), F32)],
            in_specs=[tok, tok, tok, block(group * M, 128), sums, sums, vec(hw), tok, block(half_f // steps, hw), vec(full_f)],
            out_specs=[tok, tok, block(half_f // steps, hw), vec(half_f), vec(hw), vec(hw), vec(hw)],
            compiler_params=pltpu.CompilerParams(dimension_semantics=('arbitrary',)),
            cost_estimate=pl.CostEstimate(flops=2 ** 33, bytes_accessed=64 * 2 ** 20, transcendentals=0),
            name='finish',
        )(x, dy, dxn, st, s12, s12o, smalls[1], y, gwd, gs)
        first = lax.axis_index('depth') == 0
        gwu = jnp.concatenate([jnp.where(first, gu, gu_peer), jnp.where(first, gu_peer, gu)], axis=0)
        return y, dx, ggam.reshape(-1), gbet.reshape(-1), gwu, gbup.reshape(-1), gwd, gbdn.reshape(-1)

    return jax.shard_map(
        local_pass,
        mesh=mesh,
        in_specs=(tok_spec, vec_spec, vec_spec, mat_spec, vec_spec, mat_spec, vec_spec, tok_spec),
        out_specs=(tok_spec, tok_spec, grad_vec, grad_vec, grad_mat, grad_vec, grad_mat, grad_vec),
        check_vma=False,
    )
```

```python
import functools

import jax
import jax.numpy as jnp
from jax import lax
from jax.experimental import pallas as pl
from jax.experimental.pallas import tpu as pltpu
from jax.sharding import PartitionSpec as P

LN_EPS = 1e-5
C0 = 0.7978845608
C1 = C0 * 0.044715
M = 512
FT = 512
LT = 256
SUBS = 4
BF16, F32 = jnp.bfloat16, jnp.float32
MESH = pl.DeviceIdType.MESH


def dot(lhs, rhs, lhs_dim, rhs_dim):
    return lax.dot_general(lhs, rhs, (((lhs_dim,), (rhs_dim,)), ((), ())), preferred_element_type=F32)


def gelu(v):
    t = jnp.tanh(v * (C1 * (v * v) + C0))
    h = 0.5 * v
    return h * t + h


def gelu_slope(v):
    v2 = v * v
    t = jnp.tanh(v * (C1 * v2 + C0))
    return (v * (1.0 - t * t)) * (1.5 * C1 * v2 + 0.5 * C0) + (0.5 * t + 0.5)


def fold8(v):
    return jnp.sum(v.reshape(v.shape[0] // 8, 8, v.shape[1]), axis=0)


def kernel(x_h, dy_h, wu_h, wd_h, bup_h, gam_h, bet_h, bdn_h,
           y_h, dx_h, gwd_h, gs_h, gua_h, gub_h, guo_h, st_h, dxn_h, u_h, xn_h, rdown_h, ydown_h,
           wu, wd, acc_d, acc_u, own, land, aux, xn2, tr, ub, st, da_s, act, acc, yo,
           bup8, gb8, smv, bup_s, bdn_s, s12, s12o, gd_s, gu_s, gsp, gsl,
           w_sem, wrow_s, wrow_r, wx_s, wx_r, wy_s, wy_r, wa_s, wa_r, wb_s, wb_r,
           sm_sem, land_s, land_r, ld_sem, out_sem, rd_sem, yd_sem, dl_sem, gd_sem,
           ru_s, ru_r, yu_s, yu_r, au_s, au_r, gu_sem, s12_sem, gs_sem, credit, free_row, free_dep):
    chunks = x_h.shape[0] // M
    half_f = wu_h.shape[1]
    hw = x_h.shape[1]
    full = 2 * hw
    tiles = 2 * half_f // FT
    c, r, d = lax.axis_index('col'), lax.axis_index('row'), lax.axis_index('depth')
    b = lax.rem(r + c, 2)
    peer = {'col': 1 - c, 'row': 1 - r, 'depth': 1 - d}

    def send(src, dst, s_sem, r_sem, axis):
        return pltpu.make_async_remote_copy(src_ref=src, dst_ref=dst, send_sem=s_sem, recv_sem=r_sem,
                                            device_id={axis: peer[axis]}, device_id_type=MESH)

    def local(src, dst, sem):
        return pltpu.make_async_copy(src, dst, sem)

    def rows_of(k):
        return pl.ds(pl.multiple_of(k * M, M), M)

    def pipelined(lo, hi, first, mid, last):
        first(lo)
        first(lo + 1)
        mid(lo)
        for j in range(lo, hi):
            if j + 2 < hi:
                first(j + 2)
            last(j)
            if j + 1 < hi:
                mid(j + 1)

    bar = pltpu.get_barrier_semaphore()
    for axis in ('col', 'row', 'depth'):
        pl.semaphore_signal(bar, inc=1, device_id={axis: peer[axis]}, device_id_type=MESH)
    pl.semaphore_wait(bar, 3)

    def w_cols(kind, blk, dep, s):
        if kind == 0:
            n = half_rows_u // SUBS
            return wu.at[pl.ds(pl.multiple_of(blk * hw + dep * half_rows_u + s * n, n), n), pl.ds(half_f, half_f)]
        n = half_rows_d // SUBS
        return wd.at[pl.ds(pl.multiple_of(blk * half_f + dep * half_rows_d + s * n, n), n), pl.ds(hw, hw)]

    half_rows_u, half_rows_d = hw // 2, half_f // 2
    w_srcs = (wu_h, wd_h)

    def w_src(kind, s):
        half = (half_rows_u, half_rows_d)[kind]
        n = half // SUBS
        return w_srcs[kind].at[pl.ds(pl.multiple_of(d * half + s * n, n), n), :]

    def w_own(kind):
        if kind == 0:
            return wu.at[pl.ds(pl.multiple_of(b * hw, hw), hw), pl.ds(0, half_f)]
        return wd.at[pl.ds(pl.multiple_of(b * half_f, half_f), half_f), pl.ds(0, hw)]

    def w_x(kind, s):
        return send(w_src(kind, s), w_cols(kind, 1 - b, d, s), wx_s.at[kind, s], wx_r.at[kind, s], 'col')

    def w_y(kind, s):
        return send(w_cols(kind, b, d, s), w_cols(kind, b, d, s), wy_s.at[kind, s], wy_r.at[kind, s], 'depth')

    def w_a(kind, s):
        return send(w_cols(kind, b, d, s), w_cols(kind, b, d, s), wa_s.at[kind, s], wa_r.at[kind, s], 'row')

    def w_b(kind, s):
        return send(w_cols(kind, b, 1 - d, s), w_cols(kind, b, 1 - d, s), wb_s.at[kind, s], wb_r.at[kind, s], 'row')

    def w_row(kind):
        return send(w_srcs[kind], w_own(kind), wrow_s.at[kind], wrow_r.at[kind], 'row')

    def w_load(kind):
        return local(w_srcs[kind], w_own(kind), w_sem.at[kind])

    def w_forward_x(kind):
        for s in range(SUBS):
            w_x(kind, s).wait_recv()
            w_y(kind, s).start()
            w_a(kind, s).start()

    def w_forward_y(kind):
        for s in range(SUBS):
            w_y(kind, s).wait_recv()
            w_b(kind, s).start()

    def w_finish(kind):
        for s in range(SUBS):
            w_a(kind, s).wait_recv()
            w_b(kind, s).wait_recv()
        for s in range(SUBS):
            w_x(kind, s).wait_send()
            w_y(kind, s).wait_send()
            w_a(kind, s).wait_send()
            w_b(kind, s).wait_send()

    def stream(src, k, q):
        slot = lax.rem(q, 4)
        return send(src.at[rows_of(k), :], land.at[slot], land_s.at[slot], land_r.at[slot], 'col')

    def stream_next(src, k, q):
        @pl.when(q >= 4)
        def _():
            stream(src, k, q).wait_send()
            pl.semaphore_wait(credit, 1)
        stream(src, k, q).start()

    gam_at, bet_at, bdn_at = (pl.ds(half_f + i * hw, hw) for i in range(3))
    sm_own = [local(bup_h, bup_s.at[0], sm_sem.at[2, 0]), local(gam_h, smv.at[0, :, gam_at], sm_sem.at[2, 1]),
              local(bet_h, smv.at[0, :, bet_at], sm_sem.at[2, 2]), local(bdn_h, bdn_s, sm_sem.at[2, 3])]
    sm_out = [send(bup_h, bup_s.at[1], sm_sem.at[0, 0], sm_sem.at[1, 0], 'col'),
              send(gam_h, smv.at[1, :, gam_at], sm_sem.at[0, 1], sm_sem.at[1, 1], 'col'),
              send(bet_h, smv.at[1, :, bet_at], sm_sem.at[0, 2], sm_sem.at[1, 2], 'col')]
    for cp in sm_own + sm_out:
        cp.start()
    for s in range(SUBS):
        w_x(0, s).start()
    for kind in range(2):
        w_load(kind).start()
        w_row(kind).start()
    stream(x_h, 0, 0).start()
    stream(x_h, 1, 1).start()

    def load_f(k):
        s = lax.rem(k, 2)
        return (local(x_h.at[rows_of(k), :], own.at[s], ld_sem.at[0, s]),
                local(dy_h.at[rows_of(k), :], aux.at[s], ld_sem.at[1, s]))

    for cp in load_f(0):
        cp.start()

    acc_d[...] = jnp.zeros_like(acc_d)
    acc_u[...] = jnp.zeros_like(acc_u)
    bup8[...] = jnp.zeros_like(bup8)
    gb8[...] = jnp.zeros_like(gb8)

    w_forward_x(0)
    w_forward_y(0)
    for kind in range(2):
        w_load(kind).wait()
        w_row(kind).wait()
    for cp in sm_own + sm_out:
        cp.wait()
    for i in range(half_f // 128):
        for side in range(2):
            smv[side, :, i * 128:(i + 1) * 128] = bup_s[side, i:i + 1, :].astype(F32)
    for i in range(hw // 128):
        smv[0, :, half_f + full + i * 128:half_f + full + (i + 1) * 128] = bdn_s[i:i + 1, :].astype(F32)
    w_finish(0)

    def out_f(k):
        s = lax.rem(k, 2)
        return (local(ub.at[s], u_h.at[rows_of(k), :], out_sem.at[0, s]),
                local(xn2.at[s], xn_h.at[rows_of(k), :], out_sem.at[1, s]),
                local(st.at[s], st_h.at[rows_of(k), :], out_sem.at[2, s]),
                local(yo.at[s], y_h.at[rows_of(k), :], out_sem.at[3, s]))

    def chunk_f(k, carry):
        s = lax.rem(k, 2)
        slot = lax.rem(k, 4)

        @pl.when(k < chunks - 2)
        def _():
            stream_next(x_h, k + 2, k + 2)

        @pl.when(k == chunks - 7)
        def _():
            for p in range(SUBS):
                w_x(1, p).start()

        @pl.when(k == chunks - 3)
        def _():
            w_forward_x(1)

        @pl.when(k == chunks - 1)
        def _():
            w_forward_y(1)

        @pl.when(k >= chunks - 2)
        def _():
            stream_next(dy_h, k - (chunks - 2), k + 2)

        for cp in load_f(k):
            cp.wait()

        @pl.when(k < chunks - 1)
        def _():
            for cp in load_f(k + 1):
                cp.start()

        @pl.when(k >= 2)
        def _():
            for cp in out_f(k):
                cp.wait()

        stream(x_h, k, k).wait_recv()

        gam = jnp.concatenate([smv[0, :, half_f:half_f + hw], smv[1, :, half_f:half_f + hw]], axis=1)
        bet = jnp.concatenate([smv[0, :, half_f + hw:half_f + full], smv[1, :, half_f + hw:half_f + full]], axis=1)
        step = 32
        for i in range(M // step):
            rs = slice(i * step, (i + 1) * step)
            xv = jnp.concatenate([own[s, rs, :], land[slot, rs, :]], axis=1).astype(F32)
            mean = jnp.sum(xv, axis=1, keepdims=True) * (1.0 / full)
            cen = xv - mean
            istd = lax.rsqrt(jnp.sum(cen * cen, axis=1, keepdims=True) * (1.0 / full) + LN_EPS)
            xn2[s, rs, :] = (cen * istd * gam + bet).astype(BF16)
            st[s, rs, :] = jnp.concatenate([jnp.broadcast_to(mean, (step, 64)), jnp.broadcast_to(istd, (step, 64))], axis=1)
        dyv = aux[s]
        tr[:hw, :] = dyv.T
        gb8[:, full:full + hw] += fold8(dyv.astype(F32))

        def up(j):
            js = slice(j * FT, (j + 1) * FT)
            side, at = divmod(j * FT, half_f)
            u = dot(xn2[s], wu[:, js], 1, 0) + smv[side, :, at:at + FT]
            ub[s, :, js] = u.astype(BF16)

        def mid(j):
            js = slice(j * FT, (j + 1) * FT)
            act[j % 2] = gelu(ub[s, :, js].astype(F32)).astype(BF16)

        def down(j):
            js = slice(j * FT, (j + 1) * FT)
            part = dot(act[j % 2], wd[js, :hw], 1, 0)
            acc[0] = part if j == 0 else acc[0] + part
            blk, rest = divmod(j * FT, half_f)
            qt, at = divmod(rest, half_f // 2)
            acc_d[blk, qt, :, at:at + FT] += dot(tr[:hw, :], act[j % 2], 1, 0)

        pipelined(0, tiles, up, mid, down)
        bdn = smv[0, :, half_f + full:half_f + full + hw]
        yo[s] = (own[s].astype(F32) + acc[0] + bdn).astype(BF16)
        for cp in out_f(k):
            cp.start()
        pl.semaphore_signal(credit, inc=1, device_id={'col': peer['col']}, device_id_type=MESH)
        return carry

    lax.fori_loop(0, chunks, chunk_f, 0)

    rdown = send(acc_d.at[1 - b], rdown_h, rd_sem.at[0], rd_sem.at[1], 'row')
    rdown.start()
    for k in (chunks - 2, chunks - 1):
        for cp in out_f(k):
            cp.wait()

    def load_b(k):
        s = lax.rem(k, 2)
        rs = rows_of(k)
        return (local(dy_h.at[rs, :], own.at[s], ld_sem.at[0, s]),
                local(x_h.at[rs, :], aux.at[s], ld_sem.at[1, s]),
                local(u_h.at[rs, :], ub.at[s], ld_sem.at[2, s]),
                local(xn_h.at[rs, :], xn2.at[s], ld_sem.at[3, s]),
                local(st_h.at[rs, :], st.at[s], ld_sem.at[4, s]))

    for cp in load_b(0):
        cp.start()
    w_finish(1)

    rd_load = local(rdown_h, acc_d.at[1 - b], dl_sem.at[0])
    ydown = send(acc_d.at[b, 1 - d], ydown_h, yd_sem.at[0], yd_sem.at[1], 'depth')
    yd_load = local(ydown_h, acc_d.at[1 - b, 0], dl_sem.at[1])
    half_d = half_f // 2
    gd_rows = pl.ds(pl.multiple_of(d * half_d, half_d), half_d)
    gd_own = local(gd_s, gwd_h.at[gd_rows, :], gd_sem.at[0])
    gd_far = send(gd_s, gwd_h.at[gd_rows, :], gd_sem.at[1], gd_sem.at[2], 'depth')

    def dxn_out(k):
        s = lax.rem(k, 2)
        return local(acc.at[s], dxn_h.at[rows_of(k), :], out_sem.at[0, s])

    def reduce_down(k):
        @pl.when(k == 1)
        def _():
            rdown.wait()
            rd_load.start()

        @pl.when(k == 2)
        def _():
            rd_load.wait()
            for q in range(2):
                for i in range(hw // 64):
                    rs = slice(i * 64, (i + 1) * 64)
                    acc_d[b, q, rs, :] += acc_d[1 - b, q, rs, :]

        @pl.when(k == 3)
        def _():
            ydown.start()

        @pl.when(k == 9)
        def _():
            ydown.wait()
            yd_load.start()

        @pl.when(k == 10)
        def _():
            yd_load.wait()
            for i in range(half_d // 128):
                cs = slice(i * 128, (i + 1) * 128)
                total = acc_d[b, d, :, cs] + acc_d[1 - b, 0, :, cs]
                gd_s[cs, :] = total.T.astype(BF16)

        @pl.when(k == 11)
        def _():
            gd_own.start()
            gd_far.start()
            pl.semaphore_signal(free_row, inc=1, device_id={'row': peer['row']}, device_id_type=MESH)
            pl.semaphore_signal(free_dep, inc=1, device_id={'depth': peer['depth']}, device_id_type=MESH)

    own_tiles = half_f // FT
    parts = half_f // LT
    early = parts // 2

    def grads(k, s, slot, lo, hi):
        def grad(j):
            js = slice(j * FT, (j + 1) * FT)
            dyv = jnp.concatenate([own[s], land[slot]], axis=1)
            da_s[j % 2] = dot(dyv, wd[js, :], 1, 1)

        def mid(j):
            js = slice(j * FT, (j + 1) * FT)
            du = (da_s[j % 2] * gelu_slope(ub[s, :, js].astype(F32))).astype(BF16)
            act[j % 2] = du
            if j < own_tiles:
                bup8[:, js] += fold8(du.astype(F32))

        def back(j):
            js = slice(j * FT, (j + 1) * FT)
            part = dot(act[j % 2], wu[:hw, js], 1, 1)
            acc[s] = part if j == 0 else acc[s] + part
            if j < own_tiles:
                up = dot(tr[...], act[j % 2], 1, 0)
                for i in range(4):
                    acc_u[i // 2, i % 2, :, js] += up[i * (hw // 2):(i + 1) * (hw // 2)]

        pipelined(lo, hi, grad, mid, back)

    def grads_last(s, slot, done):
        def grad(j):
            dyv = jnp.concatenate([own[s], land[slot]], axis=1)
            da_s[j % 2, :, :LT] = dot(dyv, wd[j * LT:(j + 1) * LT, :], 1, 1)

        def mid(j):
            js = slice(j * LT, (j + 1) * LT)
            du = (da_s[j % 2, :, :LT] * gelu_slope(ub[s, :, js].astype(F32))).astype(BF16)
            ub[s, :, js] = du
            bup8[:, js] += fold8(du.astype(F32))

        def back(j):
            js = slice(j * LT, (j + 1) * LT)
            up = dot(tr[...], ub[s, :, js], 1, 0)
            for i in range(4):
                acc_u[i // 2, i % 2, :, js] += up[i * (hw // 2):(i + 1) * (hw // 2)]

        grad(0)
        for j in range(parts):
            if j + 1 < parts:
                grad(j + 1)
            mid(j)
            back(j)
            done(j)

    def other_half(k, s, slot, peeled=False):
        if peeled:
            for j in range(own_tiles):
                js = slice(j * FT, (j + 1) * FT)
                part = dot(ub[s, :, js], wu[:hw, js], 1, 1)
                acc[s] = part if j == 0 else acc[s] + part
        grads(k, s, slot, own_tiles, tiles)
        gam = smv[0, :, half_f:half_f + hw]
        step = 128
        for i in range(M // step):
            rs = slice(i * step, (i + 1) * step)
            dxn = acc[s, rs, :]
            xh = (aux[s, rs, :].astype(F32) - st[s, rs, 0:1]) * st[s, rs, 64:65]
            px = dxn * xh
            gb8[:, :hw] += fold8(px)
            gb8[:, hw:full] += fold8(dxn)
            s1 = jnp.sum(dxn * gam, axis=1, keepdims=True)
            s2 = jnp.sum(px * gam, axis=1, keepdims=True)
            both = jnp.concatenate([jnp.broadcast_to(s1, (step, 64)), jnp.broadcast_to(s2, (step, 64))], axis=1).T
            s12[k, 0:4, rs] = both[0:4]
            s12[k, 4:8, rs] = both[64:68]
        dxn_out(k).start()

    last = chunks - 1

    def chunk_b(k, carry):
        s = lax.rem(k, 2)
        q = k + chunks
        slot = lax.rem(q, 4)

        @pl.when(k < chunks - 2)
        def _():
            stream_next(dy_h, k + 2, q + 2)

        reduce_down(k)
        for cp in load_b(k):
            cp.wait()
        for cp in load_b(k + 1):
            cp.start()

        @pl.when(k >= 2)
        def _():
            dxn_out(k).wait()

        stream(dy_h, k, q).wait_recv()
        tr[...] = xn2[s].T
        grads(k, s, slot, 0, own_tiles)
        other_half(k, s, slot)

        @pl.when(k < chunks - 4)
        def _():
            pl.semaphore_signal(credit, inc=1, device_id={'col': peer['col']}, device_id_type=MESH)
        return carry

    lax.fori_loop(0, last, chunk_b, 0)

    pl.semaphore_wait(free_row, 1)
    pl.semaphore_wait(free_dep, 1)
    hq = hw // 2
    wide = half_f // 2 // LT

    def ru(p):
        dst = acc_d.at[0, :, pl.ds((p // wide) * hq, hq), pl.ds((p % wide) * LT, LT)]
        return send(acc_u.at[1 - b, :, :, pl.ds(p * LT, LT)], dst, ru_s.at[p], ru_r.at[p], 'row')

    def yu(p):
        dst = acc_d.at[1, p // wide, pl.ds(0, hq), pl.ds((p % wide) * LT, LT)]
        return send(acc_u.at[b, 1 - d, :, pl.ds(p * LT, LT)], dst, yu_s.at[p], yu_r.at[p], 'depth')

    def au(p):
        ps = pl.ds(p * LT, LT)
        return send(gu_s.at[:, ps], guo_h.at[:, ps], au_s.at[p], au_r.at[p], 'depth')

    half_g = early * LT
    gua_out = local(gu_s.at[:, pl.ds(0, half_g)], gua_h, gu_sem.at[0])
    gub_out = local(gu_s.at[:, pl.ds(half_g, half_g)], gub_h, gu_sem.at[1])

    def to_depth(p):
        ru(p).wait_recv()
        for i in range(2):
            rs = slice((p // wide) * hq, (p // wide) * hq + hq)
            cs = slice((p % wide) * LT, (p % wide) * LT + LT)
            acc_u[b, i, :, p * LT:(p + 1) * LT] += acc_d[0, i, rs, cs]
        yu(p).start()

    def tile_done(p):
        ru(p).start()
        if p >= 1:
            to_depth(p - 1)

    def from_depth(p):
        yu(p).wait_recv()
        cs = slice((p % wide) * LT, (p % wide) * LT + LT)
        gu_s[:, p * LT:(p + 1) * LT] = (acc_u[b, d, :, p * LT:(p + 1) * LT] + acc_d[1, p // wide, 0:hq, cs]).astype(BF16)
        if p < early:
            au(p).start()

    slot_l, s_l = (chunks + last) % 4, last % 2
    s12_a = send(s12.at[pl.ds(0, last)], s12o.at[pl.ds(0, last)], s12_sem.at[0], s12_sem.at[1], 'col')
    s12_b = send(s12.at[last], s12o.at[last], s12_sem.at[2], s12_sem.at[3], 'col')
    for cp in load_b(last):
        cp.wait()
    dxn_out(last).wait()
    tr[...] = xn2[s_l].T
    stream(dy_h, last, chunks + last).wait_recv()
    s12_a.start()
    grads_last(s_l, slot_l, tile_done)
    to_depth(parts - 1)

    other_half(last, s_l, slot_l, True)
    s12_b.start()
    gsp[0] = jnp.concatenate([jnp.sum(bup8[...], axis=0, keepdims=True), jnp.sum(gb8[...], axis=0, keepdims=True)], axis=1)
    gs_row = send(gsp.at[0], gsl.at[0], gs_sem.at[0], gs_sem.at[1], 'row')
    gs_row.start()

    def load_t(k):
        s = lax.rem(k, 2)
        rs = rows_of(k)
        return (local(dy_h.at[rs, :], own.at[s], ld_sem.at[0, s]),
                local(x_h.at[rs, :], aux.at[s], ld_sem.at[1, s]),
                local(dxn_h.at[rs, :], da_s.at[s], ld_sem.at[2, s]),
                local(st_h.at[rs, :], st.at[s], ld_sem.at[4, s]))

    def out_t(k):
        s = lax.rem(k, 2)
        return local(yo.at[s], dx_h.at[rows_of(k), :], out_sem.at[3, s])

    for cp in load_t(0):
        cp.start()
    for k in range(4):
        stream(dy_h, k, chunks + k).wait_send()
    for k in (chunks - 2, chunks - 1):
        dxn_out(k).wait()
    gd_own.wait()
    gd_far.wait()
    for p in range(parts):
        ru(p).wait_send()
    gs_row.wait()
    gsp[1] = gsp[0] + gsl[0]
    gs_dep = send(gsp.at[1], gsl.at[1], gs_sem.at[2], gs_sem.at[3], 'depth')
    gs_dep.start()
    s12_a.wait()
    s12_b.wait()
    from_depth(0)

    def chunk_t(k, carry):
        s = lax.rem(k, 2)
        for cp in load_t(k):
            cp.wait()

        @pl.when(k < last)
        def _():
            for cp in load_t(k + 1):
                cp.start()

        @pl.when(k >= 2)
        def _():
            out_t(k).wait()

        gam = smv[0, :, half_f:half_f + hw]
        step = 128
        for i in range(M // step):
            rs = slice(i * step, (i + 1) * step)
            sums = (s12[k, :, rs] + s12o[k, :, rs]) * (1.0 / full)
            cols = jnp.concatenate([sums] * (step // 8), axis=0).T
            istd = st[s, rs, 64:65]
            xh = (aux[s, rs, :].astype(F32) - st[s, rs, 0:1]) * istd
            g = da_s[s, rs, :] * gam
            yo[s, rs, :] = (own[s, rs, :].astype(F32) + istd * (g - cols[:, 0:1] - xh * cols[:, 4:5])).astype(BF16)
        out_t(k).start()
        return carry

    lax.fori_loop(0, chunks, chunk_t, 0)
    for p in range(1, early):
        from_depth(p)
    gua_out.start()
    for k in (chunks - 2, chunks - 1):
        out_t(k).wait()
    gua_out.wait()
    for p in range(early, parts):
        from_depth(p)
    gub_out.start()
    for p in range(parts):
        yu(p).wait_send()
    gs_dep.wait()
    gsp[0] = gsp[1] + gsl[1]
    gs_out = local(gsp.at[0], gs_h, gs_sem.at[4])
    gs_out.start()
    gub_out.wait()
    gs_out.wait()
    for p in range(early):
        au(p).wait()


def finish_kernel(y_in, dx_in, gwd_in, gs, gua, gub, guo, y, dx, gwd, gwu, gbup, ggam, gbet, gbdn):
    hw = y.shape[1]
    half_f = gbup.shape[1]
    y[...] = y_in[...]
    dx[...] = dx_in[...]
    gwd[...] = gwd_in[...]
    gbup[...] = gs[:, :half_f]
    ggam[...] = gs[:, half_f:half_f + hw]
    gbet[...] = gs[:, half_f + hw:half_f + 2 * hw]
    gbdn[...] = gs[:, half_f + 2 * hw:half_f + 3 * hw]
    hq, half_g = gua.shape
    d = lax.axis_index('depth')
    mine = pl.ds(pl.multiple_of(d * hq, hq), hq)
    far = pl.ds(pl.multiple_of((1 - d) * hq, hq), hq)

    @pl.when(pl.program_id(0) == 0)
    def _():
        gwu[mine, :half_g] = gua[...]
        gwu[mine, half_g:] = gub[...]
        gwu[far, :half_g] = guo[...]
        gwu[far, half_g:] = gub[...]


def solution(mesh):
    tok_spec = P(('dp', 'depth', 'row'), 'col')
    vec_spec = P('col')
    mat_spec = P('row', 'col')
    grad_vec = P(('dp', 'col'))
    grad_mat = P(('dp', 'row'), 'col')

    def local_pass(x, gamma, beta, w_up, b_up, w_down, b_down, dy):
        rows, hw = x.shape
        half_f = b_up.shape[0]
        full_f, full = 2 * half_f, 2 * hw
        chunks = rows // M
        smalls = [b_up.reshape(-1, 128), gamma.reshape(1, -1), beta.reshape(1, -1), b_down.reshape(-1, 128)]
        hbm = pl.BlockSpec(memory_space=pltpu.HBM)
        sds = jax.ShapeDtypeStruct
        V, D, R = pltpu.VMEM, pltpu.SemaphoreType.DMA, pltpu.SemaphoreType.REGULAR
        outs = [
            sds((rows, hw), BF16), sds((rows, hw), BF16), sds((half_f, hw), BF16), sds((1, full_f), F32),
            sds((hw // 2, half_f // 2), BF16), sds((hw // 2, half_f // 2), BF16), sds((hw // 2, half_f // 2), BF16),
            sds((rows, 128), F32), sds((rows, hw), F32),
            sds((rows, full_f), BF16), sds((rows, full), BF16), sds((2, hw, half_f // 2), F32), sds((hw, half_f // 2), F32),
        ]
        parts = half_f // LT
        scratch = [
            V((full, full_f), BF16), V((full_f, full), BF16), V((2, 2, hw, half_f // 2), F32), V((2, 2, hw // 2, half_f), F32),
            V((2, M, hw), BF16), V((4, M, hw), BF16), V((2, M, hw), BF16), V((2, M, full), BF16), V((full, M), BF16),
            V((2, M, full_f), BF16), V((2, M, 128), F32), V((2, M, FT), F32), V((2, M, FT), BF16), V((2, M, hw), F32), V((2, M, hw), BF16),
            V((8, half_f), F32), V((8, half_f), F32), V((2, 1, full_f), F32),
            V((2, half_f // 128, 128), BF16), V((hw // 128, 128), BF16), V((chunks, 8, M), F32), V((chunks, 8, M), F32),
            V((half_f // 2, hw), BF16), V((hw // 2, half_f), BF16), V((2, 1, full_f), F32), V((2, 1, full_f), F32),
            D((2,)), D((2,)), D((2,)), D((2, SUBS)), D((2, SUBS)), D((2, SUBS)), D((2, SUBS)), D((2, SUBS)), D((2, SUBS)), D((2, SUBS)), D((2, SUBS)),
            D((3, 4)), D((4,)), D((4,)), D((5, 2)), D((4, 2)), D((2,)), D((2,)), D((2,)), D((3,)),
            D((parts,)), D((parts,)), D((parts,)), D((parts,)), D((parts // 2,)), D((parts // 2,)), D((2,)), D((4,)), D((5,)), R, R, R,
        ]
        res = pl.pallas_call(
            kernel,
            out_shape=outs,
            in_specs=[hbm] * 8,
            out_specs=[hbm] * len(outs),
            scratch_shapes=scratch,
            compiler_params=pltpu.CompilerParams(
                collective_id=0, has_side_effects=True, vmem_limit_bytes=67043328),
            cost_estimate=pl.CostEstimate(flops=16 * rows * full * full_f, bytes_accessed=2 ** 28, transcendentals=2 * rows * full_f),
            name='mlp_block',
        )(x, dy, w_up, w_down, *smalls)
        y, dx, gwd, gs, gua, gub, guo = res[:7]
        gub_far = lax.ppermute(gub, 'depth', ((0, 1), (1, 0)))
        steps = 8
        block = lambda n, w: pl.BlockSpec((n, w), lambda i: (i, 0))
        tok = block(rows // steps, hw)
        whole = lambda n, w: pl.BlockSpec((n, w), lambda i: (0, 0))
        part = whole(hw // 2, half_f // 2)
        y, dx, gwd, gwu, gbup, ggam, gbet, gbdn = pl.pallas_call(
            finish_kernel,
            grid=(steps,),
            out_shape=[sds((rows, hw), BF16), sds((rows, hw), BF16), sds((half_f, hw), BF16), sds((hw, half_f), BF16),
                       sds((1, half_f), F32), sds((1, hw), F32), sds((1, hw), F32), sds((1, hw), F32)],
            in_specs=[tok, tok, block(half_f // steps, hw), whole(1, full_f), part, part, part],
            out_specs=[tok, tok, block(half_f // steps, hw), whole(hw, half_f), whole(1, half_f), whole(1, hw), whole(1, hw), whole(1, hw)],
            compiler_params=pltpu.CompilerParams(dimension_semantics=('arbitrary',)),
            cost_estimate=pl.CostEstimate(flops=2 ** 33, bytes_accessed=42 * 2 ** 20, transcendentals=0),
            name='finish',
        )(y, dx, gwd, gs, gua, gub, guo)
        far = (1 - lax.axis_index('depth')) * (hw // 2)
        gwu = lax.dynamic_update_slice(gwu, gub_far, (far, half_f // 2))
        return y, dx, ggam.reshape(-1), gbet.reshape(-1), gwu, gbup.reshape(-1), gwd, gbdn.reshape(-1)

    return jax.shard_map(
        local_pass,
        mesh=mesh,
        in_specs=(tok_spec, vec_spec, vec_spec, mat_spec, vec_spec, mat_spec, vec_spec, tok_spec),
        out_specs=(tok_spec, tok_spec, grad_vec, grad_vec, grad_mat, grad_vec, grad_mat, grad_vec),
        check_vma=False,
    )
```

```python
import functools

import jax
import jax.numpy as jnp
from jax import lax
from jax.experimental import pallas as pl
from jax.experimental.pallas import tpu as pltpu
from jax.sharding import PartitionSpec as P

LN_EPS = 1e-5
C0 = 0.7978845608
C1 = C0 * 0.044715
M = 512
FT = 512
LT = 256
COPIES = 8
SUBS = 4
BF16, F32 = jnp.bfloat16, jnp.float32
MESH = pl.DeviceIdType.MESH


def dot(lhs, rhs, lhs_dim, rhs_dim):
    return lax.dot_general(lhs, rhs, (((lhs_dim,), (rhs_dim,)), ((), ())), preferred_element_type=F32)


def gelu(v):
    t = jnp.tanh(v * (C1 * (v * v) + C0))
    h = 0.5 * v
    return h * t + h


def gelu_slope(v):
    v2 = v * v
    t = jnp.tanh(v * (C1 * v2 + C0))
    return (v * (1.0 - t * t)) * (1.5 * C1 * v2 + 0.5 * C0) + (0.5 * t + 0.5)


def fold8(v):
    return jnp.sum(v.reshape(v.shape[0] // 8, 8, v.shape[1]), axis=0)


def kernel(x_h, dy_h, wu_h, wd_h, bup_h, gam_h, bet_h, bdn_h,
           y_h, dx_h, gwd_h, gs_h, gua_h, gub_h, guo_h, st_h, dxn_h, u_h, xn_h, rdown_h, ydown_h,
           wu, wd, acc_d, acc_u, own, land, aux, xn2, tr, ub, st, da_s, act, acc, yo,
           bup8, gb8, smv, bup_s, bdn_s, s12, s12o, gd_s, gu_s, gsp, gsl,
           w_sem, wrow_s, wrow_r, wx_s, wx_r, wy_s, wy_r, wa_s, wa_r, wb_s, wb_r,
           sm_sem, land_s, land_r, ld_sem, out_sem, rd_sem, yd_sem, dl_sem, gd_sem,
           ru_s, ru_r, yu_s, yu_r, au_s, au_r, gu_sem, s12_sem, gs_sem, credit, free_row, free_dep):
    chunks = x_h.shape[0] // M
    half_f = wu_h.shape[1]
    hw = x_h.shape[1]
    full = 2 * hw
    tiles = 2 * half_f // FT
    c, r, d = lax.axis_index('col'), lax.axis_index('row'), lax.axis_index('depth')
    b = lax.rem(r + c, 2)
    peer = {'col': 1 - c, 'row': 1 - r, 'depth': 1 - d}

    def send(src, dst, s_sem, r_sem, axis):
        return pltpu.make_async_remote_copy(src_ref=src, dst_ref=dst, send_sem=s_sem, recv_sem=r_sem,
                                            device_id={axis: peer[axis]}, device_id_type=MESH)

    def local(src, dst, sem):
        return pltpu.make_async_copy(src, dst, sem)

    def rows_of(k):
        return pl.ds(pl.multiple_of(k * M, M), M)

    def pipelined(lo, hi, first, mid, last):
        first(lo)
        first(lo + 1)
        mid(lo)
        for j in range(lo, hi):
            if j + 2 < hi:
                first(j + 2)
            last(j)
            if j + 1 < hi:
                mid(j + 1)

    bar = pltpu.get_barrier_semaphore()
    for axis in ('col', 'row', 'depth'):
        pl.semaphore_signal(bar, inc=1, device_id={axis: peer[axis]}, device_id_type=MESH)
    pl.semaphore_wait(bar, 3)

    def w_cols(kind, blk, dep, s):
        if kind == 0:
            n = half_rows_u // SUBS
            return wu.at[pl.ds(pl.multiple_of(blk * hw + dep * half_rows_u + s * n, n), n), pl.ds(half_f, half_f)]
        n = half_rows_d // SUBS
        return wd.at[pl.ds(pl.multiple_of(blk * half_f + dep * half_rows_d + s * n, n), n), pl.ds(hw, hw)]

    half_rows_u, half_rows_d = hw // 2, half_f // 2
    w_srcs = (wu_h, wd_h)

    def w_src(kind, s):
        half = (half_rows_u, half_rows_d)[kind]
        n = half // SUBS
        return w_srcs[kind].at[pl.ds(pl.multiple_of(d * half + s * n, n), n), :]

    def w_own(kind):
        if kind == 0:
            return wu.at[pl.ds(pl.multiple_of(b * hw, hw), hw), pl.ds(0, half_f)]
        return wd.at[pl.ds(pl.multiple_of(b * half_f, half_f), half_f), pl.ds(0, hw)]

    def w_x(kind, s):
        return send(w_src(kind, s), w_cols(kind, 1 - b, d, s), wx_s.at[kind, s], wx_r.at[kind, s], 'col')

    def w_y(kind, s):
        return send(w_cols(kind, b, d, s), w_cols(kind, b, d, s), wy_s.at[kind, s], wy_r.at[kind, s], 'depth')

    def w_a(kind, s):
        return send(w_cols(kind, b, d, s), w_cols(kind, b, d, s), wa_s.at[kind, s], wa_r.at[kind, s], 'row')

    def w_b(kind, s):
        return send(w_cols(kind, b, 1 - d, s), w_cols(kind, b, 1 - d, s), wb_s.at[kind, s], wb_r.at[kind, s], 'row')

    def w_row(kind):
        return send(w_srcs[kind], w_own(kind), wrow_s.at[kind], wrow_r.at[kind], 'row')

    def w_load(kind):
        return local(w_srcs[kind], w_own(kind), w_sem.at[kind])

    def w_forward_x(kind):
        for s in range(SUBS):
            w_x(kind, s).wait_recv()
            w_y(kind, s).start()
            w_a(kind, s).start()

    def w_forward_y(kind):
        for s in range(SUBS):
            w_y(kind, s).wait_recv()
            w_b(kind, s).start()

    def w_finish(kind):
        for s in range(SUBS):
            w_a(kind, s).wait_recv()
            w_b(kind, s).wait_recv()
        for s in range(SUBS):
            w_x(kind, s).wait_send()
            w_y(kind, s).wait_send()
            w_a(kind, s).wait_send()
            w_b(kind, s).wait_send()

    def stream(src, k, q):
        slot = lax.rem(q, 4)
        return send(src.at[rows_of(k), :], land.at[slot], land_s.at[slot], land_r.at[slot], 'col')

    def stream_next(src, k, q):
        @pl.when(q >= 4)
        def _():
            stream(src, k, q).wait_send()
            pl.semaphore_wait(credit, 1)
        stream(src, k, q).start()

    gam_at, bet_at, bdn_at = (pl.ds(half_f + i * hw, hw) for i in range(3))
    sm_own = [local(bup_h, bup_s.at[0], sm_sem.at[2, 0]), local(gam_h, smv.at[0, :, gam_at], sm_sem.at[2, 1]),
              local(bet_h, smv.at[0, :, bet_at], sm_sem.at[2, 2]), local(bdn_h, bdn_s, sm_sem.at[2, 3])]
    sm_out = [send(bup_h, bup_s.at[1], sm_sem.at[0, 0], sm_sem.at[1, 0], 'col'),
              send(gam_h, smv.at[1, :, gam_at], sm_sem.at[0, 1], sm_sem.at[1, 1], 'col'),
              send(bet_h, smv.at[1, :, bet_at], sm_sem.at[0, 2], sm_sem.at[1, 2], 'col')]
    for cp in sm_own + sm_out:
        cp.start()
    for s in range(SUBS):
        w_x(0, s).start()
    for kind in range(2):
        w_load(kind).start()
        w_row(kind).start()
    stream(x_h, 0, 0).start()
    stream(x_h, 1, 1).start()

    def load_f(k):
        s = lax.rem(k, 2)
        return (local(x_h.at[rows_of(k), :], own.at[s], ld_sem.at[0, s]),
                local(dy_h.at[rows_of(k), :], aux.at[s], ld_sem.at[1, s]))

    for cp in load_f(0):
        cp.start()

    acc_d[...] = jnp.zeros_like(acc_d)
    acc_u[...] = jnp.zeros_like(acc_u)
    bup8[...] = jnp.zeros_like(bup8)
    gb8[...] = jnp.zeros_like(gb8)

    w_forward_x(0)
    w_forward_y(0)
    for kind in range(2):
        w_load(kind).wait()
        w_row(kind).wait()
    for cp in sm_own + sm_out:
        cp.wait()
    for i in range(half_f // 128):
        for side in range(2):
            smv[side, :, i * 128:(i + 1) * 128] = bup_s[side, i:i + 1, :].astype(F32)
    for i in range(hw // 128):
        smv[0, :, half_f + full + i * 128:half_f + full + (i + 1) * 128] = bdn_s[i:i + 1, :].astype(F32)
    w_finish(0)

    def out_f(k):
        s = lax.rem(k, 2)
        return (local(ub.at[s], u_h.at[rows_of(k), :], out_sem.at[0, s]),
                local(xn2.at[s], xn_h.at[rows_of(k), :], out_sem.at[1, s]),
                local(st.at[s], st_h.at[rows_of(k), :], out_sem.at[2, s]),
                local(yo.at[s], y_h.at[rows_of(k), :], out_sem.at[3, s]))

    def chunk_f(k, carry):
        s = lax.rem(k, 2)
        slot = lax.rem(k, 4)

        @pl.when(k < chunks - 2)
        def _():
            stream_next(x_h, k + 2, k + 2)

        @pl.when(k == chunks - 7)
        def _():
            for p in range(SUBS):
                w_x(1, p).start()

        @pl.when(k == chunks - 3)
        def _():
            w_forward_x(1)

        @pl.when(k == chunks - 1)
        def _():
            w_forward_y(1)

        @pl.when(k >= chunks - 2)
        def _():
            stream_next(dy_h, k - (chunks - 2), k + 2)

        for cp in load_f(k):
            cp.wait()

        @pl.when(k < chunks - 1)
        def _():
            for cp in load_f(k + 1):
                cp.start()

        @pl.when(k >= 2)
        def _():
            for cp in out_f(k):
                cp.wait()

        stream(x_h, k, k).wait_recv()

        gam = jnp.concatenate([smv[0, :, half_f:half_f + hw], smv[1, :, half_f:half_f + hw]], axis=1)
        bet = jnp.concatenate([smv[0, :, half_f + hw:half_f + full], smv[1, :, half_f + hw:half_f + full]], axis=1)
        step = 32
        for i in range(M // step):
            rs = slice(i * step, (i + 1) * step)
            xv = jnp.concatenate([own[s, rs, :], land[slot, rs, :]], axis=1).astype(F32)
            mean = jnp.sum(xv, axis=1, keepdims=True) * (1.0 / full)
            cen = xv - mean
            istd = lax.rsqrt(jnp.sum(cen * cen, axis=1, keepdims=True) * (1.0 / full) + LN_EPS)
            xn2[s, rs, :] = (cen * istd * gam + bet).astype(BF16)
            st[s, rs, :] = jnp.concatenate([jnp.broadcast_to(mean, (step, 64)), jnp.broadcast_to(istd, (step, 64))], axis=1)
        dyv = aux[s]
        tr[:hw, :] = dyv.T
        gb8[:, full:full + hw] += fold8(dyv.astype(F32))

        def up(j):
            js = slice(j * FT, (j + 1) * FT)
            side, at = divmod(j * FT, half_f)
            u = dot(xn2[s], wu[:, js], 1, 0) + smv[side, :, at:at + FT]
            ub[s, :, js] = u.astype(BF16)

        def mid(j):
            js = slice(j * FT, (j + 1) * FT)
            act[j % 2] = gelu(ub[s, :, js].astype(F32)).astype(BF16)

        def down(j):
            js = slice(j * FT, (j + 1) * FT)
            part = dot(act[j % 2], wd[js, :hw], 1, 0)
            acc[0] = part if j == 0 else acc[0] + part
            blk, rest = divmod(j * FT, half_f)
            qt, at = divmod(rest, half_f // 2)
            acc_d[blk, qt, :, at:at + FT] += dot(tr[:hw, :], act[j % 2], 1, 0)

        pipelined(0, tiles, up, mid, down)
        bdn = smv[0, :, half_f + full:half_f + full + hw]
        yo[s] = (own[s].astype(F32) + acc[0] + bdn).astype(BF16)
        for cp in out_f(k):
            cp.start()
        pl.semaphore_signal(credit, inc=1, device_id={'col': peer['col']}, device_id_type=MESH)
        return carry

    lax.fori_loop(0, chunks, chunk_f, 0)

    rdown = send(acc_d.at[1 - b], rdown_h, rd_sem.at[0], rd_sem.at[1], 'row')
    rdown.start()
    for k in (chunks - 2, chunks - 1):
        for cp in out_f(k):
            cp.wait()

    def load_b(k):
        s = lax.rem(k, 2)
        rs = rows_of(k)
        return (local(dy_h.at[rs, :], own.at[s], ld_sem.at[0, s]),
                local(x_h.at[rs, :], aux.at[s], ld_sem.at[1, s]),
                local(u_h.at[rs, :], ub.at[s], ld_sem.at[2, s]),
                local(xn_h.at[rs, :], xn2.at[s], ld_sem.at[3, s]),
                local(st_h.at[rs, :], st.at[s], ld_sem.at[4, s]))

    for cp in load_b(0):
        cp.start()
    w_finish(1)

    rd_load = local(rdown_h, acc_d.at[1 - b], dl_sem.at[0])
    ydown = send(acc_d.at[b, 1 - d], ydown_h, yd_sem.at[0], yd_sem.at[1], 'depth')
    yd_load = local(ydown_h, acc_d.at[1 - b, 0], dl_sem.at[1])
    half_d = half_f // 2
    gd_rows = pl.ds(pl.multiple_of(d * half_d, half_d), half_d)
    gd_own = local(gd_s, gwd_h.at[gd_rows, :], gd_sem.at[0])
    gd_far = send(gd_s, gwd_h.at[gd_rows, :], gd_sem.at[1], gd_sem.at[2], 'depth')

    def dxn_out(k):
        s = lax.rem(k, 2)
        return local(acc.at[s], dxn_h.at[rows_of(k), :], out_sem.at[0, s])

    def reduce_down(k):
        @pl.when(k == 1)
        def _():
            rdown.wait()
            rd_load.start()

        @pl.when(k == 2)
        def _():
            rd_load.wait()
            for q in range(2):
                for i in range(hw // 64):
                    rs = slice(i * 64, (i + 1) * 64)
                    acc_d[b, q, rs, :] += acc_d[1 - b, q, rs, :]

        @pl.when(k == 3)
        def _():
            ydown.start()

        @pl.when(k == 9)
        def _():
            ydown.wait()
            yd_load.start()

        @pl.when(k == 10)
        def _():
            yd_load.wait()
            for i in range(half_d // 128):
                cs = slice(i * 128, (i + 1) * 128)
                total = acc_d[b, d, :, cs] + acc_d[1 - b, 0, :, cs]
                gd_s[cs, :] = total.T.astype(BF16)

        @pl.when(k == 11)
        def _():
            gd_own.start()
            gd_far.start()
            pl.semaphore_signal(free_row, inc=1, device_id={'row': peer['row']}, device_id_type=MESH)
            pl.semaphore_signal(free_dep, inc=1, device_id={'depth': peer['depth']}, device_id_type=MESH)

    own_tiles = half_f // FT
    parts = half_f // LT
    early = parts // 2

    def grads(k, s, slot, lo, hi):
        def grad(j):
            js = slice(j * FT, (j + 1) * FT)
            dyv = jnp.concatenate([own[s], land[slot]], axis=1)
            da_s[j % 2] = dot(dyv, wd[js, :], 1, 1)

        def mid(j):
            js = slice(j * FT, (j + 1) * FT)
            du = (da_s[j % 2] * gelu_slope(ub[s, :, js].astype(F32))).astype(BF16)
            act[j % 2] = du
            if j < own_tiles:
                bup8[:, js] += fold8(du.astype(F32))

        def back(j):
            js = slice(j * FT, (j + 1) * FT)
            part = dot(act[j % 2], wu[:hw, js], 1, 1)
            acc[s] = part if j == 0 else acc[s] + part
            if j < own_tiles:
                up = dot(tr[...], act[j % 2], 1, 0)
                for i in range(4):
                    acc_u[i // 2, i % 2, :, js] += up[i * (hw // 2):(i + 1) * (hw // 2)]

        pipelined(lo, hi, grad, mid, back)

    def grads_last(s, slot, done):
        def grad(j):
            dyv = jnp.concatenate([own[s], land[slot]], axis=1)
            da_s[j % 2, :, :LT] = dot(dyv, wd[j * LT:(j + 1) * LT, :], 1, 1)

        def mid(j):
            js = slice(j * LT, (j + 1) * LT)
            du = (da_s[j % 2, :, :LT] * gelu_slope(ub[s, :, js].astype(F32))).astype(BF16)
            ub[s, :, js] = du
            bup8[:, js] += fold8(du.astype(F32))

        def back(j):
            js = slice(j * LT, (j + 1) * LT)
            up = dot(tr[...], ub[s, :, js], 1, 0)
            for i in range(4):
                acc_u[i // 2, i % 2, :, js] += up[i * (hw // 2):(i + 1) * (hw // 2)]

        grad(0)
        for j in range(parts):
            if j + 1 < parts:
                grad(j + 1)
            mid(j)
            back(j)
            done(j)

    def other_half(k, s, slot, peeled=False):
        if peeled:
            for j in range(own_tiles):
                js = slice(j * FT, (j + 1) * FT)
                part = dot(ub[s, :, js], wu[:hw, js], 1, 1)
                acc[s] = part if j == 0 else acc[s] + part
        grads(k, s, slot, own_tiles, tiles)
        gam = smv[0, :, half_f:half_f + hw]
        step = 128
        for i in range(M // step):
            rs = slice(i * step, (i + 1) * step)
            dxn = acc[s, rs, :]
            xh = (aux[s, rs, :].astype(F32) - st[s, rs, 0:1]) * st[s, rs, 64:65]
            px = dxn * xh
            gb8[:, :hw] += fold8(px)
            gb8[:, hw:full] += fold8(dxn)
            s1 = jnp.sum(dxn * gam, axis=1, keepdims=True)
            s2 = jnp.sum(px * gam, axis=1, keepdims=True)
            both = jnp.concatenate([jnp.broadcast_to(s1, (step, 64)), jnp.broadcast_to(s2, (step, 64))], axis=1).T
            s12[k, 0:4, rs] = both[0:4]
            s12[k, 4:8, rs] = both[64:68]
        dxn_out(k).start()

    last = chunks - 1

    def chunk_b(k, carry):
        s = lax.rem(k, 2)
        q = k + chunks
        slot = lax.rem(q, 4)

        @pl.when(k < chunks - 2)
        def _():
            stream_next(dy_h, k + 2, q + 2)

        reduce_down(k)
        for cp in load_b(k):
            cp.wait()
        for cp in load_b(k + 1):
            cp.start()

        @pl.when(k >= 2)
        def _():
            dxn_out(k).wait()

        stream(dy_h, k, q).wait_recv()
        tr[...] = xn2[s].T
        grads(k, s, slot, 0, own_tiles)
        other_half(k, s, slot)

        @pl.when(k < chunks - 4)
        def _():
            pl.semaphore_signal(credit, inc=1, device_id={'col': peer['col']}, device_id_type=MESH)
        return carry

    lax.fori_loop(0, last, chunk_b, 0)

    pl.semaphore_wait(free_row, 1)
    pl.semaphore_wait(free_dep, 1)
    hq = hw // 2
    wide = half_f // 2 // LT

    def ru(p):
        dst = acc_d.at[0, :, pl.ds((p // wide) * hq, hq), pl.ds((p % wide) * LT, LT)]
        return send(acc_u.at[1 - b, :, :, pl.ds(p * LT, LT)], dst, ru_s.at[p], ru_r.at[p], 'row')

    def yu(p):
        dst = acc_d.at[1, p // wide, pl.ds(0, hq), pl.ds((p % wide) * LT, LT)]
        return send(acc_u.at[b, 1 - d, :, pl.ds(p * LT, LT)], dst, yu_s.at[p], yu_r.at[p], 'depth')

    def au(p):
        ps = pl.ds(p * LT, LT)
        return send(gu_s.at[:, ps], guo_h.at[:, ps], au_s.at[p], au_r.at[p], 'depth')

    half_g = early * LT
    gua_out = local(gu_s.at[:, pl.ds(0, half_g)], gua_h, gu_sem.at[0])
    gub_out = local(gu_s.at[:, pl.ds(half_g, half_g)], gub_h, gu_sem.at[1])

    def to_depth(p):
        ru(p).wait_recv()
        for i in range(2):
            rs = slice((p // wide) * hq, (p // wide) * hq + hq)
            cs = slice((p % wide) * LT, (p % wide) * LT + LT)
            acc_u[b, i, :, p * LT:(p + 1) * LT] += acc_d[0, i, rs, cs]
        yu(p).start()

    def tile_done(p):
        ru(p).start()
        if p >= 1:
            to_depth(p - 1)

    def from_depth(p):
        yu(p).wait_recv()
        cs = slice((p % wide) * LT, (p % wide) * LT + LT)
        gu_s[:, p * LT:(p + 1) * LT] = (acc_u[b, d, :, p * LT:(p + 1) * LT] + acc_d[1, p // wide, 0:hq, cs]).astype(BF16)
        if p < early:
            au(p).start()

    slot_l, s_l = (chunks + last) % 4, last % 2
    s12_a = send(s12.at[pl.ds(0, last)], s12o.at[pl.ds(0, last)], s12_sem.at[0], s12_sem.at[1], 'col')
    s12_b = send(s12.at[last], s12o.at[last], s12_sem.at[2], s12_sem.at[3], 'col')
    for cp in load_b(last):
        cp.wait()
    dxn_out(last).wait()
    tr[...] = xn2[s_l].T
    stream(dy_h, last, chunks + last).wait_recv()
    s12_a.start()
    grads_last(s_l, slot_l, tile_done)
    to_depth(parts - 1)

    other_half(last, s_l, slot_l, True)
    s12_b.start()
    gsp[0] = jnp.concatenate([jnp.sum(bup8[...], axis=0, keepdims=True), jnp.sum(gb8[...], axis=0, keepdims=True)], axis=1)
    gs_row = send(gsp.at[0], gsl.at[0], gs_sem.at[0], gs_sem.at[1], 'row')
    gs_row.start()

    def load_t(k):
        s = lax.rem(k, 2)
        rs = rows_of(k)
        return (local(dy_h.at[rs, :], own.at[s], ld_sem.at[0, s]),
                local(x_h.at[rs, :], aux.at[s], ld_sem.at[1, s]),
                local(dxn_h.at[rs, :], da_s.at[s], ld_sem.at[2, s]),
                local(st_h.at[rs, :], st.at[s], ld_sem.at[4, s]))

    def out_t(k):
        s = lax.rem(k, 2)
        return local(yo.at[s], dx_h.at[rows_of(k), :], out_sem.at[3, s])

    for cp in load_t(0):
        cp.start()
    for k in range(4):
        stream(dy_h, k, chunks + k).wait_send()
    for k in (chunks - 2, chunks - 1):
        dxn_out(k).wait()
    gd_own.wait()
    gd_far.wait()
    for p in range(parts):
        ru(p).wait_send()
    gs_row.wait()
    gsp[1] = gsp[0] + gsl[0]
    gs_dep = send(gsp.at[1], gsl.at[1], gs_sem.at[2], gs_sem.at[3], 'depth')
    gs_dep.start()
    s12_a.wait()
    s12_b.wait()
    from_depth(0)

    def chunk_t(k, carry):
        s = lax.rem(k, 2)
        for cp in load_t(k):
            cp.wait()

        @pl.when(k < last)
        def _():
            for cp in load_t(k + 1):
                cp.start()

        @pl.when(k >= 2)
        def _():
            out_t(k).wait()

        gam = smv[0, :, half_f:half_f + hw]
        step = 128
        for i in range(M // step):
            rs = slice(i * step, (i + 1) * step)
            sums = (s12[k, :, rs] + s12o[k, :, rs]) * (1.0 / full)
            cols = jnp.concatenate([sums] * (step // 8), axis=0).T
            istd = st[s, rs, 64:65]
            xh = (aux[s, rs, :].astype(F32) - st[s, rs, 0:1]) * istd
            g = da_s[s, rs, :] * gam
            yo[s, rs, :] = (own[s, rs, :].astype(F32) + istd * (g - cols[:, 0:1] - xh * cols[:, 4:5])).astype(BF16)
        out_t(k).start()
        return carry

    lax.fori_loop(0, chunks, chunk_t, 0)
    for p in range(1, early):
        from_depth(p)
    gua_out.start()
    for k in (chunks - 2, chunks - 1):
        out_t(k).wait()
    gua_out.wait()
    for p in range(early, parts):
        from_depth(p)
    gub_out.start()
    for p in range(parts):
        yu(p).wait_send()
    gs_dep.wait()
    gsp[0] = gsp[1] + gsl[1]
    gs_out = local(gsp.at[0], gs_h, gs_sem.at[4])
    gs_out.start()
    gub_out.wait()
    gs_out.wait()
    for p in range(early):
        au(p).wait()


def finish_kernel(y_in, dx_in, gwd_in, gs, gua, gub, guo, y, dx, gwd, gwu, gbup, ggam, gbet, gbdn, big, small, sums, far_s, in_sem, out_sem):
    rows, hw = y.shape
    half_f = gwd.shape[0]
    hq, half_g = gua.shape
    d = lax.axis_index('depth')
    mine = pl.ds(pl.multiple_of(d * hq, hq), hq)
    far = pl.ds(pl.multiple_of((1 - d) * hq, hq), hq)
    n = rows // COPIES
    ins, outs = [], []

    def move(src, buf, dst, more=()):
        k = len(ins)
        ins.append(pltpu.make_async_copy(src, buf, in_sem.at[k]))
        outs.append([pltpu.make_async_copy(buf, to, out_sem.at[k, i]) for i, to in enumerate((dst, *more))])

    left, right = pl.ds(0, half_g), pl.ds(half_g, half_g)
    for i in range(COPIES):
        rs = pl.ds(i * n, n)
        move(y_in.at[rs], big.at[0, rs], y.at[rs])
        move(dx_in.at[rs], big.at[1, rs], dx.at[rs])
    move(gwd_in, small, gwd)
    move(gua, far_s.at[0], gwu.at[mine, left])
    move(gub, far_s.at[1], gwu.at[mine, right], (gwu.at[far, right],))
    move(guo, far_s.at[2], gwu.at[far, left])
    at = [(0, half_f, gbup), (half_f, hw, ggam), (half_f + hw, hw, gbet), (half_f + 2 * hw, hw, gbdn)]
    for a, w, dst in at:
        move(gs.at[:, pl.ds(a, w)], sums.at[:, pl.ds(a, w)], dst)
    for cp in ins:
        cp.start()
    for cp, tos in zip(ins, outs):
        cp.wait()
        for to in tos:
            to.start()
    for tos in outs:
        for to in tos:
            to.wait()


def solution(mesh):
    tok_spec = P(('dp', 'depth', 'row'), 'col')
    vec_spec = P('col')
    mat_spec = P('row', 'col')
    grad_vec = P(('dp', 'col'))
    grad_mat = P(('dp', 'row'), 'col')

    def local_pass(x, gamma, beta, w_up, b_up, w_down, b_down, dy):
        rows, hw = x.shape
        half_f = b_up.shape[0]
        full_f, full = 2 * half_f, 2 * hw
        chunks = rows // M
        smalls = [b_up.reshape(-1, 128), gamma.reshape(1, -1), beta.reshape(1, -1), b_down.reshape(-1, 128)]
        hbm = pl.BlockSpec(memory_space=pltpu.HBM)
        sds = jax.ShapeDtypeStruct
        V, D, R = pltpu.VMEM, pltpu.SemaphoreType.DMA, pltpu.SemaphoreType.REGULAR
        outs = [
            sds((rows, hw), BF16), sds((rows, hw), BF16), sds((half_f, hw), BF16), sds((1, full_f), F32),
            sds((hw // 2, half_f // 2), BF16), sds((hw // 2, half_f // 2), BF16), sds((hw // 2, half_f // 2), BF16),
            sds((rows, 128), F32), sds((rows, hw), F32),
            sds((rows, full_f), BF16), sds((rows, full), BF16), sds((2, hw, half_f // 2), F32), sds((hw, half_f // 2), F32),
        ]
        parts = half_f // LT
        scratch = [
            V((full, full_f), BF16), V((full_f, full), BF16), V((2, 2, hw, half_f // 2), F32), V((2, 2, hw // 2, half_f), F32),
            V((2, M, hw), BF16), V((4, M, hw), BF16), V((2, M, hw), BF16), V((2, M, full), BF16), V((full, M), BF16),
            V((2, M, full_f), BF16), V((2, M, 128), F32), V((2, M, FT), F32), V((2, M, FT), BF16), V((2, M, hw), F32), V((2, M, hw), BF16),
            V((8, half_f), F32), V((8, half_f), F32), V((2, 1, full_f), F32),
            V((2, half_f // 128, 128), BF16), V((hw // 128, 128), BF16), V((chunks, 8, M), F32), V((chunks, 8, M), F32),
            V((half_f // 2, hw), BF16), V((hw // 2, half_f), BF16), V((2, 1, full_f), F32), V((2, 1, full_f), F32),
            D((2,)), D((2,)), D((2,)), D((2, SUBS)), D((2, SUBS)), D((2, SUBS)), D((2, SUBS)), D((2, SUBS)), D((2, SUBS)), D((2, SUBS)), D((2, SUBS)),
            D((3, 4)), D((4,)), D((4,)), D((5, 2)), D((4, 2)), D((2,)), D((2,)), D((2,)), D((3,)),
            D((parts,)), D((parts,)), D((parts,)), D((parts,)), D((parts // 2,)), D((parts // 2,)), D((2,)), D((4,)), D((5,)), R, R, R,
        ]
        res = pl.pallas_call(
            kernel,
            out_shape=outs,
            in_specs=[hbm] * 8,
            out_specs=[hbm] * len(outs),
            scratch_shapes=scratch,
            compiler_params=pltpu.CompilerParams(
                collective_id=0, has_side_effects=True, vmem_limit_bytes=67043328),
            cost_estimate=pl.CostEstimate(flops=16 * rows * full * full_f, bytes_accessed=2 ** 28, transcendentals=2 * rows * full_f),
            name='mlp_block',
        )(x, dy, w_up, w_down, *smalls)
        y, dx, gwd, gs, gua, gub, guo = res[:7]
        gub_far = lax.ppermute(gub, 'depth', ((0, 1), (1, 0)))
        moves = 2 * COPIES + 8
        y, dx, gwd, gwu, gbup, ggam, gbet, gbdn = pl.pallas_call(
            finish_kernel,
            out_shape=[sds((rows, hw), BF16), sds((rows, hw), BF16), sds((half_f, hw), BF16), sds((hw, half_f), BF16),
                       sds((1, half_f), F32), sds((1, hw), F32), sds((1, hw), F32), sds((1, hw), F32)],
            in_specs=[hbm] * 7,
            out_specs=[hbm] * 8,
            scratch_shapes=[V((2, rows, hw), BF16), V((half_f, hw), BF16), V((1, full_f), F32), V((3, hw // 2, half_f // 2), BF16),
                            D((moves,)), D((moves, 2))],
            compiler_params=pltpu.CompilerParams(vmem_limit_bytes=40 * 2 ** 20),
            cost_estimate=pl.CostEstimate(flops=2 ** 33, bytes_accessed=42 * 2 ** 20, transcendentals=0),
            name='finish',
        )(y, dx, gwd, gs, gua, gub, guo)
        far = (1 - lax.axis_index('depth')) * (hw // 2)
        gwu = lax.dynamic_update_slice(gwu, gub_far, (far, half_f // 2))
        return y, dx, ggam.reshape(-1), gbet.reshape(-1), gwu, gbup.reshape(-1), gwd, gbdn.reshape(-1)

    return jax.shard_map(
        local_pass,
        mesh=mesh,
        in_specs=(tok_spec, vec_spec, vec_spec, mat_spec, vec_spec, mat_spec, vec_spec, tok_spec),
        out_specs=(tok_spec, tok_spec, grad_vec, grad_vec, grad_mat, grad_vec, grad_mat, grad_vec),
        check_vma=False,
    )
```

```python
import functools

import jax
import jax.numpy as jnp
from jax import lax
from jax.experimental import pallas as pl
from jax.experimental.pallas import tpu as pltpu
from jax.sharding import PartitionSpec as P

LN_EPS = 1e-5
C0 = 0.7978845608
C1 = C0 * 0.044715
M = 512
FT = 512
LT = 256
COPIES = 8
SUBS = 4
BF16, F32 = jnp.bfloat16, jnp.float32
MESH = pl.DeviceIdType.MESH


def dot(lhs, rhs, lhs_dim, rhs_dim):
    return lax.dot_general(lhs, rhs, (((lhs_dim,), (rhs_dim,)), ((), ())), preferred_element_type=F32)


def gelu(v):
    t = jnp.tanh(v * (C1 * (v * v) + C0))
    h = 0.5 * v
    return h * t + h


def gelu_slope(v):
    v2 = v * v
    t = jnp.tanh(v * (C1 * v2 + C0))
    return (v * (1.0 - t * t)) * (1.5 * C1 * v2 + 0.5 * C0) + (0.5 * t + 0.5)


def fold8(v):
    return jnp.sum(v.reshape(v.shape[0] // 8, 8, v.shape[1]), axis=0)


def kernel(x_h, dy_h, wu_h, wd_h, bup_h, gam_h, bet_h, bdn_h,
           y_h, dx_h, gwd_h, gs_h, gua_h, gub_h, guo_h, st_h, dxn_h, u_h, xn_h, rdown_h, ydown_h,
           wu, wd, acc_d, acc_u, own, land, aux, xn2, tr, ub, st, da_s, act, acc, yo,
           bup8, gb8, smv, bup_s, bdn_s, s12, s12o, gd_s, gu_s, gsp, gsl,
           w_sem, wrow_s, wrow_r, wx_s, wx_r, wy_s, wy_r, wa_s, wa_r, wb_s, wb_r,
           sm_sem, land_s, land_r, ld_sem, out_sem, rd_sem, yd_sem, dl_sem, gd_sem,
           ru_s, ru_r, yu_s, yu_r, au_s, au_r, gu_sem, s12_sem, gs_sem, credit, free_row, free_dep):
    chunks = x_h.shape[0] // M
    half_f = wu_h.shape[1]
    hw = x_h.shape[1]
    full = 2 * hw
    tiles = 2 * half_f // FT
    c, r, d = lax.axis_index('col'), lax.axis_index('row'), lax.axis_index('depth')
    b = lax.rem(r + c, 2)
    peer = {'col': 1 - c, 'row': 1 - r, 'depth': 1 - d}

    def send(src, dst, s_sem, r_sem, axis):
        return pltpu.make_async_remote_copy(src_ref=src, dst_ref=dst, send_sem=s_sem, recv_sem=r_sem,
                                            device_id={axis: peer[axis]}, device_id_type=MESH)

    def local(src, dst, sem):
        return pltpu.make_async_copy(src, dst, sem)

    def rows_of(k):
        return pl.ds(pl.multiple_of(k * M, M), M)

    def pipelined(lo, hi, first, mid, last):
        first(lo)
        first(lo + 1)
        mid(lo)
        for j in range(lo, hi):
            if j + 2 < hi:
                first(j + 2)
            last(j)
            if j + 1 < hi:
                mid(j + 1)

    bar = pltpu.get_barrier_semaphore()
    for axis in ('col', 'row', 'depth'):
        pl.semaphore_signal(bar, inc=1, device_id={axis: peer[axis]}, device_id_type=MESH)
    pl.semaphore_wait(bar, 3)

    def w_cols(kind, blk, dep, s):
        if kind == 0:
            n = half_rows_u // SUBS
            return wu.at[pl.ds(pl.multiple_of(blk * hw + dep * half_rows_u + s * n, n), n), pl.ds(half_f, half_f)]
        n = half_rows_d // SUBS
        return wd.at[pl.ds(pl.multiple_of(blk * half_f + dep * half_rows_d + s * n, n), n), pl.ds(hw, hw)]

    half_rows_u, half_rows_d = hw // 2, half_f // 2
    w_srcs = (wu_h, wd_h)

    def w_src(kind, s):
        half = (half_rows_u, half_rows_d)[kind]
        n = half // SUBS
        return w_srcs[kind].at[pl.ds(pl.multiple_of(d * half + s * n, n), n), :]

    def w_own(kind):
        if kind == 0:
            return wu.at[pl.ds(pl.multiple_of(b * hw, hw), hw), pl.ds(0, half_f)]
        return wd.at[pl.ds(pl.multiple_of(b * half_f, half_f), half_f), pl.ds(0, hw)]

    def w_x(kind, s):
        return send(w_src(kind, s), w_cols(kind, 1 - b, d, s), wx_s.at[kind, s], wx_r.at[kind, s], 'col')

    def w_y(kind, s):
        return send(w_cols(kind, b, d, s), w_cols(kind, b, d, s), wy_s.at[kind, s], wy_r.at[kind, s], 'depth')

    def w_a(kind, s):
        return send(w_cols(kind, b, d, s), w_cols(kind, b, d, s), wa_s.at[kind, s], wa_r.at[kind, s], 'row')

    def w_b(kind, s):
        return send(w_cols(kind, b, 1 - d, s), w_cols(kind, b, 1 - d, s), wb_s.at[kind, s], wb_r.at[kind, s], 'row')

    def w_row(kind):
        return send(w_srcs[kind], w_own(kind), wrow_s.at[kind], wrow_r.at[kind], 'row')

    def w_load(kind):
        return local(w_srcs[kind], w_own(kind), w_sem.at[kind])

    def w_forward_x(kind):
        for s in range(SUBS):
            w_x(kind, s).wait_recv()
            w_y(kind, s).start()
            w_a(kind, s).start()

    def w_forward_y(kind):
        for s in range(SUBS):
            w_y(kind, s).wait_recv()
            w_b(kind, s).start()

    def w_finish(kind):
        for s in range(SUBS):
            w_a(kind, s).wait_recv()
            w_b(kind, s).wait_recv()
        for s in range(SUBS):
            w_x(kind, s).wait_send()
            w_y(kind, s).wait_send()
            w_a(kind, s).wait_send()
            w_b(kind, s).wait_send()

    def stream(src, k, q):
        slot = lax.rem(q, 4)
        return send(src.at[rows_of(k), :], land.at[slot], land_s.at[slot], land_r.at[slot], 'col')

    def stream_next(src, k, q):
        @pl.when(q >= 4)
        def _():
            stream(src, k, q).wait_send()
            pl.semaphore_wait(credit, 1)
        stream(src, k, q).start()

    gam_at, bet_at, bdn_at = (pl.ds(half_f + i * hw, hw) for i in range(3))
    sm_own = [local(bup_h, bup_s.at[0], sm_sem.at[2, 0]), local(gam_h, smv.at[0, :, gam_at], sm_sem.at[2, 1]),
              local(bet_h, smv.at[0, :, bet_at], sm_sem.at[2, 2]), local(bdn_h, bdn_s, sm_sem.at[2, 3])]
    sm_out = [send(bup_h, bup_s.at[1], sm_sem.at[0, 0], sm_sem.at[1, 0], 'col'),
              send(gam_h, smv.at[1, :, gam_at], sm_sem.at[0, 1], sm_sem.at[1, 1], 'col'),
              send(bet_h, smv.at[1, :, bet_at], sm_sem.at[0, 2], sm_sem.at[1, 2], 'col')]
    for cp in sm_own + sm_out:
        cp.start()
    for s in range(SUBS):
        w_x(0, s).start()
    for kind in range(2):
        w_load(kind).start()
        w_row(kind).start()
    stream(x_h, 0, 0).start()
    stream(x_h, 1, 1).start()

    def load_f(k):
        s = lax.rem(k, 2)
        return (local(x_h.at[rows_of(k), :], own.at[s], ld_sem.at[0, s]),
                local(dy_h.at[rows_of(k), :], aux.at[s], ld_sem.at[1, s]))

    for cp in load_f(0):
        cp.start()

    acc_d[...] = jnp.zeros_like(acc_d)
    acc_u[...] = jnp.zeros_like(acc_u)
    bup8[...] = jnp.zeros_like(bup8)
    gb8[...] = jnp.zeros_like(gb8)

    w_forward_x(0)
    w_forward_y(0)
    for kind in range(2):
        w_load(kind).wait()
        w_row(kind).wait()
    for cp in sm_own + sm_out:
        cp.wait()
    for i in range(half_f // 128):
        for side in range(2):
            smv[side, :, i * 128:(i + 1) * 128] = bup_s[side, i:i + 1, :].astype(F32)
    for i in range(hw // 128):
        smv[0, :, half_f + full + i * 128:half_f + full + (i + 1) * 128] = bdn_s[i:i + 1, :].astype(F32)
    w_finish(0)

    def out_f(k):
        s = lax.rem(k, 2)
        return (local(ub.at[s], u_h.at[rows_of(k), :], out_sem.at[0, s]),
                local(xn2.at[s], xn_h.at[rows_of(k), :], out_sem.at[1, s]),
                local(st.at[s], st_h.at[rows_of(k), :], out_sem.at[2, s]),
                local(yo.at[s], y_h.at[rows_of(k), :], out_sem.at[3, s]))

    def chunk_f(k, carry):
        s = lax.rem(k, 2)
        slot = lax.rem(k, 4)

        @pl.when(k < chunks - 2)
        def _():
            stream_next(x_h, k + 2, k + 2)

        @pl.when(k == chunks - 7)
        def _():
            for p in range(SUBS):
                w_x(1, p).start()

        @pl.when(k == chunks - 3)
        def _():
            w_forward_x(1)

        @pl.when(k == chunks - 1)
        def _():
            w_forward_y(1)

        @pl.when(k >= chunks - 2)
        def _():
            stream_next(dy_h, k - (chunks - 2), k + 2)

        for cp in load_f(k):
            cp.wait()

        @pl.when(k < chunks - 1)
        def _():
            for cp in load_f(k + 1):
                cp.start()

        @pl.when(k >= 2)
        def _():
            for cp in out_f(k):
                cp.wait()

        stream(x_h, k, k).wait_recv()

        gam = jnp.concatenate([smv[0, :, half_f:half_f + hw], smv[1, :, half_f:half_f + hw]], axis=1)
        bet = jnp.concatenate([smv[0, :, half_f + hw:half_f + full], smv[1, :, half_f + hw:half_f + full]], axis=1)
        step = 32
        for i in range(M // step):
            rs = slice(i * step, (i + 1) * step)
            xv = jnp.concatenate([own[s, rs, :], land[slot, rs, :]], axis=1).astype(F32)
            mean = jnp.sum(xv, axis=1, keepdims=True) * (1.0 / full)
            cen = xv - mean
            istd = lax.rsqrt(jnp.sum(cen * cen, axis=1, keepdims=True) * (1.0 / full) + LN_EPS)
            xn2[s, rs, :] = (cen * istd * gam + bet).astype(BF16)
            st[s, rs, :] = jnp.concatenate([jnp.broadcast_to(mean, (step, 64)), jnp.broadcast_to(istd, (step, 64))], axis=1)
        dyv = aux[s]
        tr[:hw, :] = dyv.T
        gb8[:, full:full + hw] += fold8(dyv.astype(F32))

        def up(j):
            js = slice(j * FT, (j + 1) * FT)
            side, at = divmod(j * FT, half_f)
            u = dot(xn2[s], wu[:, js], 1, 0) + smv[side, :, at:at + FT]
            ub[s, :, js] = u.astype(BF16)

        def mid(j):
            js = slice(j * FT, (j + 1) * FT)
            act[j % 2] = gelu(ub[s, :, js].astype(F32)).astype(BF16)

        def down(j):
            js = slice(j * FT, (j + 1) * FT)
            part = dot(act[j % 2], wd[js, :hw], 1, 0)
            acc[0] = part if j == 0 else acc[0] + part
            blk, rest = divmod(j * FT, half_f)
            qt, at = divmod(rest, half_f // 2)
            acc_d[blk, qt, :, at:at + FT] += dot(tr[:hw, :], act[j % 2], 1, 0)

        pipelined(0, tiles, up, mid, down)
        bdn = smv[0, :, half_f + full:half_f + full + hw]
        yo[s] = (own[s].astype(F32) + acc[0] + bdn).astype(BF16)
        for cp in out_f(k):
            cp.start()
        pl.semaphore_signal(credit, inc=1, device_id={'col': peer['col']}, device_id_type=MESH)
        return carry

    lax.fori_loop(0, chunks, chunk_f, 0)

    rdown = send(acc_d.at[1 - b], rdown_h, rd_sem.at[0], rd_sem.at[1], 'row')
    rdown.start()
    for k in (chunks - 2, chunks - 1):
        for cp in out_f(k):
            cp.wait()

    def load_b(k):
        s = lax.rem(k, 2)
        rs = rows_of(k)
        return (local(dy_h.at[rs, :], own.at[s], ld_sem.at[0, s]),
                local(x_h.at[rs, :], aux.at[s], ld_sem.at[1, s]),
                local(u_h.at[rs, :], ub.at[s], ld_sem.at[2, s]),
                local(xn_h.at[rs, :], xn2.at[s], ld_sem.at[3, s]),
                local(st_h.at[rs, :], st.at[s], ld_sem.at[4, s]))

    for cp in load_b(0):
        cp.start()
    w_finish(1)

    rd_load = local(rdown_h, acc_d.at[1 - b], dl_sem.at[0])
    ydown = send(acc_d.at[b, 1 - d], ydown_h, yd_sem.at[0], yd_sem.at[1], 'depth')
    yd_load = local(ydown_h, acc_d.at[1 - b, 0], dl_sem.at[1])
    half_d = half_f // 2
    gd_rows = pl.ds(pl.multiple_of(d * half_d, half_d), half_d)
    gd_own = local(gd_s, gwd_h.at[gd_rows, :], gd_sem.at[0])
    gd_far = send(gd_s, gwd_h.at[gd_rows, :], gd_sem.at[1], gd_sem.at[2], 'depth')

    def dxn_out(k):
        s = lax.rem(k, 2)
        return local(acc.at[s], dxn_h.at[rows_of(k), :], out_sem.at[0, s])

    def reduce_down(k):
        @pl.when(k == 1)
        def _():
            rdown.wait()
            rd_load.start()

        @pl.when(k == 2)
        def _():
            rd_load.wait()
            for q in range(2):
                for i in range(hw // 64):
                    rs = slice(i * 64, (i + 1) * 64)
                    acc_d[b, q, rs, :] += acc_d[1 - b, q, rs, :]

        @pl.when(k == 3)
        def _():
            ydown.start()

        @pl.when(k == 9)
        def _():
            ydown.wait()
            yd_load.start()

        @pl.when(k == 10)
        def _():
            yd_load.wait()
            for i in range(half_d // 128):
                cs = slice(i * 128, (i + 1) * 128)
                total = acc_d[b, d, :, cs] + acc_d[1 - b, 0, :, cs]
                gd_s[cs, :] = total.T.astype(BF16)

        @pl.when(k == 11)
        def _():
            gd_own.start()
            gd_far.start()
            pl.semaphore_signal(free_row, inc=1, device_id={'row': peer['row']}, device_id_type=MESH)
            pl.semaphore_signal(free_dep, inc=1, device_id={'depth': peer['depth']}, device_id_type=MESH)

    own_tiles = half_f // FT
    parts = half_f // LT
    early = parts // 2

    def grads(k, s, slot, lo, hi):
        def grad(j):
            js = slice(j * FT, (j + 1) * FT)
            dyv = jnp.concatenate([own[s], land[slot]], axis=1)
            da_s[j % 2] = dot(dyv, wd[js, :], 1, 1)

        def mid(j):
            js = slice(j * FT, (j + 1) * FT)
            du = (da_s[j % 2] * gelu_slope(ub[s, :, js].astype(F32))).astype(BF16)
            act[j % 2] = du
            if j < own_tiles:
                bup8[:, js] += fold8(du.astype(F32))

        def back(j):
            js = slice(j * FT, (j + 1) * FT)
            part = dot(act[j % 2], wu[:hw, js], 1, 1)
            acc[s] = part if j == 0 else acc[s] + part
            if j < own_tiles:
                up = dot(tr[...], act[j % 2], 1, 0)
                for i in range(4):
                    acc_u[i // 2, i % 2, :, js] += up[i * (hw // 2):(i + 1) * (hw // 2)]

        pipelined(lo, hi, grad, mid, back)

    def grads_last(s, slot, done):
        def grad(j):
            dyv = jnp.concatenate([own[s], land[slot]], axis=1)
            da_s[j % 2, :, :LT] = dot(dyv, wd[j * LT:(j + 1) * LT, :], 1, 1)

        def mid(j):
            js = slice(j * LT, (j + 1) * LT)
            du = (da_s[j % 2, :, :LT] * gelu_slope(ub[s, :, js].astype(F32))).astype(BF16)
            ub[s, :, js] = du
            bup8[:, js] += fold8(du.astype(F32))

        def back(j):
            js = slice(j * LT, (j + 1) * LT)
            up = dot(tr[...], ub[s, :, js], 1, 0)
            for i in range(4):
                acc_u[i // 2, i % 2, :, js] += up[i * (hw // 2):(i + 1) * (hw // 2)]

        grad(0)
        for j in range(parts):
            if j + 1 < parts:
                grad(j + 1)
            mid(j)
            back(j)
            done(j)

    def other_half(k, s, slot, peeled=False):
        if peeled:
            for j in range(own_tiles):
                js = slice(j * FT, (j + 1) * FT)
                part = dot(ub[s, :, js], wu[:hw, js], 1, 1)
                acc[s] = part if j == 0 else acc[s] + part
        grads(k, s, slot, own_tiles, tiles)
        gam = smv[0, :, half_f:half_f + hw]
        step = 128
        for i in range(M // step):
            rs = slice(i * step, (i + 1) * step)
            dxn = acc[s, rs, :]
            xh = (aux[s, rs, :].astype(F32) - st[s, rs, 0:1]) * st[s, rs, 64:65]
            px = dxn * xh
            gb8[:, :hw] += fold8(px)
            gb8[:, hw:full] += fold8(dxn)
            s1 = jnp.sum(dxn * gam, axis=1, keepdims=True)
            s2 = jnp.sum(px * gam, axis=1, keepdims=True)
            both = jnp.concatenate([jnp.broadcast_to(s1, (step, 64)), jnp.broadcast_to(s2, (step, 64))], axis=1).T
            s12[k, 0:4, rs] = both[0:4]
            s12[k, 4:8, rs] = both[64:68]
        dxn_out(k).start()

    last = chunks - 1

    def chunk_b(k, carry):
        s = lax.rem(k, 2)
        q = k + chunks
        slot = lax.rem(q, 4)

        @pl.when(k < chunks - 2)
        def _():
            stream_next(dy_h, k + 2, q + 2)

        reduce_down(k)
        for cp in load_b(k):
            cp.wait()
        for cp in load_b(k + 1):
            cp.start()

        @pl.when(k >= 2)
        def _():
            dxn_out(k).wait()

        stream(dy_h, k, q).wait_recv()
        tr[...] = xn2[s].T
        grads(k, s, slot, 0, own_tiles)
        other_half(k, s, slot)

        @pl.when(k < chunks - 4)
        def _():
            pl.semaphore_signal(credit, inc=1, device_id={'col': peer['col']}, device_id_type=MESH)
        return carry

    lax.fori_loop(0, last, chunk_b, 0)

    pl.semaphore_wait(free_row, 1)
    pl.semaphore_wait(free_dep, 1)
    hq = hw // 2
    wide = half_f // 2 // LT

    def ru(p):
        dst = acc_d.at[0, :, pl.ds((p // wide) * hq, hq), pl.ds((p % wide) * LT, LT)]
        return send(acc_u.at[1 - b, :, :, pl.ds(p * LT, LT)], dst, ru_s.at[p], ru_r.at[p], 'row')

    def yu(p):
        dst = acc_d.at[1, p // wide, pl.ds(0, hq), pl.ds((p % wide) * LT, LT)]
        return send(acc_u.at[b, 1 - d, :, pl.ds(p * LT, LT)], dst, yu_s.at[p], yu_r.at[p], 'depth')

    def au(p):
        ps = pl.ds(p * LT, LT)
        return send(gu_s.at[:, ps], guo_h.at[:, ps], au_s.at[p], au_r.at[p], 'depth')

    half_g = early * LT
    gua_out = local(gu_s.at[:, pl.ds(0, half_g)], gua_h, gu_sem.at[0])
    gub_out = local(gu_s.at[:, pl.ds(half_g, half_g)], gub_h, gu_sem.at[1])

    def to_depth(p):
        ru(p).wait_recv()
        for i in range(2):
            rs = slice((p // wide) * hq, (p // wide) * hq + hq)
            cs = slice((p % wide) * LT, (p % wide) * LT + LT)
            acc_u[b, i, :, p * LT:(p + 1) * LT] += acc_d[0, i, rs, cs]
        yu(p).start()

    def tile_done(p):
        ru(p).start()
        if p >= 1:
            to_depth(p - 1)

    def from_depth(p):
        yu(p).wait_recv()
        cs = slice((p % wide) * LT, (p % wide) * LT + LT)
        gu_s[:, p * LT:(p + 1) * LT] = (acc_u[b, d, :, p * LT:(p + 1) * LT] + acc_d[1, p // wide, 0:hq, cs]).astype(BF16)
        if p < early:
            au(p).start()

    slot_l, s_l = (chunks + last) % 4, last % 2
    s12_a = send(s12.at[pl.ds(0, last)], s12o.at[pl.ds(0, last)], s12_sem.at[0], s12_sem.at[1], 'col')
    s12_b = send(s12.at[last], s12o.at[last], s12_sem.at[2], s12_sem.at[3], 'col')
    for cp in load_b(last):
        cp.wait()
    dxn_out(last).wait()
    tr[...] = xn2[s_l].T
    stream(dy_h, last, chunks + last).wait_recv()
    s12_a.start()
    grads_last(s_l, slot_l, tile_done)
    to_depth(parts - 1)

    other_half(last, s_l, slot_l, True)
    s12_b.start()
    gsp[0] = jnp.concatenate([jnp.sum(bup8[...], axis=0, keepdims=True), jnp.sum(gb8[...], axis=0, keepdims=True)], axis=1)
    gs_row = send(gsp.at[0], gsl.at[0], gs_sem.at[0], gs_sem.at[1], 'row')
    gs_row.start()

    def load_t(k):
        s = lax.rem(k, 2)
        rs = rows_of(k)
        return (local(dy_h.at[rs, :], own.at[s], ld_sem.at[0, s]),
                local(x_h.at[rs, :], aux.at[s], ld_sem.at[1, s]),
                local(dxn_h.at[rs, :], da_s.at[s], ld_sem.at[2, s]),
                local(st_h.at[rs, :], st.at[s], ld_sem.at[4, s]))

    def out_t(k):
        s = lax.rem(k, 2)
        return local(yo.at[s], dx_h.at[rows_of(k), :], out_sem.at[3, s])

    for cp in load_t(0):
        cp.start()
    for k in range(4):
        stream(dy_h, k, chunks + k).wait_send()
    for k in (chunks - 2, chunks - 1):
        dxn_out(k).wait()
    gd_own.wait()
    gd_far.wait()
    for p in range(parts):
        ru(p).wait_send()
    gs_row.wait()
    gsp[1] = gsp[0] + gsl[0]
    gs_dep = send(gsp.at[1], gsl.at[1], gs_sem.at[2], gs_sem.at[3], 'depth')
    gs_dep.start()
    s12_a.wait()
    s12_b.wait()
    from_depth(0)

    def chunk_t(k, carry):
        s = lax.rem(k, 2)
        for cp in load_t(k):
            cp.wait()

        @pl.when(k < last)
        def _():
            for cp in load_t(k + 1):
                cp.start()

        @pl.when(k >= 2)
        def _():
            out_t(k).wait()

        gam = smv[0, :, half_f:half_f + hw]
        step = 128
        for i in range(M // step):
            rs = slice(i * step, (i + 1) * step)
            sums = (s12[k, :, rs] + s12o[k, :, rs]) * (1.0 / full)
            cols = jnp.concatenate([sums] * (step // 8), axis=0).T
            istd = st[s, rs, 64:65]
            xh = (aux[s, rs, :].astype(F32) - st[s, rs, 0:1]) * istd
            g = da_s[s, rs, :] * gam
            yo[s, rs, :] = (own[s, rs, :].astype(F32) + istd * (g - cols[:, 0:1] - xh * cols[:, 4:5])).astype(BF16)
        out_t(k).start()
        return carry

    lax.fori_loop(0, chunks, chunk_t, 0)
    for p in range(1, early):
        from_depth(p)
    gua_out.start()
    for k in (chunks - 2, chunks - 1):
        out_t(k).wait()
    gua_out.wait()
    for p in range(early, parts):
        from_depth(p)
    gub_out.start()
    for p in range(parts):
        yu(p).wait_send()
    gs_dep.wait()
    gsp[0] = gsp[1] + gsl[1]
    gs_out = local(gsp.at[0], gs_h, gs_sem.at[4])
    gs_out.start()
    gub_out.wait()
    gs_out.wait()
    for p in range(early):
        au(p).wait()


def finish_kernel(y_in, dx_in, gwd_in, gs, gua, gub, guo, y, dx, gwd, gwu, gbup, ggam, gbet, gbdn, big, small, sums, far_s, in_sem, out_sem):
    rows, hw = y.shape
    half_f = gwd.shape[0]
    hq, half_g = gua.shape
    d = lax.axis_index('depth')
    mine = pl.ds(pl.multiple_of(d * hq, hq), hq)
    far = pl.ds(pl.multiple_of((1 - d) * hq, hq), hq)
    n = rows // COPIES
    ins, outs = [], []

    def move(src, buf, dst, more=()):
        k = len(ins)
        ins.append(pltpu.make_async_copy(src, buf, in_sem.at[k]))
        outs.append([pltpu.make_async_copy(buf, to, out_sem.at[k, i]) for i, to in enumerate((dst, *more))])

    left, right = pl.ds(0, half_g), pl.ds(half_g, half_g)
    for i in range(COPIES):
        rs = pl.ds(i * n, n)
        move(y_in.at[rs], big.at[0, rs], y.at[rs])
        move(dx_in.at[rs], big.at[1, rs], dx.at[rs])
    move(gwd_in, small, gwd)
    move(gua, far_s.at[0], gwu.at[mine, left])
    move(gub, far_s.at[1], gwu.at[mine, right], (gwu.at[far, right],))
    move(guo, far_s.at[2], gwu.at[far, left])
    at = [(0, half_f, gbup), (half_f, hw, ggam), (half_f + hw, hw, gbet), (half_f + 2 * hw, hw, gbdn)]
    for a, w, dst in at:
        move(gs.at[:, pl.ds(a, w)], sums.at[:, pl.ds(a, w)], dst)
    for cp in ins:
        cp.start()
    for cp, tos in zip(ins, outs):
        cp.wait()
        for to in tos:
            to.start()
    for tos in outs:
        for to in tos:
            to.wait()


def solution(mesh):
    tok_spec = P(('dp', 'depth', 'row'), 'col')
    vec_spec = P('col')
    mat_spec = P('row', 'col')
    grad_vec = P(('dp', 'col'))
    grad_mat = P(('dp', 'row'), 'col')

    def local_pass(x, gamma, beta, w_up, b_up, w_down, b_down, dy):
        rows, hw = x.shape
        half_f = b_up.shape[0]
        full_f, full = 2 * half_f, 2 * hw
        chunks = rows // M
        smalls = [b_up.reshape(-1, 128), gamma.reshape(1, -1), beta.reshape(1, -1), b_down.reshape(-1, 128)]
        hbm = pl.BlockSpec(memory_space=pltpu.HBM)
        sds = jax.ShapeDtypeStruct
        V, D, R = pltpu.VMEM, pltpu.SemaphoreType.DMA, pltpu.SemaphoreType.REGULAR
        outs = [
            sds((rows, hw), BF16), sds((rows, hw), BF16), sds((half_f, hw), BF16), sds((1, full_f), F32),
            sds((hw // 2, half_f // 2), BF16), sds((hw // 2, half_f // 2), BF16), sds((hw // 2, half_f // 2), BF16),
            sds((rows, 128), F32), sds((rows, hw), F32),
            sds((rows, full_f), BF16), sds((rows, full), BF16), sds((2, hw, half_f // 2), F32), sds((hw, half_f // 2), F32),
        ]
        parts = half_f // LT
        scratch = [
            V((full, full_f), BF16), V((full_f, full), BF16), V((2, 2, hw, half_f // 2), F32), V((2, 2, hw // 2, half_f), F32),
            V((2, M, hw), BF16), V((4, M, hw), BF16), V((2, M, hw), BF16), V((2, M, full), BF16), V((full, M), BF16),
            V((2, M, full_f), BF16), V((2, M, 128), F32), V((2, M, FT), F32), V((2, M, FT), BF16), V((2, M, hw), F32), V((2, M, hw), BF16),
            V((8, half_f), F32), V((8, half_f), F32), V((2, 1, full_f), F32),
            V((2, half_f // 128, 128), BF16), V((hw // 128, 128), BF16), V((chunks, 8, M), F32), V((chunks, 8, M), F32),
            V((half_f // 2, hw), BF16), V((hw // 2, half_f), BF16), V((2, 1, full_f), F32), V((2, 1, full_f), F32),
            D((2,)), D((2,)), D((2,)), D((2, SUBS)), D((2, SUBS)), D((2, SUBS)), D((2, SUBS)), D((2, SUBS)), D((2, SUBS)), D((2, SUBS)), D((2, SUBS)),
            D((3, 4)), D((4,)), D((4,)), D((5, 2)), D((4, 2)), D((2,)), D((2,)), D((2,)), D((3,)),
            D((parts,)), D((parts,)), D((parts,)), D((parts,)), D((parts // 2,)), D((parts // 2,)), D((2,)), D((4,)), D((5,)), R, R, R,
        ]
        res = pl.pallas_call(
            kernel,
            out_shape=outs,
            in_specs=[hbm] * 8,
            out_specs=[hbm] * len(outs),
            scratch_shapes=scratch,
            compiler_params=pltpu.CompilerParams(
                collective_id=0, has_side_effects=True, vmem_limit_bytes=67043328),
            cost_estimate=pl.CostEstimate(flops=16 * rows * full * full_f, bytes_accessed=2 ** 28, transcendentals=2 * rows * full_f),
            name='mlp_block',
        )(x, dy, w_up, w_down, *smalls)
        y, dx, gwd, gs, gua, gub, guo = res[:7]
        gub_far = lax.ppermute(gub, 'depth', ((0, 1), (1, 0)))
        moves = 2 * COPIES + 8
        y, dx, gwd, gwu, gbup, ggam, gbet, gbdn = pl.pallas_call(
            finish_kernel,
            out_shape=[sds((rows, hw), BF16), sds((rows, hw), BF16), sds((half_f, hw), BF16), sds((hw, half_f), BF16),
                       sds((1, half_f), F32), sds((1, hw), F32), sds((1, hw), F32), sds((1, hw), F32)],
            in_specs=[hbm] * 7,
            out_specs=[hbm] * 8,
            scratch_shapes=[V((2, rows, hw), BF16), V((half_f, hw), BF16), V((1, full_f), F32), V((3, hw // 2, half_f // 2), BF16),
                            D((moves,)), D((moves, 2))],
            compiler_params=pltpu.CompilerParams(vmem_limit_bytes=67043328),
            cost_estimate=pl.CostEstimate(flops=2 ** 33, bytes_accessed=42 * 2 ** 20, transcendentals=0),
            name='finish',
        )(y, dx, gwd, gs, gua, gub, guo)
        far = (1 - lax.axis_index('depth')) * (hw // 2)
        gwu = lax.dynamic_update_slice(gwu, gub_far, (far, half_f // 2))
        return y, dx, ggam.reshape(-1), gbet.reshape(-1), gwu, gbup.reshape(-1), gwd, gbdn.reshape(-1)

    return jax.shard_map(
        local_pass,
        mesh=mesh,
        in_specs=(tok_spec, vec_spec, vec_spec, mat_spec, vec_spec, mat_spec, vec_spec, tok_spec),
        out_specs=(tok_spec, tok_spec, grad_vec, grad_vec, grad_mat, grad_vec, grad_mat, grad_vec),
        check_vma=False,
    )
```

```python
import functools

import jax
import jax.numpy as jnp
from jax import lax
from jax.experimental import pallas as pl
from jax.experimental.pallas import tpu as pltpu
from jax.sharding import PartitionSpec as P

LN_EPS = 1e-5
C0 = 0.7978845608
C1 = C0 * 0.044715
M = 512
FT = 512
LT = 256
COPIES = 4
SUBS = 2
EARLY = 3
BF16, F32 = jnp.bfloat16, jnp.float32
MESH = pl.DeviceIdType.MESH


def dot(lhs, rhs, lhs_dim, rhs_dim):
    return lax.dot_general(lhs, rhs, (((lhs_dim,), (rhs_dim,)), ((), ())), preferred_element_type=F32)


def gelu(v):
    t = jnp.tanh(v * (C1 * (v * v) + C0))
    h = 0.5 * v
    return h * t + h


def gelu_slope(v):
    v2 = v * v
    t = jnp.tanh(v * (C1 * v2 + C0))
    return (v * (1.0 - t * t)) * (1.5 * C1 * v2 + 0.5 * C0) + (0.5 * t + 0.5)


def fold8(v):
    return jnp.sum(v.reshape(v.shape[0] // 8, 8, v.shape[1]), axis=0)


def kernel(x_h, dy_h, wu_h, wd_h, bup_h, gam_h, bet_h, bdn_h,
           y_h, dx_h, gwd_h, gs_h, gua_h, gub_h, guo_h, st_h, dxn_h, u_h, xn_h, rdown_h, ydown_h,
           wu, wd, acc_d, acc_u, own, land, aux, xn2, tr, ub, st, da_s, act, acc, yo,
           bup8, gb8, smv, bup_s, bdn_s, s12, s12o, gd_s, gu_s, gsp, gsl,
           w_sem, wrow_s, wrow_r, wx_s, wx_r, wy_s, wy_r, wa_s, wa_r, wb_s, wb_r,
           sm_sem, land_s, land_r, ld_sem, out_sem, rd_sem, yd_sem, dl_sem, gd_sem,
           ru_s, ru_r, yu_s, yu_r, au_s, au_r, gu_sem, s12_sem, gs_sem, credit, free_row, free_dep):
    chunks = x_h.shape[0] // M
    half_f = wu_h.shape[1]
    hw = x_h.shape[1]
    full = 2 * hw
    tiles = 2 * half_f // FT
    c, r, d = lax.axis_index('col'), lax.axis_index('row'), lax.axis_index('depth')
    b = lax.rem(r + c, 2)
    peer = {'col': 1 - c, 'row': 1 - r, 'depth': 1 - d}

    def send(src, dst, s_sem, r_sem, axis):
        return pltpu.make_async_remote_copy(src_ref=src, dst_ref=dst, send_sem=s_sem, recv_sem=r_sem,
                                            device_id={axis: peer[axis]}, device_id_type=MESH)

    def local(src, dst, sem):
        return pltpu.make_async_copy(src, dst, sem)

    def rows_of(k):
        return pl.ds(pl.multiple_of(k * M, M), M)

    def pipelined(lo, hi, first, mid, last):
        first(lo)
        first(lo + 1)
        mid(lo)
        for j in range(lo, hi):
            if j + 2 < hi:
                first(j + 2)
            last(j)
            if j + 1 < hi:
                mid(j + 1)

    bar = pltpu.get_barrier_semaphore()
    for axis in ('col', 'row', 'depth'):
        pl.semaphore_signal(bar, inc=1, device_id={axis: peer[axis]}, device_id_type=MESH)
    pl.semaphore_wait(bar, 3)

    def w_cols(kind, blk, dep, s):
        if kind == 0:
            n = half_rows_u // SUBS
            return wu.at[pl.ds(pl.multiple_of(blk * hw + dep * half_rows_u + s * n, n), n), pl.ds(half_f, half_f)]
        n = half_rows_d // SUBS
        return wd.at[pl.ds(pl.multiple_of(blk * half_f + dep * half_rows_d + s * n, n), n), pl.ds(hw, hw)]

    half_rows_u, half_rows_d = hw // 2, half_f // 2

    def w_half(kind):
        if kind == 0:
            return wu.at[pl.ds(0, half_rows_u), pl.ds(0, half_f)]
        return wd.at[pl.ds(0, half_rows_d), pl.ds(0, hw)]

    w_srcs = (wu_h, wd_h)

    def w_src(kind, s):
        half = (half_rows_u, half_rows_d)[kind]
        n = half // SUBS
        return w_srcs[kind].at[pl.ds(pl.multiple_of(d * half + s * n, n), n), :]

    def w_own(kind):
        if kind == 0:
            return wu.at[pl.ds(pl.multiple_of(b * hw, hw), hw), pl.ds(0, half_f)]
        return wd.at[pl.ds(pl.multiple_of(b * half_f, half_f), half_f), pl.ds(0, hw)]

    def w_x(kind, s):
        return send(w_src(kind, s), w_cols(kind, 1 - b, d, s), wx_s.at[kind], wx_r.at[kind, s], 'col')

    def w_y(kind, s):
        return send(w_cols(kind, b, d, s), w_cols(kind, b, d, s), wy_s.at[kind], wy_r.at[kind, s], 'depth')

    def w_a(kind, s):
        return send(w_cols(kind, b, d, s), w_cols(kind, b, d, s), wa_s.at[kind], wa_r.at[kind, s], 'row')

    def w_b(kind, s):
        return send(w_cols(kind, b, 1 - d, s), w_cols(kind, b, 1 - d, s), wb_s.at[kind], wb_r.at[kind, s], 'row')

    def w_row(kind):
        return send(w_srcs[kind], w_own(kind), wrow_s.at[kind], wrow_r.at[kind], 'row')

    def w_load(kind):
        return local(w_srcs[kind], w_own(kind), w_sem.at[kind])

    def w_forward_x(kind):
        for s in range(SUBS):
            w_x(kind, s).wait_recv()
            w_y(kind, s).start()
            w_a(kind, s).start()

    def w_forward_y(kind):
        for s in range(SUBS):
            w_y(kind, s).wait_recv()
            w_b(kind, s).start()

    def w_finish(kind):
        for s in range(SUBS):
            w_a(kind, s).wait_recv()
            w_b(kind, s).wait_recv()
        for sems in (wx_s, wy_s, wa_s, wb_s):
            local(w_half(kind), w_half(kind), sems.at[kind]).wait()

    def stream(src, k, q):
        slot = lax.rem(q, 4)
        return send(src.at[rows_of(k), :], land.at[slot], land_s.at[slot], land_r.at[slot], 'col')

    def stream_next(src, k, q):
        @pl.when(q >= 4)
        def _():
            stream(src, k, q).wait_send()
            pl.semaphore_wait(credit, 1)
        stream(src, k, q).start()

    gam_at, bet_at, bdn_at = (pl.ds(half_f + i * hw, hw) for i in range(3))
    sm_own = [local(bup_h, bup_s.at[0], sm_sem.at[2, 0]), local(gam_h, smv.at[0, :, gam_at], sm_sem.at[2, 1]),
              local(bet_h, smv.at[0, :, bet_at], sm_sem.at[2, 2]), local(bdn_h, bdn_s, sm_sem.at[2, 3])]
    sm_out = [send(bup_h, bup_s.at[1], sm_sem.at[0, 0], sm_sem.at[1, 0], 'col'),
              send(gam_h, smv.at[1, :, gam_at], sm_sem.at[0, 1], sm_sem.at[1, 1], 'col'),
              send(bet_h, smv.at[1, :, bet_at], sm_sem.at[0, 2], sm_sem.at[1, 2], 'col')]
    for cp in sm_own + sm_out:
        cp.start()
    for s in range(SUBS):
        w_x(0, s).start()
    for kind in range(2):
        w_load(kind).start()
        w_row(kind).start()
    stream(x_h, 0, 0).start()
    stream(x_h, 1, 1).start()

    def load_f(k):
        s = lax.rem(k, 2)
        return (local(x_h.at[rows_of(k), :], own.at[s], ld_sem.at[0, s]),
                local(dy_h.at[rows_of(k), :], aux.at[s], ld_sem.at[1, s]))

    for cp in load_f(0):
        cp.start()

    acc_d[...] = jnp.zeros_like(acc_d)
    acc_u[...] = jnp.zeros_like(acc_u)
    bup8[...] = jnp.zeros_like(bup8)
    gb8[...] = jnp.zeros_like(gb8)

    w_forward_x(0)
    w_forward_y(0)
    for kind in range(2):
        w_load(kind).wait()
        w_row(kind).wait()
    for cp in sm_own + sm_out:
        cp.wait()
    for i in range(half_f // 128):
        for side in range(2):
            smv[side, :, i * 128:(i + 1) * 128] = bup_s[side, i:i + 1, :].astype(F32)
    for i in range(hw // 128):
        smv[0, :, half_f + full + i * 128:half_f + full + (i + 1) * 128] = bdn_s[i:i + 1, :].astype(F32)
    w_finish(0)

    def out_f(k):
        s = lax.rem(k, 2)
        return (local(ub.at[s], u_h.at[rows_of(k), :], out_sem.at[0, s]),
                local(xn2.at[s], xn_h.at[rows_of(k), :], out_sem.at[1, s]),
                local(st.at[s], st_h.at[rows_of(k), :], out_sem.at[2, s]),
                local(yo.at[s], y_h.at[rows_of(k), :], out_sem.at[3, s]))

    def chunk_f(k, carry):
        s = lax.rem(k, 2)
        slot = lax.rem(k, 4)

        @pl.when(k < chunks - 2)
        def _():
            stream_next(x_h, k + 2, k + 2)

        @pl.when(k == chunks - 7)
        def _():
            for p in range(SUBS):
                w_x(1, p).start()

        @pl.when(k == chunks - 3)
        def _():
            w_forward_x(1)

        @pl.when(k == chunks - 1)
        def _():
            w_forward_y(1)

        @pl.when(k >= chunks - 2)
        def _():
            stream_next(dy_h, k - (chunks - 2), k + 2)

        for cp in load_f(k):
            cp.wait()

        @pl.when(k < chunks - 1)
        def _():
            for cp in load_f(k + 1):
                cp.start()

        @pl.when(k >= 2)
        def _():
            for cp in out_f(k):
                cp.wait()

        stream(x_h, k, k).wait_recv()

        gam = jnp.concatenate([smv[0, :, half_f:half_f + hw], smv[1, :, half_f:half_f + hw]], axis=1)
        bet = jnp.concatenate([smv[0, :, half_f + hw:half_f + full], smv[1, :, half_f + hw:half_f + full]], axis=1)
        step = 32
        for i in range(M // step):
            rs = slice(i * step, (i + 1) * step)
            xv = jnp.concatenate([own[s, rs, :], land[slot, rs, :]], axis=1).astype(F32)
            mean = jnp.sum(xv, axis=1, keepdims=True) * (1.0 / full)
            cen = xv - mean
            istd = lax.rsqrt(jnp.sum(cen * cen, axis=1, keepdims=True) * (1.0 / full) + LN_EPS)
            xn2[s, rs, :] = (cen * istd * gam + bet).astype(BF16)
            st[s, rs, :] = jnp.concatenate([jnp.broadcast_to(mean, (step, 64)), jnp.broadcast_to(istd, (step, 64))], axis=1)
        dyv = aux[s]
        tr[:hw, :] = dyv.T
        gb8[:, full:full + hw] += fold8(dyv.astype(F32))

        def up(j):
            js = slice(j * FT, (j + 1) * FT)
            side, at = divmod(j * FT, half_f)
            u = dot(xn2[s], wu[:, js], 1, 0) + smv[side, :, at:at + FT]
            ub[s, :, js] = u.astype(BF16)

        def mid(j):
            js = slice(j * FT, (j + 1) * FT)
            act[j % 2] = gelu(ub[s, :, js].astype(F32)).astype(BF16)

        def down(j):
            js = slice(j * FT, (j + 1) * FT)
            part = dot(act[j % 2], wd[js, :hw], 1, 0)
            acc[0] = part if j == 0 else acc[0] + part
            blk, rest = divmod(j * FT, half_f)
            qt, at = divmod(rest, half_f // 2)
            acc_d[blk, qt, :, at:at + FT] += dot(tr[:hw, :], act[j % 2], 1, 0)

        pipelined(0, tiles, up, mid, down)
        bdn = smv[0, :, half_f + full:half_f + full + hw]
        yo[s] = (own[s].astype(F32) + acc[0] + bdn).astype(BF16)
        for cp in out_f(k):
            cp.start()
        pl.semaphore_signal(credit, inc=1, device_id={'col': peer['col']}, device_id_type=MESH)
        return carry

    lax.fori_loop(0, chunks, chunk_f, 0)

    rdown = send(acc_d.at[1 - b], rdown_h, rd_sem.at[0], rd_sem.at[1], 'row')
    rdown.start()
    for k in (chunks - 2, chunks - 1):
        for cp in out_f(k):
            cp.wait()

    def load_b(k):
        s = lax.rem(k, 2)
        rs = rows_of(k)
        return (local(dy_h.at[rs, :], own.at[s], ld_sem.at[0, s]),
                local(x_h.at[rs, :], aux.at[s], ld_sem.at[1, s]),
                local(u_h.at[rs, :], ub.at[s], ld_sem.at[2, s]),
                local(xn_h.at[rs, :], xn2.at[s], ld_sem.at[3, s]),
                local(st_h.at[rs, :], st.at[s], ld_sem.at[4, s]))

    for cp in load_b(0):
        cp.start()
    w_finish(1)

    rd_load = local(rdown_h, acc_d.at[1 - b], dl_sem.at[0])
    ydown = send(acc_d.at[b, 1 - d], ydown_h, yd_sem.at[0], yd_sem.at[1], 'depth')
    yd_load = local(ydown_h, acc_d.at[1 - b, 0], dl_sem.at[1])
    half_d = half_f // 2
    gd_rows = pl.ds(pl.multiple_of(d * half_d, half_d), half_d)
    gd_own = local(gd_s, gwd_h.at[gd_rows, :], gd_sem.at[0])
    gd_far = send(gd_s, gwd_h.at[gd_rows, :], gd_sem.at[1], gd_sem.at[2], 'depth')

    def dxn_out(k):
        s = lax.rem(k, 2)
        return local(acc.at[s], dxn_h.at[rows_of(k), :], out_sem.at[0, s])

    def reduce_down(k):
        @pl.when(k == 1)
        def _():
            rdown.wait()
            rd_load.start()

        @pl.when(k == 2)
        def _():
            rd_load.wait()
            for q in range(2):
                for i in range(hw // 64):
                    rs = slice(i * 64, (i + 1) * 64)
                    acc_d[b, q, rs, :] += acc_d[1 - b, q, rs, :]

        @pl.when(k == 3)
        def _():
            ydown.start()

        @pl.when(k == 9)
        def _():
            ydown.wait()
            yd_load.start()

        @pl.when(k == 10)
        def _():
            yd_load.wait()
            for i in range(half_d // 128):
                cs = slice(i * 128, (i + 1) * 128)
                total = acc_d[b, d, :, cs] + acc_d[1 - b, 0, :, cs]
                gd_s[cs, :] = total.T.astype(BF16)

        @pl.when(k == 11)
        def _():
            gd_own.start()
            gd_far.start()
            pl.semaphore_signal(free_row, inc=1, device_id={'row': peer['row']}, device_id_type=MESH)
            pl.semaphore_signal(free_dep, inc=1, device_id={'depth': peer['depth']}, device_id_type=MESH)

    own_tiles = half_f // FT
    parts = half_f // LT
    early = EARLY

    def grads(k, s, slot, lo, hi):
        def grad(j):
            js = slice(j * FT, (j + 1) * FT)
            dyv = jnp.concatenate([own[s], land[slot]], axis=1)
            da_s[j % 2] = dot(dyv, wd[js, :], 1, 1)

        def mid(j):
            js = slice(j * FT, (j + 1) * FT)
            du = (da_s[j % 2] * gelu_slope(ub[s, :, js].astype(F32))).astype(BF16)
            act[j % 2] = du
            if j < own_tiles:
                bup8[:, js] += fold8(du.astype(F32))

        def back(j):
            js = slice(j * FT, (j + 1) * FT)
            part = dot(act[j % 2], wu[:hw, js], 1, 1)
            acc[s] = part if j == 0 else acc[s] + part
            if j < own_tiles:
                up = dot(tr[...], act[j % 2], 1, 0)
                for i in range(4):
                    acc_u[i // 2, i % 2, :, js] += up[i * (hw // 2):(i + 1) * (hw // 2)]

        pipelined(lo, hi, grad, mid, back)

    def grads_last(s, slot, done):
        def grad(j):
            dyv = jnp.concatenate([own[s], land[slot]], axis=1)
            da_s[j % 2, :, :LT] = dot(dyv, wd[j * LT:(j + 1) * LT, :], 1, 1)

        def mid(j):
            js = slice(j * LT, (j + 1) * LT)
            du = (da_s[j % 2, :, :LT] * gelu_slope(ub[s, :, js].astype(F32))).astype(BF16)
            ub[s, :, js] = du
            bup8[:, js] += fold8(du.astype(F32))

        def back(j):
            js = slice(j * LT, (j + 1) * LT)
            up = dot(tr[...], ub[s, :, js], 1, 0)
            for i in range(4):
                acc_u[i // 2, i % 2, :, js] += up[i * (hw // 2):(i + 1) * (hw // 2)]

        grad(0)
        for j in range(parts):
            if j + 1 < parts:
                grad(j + 1)
            mid(j)
            back(j)
            done(j)

    def other_half(k, s, slot, peeled=False):
        if peeled:
            for j in range(own_tiles):
                js = slice(j * FT, (j + 1) * FT)
                part = dot(ub[s, :, js], wu[:hw, js], 1, 1)
                acc[s] = part if j == 0 else acc[s] + part
        grads(k, s, slot, own_tiles, tiles)
        gam = smv[0, :, half_f:half_f + hw]
        step = 128
        for i in range(M // step):
            rs = slice(i * step, (i + 1) * step)
            dxn = acc[s, rs, :]
            xh = (aux[s, rs, :].astype(F32) - st[s, rs, 0:1]) * st[s, rs, 64:65]
            px = dxn * xh
            gb8[:, :hw] += fold8(px)
            gb8[:, hw:full] += fold8(dxn)
            s1 = jnp.sum(dxn * gam, axis=1, keepdims=True)
            s2 = jnp.sum(px * gam, axis=1, keepdims=True)
            both = jnp.concatenate([jnp.broadcast_to(s1, (step, 64)), jnp.broadcast_to(s2, (step, 64))], axis=1).T
            s12[k, 0:4, rs] = both[0:4]
            s12[k, 4:8, rs] = both[64:68]
        dxn_out(k).start()

    last = chunks - 1

    def chunk_b(k, carry):
        s = lax.rem(k, 2)
        q = k + chunks
        slot = lax.rem(q, 4)

        @pl.when(k < chunks - 2)
        def _():
            stream_next(dy_h, k + 2, q + 2)

        reduce_down(k)
        for cp in load_b(k):
            cp.wait()
        for cp in load_b(k + 1):
            cp.start()

        @pl.when(k >= 2)
        def _():
            dxn_out(k).wait()

        stream(dy_h, k, q).wait_recv()
        tr[...] = xn2[s].T
        grads(k, s, slot, 0, own_tiles)
        other_half(k, s, slot)

        @pl.when(k < chunks - 4)
        def _():
            pl.semaphore_signal(credit, inc=1, device_id={'col': peer['col']}, device_id_type=MESH)
        return carry

    lax.fori_loop(0, last, chunk_b, 0)

    pl.semaphore_wait(free_row, 1)
    pl.semaphore_wait(free_dep, 1)
    hq = hw // 2
    wide = half_f // 2 // LT

    def ru(p):
        dst = acc_d.at[0, :, pl.ds((p // wide) * hq, hq), pl.ds((p % wide) * LT, LT)]
        return send(acc_u.at[1 - b, :, :, pl.ds(p * LT, LT)], dst, ru_s, ru_r.at[p], 'row')

    def yu(p):
        dst = acc_d.at[1, p // wide, pl.ds(0, hq), pl.ds((p % wide) * LT, LT)]
        return send(acc_u.at[b, 1 - d, :, pl.ds(p * LT, LT)], dst, yu_s, yu_r.at[p], 'depth')

    def au(p):
        ps = pl.ds(p * LT, LT)
        return send(gu_s.at[:, ps], guo_h.at[:, ps], au_s, au_r, 'depth')

    half_g = early * LT
    gua_out = local(gu_s.at[:, pl.ds(0, half_g)], gua_h, gu_sem.at[0])
    gub_out = local(gu_s.at[:, pl.ds(half_g, half_f - half_g)], gub_h, gu_sem.at[1])

    def to_depth(p):
        ru(p).wait_recv()
        for i in range(2):
            rs = slice((p // wide) * hq, (p // wide) * hq + hq)
            cs = slice((p % wide) * LT, (p % wide) * LT + LT)
            acc_u[b, i, :, p * LT:(p + 1) * LT] += acc_d[0, i, rs, cs]
        yu(p).start()

    def tile_done(p):
        ru(p).start()
        if p >= 1:
            to_depth(p - 1)

    def from_depth(p):
        yu(p).wait_recv()
        cs = slice((p % wide) * LT, (p % wide) * LT + LT)
        gu_s[:, p * LT:(p + 1) * LT] = (acc_u[b, d, :, p * LT:(p + 1) * LT] + acc_d[1, p // wide, 0:hq, cs]).astype(BF16)
        if p < early:
            au(p).start()

    slot_l, s_l = (chunks + last) % 4, last % 2
    s12_a = send(s12.at[pl.ds(0, last)], s12o.at[pl.ds(0, last)], s12_sem.at[0], s12_sem.at[1], 'col')
    s12_b = send(s12.at[last], s12o.at[last], s12_sem.at[2], s12_sem.at[3], 'col')
    for cp in load_b(last):
        cp.wait()
    dxn_out(last).wait()
    tr[...] = xn2[s_l].T
    stream(dy_h, last, chunks + last).wait_recv()
    s12_a.start()
    grads_last(s_l, slot_l, tile_done)
    to_depth(parts - 1)

    other_half(last, s_l, slot_l, True)
    s12_b.start()
    gsp[0] = jnp.concatenate([jnp.sum(bup8[...], axis=0, keepdims=True), jnp.sum(gb8[...], axis=0, keepdims=True)], axis=1)
    gs_row = send(gsp.at[0], gsl.at[0], gs_sem.at[0], gs_sem.at[1], 'row')
    gs_row.start()

    def load_t(k):
        s = lax.rem(k, 2)
        rs = rows_of(k)
        return (local(dy_h.at[rs, :], own.at[s], ld_sem.at[0, s]),
                local(x_h.at[rs, :], aux.at[s], ld_sem.at[1, s]),
                local(dxn_h.at[rs, :], da_s.at[s], ld_sem.at[2, s]),
                local(st_h.at[rs, :], st.at[s], ld_sem.at[4, s]))

    def out_t(k):
        s = lax.rem(k, 2)
        return local(yo.at[s], dx_h.at[rows_of(k), :], out_sem.at[3, s])

    for cp in load_t(0):
        cp.start()
    for k in range(4):
        stream(dy_h, k, chunks + k).wait_send()
    for k in (chunks - 2, chunks - 1):
        dxn_out(k).wait()
    gd_own.wait()
    gd_far.wait()
    local(acc_u.at[1 - b], acc_u.at[1 - b], ru_s).wait()
    gs_row.wait()
    gsp[1] = gsp[0] + gsl[0]
    gs_dep = send(gsp.at[1], gsl.at[1], gs_sem.at[2], gs_sem.at[3], 'depth')
    gs_dep.start()
    s12_a.wait()
    s12_b.wait()
    from_depth(0)

    def chunk_t(k, carry):
        s = lax.rem(k, 2)
        for cp in load_t(k):
            cp.wait()

        @pl.when(k < last)
        def _():
            for cp in load_t(k + 1):
                cp.start()

        @pl.when(k >= 2)
        def _():
            out_t(k).wait()

        gam = smv[0, :, half_f:half_f + hw]
        step = 128
        for i in range(M // step):
            rs = slice(i * step, (i + 1) * step)
            sums = (s12[k, :, rs] + s12o[k, :, rs]) * (1.0 / full)
            cols = jnp.concatenate([sums] * (step // 8), axis=0).T
            istd = st[s, rs, 64:65]
            xh = (aux[s, rs, :].astype(F32) - st[s, rs, 0:1]) * istd
            g = da_s[s, rs, :] * gam
            yo[s, rs, :] = (own[s, rs, :].astype(F32) + istd * (g - cols[:, 0:1] - xh * cols[:, 4:5])).astype(BF16)
        out_t(k).start()
        return carry

    lax.fori_loop(0, chunks, chunk_t, 0)
    for p in range(1, early):
        from_depth(p)
    gua_out.start()
    for k in (chunks - 2, chunks - 1):
        out_t(k).wait()
    gua_out.wait()
    for p in range(early, parts):
        from_depth(p)
    gub_out.start()
    local(acc_u.at[b, 1 - d], acc_u.at[b, 1 - d], yu_s).wait()
    gs_dep.wait()
    gsp[0] = gsp[1] + gsl[1]
    gs_out = local(gsp.at[0], gs_h, gs_sem.at[4])
    gs_out.start()
    gub_out.wait()
    gs_out.wait()
    for sem in (au_s, au_r):
        local(guo_h, guo_h, sem).wait()


def finish_kernel(y_in, dx_in, gwd_in, gs, gua, gub, guo, y, dx, gwd, gwu, gbup, ggam, gbet, gbdn, big, small, sums, far_s, in_sem, out_sem):
    rows, hw = y.shape
    half_f = gwd.shape[0]
    hq, half_g = gua.shape
    d = lax.axis_index('depth')
    mine = pl.ds(pl.multiple_of(d * hq, hq), hq)
    far = pl.ds(pl.multiple_of((1 - d) * hq, hq), hq)
    n = rows // COPIES
    ins, outs = [], []

    def move(src, buf, *dst):
        ins.append(pltpu.make_async_copy(src, buf, in_sem.at[len(ins)]))
        outs.append([pltpu.make_async_copy(buf, to, out_sem) for to in dst])

    left, right = pl.ds(0, half_g), pl.ds(half_g, half_f - half_g)
    for i in range(COPIES):
        rs = pl.ds(i * n, n)
        move(y_in.at[rs], big.at[0, rs], y.at[rs])
        move(dx_in.at[rs], big.at[1, rs], dx.at[rs])
    move(gwd_in, small, gwd)
    move(gua, far_s.at[0, :, left], gwu.at[mine, left])
    move(gub, far_s.at[0, :, right], gwu.at[mine, right], gwu.at[far, right])
    move(guo, far_s.at[1, :, left], gwu.at[far, left])
    parts = [(0, half_f, gbup), (half_f, hw, ggam), (half_f + hw, hw, gbet), (half_f + 2 * hw, hw, gbdn)]
    move(gs, sums)
    outs[-1] = [pltpu.make_async_copy(sums.at[:, pl.ds(a, w)], dst, out_sem) for a, w, dst in parts]
    for cp in ins:
        cp.start()
    for cp, tos in zip(ins, outs):
        cp.wait()
        for to in tos:
            to.start()
    for tos in outs:
        for to in tos:
            to.wait()


def solution(mesh):
    tok_spec = P(('dp', 'depth', 'row'), 'col')
    vec_spec = P('col')
    mat_spec = P('row', 'col')
    grad_vec = P(('dp', 'col'))
    grad_mat = P(('dp', 'row'), 'col')

    def local_pass(x, gamma, beta, w_up, b_up, w_down, b_down, dy):
        rows, hw = x.shape
        half_f = b_up.shape[0]
        full_f, full = 2 * half_f, 2 * hw
        chunks = rows // M
        smalls = [b_up.reshape(-1, 128), gamma.reshape(1, -1), beta.reshape(1, -1), b_down.reshape(-1, 128)]
        hbm = pl.BlockSpec(memory_space=pltpu.HBM)
        sds = jax.ShapeDtypeStruct
        V, D, R = pltpu.VMEM, pltpu.SemaphoreType.DMA, pltpu.SemaphoreType.REGULAR
        sent = EARLY * LT
        outs = [
            sds((rows, hw), BF16), sds((rows, hw), BF16), sds((half_f, hw), BF16), sds((1, full_f), F32),
            sds((hw // 2, sent), BF16), sds((hw // 2, half_f - sent), BF16), sds((hw // 2, sent), BF16),
            sds((rows, 128), F32), sds((rows, hw), F32),
            sds((rows, full_f), BF16), sds((rows, full), BF16), sds((2, hw, half_f // 2), F32), sds((hw, half_f // 2), F32),
        ]
        parts = half_f // LT
        scratch = [
            V((full, full_f), BF16), V((full_f, full), BF16), V((2, 2, hw, half_f // 2), F32), V((2, 2, hw // 2, half_f), F32),
            V((2, M, hw), BF16), V((4, M, hw), BF16), V((2, M, hw), BF16), V((2, M, full), BF16), V((full, M), BF16),
            V((2, M, full_f), BF16), V((2, M, 128), F32), V((2, M, FT), F32), V((2, M, FT), BF16), V((2, M, hw), F32), V((2, M, hw), BF16),
            V((8, half_f), F32), V((8, half_f), F32), V((2, 1, full_f), F32),
            V((2, half_f // 128, 128), BF16), V((hw // 128, 128), BF16), V((chunks, 8, M), F32), V((chunks, 8, M), F32),
            V((half_f // 2, hw), BF16), V((hw // 2, half_f), BF16), V((2, 1, full_f), F32), V((2, 1, full_f), F32),
            D((2,)), D((2,)), D((2,)), D((2,)), D((2, SUBS)), D((2,)), D((2, SUBS)), D((2,)), D((2, SUBS)), D((2,)), D((2, SUBS)),
            D((3, 4)), D((4,)), D((4,)), D((5, 2)), D((4, 2)), D((2,)), D((2,)), D((2,)), D((3,)),
            D(()), D((parts,)), D(()), D((parts,)), D(()), D(()), D((2,)), D((4,)), D((5,)), R, R, R,
        ]
        res = pl.pallas_call(
            kernel,
            out_shape=outs,
            in_specs=[hbm] * 8,
            out_specs=[hbm] * len(outs),
            scratch_shapes=scratch,
            compiler_params=pltpu.CompilerParams(
                collective_id=0, has_side_effects=True, vmem_limit_bytes=67043328),
            cost_estimate=pl.CostEstimate(flops=16 * rows * full * full_f, bytes_accessed=2 ** 28, transcendentals=2 * rows * full_f),
            name='mlp_block',
        )(x, dy, w_up, w_down, *smalls)
        y, dx, gwd, gs, gua, gub, guo = res[:7]
        gub_far = lax.ppermute(gub, 'depth', ((0, 1), (1, 0)))
        moves = 2 * COPIES + 5
        y, dx, gwd, gwu, gbup, ggam, gbet, gbdn = pl.pallas_call(
            finish_kernel,
            out_shape=[sds((rows, hw), BF16), sds((rows, hw), BF16), sds((half_f, hw), BF16), sds((hw, half_f), BF16),
                       sds((1, half_f), F32), sds((1, hw), F32), sds((1, hw), F32), sds((1, hw), F32)],
            in_specs=[hbm] * 7,
            out_specs=[hbm] * 8,
            scratch_shapes=[V((2, rows, hw), BF16), V((half_f, hw), BF16), V((1, full_f), F32), V((2, hw // 2, half_f), BF16),
                            D((moves,)), D(())],
            compiler_params=pltpu.CompilerParams(vmem_limit_bytes=67043328),
            cost_estimate=pl.CostEstimate(flops=2 ** 33, bytes_accessed=42 * 2 ** 20, transcendentals=0),
            name='finish',
        )(y, dx, gwd, gs, gua, gub, guo)
        far = (1 - lax.axis_index('depth')) * (hw // 2)
        gwu = lax.dynamic_update_slice(gwu, gub_far, (far, sent))
        return y, dx, ggam.reshape(-1), gbet.reshape(-1), gwu, gbup.reshape(-1), gwd, gbdn.reshape(-1)

    return jax.shard_map(
        local_pass,
        mesh=mesh,
        in_specs=(tok_spec, vec_spec, vec_spec, mat_spec, vec_spec, mat_spec, vec_spec, tok_spec),
        out_specs=(tok_spec, tok_spec, grad_vec, grad_vec, grad_mat, grad_vec, grad_mat, grad_vec),
        check_vma=False,
    )
```

```python
import jax
import jax.numpy as jnp
from jax import lax
from jax.experimental import pallas as pl
from jax.experimental.pallas import tpu as pltpu
from jax.sharding import PartitionSpec as P

LN_EPS = 1e-5
C0 = 0.7978845608
C1 = C0 * 0.044715
M = 512
FT = 512
SUBS = 2
RING = 6
LATE = 2
PROMPT = 2
COPIES = 4
BF16, F32 = jnp.bfloat16, jnp.float32
MESH = pl.DeviceIdType.MESH


def dot(lhs, rhs, rhs_dim=0):
    return lax.dot_general(lhs, rhs, (((1,), (rhs_dim,)), ((), ())), preferred_element_type=F32)


def dot_t(lhs, rhs):
    return dot(lhs, rhs, 1)


def odd(n):
    return lax.rem(n, 2)


def cat(*parts):
    return jnp.concatenate(parts, axis=1)


def row_sum(v):
    return jnp.sum(v, axis=1, keepdims=True)


def col_sum(v):
    return jnp.sum(v, axis=0, keepdims=True)


def head(n):
    return pl.ds(0, n)


def tile(i, n):
    return slice(i * n, (i + 1) * n)


def gelu(v):
    t = jnp.tanh(v * (C1 * (v * v) + C0))
    h = 0.5 * v
    return h * t + h


def gelu_and_slope(v):
    v2 = v * v
    t = jnp.tanh(v * (C1 * v2 + C0))
    h = 0.5 * v
    slope = (v * (1.0 - t * t)) * (1.5 * C1 * v2 + 0.5 * C0) + (0.5 * t + 0.5)
    return h * t + h, slope


def fold8(v):
    return jnp.sum(v.reshape(v.shape[0] // 8, 8, v.shape[1]), axis=0)


def kernel(x_h, dy_h, wu_h, wd_h, bup_h, gam_h, bet_h, bdn_h,
           y_h, dx_h, dxl_h, gs_h, gu_h, gd_h, dxo_h, rrow_h, ryu_h, rx_h, rdn_h, ydn_h, xo_h, dyo_h, dxn_h, st_h,
           wu, wd, acc_d, acc_u, own, land, aux, xn, trx, trd, st, us, da_s, act, du_s, yacc, dxn, yo, dxa, dxb,
           bup8, gb8, smv, bup_s, bdn_s, gso, gsp, gsl,
           wrow_s, wrow_r, wx_s, wx_r, wy_s, wy_r, wa_s, wa_r, wb_s, wb_r, sm_s, sm_r,
           land_s, land_r, ld_sem, out_sem, sv_sem, t_sem, ru_s, ru_r, yu_s, yu_r, rx_s, rx_r, ag_s, ag_r, rdn_s, rdn_r,
           ydn_s, ydn_r, dx_s, dx_r, gs_s, gs_r, credit):
    chunks = x_h.shape[0] // M
    half_n = chunks // 2
    half_f = wu_h.shape[1]
    hw = x_h.shape[1]
    full = 2 * hw
    hq = hw // 2
    half_d = half_f // 2
    tiles = 2 * half_f // FT
    own_tiles = tiles // 2
    c, r, d = lax.axis_index('col'), lax.axis_index('row'), lax.axis_index('depth')
    b = lax.rem(r + c, 2)
    peer = {'col': 1 - c, 'row': 1 - r, 'depth': 1 - d}
    mine0, theirs0 = c * half_n, (1 - c) * half_n

    def send(src, dst, s_sem, r_sem, axis):
        return pltpu.make_async_remote_copy(src_ref=src, dst_ref=dst, send_sem=s_sem, recv_sem=r_sem,
                                            device_id={axis: peer[axis]}, device_id_type=MESH)

    def local(src, dst, sem):
        return pltpu.make_async_copy(src, dst, sem)

    def all_of(ref, sem):
        return pltpu.make_async_copy(ref, ref, sem)

    def rows_of(k):
        return pl.ds(pl.multiple_of(k * M, M), M)

    def chunk_at(n):
        return lax.rem(mine0 + n, chunks)

    bar = pltpu.get_barrier_semaphore()
    for axis in ('col', 'row', 'depth'):
        pl.semaphore_signal(bar, inc=1, device_id={axis: peer[axis]}, device_id_type=MESH)
    pl.semaphore_wait(bar, 3)

    half_rows = (hq, half_d)
    w_srcs = (wu_h, wd_h)

    def w_cols(kind, blk, dep, s):
        n = half_rows[kind] // SUBS
        if kind == 0:
            return wu.at[pl.ds(pl.multiple_of(blk * hw + dep * hq + s * n, n), n), pl.ds(half_f, half_f)]
        return wd.at[pl.ds(pl.multiple_of(blk * half_f + dep * half_d + s * n, n), n), pl.ds(hw, hw)]

    def w_half(kind):
        return wu.at[head(hq), head(half_f)] if kind == 0 else wd.at[head(half_d), head(hw)]

    def w_own(kind):
        if kind == 0:
            return wu.at[pl.ds(pl.multiple_of(b * hw, hw), hw), head(half_f)]
        return wd.at[pl.ds(pl.multiple_of(b * half_f, half_f), half_f), head(hw)]

    def w_x(kind, s):
        n = half_rows[kind] // SUBS
        src = w_srcs[kind].at[pl.ds(pl.multiple_of(d * half_rows[kind] + s * n, n), n), :]
        return send(src, w_cols(kind, 1 - b, d, s), wx_s.at[kind], wx_r.at[kind, s], 'col')

    def w_y(kind, s):
        return send(w_cols(kind, b, d, s), w_cols(kind, b, d, s), wy_s.at[kind], wy_r.at[kind, s], 'depth')

    def w_a(kind, s):
        return send(w_cols(kind, b, d, s), w_cols(kind, b, d, s), wa_s.at[kind], wa_r.at[kind, s], 'row')

    def w_b(kind, s):
        return send(w_cols(kind, b, 1 - d, s), w_cols(kind, b, 1 - d, s), wb_s.at[kind], wb_r.at[kind, s], 'row')

    def w_row(kind):
        return send(w_srcs[kind], w_own(kind), wrow_s.at[kind], wrow_r.at[kind], 'row')

    def w_load(kind):
        return local(w_srcs[kind], w_own(kind), out_sem.at[kind])

    def stream(src, k, q):
        slot = lax.rem(q, RING)
        return send(src.at[rows_of(k), :], land.at[slot], land_s.at[slot], land_r.at[slot], 'col')

    def stream_next(src, k, q):
        @pl.when(q >= RING)
        def _():
            stream(src, k, q).wait_send()
            pl.semaphore_wait(credit, 1)
        stream(src, k, q).start()

    def give(n):
        for _ in range(n):
            pl.semaphore_signal(credit, inc=1, device_id={'col': peer['col']}, device_id_type=MESH)

    gam_at, bet_at = pl.ds(half_f, hw), pl.ds(half_f + hw, hw)
    sm_own = [local(bup_h, bup_s.at[0], ld_sem.at[0, 0]), local(gam_h, smv.at[0, :, gam_at], ld_sem.at[0, 1]),
              local(bet_h, smv.at[0, :, bet_at], ld_sem.at[1, 0]), local(bdn_h, bdn_s, ld_sem.at[1, 1])]
    sm_out = [send(bup_h, bup_s.at[1], sm_s.at[0], sm_r.at[0], 'col'),
              send(gam_h, smv.at[1, :, gam_at], sm_s.at[1], sm_r.at[1], 'col'),
              send(bet_h, smv.at[1, :, bet_at], sm_s.at[2], sm_r.at[2], 'col')]
    for cp in sm_own + sm_out:
        cp.start()
    for kind in range(2):
        for s in range(SUBS):
            w_x(kind, s).start()
    for kind in range(2):
        w_load(kind).start()
        w_row(kind).start()
    for i in range(2):
        stream(x_h, theirs0 + i, 2 * i).start()
        stream(dy_h, theirs0 + i, 2 * i + 1).start()

    acc_d[...] = jnp.zeros_like(acc_d)
    acc_u[...] = jnp.zeros_like(acc_u)
    bup8[...] = jnp.zeros_like(bup8)
    gb8[...] = jnp.zeros_like(gb8)
    for cp in sm_own:
        cp.wait()

    def load(n):
        s = odd(n)
        rs = rows_of(chunk_at(n))
        return (local(x_h.at[rs, :], own.at[s], ld_sem.at[0, s]), local(dy_h.at[rs, :], aux.at[s], ld_sem.at[1, s]))

    for cp in load(0):
        cp.start()
    for kind in range(2):
        for s in range(SUBS):
            w_x(kind, s).wait_recv()
            w_y(kind, s).start()
            w_a(kind, s).start()
        for s in range(SUBS):
            w_y(kind, s).wait_recv()
            w_b(kind, s).start()
    for kind in range(2):
        w_load(kind).wait()
        w_row(kind).wait()
        for s in range(SUBS):
            w_a(kind, s).wait_recv()
            w_b(kind, s).wait_recv()
        for sems in (wx_s, wy_s, wa_s, wb_s):
            all_of(w_half(kind), sems.at[kind]).wait()
    for cp in sm_out:
        cp.wait()
    for i in range(half_f // 128):
        for side in range(2):
            smv[side, :, tile(i, 128)] = bup_s[side, i:i + 1, :].astype(F32)
    for i in range(hw // 128):
        smv[0, :, half_f + full + i * 128:half_f + full + (i + 1) * 128] = bdn_s[i:i + 1, :].astype(F32)

    def wide(at):
        return cat(smv[0, :, half_f + at:half_f + at + hw], smv[1, :, half_f + at:half_f + at + hw])

    def norm(s, slot, keep):
        gam, bet = wide(0), wide(hw)
        step = 32
        for i in range(M // step):
            rs = tile(i, step)
            xv = cat(own[s, rs, :], land[slot, rs, :]).astype(F32)
            mean = row_sum(xv) * (1.0 / full)
            cen = xv - mean
            istd = lax.rsqrt(row_sum(cen * cen) * (1.0 / full) + LN_EPS)
            xn[rs, :] = (cen * istd * gam + bet).astype(BF16)
            if keep:
                st[i * step // hq, i * step % hq:i * step % hq + step, :] = cat(jnp.broadcast_to(mean, (step, 64)), jnp.broadcast_to(istd, (step, 64)))
        dyv = aux[s]
        trd[...] = dyv.T
        gb8[:, 2 * full:2 * full + hw] += fold8(dyv.astype(F32))

    def write_y(s):
        bdn = smv[0, :, half_f + full:half_f + full + hw]
        yo[...] = (own[s].astype(F32) + yacc[...] + bdn).astype(BF16)

    def y_out(n):
        return local(yo, y_h.at[rows_of(chunk_at(n)), :], out_sem.at[0])

    def dx_out(n):
        return local(dxa, dx_h.at[rows_of(chunk_at(n)), :], out_sem.at[1])

    def dxo_out(n):
        return local(dxb, dxo_h.at[rows_of(n), :], out_sem.at[2])

    def dxl_out(n):
        return local(dxb, dxl_h.at[rows_of(n - (half_n - LATE)), :], out_sem.at[2])

    def saves(n, slot_x, slot_d):
        rs = rows_of(n)
        return (local(land.at[slot_x], xo_h.at[rs, :], sv_sem.at[0]), local(land.at[slot_d], dyo_h.at[rs, :], sv_sem.at[1]),
                local(dxn, dxn_h.at[n], sv_sem.at[2]), local(st, st_h.at[n], sv_sem.at[3]))

    def finish_dx(grads, xs, dys, stats):
        gam = wide(0)
        step = 32
        for i in range(M // step):
            rs = tile(i, step)
            h, hs = i * step // hq, slice(i * step % hq, i * step % hq + step)
            istd = stats[h, hs, 64:65]
            xh = (xs(rs).astype(F32) - stats[h, hs, 0:1]) * istd
            dv = grads(h, hs)
            px = dv * xh
            gb8[:, :full] += fold8(px)
            gb8[:, full:2 * full] += fold8(dv)
            m1 = row_sum(dv * gam) * (1.0 / full)
            m2 = row_sum(px * gam) * (1.0 / full)
            dxv = (dys(rs).astype(F32) + istd * (dv * gam - m1 - xh * m2)).astype(BF16)
            dxa[rs, :] = dxv[:, :hw]
            dxb[rs, :] = dxv[:, hw:]

    def chunk_mine(n, carry):
        s = odd(n)
        slot_x, slot_d = lax.rem(2 * n, RING), lax.rem(2 * n + 1, RING)

        @pl.when(n < half_n - 2)
        def _():
            stream_next(x_h, theirs0 + n + 2, 2 * n + 4)
            stream_next(dy_h, theirs0 + n + 2, 2 * n + 5)

        @pl.when(n >= half_n - 2)
        def _():
            k = 2 * (n - (half_n - 2))
            stream_next(x_h, mine0 + k, chunks + k)
            stream_next(x_h, mine0 + k + 1, chunks + k + 1)

        for cp in load(n):
            cp.wait()
        for cp in load(n + 1):
            cp.start()

        @pl.when(n >= 1)
        def _():
            y_out(n).wait()
            for cp in saves(n, slot_x, slot_d)[2:]:
                cp.wait()

        @pl.when((n >= 1) & (n <= PROMPT))
        def _():
            dx_out(n).wait()
            dxo_out(n).wait()

        stream(x_h, n, 2 * n).wait_recv()
        stream(dy_h, n, 2 * n + 1).wait_recv()
        save = saves(n, slot_x, slot_d)
        save[0].start()
        save[1].start()
        norm(s, slot_x, True)
        save[3].start()
        trx[...] = xn[...].T
        yacc[...] = jnp.zeros_like(yacc)
        dxn[...] = jnp.zeros_like(dxn)

        def quad(jj, inner):
            cols = [pl.ds(pl.multiple_of((own_tiles * jj + t) * FT, FT), FT) for t in range(own_tiles)]

            def first(t):
                bias = smv[jj, :, tile(t, FT)]
                us[t % 2] = (dot(xn[...], wu[:, cols[t]]) + bias).astype(BF16)
                dyv = cat(aux[s], land[slot_d])
                da_s[t % 2] = dot_t(dyv, wd[cols[t], :]).reshape(2, hq, FT)

            def mid(t):
                a, slope = gelu_and_slope(us[t % 2].astype(F32))
                act[t % 2] = a.astype(BF16)
                du = (da_s[t % 2].reshape(M, FT) * slope).astype(BF16)
                du_s[t % 2] = du
                bup8[:, cols[t]] += fold8(du.astype(F32))

            def last(t):
                yacc[...] += dot(act[t % 2], wd[cols[t], :hw])
                at = t * FT % half_d
                acc_d[jj, t * FT // half_d, :, at:at + FT] += dot(trd[...], act[t % 2])
                dxn[...] += dot_t(du_s[t % 2], wu[:, cols[t]]).reshape(2, hq, full)
                part = dot(trx[...], du_s[t % 2])
                for i in range(4):
                    acc_u[i // 2, i % 2, :, cols[t]] += part[tile(i, hq)]

            first(0)
            first(1)
            mid(0)
            for t in range(own_tiles):
                last(t)
                if t + 2 < own_tiles:
                    first(t + 2)
                if t + 1 < own_tiles:
                    mid(t + 1)
            return inner

        lax.fori_loop(0, 2, quad, 0)
        write_y(s)
        y_out(n).start()
        save[2].start()

        @pl.when(n < PROMPT)
        def _():
            finish_dx(lambda h, rs: dxn[h, rs, :],
                      lambda rs: cat(own[s, rs, :], land[slot_x, rs, :]),
                      lambda rs: cat(aux[s, rs, :], land[slot_d, rs, :]), st)
            dx_out(n).start()
            dxo_out(n).start()

        save[0].wait()
        save[1].wait()
        give(2)
        return carry

    lax.fori_loop(0, half_n, chunk_mine, 0)

    order = [*range(own_tiles, tiles), *range(own_tiles)]

    def ru(p):
        return send(acc_u.at[1 - b, :, :, pl.ds(p * FT, FT)], rrow_h.at[p], ru_s, ru_r.at[p], 'row')

    def yu(p):
        return send(acc_u.at[b, 1 - d, :, pl.ds(p * FT, FT)], ryu_h.at[p], yu_s, yu_r.at[p], 'depth')

    def rx(k):
        return send(acc_u.at[b, d, :, pl.ds((own_tiles + k) * FT, FT)], rx_h.at[k], rx_s, rx_r.at[k], 'col')

    gu_rows = pl.ds(pl.multiple_of(d * hq, hq), hq)

    def ag(k):
        ps = pl.ds(k * FT, FT)
        return send(trx.at[pl.ds(k * hq, hq), :], gu_h.at[gu_rows, ps], ag_s, ag_r, 'depth')

    def gu_out(k):
        return local(trx.at[pl.ds(k * hq, hq), :], gu_h.at[gu_rows, pl.ds(k * FT, FT)], out_sem.at[3])

    def row_load(i, p):
        return local(rrow_h.at[p], da_s.at[i % 2], t_sem.at[i % 2, 0])

    for p in order:
        ru(p).start()
    y_out(0).wait()
    for cp in saves(half_n - 1, 0, 0)[2:]:
        cp.wait()
    ru(order[0]).wait_recv()
    row_load(0, order[0]).start()
    for i, p in enumerate(order):
        if i + 1 < tiles:
            ru(order[i + 1]).wait_recv()
            row_load(i + 1, order[i + 1]).start()
        row_load(i, p).wait()
        for h in range(2):
            acc_u[b, h, :, tile(p, FT)] += da_s[i % 2, h]
        yu(p).start()

    def oth_load(k):
        yu(own_tiles + k).wait_recv()
        local(ryu_h.at[own_tiles + k], da_s.at[k % 2, 0], t_sem.at[k % 2, 0]).start()

    def oth_send(k):
        p = own_tiles + k
        local(ryu_h.at[p], da_s.at[k % 2, 0], t_sem.at[k % 2, 0]).wait()
        acc_u[b, d, :, tile(p, FT)] += da_s[k % 2, 0]
        rx(k).start()

    def own_loads(k):
        return (local(ryu_h.at[k], da_s.at[k % 2, 0], t_sem.at[k % 2, 0]),
                local(rx_h.at[k], da_s.at[k % 2, 1], t_sem.at[k % 2, 1]))

    def own_load(k):
        yu(k).wait_recv()
        rx(k).wait_recv()
        for cp in own_loads(k):
            cp.start()

    def own_send(k):
        for cp in own_loads(k):
            cp.wait()
        trx[tile(k, hq), :] = (acc_u[b, d, :, tile(k, FT)] + da_s[k % 2, 0] + da_s[k % 2, 1]).astype(BF16)
        ag(k).start()

    def dx_far(m):
        return send(dxo_h.at[rows_of(m), :], dx_h.at[rows_of(mine0 + m), :], dx_s, dx_r, 'col')

    def background(n):
        for k in range(own_tiles):
            @pl.when(n == half_n + 2 + k)
            def _():
                oth_send(k)

            @pl.when(n == half_n + 1 + k)
            def _():
                oth_load(k)

        for k in range(own_tiles - 1):
            @pl.when(n == half_n + 6 + k)
            def _():
                own_send(k)

            @pl.when(n == half_n + 5 + k)
            def _():
                if k >= 1:
                    pass
                own_load(k)

        for m in range(PROMPT):
            @pl.when(n == half_n + 6 + m)
            def _():
                dx_far(m).start()

    def chunk_theirs(n, carry):
        s = odd(n)
        q = n + half_n
        slot = lax.rem(q, RING)

        @pl.when(n == half_n)
        def _():
            stream_next(x_h, mine0 + 4, chunks + 4)

        @pl.when(n <= half_n + 2)
        def _():
            stream_next(x_h, mine0 + 5 + (n - half_n), chunks + 5 + (n - half_n))

        background(n)
        for cp in load(n):
            cp.wait()

        @pl.when(n < chunks - 1)
        def _():
            for cp in load(n + 1):
                cp.start()

        @pl.when(n > half_n)
        def _():
            y_out(n).wait()

        stream(x_h, n, q).wait_recv()
        norm(s, slot, False)

        def up(j):
            side, at = divmod(j * FT, half_f)
            us[j % 2] = (dot(xn[...], wu[:, tile(j, FT)]) + smv[side, :, at:at + FT]).astype(BF16)

        def mid(j):
            act[j % 2] = gelu(us[j % 2].astype(F32)).astype(BF16)

        def down(j):
            part = dot(act[j % 2], wd[tile(j, FT), :hw])
            yacc[...] = part if j == 0 else yacc[...] + part
            blk, rest = divmod(j * FT, half_f)
            qt, at = divmod(rest, half_d)
            acc_d[blk, qt, :, at:at + FT] += dot(trd[...], act[j % 2])

        up(0)
        up(1)
        mid(0)
        for j in range(tiles):
            if j + 2 < tiles:
                up(j + 2)
            down(j)
            if j + 1 < tiles:
                mid(j + 1)
        write_y(s)
        y_out(n).start()

        @pl.when(n < half_n + 2)
        def _():
            give(1)
        return carry

    lax.fori_loop(half_n, chunks, chunk_theirs, 0)

    rdn = send(acc_d.at[1 - b], rdn_h, rdn_s, rdn_r, 'row')
    rdn.start()
    k = own_tiles - 1
    own_send(k - 1)
    own_load(k)
    own_send(k)
    for k in range(own_tiles):
        gu_out(k).start()
    rdn.wait()
    rd_load = local(rdn_h, acc_d.at[1 - b], t_sem.at[0, 0])
    rd_load.start()
    rd_load.wait()
    steps = hw // 128

    def ydn(i):
        return send(acc_d.at[b, 1 - d, pl.ds(i * 128, 128), :], ydn_h.at[i], ydn_s, ydn_r.at[i], 'depth')

    for i in range(steps):
        rs = tile(i, 128)
        for qt in range(2):
            acc_d[b, qt, rs, :] += acc_d[1 - b, qt, rs, :]
        ydn(i).start()
    y_out(chunks - 1).wait()
    all_of(acc_u.at[1 - b], ru_s).wait()

    def load_dx(n):
        s = odd(n)
        rs, ks = rows_of(n), rows_of(mine0 + n)
        return (local(x_h.at[ks, :], own.at[s], ld_sem.at[0, s]), local(dy_h.at[ks, :], aux.at[s], ld_sem.at[1, s]),
                local(xo_h.at[rs, :], land.at[2 * s], ld_sem.at[2, s]), local(dyo_h.at[rs, :], land.at[2 * s + 1], ld_sem.at[3, s]),
                local(dxn_h.at[n], acc_u.at[1 - b, :, :, pl.ds(pl.multiple_of(s * full, full), full)], ld_sem.at[4, s]),
                local(st_h.at[n], da_s.at[s, :, :, head(128)], ld_sem.at[5, s]))

    held = 2

    def chunk_dx(n, carry):
        s = odd(n)
        for cp in load_dx(n):
            cp.wait()

        @pl.when(n < half_n - 1)
        def _():
            for cp in load_dx(n + 1):
                cp.start()

        @pl.when(n > PROMPT)
        def _():
            dx_out(n).wait()
            dxo_out(n).wait()

        @pl.when((n > PROMPT) & (n <= half_n - LATE - held))
        def _():
            dx_far(n - 1).start()

        finish_dx(lambda h, rs: acc_u[1 - b, h, rs, pl.ds(pl.multiple_of(s * full, full), full)],
                  lambda rs: cat(own[s, rs, :], land[2 * s, rs, :]),
                  lambda rs: cat(aux[s, rs, :], land[2 * s + 1, rs, :]), da_s.at[s, :, :, head(128)])
        dx_out(n).start()

        @pl.when(n < half_n - LATE)
        def _():
            dxo_out(n).start()

        @pl.when(n >= half_n - LATE)
        def _():
            dxl_out(n).start()
        return carry

    for cp in load_dx(PROMPT):
        cp.start()
    lax.fori_loop(PROMPT, half_n, chunk_dx, 0)
    oth = lambda at, n: [col_sum(ref[:, a:a + n]) for ref, a in at]
    gso[...] = jnp.concatenate(oth(((bup8, half_f),), half_f) + oth(((gb8, hw), (gb8, full + hw)), hw)
                               + [jnp.zeros((1, half_f - full), F32)], axis=1)
    gs_col = send(gso, gsl.at[0], gs_s.at[0], gs_r.at[0], 'col')
    gs_col.start()
    for m in range(half_n - LATE - held, half_n - LATE):
        dx_far(m).start()
    dx_out(half_n - 1).wait()
    dxl_out(half_n - 1).wait()
    gs_col.wait()
    gsp[0] = jnp.concatenate(oth(((bup8, 0),), half_f) + oth(((gb8, 0), (gb8, full), (gb8, 2 * full)), hw)
                             + [jnp.zeros((1, half_f - 3 * hw), F32)], axis=1) + gsl[0]
    gs_row = send(gsp.at[0], gsl.at[1], gs_s.at[1], gs_r.at[1], 'row')
    gs_row.start()
    gs_row.wait()
    gsp[1] = gsp[0] + gsl[1]
    gs_dep = send(gsp.at[1], gsl.at[2], gs_s.at[2], gs_r.at[2], 'depth')
    gs_dep.start()
    for q in range(3 * half_n - RING, 3 * half_n):
        stream(x_h, 0, q).wait_send()
    all_of(acc_u.at[b, 1 - d], yu_s).wait()
    all_of(acc_u.at[b, d, :, pl.ds(half_f, half_f)], rx_s).wait()
    all_of(trx, out_sem.at[3]).wait()
    for i in range(steps):
        ydn(i).wait_recv()
        dn_load = local(ydn_h.at[i], acc_d.at[1 - b, 0, pl.ds(i * 128, 128), :], t_sem.at[1, 0])
        dn_load.start()
        dn_load.wait()
        rs = tile(i, 128)
        for j in range(half_d // 128):
            cs = tile(j, 128)
            total = acc_d[b, d, rs, cs] + acc_d[1 - b, 0, rs, cs]
            us[j * 128 // M, j * 128 % M:j * 128 % M + 128, rs] = total.T.astype(BF16)
    gd_out = [local(us.at[i], gd_h.at[pl.ds(i * M, M), :], t_sem.at[i, 1]) for i in range(2)]
    for cp in gd_out:
        cp.start()
    gs_dep.wait()
    gsp[0] = gsp[1] + gsl[2]
    gs_out = local(gsp.at[0], gs_h, out_sem.at[0])
    gs_out.start()
    all_of(acc_d.at[b, 1 - d], ydn_s).wait()
    for sem in (ag_s, ag_r):
        all_of(trx, sem).wait()
    sent = dxo_h.at[head((half_n - LATE) * M), :]
    for sem in (dx_s, dx_r):
        all_of(sent, sem).wait()
    for cp in gd_out:
        cp.wait()
    gs_out.wait()


def finish_kernel(y_in, dx_in, gwu_in, gd, gs, y, dx, gwu, gwd, gbup, ggam, gbet, gbdn, big, small, sums, in_sem, out_sem):
    rows, hw = y.shape
    half_f = gwd.shape[0]
    d = lax.axis_index('depth')
    n = rows // COPIES
    ins, outs = [], []

    def move(src, buf, *dst):
        ins.append(pltpu.make_async_copy(src, buf, in_sem.at[len(ins)]))
        outs.append([pltpu.make_async_copy(buf, to, out_sem) for to in dst])

    for i in range(COPIES):
        rs = pl.ds(i * n, n)
        move(y_in.at[rs], big.at[0, rs], y.at[rs])
        move(dx_in.at[rs], big.at[1, rs], dx.at[rs])
    move(gwu_in, small.at[:, head(half_f)], gwu)
    move(gd, big.at[2, head(half_f // 2)], gwd.at[pl.ds(pl.multiple_of(d * (half_f // 2), half_f // 2), half_f // 2)])
    parts = [(0, half_f, gbup), (half_f, hw, ggam), (half_f + hw, hw, gbet), (half_f + 2 * hw, hw, gbdn)]
    move(gs, sums)
    outs[-1] = [pltpu.make_async_copy(sums.at[:, pl.ds(a, w)], dst, out_sem) for a, w, dst in parts]
    for cp in ins:
        cp.start()
    for cp, tos in zip(ins, outs):
        cp.wait()
        for to in tos:
            to.start()
    for tos in outs:
        for to in tos:
            to.wait()


def solution(mesh):
    tok_spec = P(('dp', 'depth', 'row'), 'col')
    vec_spec = P('col')
    mat_spec = P('row', 'col')
    grad_vec = P(('dp', 'col'))
    grad_mat = P(('dp', 'row'), 'col')
    swap = ((0, 1), (1, 0))

    def local_pass(x, gamma, beta, w_up, b_up, w_down, b_down, dy):
        rows, hw = x.shape
        half_f = b_up.shape[0]
        full_f, full, hq = 2 * half_f, 2 * hw, hw // 2
        chunks = rows // M
        late = LATE * M
        hbm = pl.BlockSpec(memory_space=pltpu.HBM)
        sds = jax.ShapeDtypeStruct
        V, D = pltpu.VMEM, pltpu.SemaphoreType.DMA
        D2, D3, D4, D2S = D((2,)), D((3,)), D((4,)), D((2, SUBS))
        tiles, own_tiles = full_f // FT, half_f // FT
        outs = [
            sds((rows, hw), BF16), sds((rows, hw), BF16), sds((late, hw), BF16), sds((1, full_f), F32), sds((hw, half_f), BF16),
            sds((half_f // 2, hw), BF16),
            sds((rows // 2, hw), BF16), sds((tiles, 2, hq, FT), F32), sds((tiles, hq, FT), F32), sds((own_tiles, hq, FT), F32),
            sds((2, hw, half_f // 2), F32), sds((hw // 128, 128, half_f // 2), F32),
            sds((rows // 2, hw), BF16), sds((rows // 2, hw), BF16), sds((chunks // 2, 2, hq, full), F32), sds((chunks // 2, 2, hq, 128), F32),
        ]
        scratch = [
            V((full, full_f), BF16), V((full_f, full), BF16), V((2, 2, hw, half_f // 2), F32), V((2, 2, hq, full_f), F32),
            V((2, M, hw), BF16), V((RING, M, hw), BF16), V((2, M, hw), BF16), V((M, full), BF16), V((full, M), BF16), V((hw, M), BF16),
            V((2, hq, 128), F32), V((2, M, FT), BF16), V((2, 2, hq, FT), F32), V((2, M, FT), BF16), V((2, M, FT), BF16),
            V((M, hw), F32), V((2, hq, full), F32), V((M, hw), BF16), V((M, hw), BF16), V((M, hw), BF16),
            V((8, full_f), F32), V((8, 2 * full + hw), F32), V((2, 1, full_f), F32), V((2, half_f // 128, 128), BF16), V((hw // 128, 128), BF16),
            V((1, full_f), F32), V((2, 1, full_f), F32), V((3, 1, full_f), F32),
            D2, D2, D2, D2S, D2, D2S, D2, D2S, D2, D2S, D3, D3,
            D((RING,)), D((RING,)), D((6, 2)), D4, D4, D((2, 2)), D(()), D((tiles,)), D(()), D((tiles,)), D(()), D((own_tiles,)),
            D(()), D(()), D(()), D(()), D(()), D((hw // 128,)), D(()), D(()), D3, D3, pltpu.SemaphoreType.REGULAR,
        ]
        res = pl.pallas_call(
            kernel,
            out_shape=outs,
            in_specs=[hbm] * 8,
            out_specs=[hbm] * len(outs),
            scratch_shapes=scratch,
            compiler_params=pltpu.CompilerParams(
                collective_id=0, has_side_effects=True, vmem_limit_bytes=67043328),
            cost_estimate=pl.CostEstimate(flops=14 * rows * full * full_f, bytes_accessed=2 ** 27, transcendentals=rows * full_f),
            name='mlp_block',
        )(x, dy, w_up, w_down, b_up.reshape(-1, 128), gamma.reshape(1, -1), beta.reshape(1, -1), b_down.reshape(-1, 128))
        y, dx, dxl, gs, gwu, gd = res[:6]
        gd_far = lax.ppermute(gd, 'depth', swap)
        dx_far = lax.ppermute(dxl, 'col', swap)
        moves = 2 * COPIES + 3
        y, dx, gwu, gwd, gbup, ggam, gbet, gbdn = pl.pallas_call(
            finish_kernel,
            out_shape=[sds((rows, hw), BF16), sds((rows, hw), BF16), sds((hw, half_f), BF16), sds((half_f, hw), BF16),
                       sds((1, half_f), F32), sds((1, hw), F32), sds((1, hw), F32), sds((1, hw), F32)],
            in_specs=[hbm] * 5,
            out_specs=[hbm] * 8,
            scratch_shapes=[V((3, rows, hw), BF16), V((hw, half_f), BF16), V((1, full_f), F32), D((moves,)), D(())],
            compiler_params=pltpu.CompilerParams(vmem_limit_bytes=62000000),
            cost_estimate=pl.CostEstimate(flops=2 ** 33, bytes_accessed=42 * 2 ** 20, transcendentals=0),
            name='finish',
        )(y, dx, gwu, gd, gs)
        gwd = lax.dynamic_update_slice(gwd, gd_far, ((1 - lax.axis_index('depth')) * (half_f // 2), 0))
        dx = lax.dynamic_update_slice(dx, dx_far, ((1 - lax.axis_index('col')) * (rows // 2) + rows // 2 - late, 0))
        return y, dx, ggam.reshape(-1), gbet.reshape(-1), gwu, gbup.reshape(-1), gwd, gbdn.reshape(-1)

    return jax.shard_map(
        local_pass,
        mesh=mesh,
        in_specs=(tok_spec, vec_spec, vec_spec, mat_spec, vec_spec, mat_spec, vec_spec, tok_spec),
        out_specs=(tok_spec, tok_spec, grad_vec, grad_vec, grad_mat, grad_vec, grad_mat, grad_vec),
        check_vma=False,
    )
```

```python
import jax
import jax.numpy as jnp
from jax import lax
from jax.experimental import pallas as pl
from jax.experimental.pallas import tpu as pltpu
from jax.sharding import PartitionSpec as P

LN_EPS = 1e-5
C0 = 0.7978845608
C1 = C0 * 0.044715
M = 512
FT = 512
SUBS = 2
RING = 6
LATE = 2
PROMPT = 2
COPIES = 4
BF16, F32 = jnp.bfloat16, jnp.float32
MESH = pl.DeviceIdType.MESH


def dot(lhs, rhs, rhs_dim=0):
    return lax.dot_general(lhs, rhs, (((1,), (rhs_dim,)), ((), ())), preferred_element_type=F32)


def dot_t(lhs, rhs):
    return dot(lhs, rhs, 1)


def odd(n):
    return lax.rem(n, 2)


def cat(*parts):
    return jnp.concatenate(parts, axis=1)


def row_sum(v):
    return jnp.sum(v, axis=1, keepdims=True)


def col_sum(v):
    return jnp.sum(v, axis=0, keepdims=True)


def head(n):
    return pl.ds(0, n)


def tile(i, n):
    return slice(i * n, (i + 1) * n)


def gelu(v):
    t = jnp.tanh(v * (C1 * (v * v) + C0))
    h = 0.5 * v
    return h * t + h


def gelu_and_slope(v):
    v2 = v * v
    t = jnp.tanh(v * (C1 * v2 + C0))
    h = 0.5 * v
    slope = (v * (1.0 - t * t)) * (1.5 * C1 * v2 + 0.5 * C0) + (0.5 * t + 0.5)
    return h * t + h, slope


def fold8(v):
    return jnp.sum(v.reshape(v.shape[0] // 8, 8, v.shape[1]), axis=0)


def kernel(x_h, dy_h, wu_h, wd_h, bup_h, gam_h, bet_h, bdn_h,
           y_h, dx_h, dxl_h, gs_h, gu_h, gd_h, dxo_h, rrow_h, ryu_h, rx_h, rdn_h, ydn_h, xo_h, dyo_h, dxn_h, st_h,
           wu, wd, acc_d, acc_u, own, land, aux, xn, trx, trd, st, us, da_s, act, du_s, yacc, dxn, yo, dxa, dxb,
           bup8, gb8, smv, bup_s, bdn_s, gso, gsp, gsl,
           wrow_s, wrow_r, wx_s, wx_r, wy_s, wy_r, wa_s, wa_r, wb_s, wb_r, sm_s, sm_r,
           land_s, land_r, ld_sem, out_sem, sv_sem, t_sem, ru_s, ru_r, yu_s, yu_r, rx_s, rx_r, ag_s, ag_r, rdn_s, rdn_r,
           ydn_s, ydn_r, dx_s, dx_r, gs_s, gs_r, credit):
    chunks = x_h.shape[0] // M
    half_n = chunks // 2
    half_f = wu_h.shape[1]
    hw = x_h.shape[1]
    full = 2 * hw
    hq = hw // 2
    half_d = half_f // 2
    tiles = 2 * half_f // FT
    own_tiles = tiles // 2
    c, r, d = lax.axis_index('col'), lax.axis_index('row'), lax.axis_index('depth')
    b = lax.rem(r + c, 2)
    peer = {'col': 1 - c, 'row': 1 - r, 'depth': 1 - d}
    mine0, theirs0 = c * half_n, (1 - c) * half_n

    def send(src, dst, s_sem, r_sem, axis):
        return pltpu.make_async_remote_copy(src_ref=src, dst_ref=dst, send_sem=s_sem, recv_sem=r_sem,
                                            device_id={axis: peer[axis]}, device_id_type=MESH)

    def local(src, dst, sem):
        return pltpu.make_async_copy(src, dst, sem)

    def all_of(ref, sem):
        return pltpu.make_async_copy(ref, ref, sem)

    def rows_of(k):
        return pl.ds(pl.multiple_of(k * M, M), M)

    def chunk_at(n):
        return lax.rem(mine0 + n, chunks)

    bar = pltpu.get_barrier_semaphore()
    for axis in ('col', 'row', 'depth'):
        pl.semaphore_signal(bar, inc=1, device_id={axis: peer[axis]}, device_id_type=MESH)
    pl.semaphore_wait(bar, 3)

    half_rows = (hq, half_d)
    w_srcs = (wu_h, wd_h)

    def w_cols(kind, blk, dep, s):
        n = half_rows[kind] // SUBS
        if kind == 0:
            return wu.at[pl.ds(pl.multiple_of(blk * hw + dep * hq + s * n, n), n), pl.ds(half_f, half_f)]
        return wd.at[pl.ds(pl.multiple_of(blk * half_f + dep * half_d + s * n, n), n), pl.ds(hw, hw)]

    def w_half(kind):
        return wu.at[head(hq), head(half_f)] if kind == 0 else wd.at[head(half_d), head(hw)]

    def w_own(kind):
        if kind == 0:
            return wu.at[pl.ds(pl.multiple_of(b * hw, hw), hw), head(half_f)]
        return wd.at[pl.ds(pl.multiple_of(b * half_f, half_f), half_f), head(hw)]

    def w_x(kind, s):
        n = half_rows[kind] // SUBS
        src = w_srcs[kind].at[pl.ds(pl.multiple_of(d * half_rows[kind] + s * n, n), n), :]
        return send(src, w_cols(kind, 1 - b, d, s), wx_s.at[kind], wx_r.at[kind, s], 'col')

    def w_y(kind, s):
        return send(w_cols(kind, b, d, s), w_cols(kind, b, d, s), wy_s.at[kind], wy_r.at[kind, s], 'depth')

    def w_a(kind, s):
        return send(w_cols(kind, b, d, s), w_cols(kind, b, d, s), wa_s.at[kind], wa_r.at[kind, s], 'row')

    def w_b(kind, s):
        return send(w_cols(kind, b, 1 - d, s), w_cols(kind, b, 1 - d, s), wb_s.at[kind], wb_r.at[kind, s], 'row')

    def w_row(kind):
        return send(w_srcs[kind], w_own(kind), wrow_s.at[kind], wrow_r.at[kind], 'row')

    def w_load(kind):
        return local(w_srcs[kind], w_own(kind), out_sem.at[kind])

    def stream(src, k, q):
        slot = lax.rem(q, RING)
        return send(src.at[rows_of(k), :], land.at[slot], land_s.at[slot], land_r.at[slot], 'col')

    def stream_next(src, k, q):
        @pl.when(q >= RING)
        def _():
            stream(src, k, q).wait_send()
            pl.semaphore_wait(credit, 1)
        stream(src, k, q).start()

    def give(n):
        for _ in range(n):
            pl.semaphore_signal(credit, inc=1, device_id={'col': peer['col']}, device_id_type=MESH)

    gam_at, bet_at = pl.ds(half_f, hw), pl.ds(half_f + hw, hw)
    sm_own = [local(bup_h, bup_s.at[0], ld_sem.at[0, 0]), local(gam_h, smv.at[0, :, gam_at], ld_sem.at[0, 1]),
              local(bet_h, smv.at[0, :, bet_at], ld_sem.at[1, 0]), local(bdn_h, bdn_s, ld_sem.at[1, 1])]
    sm_out = [send(bup_h, bup_s.at[1], sm_s.at[0], sm_r.at[0], 'col'),
              send(gam_h, smv.at[1, :, gam_at], sm_s.at[1], sm_r.at[1], 'col'),
              send(bet_h, smv.at[1, :, bet_at], sm_s.at[2], sm_r.at[2], 'col')]
    for cp in sm_own + sm_out:
        cp.start()
    for kind in range(2):
        for s in range(SUBS):
            w_x(kind, s).start()
    for kind in range(2):
        w_load(kind).start()
        w_row(kind).start()
    for i in range(2):
        stream(x_h, theirs0 + i, 2 * i).start()
        stream(dy_h, theirs0 + i, 2 * i + 1).start()

    acc_d[...] = jnp.zeros_like(acc_d)
    acc_u[...] = jnp.zeros_like(acc_u)
    bup8[...] = jnp.zeros_like(bup8)
    gb8[...] = jnp.zeros_like(gb8)
    for cp in sm_own:
        cp.wait()

    def load(n):
        s = odd(n)
        rs = rows_of(chunk_at(n))
        return (local(x_h.at[rs, :], own.at[s], ld_sem.at[0, s]), local(dy_h.at[rs, :], aux.at[s], ld_sem.at[1, s]))

    for cp in load(0):
        cp.start()
    for kind in range(2):
        for s in range(SUBS):
            w_x(kind, s).wait_recv()
            w_y(kind, s).start()
            w_a(kind, s).start()
        for s in range(SUBS):
            w_y(kind, s).wait_recv()
            w_b(kind, s).start()
    for kind in range(2):
        w_load(kind).wait()
        w_row(kind).wait()
        for s in range(SUBS):
            w_a(kind, s).wait_recv()
            w_b(kind, s).wait_recv()
        for sems in (wx_s, wy_s, wa_s, wb_s):
            all_of(w_half(kind), sems.at[kind]).wait()
    for cp in sm_out:
        cp.wait()
    for i in range(half_f // 128):
        for side in range(2):
            smv[side, :, tile(i, 128)] = bup_s[side, i:i + 1, :].astype(F32)
    for i in range(hw // 128):
        smv[0, :, half_f + full + i * 128:half_f + full + (i + 1) * 128] = bdn_s[i:i + 1, :].astype(F32)

    def wide(at):
        return cat(smv[0, :, half_f + at:half_f + at + hw], smv[1, :, half_f + at:half_f + at + hw])

    def norm(s, slot, keep):
        gam, bet = wide(0), wide(hw)
        step = 32
        for i in range(M // step):
            rs = tile(i, step)
            xv = cat(own[s, rs, :], land[slot, rs, :]).astype(F32)
            mean = row_sum(xv) * (1.0 / full)
            cen = xv - mean
            istd = lax.rsqrt(row_sum(cen * cen) * (1.0 / full) + LN_EPS)
            xn[rs, :] = (cen * istd * gam + bet).astype(BF16)
            if keep:
                st[i * step // hq, i * step % hq:i * step % hq + step, :] = cat(jnp.broadcast_to(mean, (step, 64)), jnp.broadcast_to(istd, (step, 64)))
        dyv = aux[s]
        trd[...] = dyv.T
        gb8[:, 2 * full:2 * full + hw] += fold8(dyv.astype(F32))

    def write_y(s):
        bdn = smv[0, :, half_f + full:half_f + full + hw]
        yo[...] = (own[s].astype(F32) + yacc[...] + bdn).astype(BF16)

    def y_out(n):
        return local(yo, y_h.at[rows_of(chunk_at(n)), :], out_sem.at[0])

    def dx_out(n):
        return local(dxa, dx_h.at[rows_of(chunk_at(n)), :], out_sem.at[1])

    def dxo_out(n):
        return local(dxb, dxo_h.at[rows_of(n), :], out_sem.at[2])

    def dxl_out(n):
        return local(dxb, dxl_h.at[rows_of(n - (half_n - LATE)), :], out_sem.at[2])

    def saves(n, slot_x, slot_d):
        rs = rows_of(n)
        return (local(land.at[slot_x], xo_h.at[rs, :], sv_sem.at[0]), local(land.at[slot_d], dyo_h.at[rs, :], sv_sem.at[1]),
                local(dxn, dxn_h.at[n], sv_sem.at[2]), local(st, st_h.at[n], sv_sem.at[3]))

    def finish_dx(grads, xs, dys, stats):
        gam = wide(0)
        step = 32
        for i in range(M // step):
            rs = tile(i, step)
            h, hs = i * step // hq, slice(i * step % hq, i * step % hq + step)
            istd = stats[h, hs, 64:65]
            xh = (xs(rs).astype(F32) - stats[h, hs, 0:1]) * istd
            dv = grads(h, hs)
            px = dv * xh
            gb8[:, :full] += fold8(px)
            gb8[:, full:2 * full] += fold8(dv)
            m1 = row_sum(dv * gam) * (1.0 / full)
            m2 = row_sum(px * gam) * (1.0 / full)
            dxv = (dys(rs).astype(F32) + istd * (dv * gam - m1 - xh * m2)).astype(BF16)
            dxa[rs, :] = dxv[:, :hw]
            dxb[rs, :] = dxv[:, hw:]

    def dx_far(m):
        return send(dxo_h.at[rows_of(m), :], dx_h.at[rows_of(mine0 + m), :], dx_s, dx_r, 'col')

    def chunk_mine(n, carry):
        s = odd(n)
        slot_x, slot_d = lax.rem(2 * n, RING), lax.rem(2 * n + 1, RING)

        @pl.when(n < half_n - 2)
        def _():
            stream_next(x_h, theirs0 + n + 2, 2 * n + 4)
            stream_next(dy_h, theirs0 + n + 2, 2 * n + 5)

        @pl.when(n >= half_n - 2)
        def _():
            k = 2 * (n - (half_n - 2))
            stream_next(x_h, mine0 + k, chunks + k)
            stream_next(x_h, mine0 + k + 1, chunks + k + 1)

        for cp in load(n):
            cp.wait()
        for cp in load(n + 1):
            cp.start()

        for m in range(PROMPT):
            @pl.when(n == half_n // 2 + 2 * m - 1)
            def _():
                dx_far(m).start()

        stream(x_h, n, 2 * n).wait_recv()
        stream(dy_h, n, 2 * n + 1).wait_recv()
        save = saves(n, slot_x, slot_d)
        save[0].start()
        save[1].start()

        @pl.when(n > 0)
        def _():
            save[3].wait()

        norm(s, slot_x, True)
        save[3].start()
        trx[...] = xn[...].T

        @pl.when(n > 0)
        def _():
            save[2].wait()

        @pl.when((n > 0) & (n <= PROMPT))
        def _():
            dx_out(n).wait()
            dxo_out(n).wait()

        yacc[...] = jnp.zeros_like(yacc)
        dxn[...] = jnp.zeros_like(dxn)

        def quad(jj, inner):
            cols = [pl.ds(pl.multiple_of((own_tiles * jj + t) * FT, FT), FT) for t in range(own_tiles)]

            def first(t):
                bias = smv[jj, :, tile(t, FT)]
                us[t % 2] = (dot(xn[...], wu[:, cols[t]]) + bias).astype(BF16)
                dyv = cat(aux[s], land[slot_d])
                da_s[t % 2] = dot_t(dyv, wd[cols[t], :]).reshape(2, hq, FT)

            def mid(t):
                a, slope = gelu_and_slope(us[t % 2].astype(F32))
                act[t % 2] = a.astype(BF16)
                du = (da_s[t % 2].reshape(M, FT) * slope).astype(BF16)
                du_s[t % 2] = du
                bup8[:, cols[t]] += fold8(du.astype(F32))

            def last(t):
                yacc[...] += dot(act[t % 2], wd[cols[t], :hw])
                at = t * FT % half_d
                acc_d[jj, t * FT // half_d, :, at:at + FT] += dot(trd[...], act[t % 2])
                dxn[...] += dot_t(du_s[t % 2], wu[:, cols[t]]).reshape(2, hq, full)
                part = dot(trx[...], du_s[t % 2])
                for i in range(4):
                    acc_u[i // 2, i % 2, :, cols[t]] += part[tile(i, hq)]

            first(0)
            first(1)
            mid(0)
            for t in range(own_tiles):
                last(t)
                if t + 2 < own_tiles:
                    first(t + 2)
                if t + 1 < own_tiles:
                    mid(t + 1)
            return inner

        lax.fori_loop(0, 2, quad, 0)

        @pl.when(n > 0)
        def _():
            y_out(n).wait()

        write_y(s)
        y_out(n).start()
        save[2].start()

        @pl.when(n < PROMPT)
        def _():
            finish_dx(lambda h, rs: dxn[h, rs, :],
                      lambda rs: cat(own[s, rs, :], land[slot_x, rs, :]),
                      lambda rs: cat(aux[s, rs, :], land[slot_d, rs, :]), st)
            dx_out(n).start()
            dxo_out(n).start()

        save[0].wait()
        save[1].wait()
        give(2)
        return carry

    lax.fori_loop(0, half_n, chunk_mine, 0)

    order = [*range(own_tiles, tiles), *range(own_tiles)]

    def ru(p):
        return send(acc_u.at[1 - b, :, :, pl.ds(p * FT, FT)], rrow_h.at[p], ru_s, ru_r.at[p], 'row')

    def yu(p):
        return send(acc_u.at[b, 1 - d, :, pl.ds(p * FT, FT)], ryu_h.at[p], yu_s, yu_r.at[p], 'depth')

    def rx(k):
        return send(acc_u.at[b, d, :, pl.ds((own_tiles + k) * FT, FT)], rx_h.at[k], rx_s, rx_r.at[k], 'col')

    gu_rows = pl.ds(pl.multiple_of(d * hq, hq), hq)

    def ag(k):
        ps = pl.ds(k * FT, FT)
        return send(trx.at[pl.ds(k * hq, hq), :], gu_h.at[gu_rows, ps], ag_s, ag_r, 'depth')

    def gu_out(k):
        return local(trx.at[pl.ds(k * hq, hq), :], gu_h.at[gu_rows, pl.ds(k * FT, FT)], out_sem.at[3])

    def row_load(i, p):
        return local(rrow_h.at[p], da_s.at[i % 2], t_sem.at[i % 2, 0])

    for p in order:
        ru(p).start()
    y_out(0).wait()
    for cp in saves(half_n - 1, 0, 0)[2:]:
        cp.wait()
    ru(order[0]).wait_recv()
    row_load(0, order[0]).start()
    for i, p in enumerate(order):
        if i + 1 < tiles:
            ru(order[i + 1]).wait_recv()
            row_load(i + 1, order[i + 1]).start()
        row_load(i, p).wait()
        for h in range(2):
            acc_u[b, h, :, tile(p, FT)] += da_s[i % 2, h]
        yu(p).start()

    def oth_load(k):
        yu(own_tiles + k).wait_recv()
        local(ryu_h.at[own_tiles + k], da_s.at[k % 2, 0], t_sem.at[k % 2, 0]).start()

    def oth_send(k):
        p = own_tiles + k
        local(ryu_h.at[p], da_s.at[k % 2, 0], t_sem.at[k % 2, 0]).wait()
        acc_u[b, d, :, tile(p, FT)] += da_s[k % 2, 0]
        rx(k).start()

    def own_loads(k):
        return (local(ryu_h.at[k], da_s.at[k % 2, 0], t_sem.at[k % 2, 0]),
                local(rx_h.at[k], da_s.at[k % 2, 1], t_sem.at[k % 2, 1]))

    def own_load(k):
        yu(k).wait_recv()
        rx(k).wait_recv()
        for cp in own_loads(k):
            cp.start()

    def own_send(k):
        for cp in own_loads(k):
            cp.wait()
        trx[tile(k, hq), :] = (acc_u[b, d, :, tile(k, FT)] + da_s[k % 2, 0] + da_s[k % 2, 1]).astype(BF16)
        ag(k).start()

    def background(n):
        for k in range(own_tiles):
            @pl.when(n == half_n + 2 + k)
            def _():
                oth_send(k)

            @pl.when(n == half_n + 1 + k)
            def _():
                oth_load(k)

        for k in range(own_tiles - 1):
            @pl.when(n == half_n + 6 + k)
            def _():
                own_send(k)

            @pl.when(n == half_n + 5 + k)
            def _():
                if k >= 1:
                    pass
                own_load(k)

    def chunk_theirs(n, carry):
        s = odd(n)
        q = n + half_n
        slot = lax.rem(q, RING)

        @pl.when(n == half_n)
        def _():
            stream_next(x_h, mine0 + 4, chunks + 4)

        @pl.when(n <= half_n + 2)
        def _():
            stream_next(x_h, mine0 + 5 + (n - half_n), chunks + 5 + (n - half_n))

        background(n)
        for cp in load(n):
            cp.wait()

        @pl.when(n < chunks - 1)
        def _():
            for cp in load(n + 1):
                cp.start()

        stream(x_h, n, q).wait_recv()
        norm(s, slot, False)

        def up(j):
            side, at = divmod(j * FT, half_f)
            us[j % 2] = (dot(xn[...], wu[:, tile(j, FT)]) + smv[side, :, at:at + FT]).astype(BF16)

        def mid(j):
            act[j % 2] = gelu(us[j % 2].astype(F32)).astype(BF16)

        def down(j):
            part = dot(act[j % 2], wd[tile(j, FT), :hw])
            yacc[...] = part if j == 0 else yacc[...] + part
            blk, rest = divmod(j * FT, half_f)
            qt, at = divmod(rest, half_d)
            acc_d[blk, qt, :, at:at + FT] += dot(trd[...], act[j % 2])

        up(0)
        up(1)
        mid(0)
        for j in range(tiles):
            if j + 2 < tiles:
                up(j + 2)
            down(j)
            if j + 1 < tiles:
                mid(j + 1)

        @pl.when(n > half_n)
        def _():
            y_out(n).wait()

        write_y(s)
        y_out(n).start()

        @pl.when(n < half_n + 2)
        def _():
            give(1)
        return carry

    lax.fori_loop(half_n, chunks, chunk_theirs, 0)

    rdn = send(acc_d.at[1 - b], rdn_h, rdn_s, rdn_r, 'row')
    rdn.start()
    k = own_tiles - 1
    own_send(k - 1)
    own_load(k)
    own_send(k)
    for k in range(own_tiles):
        gu_out(k).start()
    rdn.wait()
    rd_load = local(rdn_h, acc_d.at[1 - b], t_sem.at[0, 0])
    rd_load.start()
    rd_load.wait()
    steps = hw // 128

    def ydn(i):
        return send(acc_d.at[b, 1 - d, pl.ds(i * 128, 128), :], ydn_h.at[i], ydn_s, ydn_r.at[i], 'depth')

    for i in range(steps):
        rs = tile(i, 128)
        for qt in range(2):
            acc_d[b, qt, rs, :] += acc_d[1 - b, qt, rs, :]
        ydn(i).start()
    y_out(chunks - 1).wait()
    all_of(acc_u.at[1 - b], ru_s).wait()

    def load_dx(n):
        s = odd(n)
        rs, ks = rows_of(n), rows_of(mine0 + n)
        return (local(x_h.at[ks, :], own.at[s], ld_sem.at[0, s]), local(dy_h.at[ks, :], aux.at[s], ld_sem.at[1, s]),
                local(xo_h.at[rs, :], land.at[2 * s], ld_sem.at[2, s]), local(dyo_h.at[rs, :], land.at[2 * s + 1], ld_sem.at[3, s]),
                local(dxn_h.at[n], acc_u.at[1 - b, :, :, pl.ds(pl.multiple_of(s * full, full), full)], ld_sem.at[4, s]),
                local(st_h.at[n], da_s.at[s, :, :, head(128)], ld_sem.at[5, s]))

    held = 2

    def chunk_dx(n, carry):
        s = odd(n)
        for cp in load_dx(n):
            cp.wait()

        @pl.when(n < half_n - 1)
        def _():
            for cp in load_dx(n + 1):
                cp.start()

        @pl.when(n > PROMPT)
        def _():
            dx_out(n).wait()
            dxo_out(n).wait()

        @pl.when((n > PROMPT) & (n <= half_n - LATE - held))
        def _():
            dx_far(n - 1).start()

        finish_dx(lambda h, rs: acc_u[1 - b, h, rs, pl.ds(pl.multiple_of(s * full, full), full)],
                  lambda rs: cat(own[s, rs, :], land[2 * s, rs, :]),
                  lambda rs: cat(aux[s, rs, :], land[2 * s + 1, rs, :]), da_s.at[s, :, :, head(128)])
        dx_out(n).start()

        @pl.when(n < half_n - LATE)
        def _():
            dxo_out(n).start()

        @pl.when(n >= half_n - LATE)
        def _():
            dxl_out(n).start()
        return carry

    for cp in load_dx(PROMPT):
        cp.start()
    lax.fori_loop(PROMPT, half_n, chunk_dx, 0)
    oth = lambda at, n: [col_sum(ref[:, a:a + n]) for ref, a in at]
    gso[...] = jnp.concatenate(oth(((bup8, half_f),), half_f) + oth(((gb8, hw), (gb8, full + hw)), hw)
                               + [jnp.zeros((1, half_f - full), F32)], axis=1)
    gs_col = send(gso, gsl.at[0], gs_s.at[0], gs_r.at[0], 'col')
    gs_col.start()
    for m in range(half_n - LATE - held, half_n - LATE):
        dx_far(m).start()
    dx_out(half_n - 1).wait()
    dxl_out(half_n - 1).wait()
    gs_col.wait()
    gsp[0] = jnp.concatenate(oth(((bup8, 0),), half_f) + oth(((gb8, 0), (gb8, full), (gb8, 2 * full)), hw)
                             + [jnp.zeros((1, half_f - 3 * hw), F32)], axis=1) + gsl[0]
    gs_row = send(gsp.at[0], gsl.at[1], gs_s.at[1], gs_r.at[1], 'row')
    gs_row.start()
    gs_row.wait()
    gsp[1] = gsp[0] + gsl[1]
    gs_dep = send(gsp.at[1], gsl.at[2], gs_s.at[2], gs_r.at[2], 'depth')
    gs_dep.start()
    for q in range(3 * half_n - RING, 3 * half_n):
        stream(x_h, 0, q).wait_send()
    all_of(acc_u.at[b, 1 - d], yu_s).wait()
    all_of(acc_u.at[b, d, :, pl.ds(half_f, half_f)], rx_s).wait()
    all_of(trx, out_sem.at[3]).wait()
    for i in range(steps):
        ydn(i).wait_recv()
        dn_load = local(ydn_h.at[i], acc_d.at[1 - b, 0, pl.ds(i * 128, 128), :], t_sem.at[1, 0])
        dn_load.start()
        dn_load.wait()
        rs = tile(i, 128)
        for j in range(half_d // 128):
            cs = tile(j, 128)
            total = acc_d[b, d, rs, cs] + acc_d[1 - b, 0, rs, cs]
            us[j * 128 // M, j * 128 % M:j * 128 % M + 128, rs] = total.T.astype(BF16)
    gd_out = [local(us.at[i], gd_h.at[pl.ds(i * M, M), :], t_sem.at[i, 1]) for i in range(2)]
    for cp in gd_out:
        cp.start()
    gs_dep.wait()
    gsp[0] = gsp[1] + gsl[2]
    gs_out = local(gsp.at[0], gs_h, out_sem.at[0])
    gs_out.start()
    all_of(acc_d.at[b, 1 - d], ydn_s).wait()
    for sem in (ag_s, ag_r):
        all_of(trx, sem).wait()
    sent = dxo_h.at[head((half_n - LATE) * M), :]
    for sem in (dx_s, dx_r):
        all_of(sent, sem).wait()
    for cp in gd_out:
        cp.wait()
    gs_out.wait()


def finish_kernel(y_in, dx_in, gwu_in, gd, gs, y, dx, gwu, gwd, gbup, ggam, gbet, gbdn, big, small, sums, in_sem, out_sem):
    rows, hw = y.shape
    half_f = gwd.shape[0]
    d = lax.axis_index('depth')
    n = rows // COPIES
    ins, outs = [], []

    def move(src, buf, *dst):
        ins.append(pltpu.make_async_copy(src, buf, in_sem.at[len(ins)]))
        outs.append([pltpu.make_async_copy(buf, to, out_sem) for to in dst])

    for i in range(COPIES):
        rs = pl.ds(i * n, n)
        move(y_in.at[rs], big.at[0, rs], y.at[rs])
        move(dx_in.at[rs], big.at[1, rs], dx.at[rs])
    move(gwu_in, small.at[:, head(half_f)], gwu)
    move(gd, big.at[2, head(half_f // 2)], gwd.at[pl.ds(pl.multiple_of(d * (half_f // 2), half_f // 2), half_f // 2)])
    parts = [(0, half_f, gbup), (half_f, hw, ggam), (half_f + hw, hw, gbet), (half_f + 2 * hw, hw, gbdn)]
    move(gs, sums)
    outs[-1] = [pltpu.make_async_copy(sums.at[:, pl.ds(a, w)], dst, out_sem) for a, w, dst in parts]
    for cp in ins:
        cp.start()
    for cp, tos in zip(ins, outs):
        cp.wait()
        for to in tos:
            to.start()
    for tos in outs:
        for to in tos:
            to.wait()


def solution(mesh):
    tok_spec = P(('dp', 'depth', 'row'), 'col')
    vec_spec = P('col')
    mat_spec = P('row', 'col')
    grad_vec = P(('dp', 'col'))
    grad_mat = P(('dp', 'row'), 'col')
    swap = ((0, 1), (1, 0))

    def local_pass(x, gamma, beta, w_up, b_up, w_down, b_down, dy):
        rows, hw = x.shape
        half_f = b_up.shape[0]
        full_f, full, hq = 2 * half_f, 2 * hw, hw // 2
        chunks = rows // M
        late = LATE * M
        hbm = pl.BlockSpec(memory_space=pltpu.HBM)
        sds = jax.ShapeDtypeStruct
        V, D = pltpu.VMEM, pltpu.SemaphoreType.DMA
        D2, D3, D4, D2S = D((2,)), D((3,)), D((4,)), D((2, SUBS))
        tiles, own_tiles = full_f // FT, half_f // FT
        outs = [
            sds((rows, hw), BF16), sds((rows, hw), BF16), sds((late, hw), BF16), sds((1, full_f), F32), sds((hw, half_f), BF16),
            sds((half_f // 2, hw), BF16),
            sds((rows // 2, hw), BF16), sds((tiles, 2, hq, FT), F32), sds((tiles, hq, FT), F32), sds((own_tiles, hq, FT), F32),
            sds((2, hw, half_f // 2), F32), sds((hw // 128, 128, half_f // 2), F32),
            sds((rows // 2, hw), BF16), sds((rows // 2, hw), BF16), sds((chunks // 2, 2, hq, full), F32), sds((chunks // 2, 2, hq, 128), F32),
        ]
        scratch = [
            V((full, full_f), BF16), V((full_f, full), BF16), V((2, 2, hw, half_f // 2), F32), V((2, 2, hq, full_f), F32),
            V((2, M, hw), BF16), V((RING, M, hw), BF16), V((2, M, hw), BF16), V((M, full), BF16), V((full, M), BF16), V((hw, M), BF16),
            V((2, hq, 128), F32), V((2, M, FT), BF16), V((2, 2, hq, FT), F32), V((2, M, FT), BF16), V((2, M, FT), BF16),
            V((M, hw), F32), V((2, hq, full), F32), V((M, hw), BF16), V((M, hw), BF16), V((M, hw), BF16),
            V((8, full_f), F32), V((8, 2 * full + hw), F32), V((2, 1, full_f), F32), V((2, half_f // 128, 128), BF16), V((hw // 128, 128), BF16),
            V((1, full_f), F32), V((2, 1, full_f), F32), V((3, 1, full_f), F32),
            D2, D2, D2, D2S, D2, D2S, D2, D2S, D2, D2S, D3, D3,
            D((RING,)), D((RING,)), D((6, 2)), D4, D4, D((2, 2)), D(()), D((tiles,)), D(()), D((tiles,)), D(()), D((own_tiles,)),
            D(()), D(()), D(()), D(()), D(()), D((hw // 128,)), D(()), D(()), D3, D3, pltpu.SemaphoreType.REGULAR,
        ]
        res = pl.pallas_call(
            kernel,
            out_shape=outs,
            in_specs=[hbm] * 8,
            out_specs=[hbm] * len(outs),
            scratch_shapes=scratch,
            compiler_params=pltpu.CompilerParams(
                collective_id=0, has_side_effects=True, vmem_limit_bytes=67043328),
            cost_estimate=pl.CostEstimate(flops=14 * rows * full * full_f, bytes_accessed=2 ** 27, transcendentals=rows * full_f),
            name='mlp_block',
        )(x, dy, w_up, w_down, b_up.reshape(-1, 128), gamma.reshape(1, -1), beta.reshape(1, -1), b_down.reshape(-1, 128))
        y, dx, dxl, gs, gwu, gd = res[:6]
        gd_far = lax.ppermute(gd, 'depth', swap)
        dx_far = lax.ppermute(dxl, 'col', swap)
        moves = 2 * COPIES + 3
        y, dx, gwu, gwd, gbup, ggam, gbet, gbdn = pl.pallas_call(
            finish_kernel,
            out_shape=[sds((rows, hw), BF16), sds((rows, hw), BF16), sds((hw, half_f), BF16), sds((half_f, hw), BF16),
                       sds((1, half_f), F32), sds((1, hw), F32), sds((1, hw), F32), sds((1, hw), F32)],
            in_specs=[hbm] * 5,
            out_specs=[hbm] * 8,
            scratch_shapes=[V((3, rows, hw), BF16), V((hw, half_f), BF16), V((1, full_f), F32), D((moves,)), D(())],
            compiler_params=pltpu.CompilerParams(vmem_limit_bytes=62000000),
            cost_estimate=pl.CostEstimate(flops=2 ** 33, bytes_accessed=42 * 2 ** 20, transcendentals=0),
            name='finish',
        )(y, dx, gwu, gd, gs)
        gwd = lax.dynamic_update_slice(gwd, gd_far, ((1 - lax.axis_index('depth')) * (half_f // 2), 0))
        dx = lax.dynamic_update_slice(dx, dx_far, ((1 - lax.axis_index('col')) * (rows // 2) + rows // 2 - late, 0))
        return y, dx, ggam.reshape(-1), gbet.reshape(-1), gwu, gbup.reshape(-1), gwd, gbdn.reshape(-1)

    return jax.shard_map(
        local_pass,
        mesh=mesh,
        in_specs=(tok_spec, vec_spec, vec_spec, mat_spec, vec_spec, mat_spec, vec_spec, tok_spec),
        out_specs=(tok_spec, tok_spec, grad_vec, grad_vec, grad_mat, grad_vec, grad_mat, grad_vec),
        check_vma=False,
    )
```

```python
import jax
import jax.numpy as jnp
from jax import lax
from jax.experimental import pallas as pl
from jax.experimental.pallas import tpu as pltpu
from jax.sharding import PartitionSpec as P

LN_EPS = 1e-5
C0 = 0.7978845608
C1 = C0 * 0.044715
M = 512
FT = 512
SUBS = 2
RING = 6
LATE = 2
PROMPT = 2
COPIES = 4
LANES = 128
BF16, F32 = jnp.bfloat16, jnp.float32
MESH = pl.DeviceIdType.MESH


def dot(lhs, rhs, rhs_dim=0):
    return lax.dot_general(lhs, rhs, (((1,), (rhs_dim,)), ((), ())), preferred_element_type=F32)


def dot_t(lhs, rhs):
    return dot(lhs, rhs, 1)


def odd(n):
    return lax.rem(n, 2)


def cat(*parts):
    return jnp.concatenate(parts, axis=1)


def row_sum(v):
    return jnp.sum(v, axis=1, keepdims=True)


def col_sum(v):
    return jnp.sum(v, axis=0, keepdims=True)


def head(n):
    return pl.ds(0, n)


def tile(i, n):
    return slice(i * n, (i + 1) * n)


def gelu(v):
    t = jnp.tanh(v * (C1 * (v * v) + C0))
    h = 0.5 * v
    return h * t + h


def gelu_and_slope(v):
    v2 = v * v
    t = jnp.tanh(v * (C1 * v2 + C0))
    h = 0.5 * v
    slope = (v * (1.0 - t * t)) * (1.5 * C1 * v2 + 0.5 * C0) + (0.5 * t + 0.5)
    return h * t + h, slope


def fold8(v):
    return jnp.sum(v.reshape(v.shape[0] // 8, 8, v.shape[1]), axis=0)


def kernel(x_h, dy_h, wu_h, wd_h, bup_h, gam_h, bet_h, bdn_h,
           y_h, dx_h, dxl_h, gs_h, gu_h, gd_h, dxo_h, rrow_h, ryu_h, rx_h, rdn_h, ydn_h, xo_h, dyo_h, dxn_h, st_h,
           wu, wd, acc_d, acc_u, own, land, aux, xn, trx, trd, st, us, da_s, act, du_s, yacc, dxn, yo, dxa, dxb,
           bup8, gb8, smv, bup_s, bdn_s, gso, gsp, gsl,
           wrow_s, wrow_r, wx_s, wx_r, wy_s, wy_r, wa_s, wa_r, wb_s, wb_r, sm_s, sm_r,
           land_s, land_r, ld_sem, out_sem, sv_sem, t_sem, ru_s, ru_r, yu_s, yu_r, rx_s, rx_r, ag_s, ag_r, rdn_s, rdn_r,
           ydn_s, ydn_r, dx_s, dx_r, gs_s, gs_r, credit):
    chunks = x_h.shape[0] // M
    half_n = chunks // 2
    half_f = wu_h.shape[1]
    hw = x_h.shape[1]
    full = 2 * hw
    hq = hw // 2
    half_d = half_f // 2
    tiles = 2 * half_f // FT
    own_tiles = tiles // 2
    c, r, d = lax.axis_index('col'), lax.axis_index('row'), lax.axis_index('depth')
    b = lax.rem(r + c, 2)
    peer = {'col': 1 - c, 'row': 1 - r, 'depth': 1 - d}
    mine0, theirs0 = c * half_n, (1 - c) * half_n

    def send(src, dst, s_sem, r_sem, axis):
        return pltpu.make_async_remote_copy(src_ref=src, dst_ref=dst, send_sem=s_sem, recv_sem=r_sem,
                                            device_id={axis: peer[axis]}, device_id_type=MESH)

    def local(src, dst, sem):
        return pltpu.make_async_copy(src, dst, sem)

    def all_of(ref, sem):
        return pltpu.make_async_copy(ref, ref, sem)

    def rows_of(k):
        return pl.ds(pl.multiple_of(k * M, M), M)

    def chunk_at(n):
        return lax.rem(mine0 + n, chunks)

    bar = pltpu.get_barrier_semaphore()
    for axis in ('col', 'row', 'depth'):
        pl.semaphore_signal(bar, inc=1, device_id={axis: peer[axis]}, device_id_type=MESH)
    pl.semaphore_wait(bar, 3)

    half_rows = (hq, half_d)
    w_srcs = (wu_h, wd_h)

    def w_cols(kind, blk, dep, s):
        n = half_rows[kind] // SUBS
        if kind == 0:
            return wu.at[pl.ds(pl.multiple_of(blk * hw + dep * hq + s * n, n), n), pl.ds(half_f, half_f)]
        return wd.at[pl.ds(pl.multiple_of(blk * half_f + dep * half_d + s * n, n), n), pl.ds(hw, hw)]

    def w_half(kind):
        return wu.at[head(hq), head(half_f)] if kind == 0 else wd.at[head(half_d), head(hw)]

    def w_own(kind):
        if kind == 0:
            return wu.at[pl.ds(pl.multiple_of(b * hw, hw), hw), head(half_f)]
        return wd.at[pl.ds(pl.multiple_of(b * half_f, half_f), half_f), head(hw)]

    def w_x(kind, s):
        n = half_rows[kind] // SUBS
        src = w_srcs[kind].at[pl.ds(pl.multiple_of(d * half_rows[kind] + s * n, n), n), :]
        return send(src, w_cols(kind, 1 - b, d, s), wx_s.at[kind], wx_r.at[kind, s], 'col')

    def w_y(kind, s):
        return send(w_cols(kind, b, d, s), w_cols(kind, b, d, s), wy_s.at[kind], wy_r.at[kind, s], 'depth')

    def w_a(kind, s):
        return send(w_cols(kind, b, d, s), w_cols(kind, b, d, s), wa_s.at[kind], wa_r.at[kind, s], 'row')

    def w_b(kind, s):
        return send(w_cols(kind, b, 1 - d, s), w_cols(kind, b, 1 - d, s), wb_s.at[kind], wb_r.at[kind, s], 'row')

    def w_row(kind):
        return send(w_srcs[kind], w_own(kind), wrow_s.at[kind], wrow_r.at[kind], 'row')

    def w_load(kind):
        return local(w_srcs[kind], w_own(kind), out_sem.at[kind])

    def w_cross(kind):
        for s in range(SUBS):
            w_x(kind, s).start()

    def w_forward(kind):
        for s in range(SUBS):
            w_x(kind, s).wait_recv()
            w_y(kind, s).start()
            w_a(kind, s).start()
        for s in range(SUBS):
            w_y(kind, s).wait_recv()
            w_b(kind, s).start()

    def w_arrive(kind):
        for s in range(SUBS):
            w_a(kind, s).wait_recv()
            w_b(kind, s).wait_recv()

    def stream(src, k, q):
        slot = lax.rem(q, RING)
        return send(src.at[rows_of(k), :], land.at[slot], land_s.at[slot], land_r.at[slot], 'col')

    def stream_next(src, k, q):
        @pl.when(q >= RING)
        def _():
            stream(src, k, q).wait_send()
            pl.semaphore_wait(credit, 1)
        stream(src, k, q).start()

    def give(n):
        for _ in range(n):
            pl.semaphore_signal(credit, inc=1, device_id={'col': peer['col']}, device_id_type=MESH)

    gam_at, bet_at = pl.ds(half_f, hw), pl.ds(half_f + hw, hw)
    sm_own = [local(bup_h, bup_s.at[0], ld_sem.at[0, 0]), local(gam_h, smv.at[0, :, gam_at], ld_sem.at[0, 1]),
              local(bet_h, smv.at[0, :, bet_at], ld_sem.at[1, 0]), local(bdn_h, bdn_s, ld_sem.at[1, 1])]
    sm_out = [send(bup_h, bup_s.at[1], sm_s.at[0], sm_r.at[0], 'col'),
              send(gam_h, smv.at[1, :, gam_at], sm_s.at[1], sm_r.at[1], 'col'),
              send(bet_h, smv.at[1, :, bet_at], sm_s.at[2], sm_r.at[2], 'col')]
    for cp in sm_own + sm_out:
        cp.start()
    @pl.when(b == 1)
    def _():
        w_cross(1)

    for kind in range(2):
        w_load(kind).start()
        w_row(kind).start()
    stream(x_h, theirs0, 0).start()
    stream(dy_h, theirs0, 1).start()
    w_cross(0)

    @pl.when(b == 0)
    def _():
        w_cross(1)

    stream(x_h, theirs0 + 1, 2).start()
    stream(dy_h, theirs0 + 1, 3).start()

    acc_d[...] = jnp.zeros_like(acc_d)
    acc_u[...] = jnp.zeros_like(acc_u)
    bup8[...] = jnp.zeros_like(bup8)
    gb8[...] = jnp.zeros_like(gb8)
    for cp in sm_own:
        cp.wait()

    def load(n):
        s = odd(n)
        rs = rows_of(chunk_at(n))
        return (local(x_h.at[rs, :], own.at[s], ld_sem.at[0, s]), local(dy_h.at[rs, :], aux.at[s], ld_sem.at[1, s]))

    for cp in load(0):
        cp.start()
    for kind in range(2):
        w_load(kind).wait()
        w_row(kind).wait()

    @pl.when(b == 0)
    def _():
        w_forward(1)

    @pl.when(b == 1)
    def _():
        w_arrive(1)

    def w_rest():
        w_forward(0)

        @pl.when(b == 1)
        def _():
            w_forward(1)

        @pl.when(b == 0)
        def _():
            w_arrive(1)

        w_arrive(0)
        for kind in range(2):
            for sems in (wx_s, wy_s, wa_s, wb_s):
                all_of(w_half(kind), sems.at[kind]).wait()

    for cp in sm_out:
        cp.wait()
    for i in range(half_f // LANES):
        for side in range(2):
            smv[side, :, tile(i, LANES)] = bup_s[side, i:i + 1, :].astype(F32)
    for i in range(hw // LANES):
        smv[0, :, half_f + full + i * LANES:half_f + full + (i + 1) * LANES] = bdn_s[i:i + 1, :].astype(F32)

    def wide(at):
        return cat(smv[0, :, half_f + at:half_f + at + hw], smv[1, :, half_f + at:half_f + at + hw])

    def norm(s, slot, keep):
        gam, bet = wide(0), wide(hw)
        step = 32
        for i in range(M // step):
            rs = tile(i, step)
            xv = cat(own[s, rs, :], land[slot, rs, :]).astype(F32)
            mean = row_sum(xv) * (1.0 / full)
            cen = xv - mean
            istd = lax.rsqrt(row_sum(cen * cen) * (1.0 / full) + LN_EPS)
            xn[rs, :] = (cen * istd * gam + bet).astype(BF16)
            if keep:
                st[i * step // hq, i * step % hq:i * step % hq + step, :] = cat(jnp.broadcast_to(mean, (step, 64)), jnp.broadcast_to(istd, (step, 64)))
        dyv = aux[s]
        trd[...] = dyv.T
        gb8[:, 2 * full:2 * full + hw] += fold8(dyv.astype(F32))

    def write_y(s):
        bdn = smv[0, :, half_f + full:half_f + full + hw]
        yo[...] = (own[s].astype(F32) + yacc[...] + bdn).astype(BF16)

    def y_out(n):
        return local(yo, y_h.at[rows_of(chunk_at(n)), :], out_sem.at[0])

    def dx_out(n):
        return local(dxa, dx_h.at[rows_of(chunk_at(n)), :], out_sem.at[1])

    def dxo_out(n):
        return local(dxb, dxo_h.at[rows_of(n), :], out_sem.at[2])

    def dxl_out(n):
        return local(dxb, dxl_h.at[rows_of(n - (half_n - LATE)), :], out_sem.at[2])

    def saves(n, slot_x, slot_d):
        rs = rows_of(n)
        return (local(land.at[slot_x], xo_h.at[rs, :], sv_sem.at[0]), local(land.at[slot_d], dyo_h.at[rs, :], sv_sem.at[1]),
                local(dxn, dxn_h.at[n], sv_sem.at[2]), local(st, st_h.at[n], sv_sem.at[3]))

    def finish_dx(grads, xs, dys, stats):
        gam = wide(0)
        step = 32
        for i in range(M // step):
            rs = tile(i, step)
            h, hs = i * step // hq, slice(i * step % hq, i * step % hq + step)
            istd = stats[h, hs, 64:65]
            xh = (xs(rs).astype(F32) - stats[h, hs, 0:1]) * istd
            dv = grads(h, hs)
            px = dv * xh
            gb8[:, :full] += fold8(px)
            gb8[:, full:2 * full] += fold8(dv)
            m1 = row_sum(dv * gam) * (1.0 / full)
            m2 = row_sum(px * gam) * (1.0 / full)
            dxv = (dys(rs).astype(F32) + istd * (dv * gam - m1 - xh * m2)).astype(BF16)
            dxa[rs, :] = dxv[:, :hw]
            dxb[rs, :] = dxv[:, hw:]

    def dx_far(m):
        return send(dxo_h.at[rows_of(m), :], dx_h.at[rows_of(mine0 + m), :], dx_s, dx_r, 'col')

    def chunk_mine(n, carry):
        s = odd(n)
        slot_x, slot_d = lax.rem(2 * n, RING), lax.rem(2 * n + 1, RING)

        @pl.when(n < half_n - 2)
        def _():
            stream_next(x_h, theirs0 + n + 2, 2 * n + 4)
            stream_next(dy_h, theirs0 + n + 2, 2 * n + 5)

        @pl.when(n >= half_n - 2)
        def _():
            k = 2 * (n - (half_n - 2))
            stream_next(x_h, mine0 + k, chunks + k)
            stream_next(x_h, mine0 + k + 1, chunks + k + 1)

        for cp in load(n):
            cp.wait()
        for cp in load(n + 1):
            cp.start()

        for m in range(PROMPT):
            @pl.when(n == half_n // 2 + 2 * m - 1)
            def _():
                dx_far(m).start()

        stream(x_h, n, 2 * n).wait_recv()
        stream(dy_h, n, 2 * n + 1).wait_recv()
        save = saves(n, slot_x, slot_d)
        save[0].start()
        save[1].start()

        @pl.when(n > 0)
        def _():
            save[3].wait()

        norm(s, slot_x, True)
        save[3].start()
        trx[...] = xn[...].T

        @pl.when(n > 0)
        def _():
            save[2].wait()

        @pl.when((n > 0) & (n <= PROMPT))
        def _():
            dx_out(n).wait()
            dxo_out(n).wait()

        yacc[...] = jnp.zeros_like(yacc)
        dxn[...] = jnp.zeros_like(dxn)

        def quad(jj, inner):
            @pl.when((n == 0) & (jj == 1))
            def _():
                w_rest()

            cols = [pl.ds(pl.multiple_of((own_tiles * jj + t) * FT, FT), FT) for t in range(own_tiles)]

            def first(t):
                bias = smv[jj, :, tile(t, FT)]
                us[t % 2] = (dot(xn[...], wu[:, cols[t]]) + bias).astype(BF16)
                dyv = cat(aux[s], land[slot_d])
                da_s[t % 2] = dot_t(dyv, wd[cols[t], :]).reshape(2, hq, FT)

            def mid(t):
                a, slope = gelu_and_slope(us[t % 2].astype(F32))
                act[t % 2] = a.astype(BF16)
                du = (da_s[t % 2].reshape(M, FT) * slope).astype(BF16)
                du_s[t % 2] = du
                bup8[:, cols[t]] += fold8(du.astype(F32))

            def last(t):
                yacc[...] += dot(act[t % 2], wd[cols[t], :hw])
                at = t * FT % half_d
                acc_d[jj, t * FT // half_d, :, at:at + FT] += dot(trd[...], act[t % 2])
                dxn[...] += dot_t(du_s[t % 2], wu[:, cols[t]]).reshape(2, hq, full)
                part = dot(trx[...], du_s[t % 2])
                for i in range(4):
                    acc_u[i // 2, i % 2, :, cols[t]] += part[tile(i, hq)]

            first(0)
            first(1)
            mid(0)
            for t in range(own_tiles):
                last(t)
                if t + 2 < own_tiles:
                    first(t + 2)
                if t + 1 < own_tiles:
                    mid(t + 1)
            return inner

        lax.fori_loop(0, 2, quad, 0)

        @pl.when(n > 0)
        def _():
            y_out(n).wait()

        write_y(s)
        y_out(n).start()
        save[2].start()

        @pl.when(n < PROMPT)
        def _():
            finish_dx(lambda h, rs: dxn[h, rs, :],
                      lambda rs: cat(own[s, rs, :], land[slot_x, rs, :]),
                      lambda rs: cat(aux[s, rs, :], land[slot_d, rs, :]), st)
            dx_out(n).start()
            dxo_out(n).start()

        save[0].wait()
        save[1].wait()
        give(2)
        return carry

    lax.fori_loop(0, half_n, chunk_mine, 0)

    order = [*range(own_tiles, tiles), *range(own_tiles)]

    def ru(p):
        return send(acc_u.at[1 - b, :, :, pl.ds(p * FT, FT)], rrow_h.at[p], ru_s, ru_r.at[p], 'row')

    def yu(p):
        return send(acc_u.at[b, 1 - d, :, pl.ds(p * FT, FT)], ryu_h.at[p], yu_s, yu_r.at[p], 'depth')

    def rx(k):
        return send(acc_u.at[b, d, :, pl.ds((own_tiles + k) * FT, FT)], rx_h.at[k], rx_s, rx_r.at[k], 'col')

    gu_rows = pl.ds(pl.multiple_of(d * hq, hq), hq)

    def ag(k):
        ps = pl.ds(k * FT, FT)
        return send(trx.at[pl.ds(k * hq, hq), :], gu_h.at[gu_rows, ps], ag_s, ag_r, 'depth')

    def gu_out(k):
        return local(trx.at[pl.ds(k * hq, hq), :], gu_h.at[gu_rows, pl.ds(k * FT, FT)], out_sem.at[3])

    def row_load(i, p):
        return local(rrow_h.at[p], da_s.at[i % 2], t_sem.at[i % 2, 0])

    for p in order:
        ru(p).start()
    y_out(0).wait()
    for cp in saves(half_n - 1, 0, 0)[2:]:
        cp.wait()
    ru(order[0]).wait_recv()
    row_load(0, order[0]).start()
    for i, p in enumerate(order):
        if i + 1 < tiles:
            ru(order[i + 1]).wait_recv()
            row_load(i + 1, order[i + 1]).start()
        row_load(i, p).wait()
        for h in range(2):
            acc_u[b, h, :, tile(p, FT)] += da_s[i % 2, h]
        yu(p).start()

    def oth_load(k):
        yu(own_tiles + k).wait_recv()
        local(ryu_h.at[own_tiles + k], da_s.at[k % 2, 0], t_sem.at[k % 2, 0]).start()

    def oth_send(k):
        p = own_tiles + k
        local(ryu_h.at[p], da_s.at[k % 2, 0], t_sem.at[k % 2, 0]).wait()
        acc_u[b, d, :, tile(p, FT)] += da_s[k % 2, 0]
        rx(k).start()

    def own_loads(k):
        return (local(ryu_h.at[k], da_s.at[k % 2, 0], t_sem.at[k % 2, 0]),
                local(rx_h.at[k], da_s.at[k % 2, 1], t_sem.at[k % 2, 1]))

    def own_load(k):
        yu(k).wait_recv()
        rx(k).wait_recv()
        for cp in own_loads(k):
            cp.start()

    def own_send(k):
        for cp in own_loads(k):
            cp.wait()
        trx[tile(k, hq), :] = (acc_u[b, d, :, tile(k, FT)] + da_s[k % 2, 0] + da_s[k % 2, 1]).astype(BF16)
        ag(k).start()

    def background(n):
        for k in range(own_tiles):
            @pl.when(n == half_n + 2 + k)
            def _():
                oth_send(k)

            @pl.when(n == half_n + 1 + k)
            def _():
                oth_load(k)

        for k in range(own_tiles - 1):
            @pl.when(n == half_n + 6 + k)
            def _():
                own_send(k)

            @pl.when(n == half_n + 5 + k)
            def _():
                if k >= 1:
                    pass
                own_load(k)

    def chunk_theirs(n, carry):
        s = odd(n)
        q = n + half_n
        slot = lax.rem(q, RING)

        @pl.when(n == half_n)
        def _():
            stream_next(x_h, mine0 + 4, chunks + 4)

        @pl.when(n <= half_n + 2)
        def _():
            stream_next(x_h, mine0 + 5 + (n - half_n), chunks + 5 + (n - half_n))

        background(n)
        for cp in load(n):
            cp.wait()

        @pl.when(n < chunks - 1)
        def _():
            for cp in load(n + 1):
                cp.start()

        stream(x_h, n, q).wait_recv()
        norm(s, slot, False)

        def up(j):
            side, at = divmod(j * FT, half_f)
            us[j % 2] = (dot(xn[...], wu[:, tile(j, FT)]) + smv[side, :, at:at + FT]).astype(BF16)

        def mid(j):
            act[j % 2] = gelu(us[j % 2].astype(F32)).astype(BF16)

        def down(j):
            part = dot(act[j % 2], wd[tile(j, FT), :hw])
            yacc[...] = part if j == 0 else yacc[...] + part
            blk, rest = divmod(j * FT, half_f)
            qt, at = divmod(rest, half_d)
            acc_d[blk, qt, :, at:at + FT] += dot(trd[...], act[j % 2])

        up(0)
        up(1)
        mid(0)
        for j in range(tiles):
            if j + 2 < tiles:
                up(j + 2)
            down(j)
            if j + 1 < tiles:
                mid(j + 1)

        @pl.when(n > half_n)
        def _():
            y_out(n).wait()

        write_y(s)
        y_out(n).start()

        @pl.when(n < half_n + 2)
        def _():
            give(1)
        return carry

    lax.fori_loop(half_n, chunks, chunk_theirs, 0)

    rdn = send(acc_d.at[1 - b], rdn_h, rdn_s, rdn_r, 'row')
    rdn.start()
    k = own_tiles - 1
    own_send(k - 1)
    own_load(k)
    own_send(k)
    for k in range(own_tiles):
        gu_out(k).start()
    all_of(acc_u.at[1 - b], ru_s).wait()

    def load_dx(n):
        s = odd(n)
        rs, ks = rows_of(n), rows_of(mine0 + n)
        return (local(x_h.at[ks, :], own.at[s], ld_sem.at[0, s]), local(dy_h.at[ks, :], aux.at[s], ld_sem.at[1, s]),
                local(xo_h.at[rs, :], land.at[2 * s], ld_sem.at[2, s]), local(dyo_h.at[rs, :], land.at[2 * s + 1], ld_sem.at[3, s]),
                local(dxn_h.at[n], acc_u.at[1 - b, :, :, pl.ds(pl.multiple_of(s * full, full), full)], ld_sem.at[4, s]),
                local(st_h.at[n], da_s.at[s, :, :, head(LANES)], ld_sem.at[5, s]))

    held = 2

    def chunk_dx(n, carry):
        s = odd(n)
        for cp in load_dx(n):
            cp.wait()

        @pl.when(n < half_n - 1)
        def _():
            for cp in load_dx(n + 1):
                cp.start()

        @pl.when(n > PROMPT)
        def _():
            dx_out(n).wait()
            dxo_out(n).wait()

        @pl.when((n > PROMPT) & (n <= half_n - LATE - held))
        def _():
            dx_far(n - 1).start()

        finish_dx(lambda h, rs: acc_u[1 - b, h, rs, pl.ds(pl.multiple_of(s * full, full), full)],
                  lambda rs: cat(own[s, rs, :], land[2 * s, rs, :]),
                  lambda rs: cat(aux[s, rs, :], land[2 * s + 1, rs, :]), da_s.at[s, :, :, head(LANES)])
        dx_out(n).start()

        @pl.when(n < half_n - LATE)
        def _():
            dxo_out(n).start()

        @pl.when(n >= half_n - LATE)
        def _():
            dxl_out(n).start()
        return carry

    for cp in load_dx(PROMPT):
        cp.start()
    lax.fori_loop(PROMPT, 2 * PROMPT, chunk_dx, 0)
    rdn.wait()
    rd_load = local(rdn_h, acc_d.at[1 - b], t_sem.at[0, 0])
    rd_load.start()
    rd_load.wait()
    steps = hw // LANES

    def ydn(i):
        return send(acc_d.at[b, 1 - d, pl.ds(i * LANES, LANES), :], ydn_h.at[i], ydn_s, ydn_r.at[i], 'depth')

    for i in range(steps):
        rs = tile(i, LANES)
        for qt in range(2):
            acc_d[b, qt, rs, :] += acc_d[1 - b, qt, rs, :]
        ydn(i).start()
    lax.fori_loop(2 * PROMPT, half_n, chunk_dx, 0)
    y_out(chunks - 1).wait()
    oth = lambda at, n: [col_sum(ref[:, a:a + n]) for ref, a in at]
    gso[...] = jnp.concatenate(oth(((bup8, half_f),), half_f) + oth(((gb8, hw), (gb8, full + hw)), hw)
                               + [jnp.zeros((1, half_f - full), F32)], axis=1)
    gs_col = send(gso, gsl.at[0], gs_s.at[0], gs_r.at[0], 'col')
    gs_col.start()
    for m in range(half_n - LATE - held, half_n - LATE):
        dx_far(m).start()
    dx_out(half_n - 1).wait()
    dxl_out(half_n - 1).wait()
    gs_col.wait()
    gsp[0] = jnp.concatenate(oth(((bup8, 0),), half_f) + oth(((gb8, 0), (gb8, full), (gb8, 2 * full)), hw)
                             + [jnp.zeros((1, half_f - 3 * hw), F32)], axis=1) + gsl[0]
    gs_row = send(gsp.at[0], gsl.at[1], gs_s.at[1], gs_r.at[1], 'row')
    gs_row.start()
    gs_row.wait()
    gsp[1] = gsp[0] + gsl[1]
    gs_dep = send(gsp.at[1], gsl.at[2], gs_s.at[2], gs_r.at[2], 'depth')
    gs_dep.start()
    for q in range(3 * half_n - RING, 3 * half_n):
        stream(x_h, 0, q).wait_send()
    all_of(acc_u.at[b, 1 - d], yu_s).wait()
    all_of(acc_u.at[b, d, :, pl.ds(half_f, half_f)], rx_s).wait()
    all_of(trx, out_sem.at[3]).wait()
    for i in range(steps):
        ydn(i).wait_recv()
        dn_load = local(ydn_h.at[i], acc_d.at[1 - b, 0, pl.ds(i * LANES, LANES), :], t_sem.at[1, 0])
        dn_load.start()
        dn_load.wait()
        rs = tile(i, LANES)
        for j in range(half_d // LANES):
            cs = tile(j, LANES)
            total = acc_d[b, d, rs, cs] + acc_d[1 - b, 0, rs, cs]
            us[j * LANES // M, j * LANES % M:j * LANES % M + LANES, rs] = total.T.astype(BF16)
    gd_out = [local(us.at[i], gd_h.at[pl.ds(i * M, M), :], t_sem.at[i, 1]) for i in range(2)]
    for cp in gd_out:
        cp.start()
    gs_dep.wait()
    gsp[0] = gsp[1] + gsl[2]
    gs_out = local(gsp.at[0], gs_h, out_sem.at[0])
    gs_out.start()
    all_of(acc_d.at[b, 1 - d], ydn_s).wait()
    for sem in (ag_s, ag_r):
        all_of(trx, sem).wait()
    sent = dxo_h.at[head((half_n - LATE) * M), :]
    for sem in (dx_s, dx_r):
        all_of(sent, sem).wait()
    for cp in gd_out:
        cp.wait()
    gs_out.wait()


def finish_kernel(y_in, dx_in, gwu_in, gd, gs, y, dx, gwu, gwd, gbup, ggam, gbet, gbdn, big, small, sums, in_sem, out_sem):
    rows, hw = y.shape
    half_f = gwd.shape[0]
    d = lax.axis_index('depth')
    n = rows // COPIES
    ins, outs = [], []

    def move(src, buf, *dst):
        ins.append(pltpu.make_async_copy(src, buf, in_sem.at[len(ins)]))
        outs.append([pltpu.make_async_copy(buf, to, out_sem) for to in dst])

    for i in range(COPIES):
        rs = pl.ds(i * n, n)
        move(y_in.at[rs], big.at[0, rs], y.at[rs])
        move(dx_in.at[rs], big.at[1, rs], dx.at[rs])
    move(gwu_in, small.at[:, head(half_f)], gwu)
    move(gd, big.at[2, head(half_f // 2)], gwd.at[pl.ds(pl.multiple_of(d * (half_f // 2), half_f // 2), half_f // 2)])
    parts = [(0, half_f, gbup), (half_f, hw, ggam), (half_f + hw, hw, gbet), (half_f + 2 * hw, hw, gbdn)]
    move(gs, sums)
    outs[-1] = [pltpu.make_async_copy(sums.at[:, pl.ds(a, w)], dst, out_sem) for a, w, dst in parts]
    for cp in ins:
        cp.start()
    for cp, tos in zip(ins, outs):
        cp.wait()
        for to in tos:
            to.start()
    for tos in outs:
        for to in tos:
            to.wait()


def solution(mesh):
    tok_spec = P(('dp', 'depth', 'row'), 'col')
    vec_spec = P('col')
    mat_spec = P('row', 'col')
    grad_vec = P(('dp', 'col'))
    grad_mat = P(('dp', 'row'), 'col')
    swap = ((0, 1), (1, 0))

    def local_pass(x, gamma, beta, w_up, b_up, w_down, b_down, dy):
        rows, hw = x.shape
        half_f = b_up.shape[0]
        full_f, full, hq = 2 * half_f, 2 * hw, hw // 2
        chunks = rows // M
        late = LATE * M
        hbm = pl.BlockSpec(memory_space=pltpu.HBM)
        sds = jax.ShapeDtypeStruct
        V, D = pltpu.VMEM, pltpu.SemaphoreType.DMA
        D2, D3, D4, D2S = D((2,)), D((3,)), D((4,)), D((2, SUBS))
        tiles, own_tiles = full_f // FT, half_f // FT
        outs = [
            sds((rows, hw), BF16), sds((rows, hw), BF16), sds((late, hw), BF16), sds((1, full_f), F32), sds((hw, half_f), BF16),
            sds((half_f // 2, hw), BF16),
            sds((rows // 2, hw), BF16), sds((tiles, 2, hq, FT), F32), sds((tiles, hq, FT), F32), sds((own_tiles, hq, FT), F32),
            sds((2, hw, half_f // 2), F32), sds((hw // LANES, LANES, half_f // 2), F32),
            sds((rows // 2, hw), BF16), sds((rows // 2, hw), BF16), sds((chunks // 2, 2, hq, full), F32), sds((chunks // 2, 2, hq, LANES), F32),
        ]
        scratch = [
            V((full, full_f), BF16), V((full_f, full), BF16), V((2, 2, hw, half_f // 2), F32), V((2, 2, hq, full_f), F32),
            V((2, M, hw), BF16), V((RING, M, hw), BF16), V((2, M, hw), BF16), V((M, full), BF16), V((full, M), BF16), V((hw, M), BF16),
            V((2, hq, LANES), F32), V((2, M, FT), BF16), V((2, 2, hq, FT), F32), V((2, M, FT), BF16), V((2, M, FT), BF16),
            V((M, hw), F32), V((2, hq, full), F32), V((M, hw), BF16), V((M, hw), BF16), V((M, hw), BF16),
            V((8, full_f), F32), V((8, 2 * full + hw), F32), V((2, 1, full_f), F32), V((2, half_f // LANES, LANES), BF16), V((hw // LANES, LANES), BF16),
            V((1, full_f), F32), V((2, 1, full_f), F32), V((3, 1, full_f), F32),
            D2, D2, D2, D2S, D2, D2S, D2, D2S, D2, D2S, D3, D3,
            D((RING,)), D((RING,)), D((6, 2)), D4, D4, D((2, 2)), D(()), D((tiles,)), D(()), D((tiles,)), D(()), D((own_tiles,)),
            D(()), D(()), D(()), D(()), D(()), D((hw // LANES,)), D(()), D(()), D3, D3, pltpu.SemaphoreType.REGULAR,
        ]
        res = pl.pallas_call(
            kernel,
            out_shape=outs,
            in_specs=[hbm] * 8,
            out_specs=[hbm] * len(outs),
            scratch_shapes=scratch,
            compiler_params=pltpu.CompilerParams(
                collective_id=0, has_side_effects=True, vmem_limit_bytes=67043328),
            cost_estimate=pl.CostEstimate(flops=14 * rows * full * full_f, bytes_accessed=2 ** 27, transcendentals=rows * full_f),
            name='mlp_block',
        )(x, dy, w_up, w_down, b_up.reshape(-1, LANES), gamma.reshape(1, -1), beta.reshape(1, -1), b_down.reshape(-1, LANES))
        y, dx, dxl, gs, gwu, gd = res[:6]
        gd_far = lax.ppermute(gd, 'depth', swap)
        dx_far = lax.ppermute(dxl, 'col', swap)
        moves = 2 * COPIES + 3
        y, dx, gwu, gwd, gbup, ggam, gbet, gbdn = pl.pallas_call(
            finish_kernel,
            out_shape=[sds((rows, hw), BF16), sds((rows, hw), BF16), sds((hw, half_f), BF16), sds((half_f, hw), BF16),
                       sds((1, half_f), F32), sds((1, hw), F32), sds((1, hw), F32), sds((1, hw), F32)],
            in_specs=[hbm] * 5,
            out_specs=[hbm] * 8,
            scratch_shapes=[V((3, rows, hw), BF16), V((hw, half_f), BF16), V((1, full_f), F32), D((moves,)), D(())],
            compiler_params=pltpu.CompilerParams(vmem_limit_bytes=62000000),
            cost_estimate=pl.CostEstimate(flops=2 ** 33, bytes_accessed=42 * 2 ** 20, transcendentals=0),
            name='finish',
        )(y, dx, gwu, gd, gs)
        gwd = lax.dynamic_update_slice(gwd, gd_far, ((1 - lax.axis_index('depth')) * (half_f // 2), 0))
        dx = lax.dynamic_update_slice(dx, dx_far, ((1 - lax.axis_index('col')) * (rows // 2) + rows // 2 - late, 0))
        return y, dx, ggam.reshape(-1), gbet.reshape(-1), gwu, gbup.reshape(-1), gwd, gbdn.reshape(-1)

    return jax.shard_map(
        local_pass,
        mesh=mesh,
        in_specs=(tok_spec, vec_spec, vec_spec, mat_spec, vec_spec, mat_spec, vec_spec, tok_spec),
        out_specs=(tok_spec, tok_spec, grad_vec, grad_vec, grad_mat, grad_vec, grad_mat, grad_vec),
        check_vma=False,
    )
```

```python
import jax
import jax.numpy as jnp
from jax import lax
from jax.experimental import pallas as pl
from jax.experimental.pallas import tpu as pltpu
from jax.sharding import PartitionSpec as P

LN_EPS = 1e-5
C0 = 0.7978845608
C1 = C0 * 0.044715
M = 512
FT = 512
SUBS = 4
RING = 6
LATE = 2
PROMPT = 2
COPIES = 4
LANES = 128
BF16, F32 = jnp.bfloat16, jnp.float32
MESH = pl.DeviceIdType.MESH


def dot(lhs, rhs, rhs_dim=0):
    return lax.dot_general(lhs, rhs, (((1,), (rhs_dim,)), ((), ())), preferred_element_type=F32)


def dot_t(lhs, rhs):
    return dot(lhs, rhs, 1)


def odd(n):
    return lax.rem(n, 2)


def cat(*parts):
    return jnp.concatenate(parts, axis=1)


def row_sum(v):
    return jnp.sum(v, axis=1, keepdims=True)


def col_sum(v):
    return jnp.sum(v, axis=0, keepdims=True)


def head(n):
    return pl.ds(0, n)


def tile(i, n):
    return slice(i * n, (i + 1) * n)


def gelu(v):
    t = jnp.tanh(v * (C1 * (v * v) + C0))
    h = 0.5 * v
    return h * t + h


def gelu_and_slope(v):
    v2 = v * v
    t = jnp.tanh(v * (C1 * v2 + C0))
    h = 0.5 * v
    slope = (v * (1.0 - t * t)) * (1.5 * C1 * v2 + 0.5 * C0) + (0.5 * t + 0.5)
    return h * t + h, slope


def fold8(v):
    return jnp.sum(v.reshape(v.shape[0] // 8, 8, v.shape[1]), axis=0)


def kernel(x_h, dy_h, wu_h, wd_h, bup_h, gam_h, bet_h, bdn_h,
           y_h, dx_h, dxl_h, gs_h, gu_h, gd_h, dxo_h, rrow_h, ryu_h, rx_h, rdn_h, ydn_h, xo_h, dyo_h, dxn_h, st_h,
           wu, wd, acc_d, acc_u, own, land, aux, xn, trx, trd, st, us, da_s, act, du_s, yacc, dxn, yo, dxa, dxb,
           bup8, gb8, smv, bup_s, bdn_s, gso, gsp, gsl,
           wrow_s, wrow_r, wx_s, wx_r, wy_s, wy_r, wa_s, wa_r, wb_s, wb_r, sm_s, sm_r,
           land_s, land_r, ld_sem, out_sem, sv_sem, t_sem, ru_s, ru_r, yu_s, yu_r, rx_s, rx_r, ag_s, ag_r, rdn_s, rdn_r,
           ydn_s, ydn_r, dx_s, dx_r, gs_s, gs_r, credit):
    chunks = x_h.shape[0] // M
    half_n = chunks // 2
    half_f = wu_h.shape[1]
    hw = x_h.shape[1]
    full = 2 * hw
    hq = hw // 2
    half_d = half_f // 2
    tiles = 2 * half_f // FT
    own_tiles = tiles // 2
    c, r, d = lax.axis_index('col'), lax.axis_index('row'), lax.axis_index('depth')
    b = lax.rem(r + c, 2)
    peer = {'col': 1 - c, 'row': 1 - r, 'depth': 1 - d}
    mine0, theirs0 = c * half_n, (1 - c) * half_n

    def send(src, dst, s_sem, r_sem, axis):
        return pltpu.make_async_remote_copy(src_ref=src, dst_ref=dst, send_sem=s_sem, recv_sem=r_sem,
                                            device_id={axis: peer[axis]}, device_id_type=MESH)

    def local(src, dst, sem):
        return pltpu.make_async_copy(src, dst, sem)

    def all_of(ref, sem):
        return pltpu.make_async_copy(ref, ref, sem)

    def rows_of(k):
        return pl.ds(pl.multiple_of(k * M, M), M)

    def chunk_at(n):
        return lax.rem(mine0 + n, chunks)

    bar = pltpu.get_barrier_semaphore()
    for axis in ('col', 'row', 'depth'):
        pl.semaphore_signal(bar, inc=1, device_id={axis: peer[axis]}, device_id_type=MESH)
    pl.semaphore_wait(bar, 3)

    half_rows = (hq, half_d)
    w_srcs = (wu_h, wd_h)

    def w_cols(kind, blk, dep, s):
        n = half_rows[kind] // SUBS
        if kind == 0:
            return wu.at[pl.ds(pl.multiple_of(blk * hw + dep * hq + s * n, n), n), pl.ds(half_f, half_f)]
        return wd.at[pl.ds(pl.multiple_of(blk * half_f + dep * half_d + s * n, n), n), pl.ds(hw, hw)]

    def w_half(kind):
        return wu.at[head(hq), head(half_f)] if kind == 0 else wd.at[head(half_d), head(hw)]

    def w_own(kind):
        if kind == 0:
            return wu.at[pl.ds(pl.multiple_of(b * hw, hw), hw), head(half_f)]
        return wd.at[pl.ds(pl.multiple_of(b * half_f, half_f), half_f), head(hw)]

    def w_x(kind, s):
        n = half_rows[kind] // SUBS
        src = w_srcs[kind].at[pl.ds(pl.multiple_of(d * half_rows[kind] + s * n, n), n), :]
        return send(src, w_cols(kind, 1 - b, d, s), wx_s.at[kind], wx_r.at[kind, s], 'col')

    def w_y(kind, s):
        return send(w_cols(kind, b, d, s), w_cols(kind, b, d, s), wy_s.at[kind], wy_r.at[kind, s], 'depth')

    def w_a(kind, s):
        return send(w_cols(kind, b, d, s), w_cols(kind, b, d, s), wa_s.at[kind], wa_r.at[kind, s], 'row')

    def w_b(kind, s):
        return send(w_cols(kind, b, 1 - d, s), w_cols(kind, b, 1 - d, s), wb_s.at[kind], wb_r.at[kind, s], 'row')

    def w_row(kind):
        return send(w_srcs[kind], w_own(kind), wrow_s.at[kind], wrow_r.at[kind], 'row')

    def w_load(kind):
        return local(w_srcs[kind], w_own(kind), out_sem.at[kind])

    def w_cross(kind):
        for s in range(SUBS):
            w_x(kind, s).start()

    def w_forward_x(kind):
        for s in range(SUBS):
            w_x(kind, s).wait_recv()
            w_y(kind, s).start()
            w_a(kind, s).start()

    def w_forward_y(kind):
        for s in range(SUBS):
            w_y(kind, s).wait_recv()
            w_b(kind, s).start()

    def w_arrive(kind):
        for s in range(SUBS):
            w_a(kind, s).wait_recv()
            w_b(kind, s).wait_recv()

    def stream(src, k, q):
        slot = lax.rem(q, RING)
        return send(src.at[rows_of(k), :], land.at[slot], land_s.at[slot], land_r.at[slot], 'col')

    def stream_next(src, k, q):
        @pl.when(q >= RING)
        def _():
            stream(src, k, q).wait_send()
            pl.semaphore_wait(credit, 1)
        stream(src, k, q).start()

    def give(n):
        for _ in range(n):
            pl.semaphore_signal(credit, inc=1, device_id={'col': peer['col']}, device_id_type=MESH)

    gam_at, bet_at = pl.ds(half_f, hw), pl.ds(half_f + hw, hw)
    sm_own = [local(bup_h, bup_s.at[0], ld_sem.at[0, 0]), local(gam_h, smv.at[0, :, gam_at], ld_sem.at[0, 1]),
              local(bet_h, smv.at[0, :, bet_at], ld_sem.at[1, 0]), local(bdn_h, bdn_s, ld_sem.at[1, 1])]
    sm_out = [send(bup_h, bup_s.at[1], sm_s.at[0], sm_r.at[0], 'col'),
              send(gam_h, smv.at[1, :, gam_at], sm_s.at[1], sm_r.at[1], 'col'),
              send(bet_h, smv.at[1, :, bet_at], sm_s.at[2], sm_r.at[2], 'col')]
    for cp in sm_own + sm_out:
        cp.start()
    @pl.when(b == 1)
    def _():
        w_cross(1)

    for kind in range(2):
        w_load(kind).start()
        w_row(kind).start()
    stream(x_h, theirs0, 0).start()
    stream(dy_h, theirs0, 1).start()
    w_cross(0)

    @pl.when(b == 0)
    def _():
        w_cross(1)

    stream(x_h, theirs0 + 1, 2).start()
    stream(dy_h, theirs0 + 1, 3).start()

    acc_d[...] = jnp.zeros_like(acc_d)
    acc_u[...] = jnp.zeros_like(acc_u)
    bup8[...] = jnp.zeros_like(bup8)
    gb8[...] = jnp.zeros_like(gb8)
    for cp in sm_own:
        cp.wait()

    def load(n):
        s = odd(n)
        rs = rows_of(chunk_at(n))
        return (local(x_h.at[rs, :], own.at[s], ld_sem.at[0, s]), local(dy_h.at[rs, :], aux.at[s], ld_sem.at[1, s]))

    for cp in load(0):
        cp.start()
    for kind in range(2):
        w_load(kind).wait()
        w_row(kind).wait()

    @pl.when(b == 0)
    def _():
        w_forward_x(1)
        w_forward_y(1)

    @pl.when(b == 1)
    def _():
        w_arrive(1)

    def w_rest():
        w_forward_x(0)

        @pl.when(b == 1)
        def _():
            w_forward_x(1)

        w_forward_y(0)

        @pl.when(b == 1)
        def _():
            w_forward_y(1)

        @pl.when(b == 0)
        def _():
            w_arrive(1)

        w_arrive(0)
        for kind in range(2):
            for sems in (wx_s, wy_s, wa_s, wb_s):
                all_of(w_half(kind), sems.at[kind]).wait()

    for cp in sm_out:
        cp.wait()
    for i in range(half_f // LANES):
        for side in range(2):
            smv[side, :, tile(i, LANES)] = bup_s[side, i:i + 1, :].astype(F32)
    for i in range(hw // LANES):
        smv[0, :, half_f + full + i * LANES:half_f + full + (i + 1) * LANES] = bdn_s[i:i + 1, :].astype(F32)

    def wide(at):
        return cat(smv[0, :, half_f + at:half_f + at + hw], smv[1, :, half_f + at:half_f + at + hw])

    def norm(s, slot, keep):
        gam, bet = wide(0), wide(hw)
        step = 32
        for i in range(M // step):
            rs = tile(i, step)
            xv = cat(own[s, rs, :], land[slot, rs, :]).astype(F32)
            mean = row_sum(xv) * (1.0 / full)
            cen = xv - mean
            istd = lax.rsqrt(row_sum(cen * cen) * (1.0 / full) + LN_EPS)
            xn[rs, :] = (cen * istd * gam + bet).astype(BF16)
            if keep:
                st[i * step // hq, i * step % hq:i * step % hq + step, :] = cat(jnp.broadcast_to(mean, (step, 64)), jnp.broadcast_to(istd, (step, 64)))
        dyv = aux[s]
        trd[...] = dyv.T
        gb8[:, 2 * full:2 * full + hw] += fold8(dyv.astype(F32))

    def write_y(s):
        bdn = smv[0, :, half_f + full:half_f + full + hw]
        yo[...] = (own[s].astype(F32) + yacc[...] + bdn).astype(BF16)

    def y_out(n):
        return local(yo, y_h.at[rows_of(chunk_at(n)), :], out_sem.at[0])

    def dx_out(n):
        return local(dxa, dx_h.at[rows_of(chunk_at(n)), :], out_sem.at[1])

    def dxo_out(n):
        return local(dxb, dxo_h.at[rows_of(n), :], out_sem.at[2])

    def dxl_out(n):
        return local(dxb, dxl_h.at[rows_of(n - (half_n - LATE)), :], out_sem.at[2])

    def saves(n, slot_x, slot_d):
        rs = rows_of(n)
        return (local(land.at[slot_x], xo_h.at[rs, :], sv_sem.at[0]), local(land.at[slot_d], dyo_h.at[rs, :], sv_sem.at[1]),
                local(dxn, dxn_h.at[n], sv_sem.at[2]), local(st, st_h.at[n], sv_sem.at[3]))

    def finish_dx(grads, xs, dys, stats):
        gam = wide(0)
        step = 32
        for i in range(M // step):
            rs = tile(i, step)
            h, hs = i * step // hq, slice(i * step % hq, i * step % hq + step)
            istd = stats[h, hs, 64:65]
            xh = (xs(rs).astype(F32) - stats[h, hs, 0:1]) * istd
            dv = grads(h, hs)
            px = dv * xh
            gb8[:, :full] += fold8(px)
            gb8[:, full:2 * full] += fold8(dv)
            m1 = row_sum(dv * gam) * (1.0 / full)
            m2 = row_sum(px * gam) * (1.0 / full)
            dxv = (dys(rs).astype(F32) + istd * (dv * gam - m1 - xh * m2)).astype(BF16)
            dxa[rs, :] = dxv[:, :hw]
            dxb[rs, :] = dxv[:, hw:]

    def dx_far(m):
        return send(dxo_h.at[rows_of(m), :], dx_h.at[rows_of(mine0 + m), :], dx_s, dx_r, 'col')

    def chunk_mine(n, carry):
        s = odd(n)
        slot_x, slot_d = lax.rem(2 * n, RING), lax.rem(2 * n + 1, RING)

        for cp in load(n):
            cp.wait()
        for cp in load(n + 1):
            cp.start()

        for m in range(PROMPT):
            @pl.when(n == half_n // 2 + 2 * m - 1)
            def _():
                dx_far(m).start()

        stream(x_h, n, 2 * n).wait_recv()
        stream(dy_h, n, 2 * n + 1).wait_recv()
        save = saves(n, slot_x, slot_d)
        save[0].start()
        save[1].start()

        @pl.when(n > 0)
        def _():
            save[3].wait()

        norm(s, slot_x, True)
        save[3].start()
        trx[...] = xn[...].T

        @pl.when(n > 0)
        def _():
            save[2].wait()

        @pl.when((n > 0) & (n <= PROMPT))
        def _():
            dx_out(n).wait()
            dxo_out(n).wait()

        yacc[...] = jnp.zeros_like(yacc)
        dxn[...] = jnp.zeros_like(dxn)

        def quad(jj, inner):
            @pl.when((n == 0) & (jj == 1))
            def _():
                w_rest()

            @pl.when((n < half_n - 2) & (jj == 1))
            def _():
                stream_next(x_h, theirs0 + n + 2, 2 * n + 4)
                stream_next(dy_h, theirs0 + n + 2, 2 * n + 5)

            @pl.when((n >= half_n - 2) & (jj == 1))
            def _():
                k = 2 * (n - (half_n - 2))
                stream_next(x_h, mine0 + k, chunks + k)
                stream_next(x_h, mine0 + k + 1, chunks + k + 1)

            cols = [pl.ds(pl.multiple_of((own_tiles * jj + t) * FT, FT), FT) for t in range(own_tiles)]

            def first(t):
                bias = smv[jj, :, tile(t, FT)]
                us[t % 2] = (dot(xn[...], wu[:, cols[t]]) + bias).astype(BF16)
                dyv = cat(aux[s], land[slot_d])
                da_s[t % 2] = dot_t(dyv, wd[cols[t], :]).reshape(2, hq, FT)

            def mid(t):
                a, slope = gelu_and_slope(us[t % 2].astype(F32))
                act[t % 2] = a.astype(BF16)
                du = (da_s[t % 2].reshape(M, FT) * slope).astype(BF16)
                du_s[t % 2] = du
                bup8[:, cols[t]] += fold8(du.astype(F32))

            def last(t):
                yacc[...] += dot(act[t % 2], wd[cols[t], :hw])
                at = t * FT % half_d
                acc_d[jj, t * FT // half_d, :, at:at + FT] += dot(trd[...], act[t % 2])
                dxn[...] += dot_t(du_s[t % 2], wu[:, cols[t]]).reshape(2, hq, full)
                part = dot(trx[...], du_s[t % 2])
                for i in range(4):
                    acc_u[i // 2, i % 2, :, cols[t]] += part[tile(i, hq)]

            first(0)
            first(1)
            mid(0)
            for t in range(own_tiles):
                last(t)
                if t + 2 < own_tiles:
                    first(t + 2)
                if t + 1 < own_tiles:
                    mid(t + 1)
            return inner

        lax.fori_loop(0, 2, quad, 0)

        @pl.when(n > 0)
        def _():
            y_out(n).wait()

        write_y(s)
        y_out(n).start()
        save[2].start()

        @pl.when(n < PROMPT)
        def _():
            finish_dx(lambda h, rs: dxn[h, rs, :],
                      lambda rs: cat(own[s, rs, :], land[slot_x, rs, :]),
                      lambda rs: cat(aux[s, rs, :], land[slot_d, rs, :]), st)
            dx_out(n).start()
            dxo_out(n).start()

        save[0].wait()
        save[1].wait()
        give(2)
        return carry

    lax.fori_loop(0, half_n, chunk_mine, 0)

    order = [*range(own_tiles, tiles), *range(own_tiles)]

    def ru(p):
        return send(acc_u.at[1 - b, :, :, pl.ds(p * FT, FT)], rrow_h.at[p], ru_s, ru_r.at[p], 'row')

    def yu(p):
        return send(acc_u.at[b, 1 - d, :, pl.ds(p * FT, FT)], ryu_h.at[p], yu_s, yu_r.at[p], 'depth')

    def rx(k):
        return send(acc_u.at[b, d, :, pl.ds((own_tiles + k) * FT, FT)], rx_h.at[k], rx_s, rx_r.at[k], 'col')

    gu_rows = pl.ds(pl.multiple_of(d * hq, hq), hq)

    def ag(k):
        ps = pl.ds(k * FT, FT)
        return send(trx.at[pl.ds(k * hq, hq), :], gu_h.at[gu_rows, ps], ag_s, ag_r, 'depth')

    def gu_out(k):
        return local(trx.at[pl.ds(k * hq, hq), :], gu_h.at[gu_rows, pl.ds(k * FT, FT)], out_sem.at[3])

    def row_load(i, p):
        return local(rrow_h.at[p], da_s.at[i % 2], t_sem.at[i % 2, 0])

    for p in order:
        ru(p).start()
    y_out(0).wait()
    for cp in saves(half_n - 1, 0, 0)[2:]:
        cp.wait()
    ru(order[0]).wait_recv()
    row_load(0, order[0]).start()
    for i, p in enumerate(order):
        if i + 1 < tiles:
            ru(order[i + 1]).wait_recv()
            row_load(i + 1, order[i + 1]).start()
        row_load(i, p).wait()
        for h in range(2):
            acc_u[b, h, :, tile(p, FT)] += da_s[i % 2, h]
        yu(p).start()

    def oth_load(k):
        yu(own_tiles + k).wait_recv()
        local(ryu_h.at[own_tiles + k], da_s.at[k % 2, 0], t_sem.at[k % 2, 0]).start()

    def oth_send(k):
        p = own_tiles + k
        local(ryu_h.at[p], da_s.at[k % 2, 0], t_sem.at[k % 2, 0]).wait()
        acc_u[b, d, :, tile(p, FT)] += da_s[k % 2, 0]
        rx(k).start()

    def own_loads(k):
        return (local(ryu_h.at[k], da_s.at[k % 2, 0], t_sem.at[k % 2, 0]),
                local(rx_h.at[k], da_s.at[k % 2, 1], t_sem.at[k % 2, 1]))

    def own_load(k):
        yu(k).wait_recv()
        rx(k).wait_recv()
        for cp in own_loads(k):
            cp.start()

    def own_send(k):
        for cp in own_loads(k):
            cp.wait()
        trx[tile(k, hq), :] = (acc_u[b, d, :, tile(k, FT)] + da_s[k % 2, 0] + da_s[k % 2, 1]).astype(BF16)
        ag(k).start()

    def background(n):
        for k in range(own_tiles):
            @pl.when(n == half_n + 2 + k)
            def _():
                oth_send(k)

            @pl.when(n == half_n + 1 + k)
            def _():
                oth_load(k)

        for k in range(own_tiles - 1):
            @pl.when(n == half_n + 6 + k)
            def _():
                own_send(k)

            @pl.when(n == half_n + 5 + k)
            def _():
                if k >= 1:
                    pass
                own_load(k)

    def chunk_theirs(n, carry):
        s = odd(n)
        q = n + half_n
        slot = lax.rem(q, RING)

        @pl.when(n == half_n)
        def _():
            stream_next(x_h, mine0 + 4, chunks + 4)

        @pl.when(n <= half_n + 2)
        def _():
            stream_next(x_h, mine0 + 5 + (n - half_n), chunks + 5 + (n - half_n))

        background(n)
        for cp in load(n):
            cp.wait()

        @pl.when(n < chunks - 1)
        def _():
            for cp in load(n + 1):
                cp.start()

        stream(x_h, n, q).wait_recv()
        norm(s, slot, False)

        def up(j):
            side, at = divmod(j * FT, half_f)
            us[j % 2] = (dot(xn[...], wu[:, tile(j, FT)]) + smv[side, :, at:at + FT]).astype(BF16)

        def mid(j):
            act[j % 2] = gelu(us[j % 2].astype(F32)).astype(BF16)

        def down(j):
            part = dot(act[j % 2], wd[tile(j, FT), :hw])
            yacc[...] = part if j == 0 else yacc[...] + part
            blk, rest = divmod(j * FT, half_f)
            qt, at = divmod(rest, half_d)
            acc_d[blk, qt, :, at:at + FT] += dot(trd[...], act[j % 2])

        up(0)
        up(1)
        mid(0)
        for j in range(tiles):
            if j + 2 < tiles:
                up(j + 2)
            down(j)
            if j + 1 < tiles:
                mid(j + 1)

        @pl.when(n > half_n)
        def _():
            y_out(n).wait()

        write_y(s)
        y_out(n).start()

        @pl.when(n < half_n + 2)
        def _():
            give(1)
        return carry

    lax.fori_loop(half_n, chunks, chunk_theirs, 0)

    rdn = send(acc_d.at[1 - b], rdn_h, rdn_s, rdn_r, 'row')
    rdn.start()
    k = own_tiles - 1
    own_send(k - 1)
    own_load(k)
    own_send(k)
    for k in range(own_tiles):
        gu_out(k).start()
    all_of(acc_u.at[1 - b], ru_s).wait()

    def load_dx(n):
        s = odd(n)
        rs, ks = rows_of(n), rows_of(mine0 + n)
        return (local(x_h.at[ks, :], own.at[s], ld_sem.at[0, s]), local(dy_h.at[ks, :], aux.at[s], ld_sem.at[1, s]),
                local(xo_h.at[rs, :], land.at[2 * s], ld_sem.at[2, s]), local(dyo_h.at[rs, :], land.at[2 * s + 1], ld_sem.at[3, s]),
                local(dxn_h.at[n], acc_u.at[1 - b, :, :, pl.ds(pl.multiple_of(s * full, full), full)], ld_sem.at[4, s]),
                local(st_h.at[n], da_s.at[s, :, :, head(LANES)], ld_sem.at[5, s]))

    held = 2

    def chunk_dx(n, carry):
        s = odd(n)
        for cp in load_dx(n):
            cp.wait()

        @pl.when(n < half_n - 1)
        def _():
            for cp in load_dx(n + 1):
                cp.start()

        @pl.when(n > PROMPT)
        def _():
            dx_out(n).wait()
            dxo_out(n).wait()

        @pl.when((n > PROMPT) & (n <= half_n - LATE - held))
        def _():
            dx_far(n - 1).start()

        finish_dx(lambda h, rs: acc_u[1 - b, h, rs, pl.ds(pl.multiple_of(s * full, full), full)],
                  lambda rs: cat(own[s, rs, :], land[2 * s, rs, :]),
                  lambda rs: cat(aux[s, rs, :], land[2 * s + 1, rs, :]), da_s.at[s, :, :, head(LANES)])
        dx_out(n).start()

        @pl.when(n < half_n - LATE)
        def _():
            dxo_out(n).start()

        @pl.when(n >= half_n - LATE)
        def _():
            dxl_out(n).start()
        return carry

    for cp in load_dx(PROMPT):
        cp.start()
    lax.fori_loop(PROMPT, 2 * PROMPT, chunk_dx, 0)
    rdn.wait()
    rd_load = local(rdn_h, acc_d.at[1 - b], t_sem.at[0, 0])
    rd_load.start()
    rd_load.wait()
    steps = hw // LANES

    def ydn(i):
        return send(acc_d.at[b, 1 - d, pl.ds(i * LANES, LANES), :], ydn_h.at[i], ydn_s, ydn_r.at[i], 'depth')

    for i in range(steps):
        rs = tile(i, LANES)
        for qt in range(2):
            acc_d[b, qt, rs, :] += acc_d[1 - b, qt, rs, :]
        ydn(i).start()
    lax.fori_loop(2 * PROMPT, half_n, chunk_dx, 0)
    y_out(chunks - 1).wait()
    oth = lambda at, n: [col_sum(ref[:, a:a + n]) for ref, a in at]
    gso[...] = jnp.concatenate(oth(((bup8, half_f),), half_f) + oth(((gb8, hw), (gb8, full + hw)), hw)
                               + [jnp.zeros((1, half_f - full), F32)], axis=1)
    gs_col = send(gso, gsl.at[0], gs_s.at[0], gs_r.at[0], 'col')
    gs_col.start()
    for m in range(half_n - LATE - held, half_n - LATE):
        dx_far(m).start()
    dx_out(half_n - 1).wait()
    dxl_out(half_n - 1).wait()
    gs_col.wait()
    gsp[0] = jnp.concatenate(oth(((bup8, 0),), half_f) + oth(((gb8, 0), (gb8, full), (gb8, 2 * full)), hw)
                             + [jnp.zeros((1, half_f - 3 * hw), F32)], axis=1) + gsl[0]
    gs_row = send(gsp.at[0], gsl.at[1], gs_s.at[1], gs_r.at[1], 'row')
    gs_row.start()
    gs_row.wait()
    gsp[1] = gsp[0] + gsl[1]
    gs_dep = send(gsp.at[1], gsl.at[2], gs_s.at[2], gs_r.at[2], 'depth')
    gs_dep.start()
    for q in range(3 * half_n - RING, 3 * half_n):
        stream(x_h, 0, q).wait_send()
    all_of(acc_u.at[b, 1 - d], yu_s).wait()
    all_of(acc_u.at[b, d, :, pl.ds(half_f, half_f)], rx_s).wait()
    all_of(trx, out_sem.at[3]).wait()
    for i in range(steps):
        ydn(i).wait_recv()
        dn_load = local(ydn_h.at[i], acc_d.at[1 - b, 0, pl.ds(i * LANES, LANES), :], t_sem.at[1, 0])
        dn_load.start()
        dn_load.wait()
        rs = tile(i, LANES)
        for j in range(half_d // LANES):
            cs = tile(j, LANES)
            total = acc_d[b, d, rs, cs] + acc_d[1 - b, 0, rs, cs]
            us[j * LANES // M, j * LANES % M:j * LANES % M + LANES, rs] = total.T.astype(BF16)
    gd_out = [local(us.at[i], gd_h.at[pl.ds(i * M, M), :], t_sem.at[i, 1]) for i in range(2)]
    for cp in gd_out:
        cp.start()
    gs_dep.wait()
    gsp[0] = gsp[1] + gsl[2]
    gs_out = local(gsp.at[0], gs_h, out_sem.at[0])
    gs_out.start()
    all_of(acc_d.at[b, 1 - d], ydn_s).wait()
    for sem in (ag_s, ag_r):
        all_of(trx, sem).wait()
    sent = dxo_h.at[head((half_n - LATE) * M), :]
    for sem in (dx_s, dx_r):
        all_of(sent, sem).wait()
    for cp in gd_out:
        cp.wait()
    gs_out.wait()


def finish_kernel(y_in, dx_in, gwu_in, gd, gs, y, dx, gwu, gwd, gbup, ggam, gbet, gbdn, big, small, sums, in_sem, out_sem):
    rows, hw = y.shape
    half_f = gwd.shape[0]
    d = lax.axis_index('depth')
    n = rows // COPIES
    ins, outs = [], []

    def move(src, buf, *dst):
        ins.append(pltpu.make_async_copy(src, buf, in_sem.at[len(ins)]))
        outs.append([pltpu.make_async_copy(buf, to, out_sem) for to in dst])

    for i in range(COPIES):
        rs = pl.ds(i * n, n)
        move(y_in.at[rs], big.at[0, rs], y.at[rs])
        move(dx_in.at[rs], big.at[1, rs], dx.at[rs])
    move(gwu_in, small.at[:, head(half_f)], gwu)
    move(gd, big.at[2, head(half_f // 2)], gwd.at[pl.ds(pl.multiple_of(d * (half_f // 2), half_f // 2), half_f // 2)])
    parts = [(0, half_f, gbup), (half_f, hw, ggam), (half_f + hw, hw, gbet), (half_f + 2 * hw, hw, gbdn)]
    move(gs, sums)
    outs[-1] = [pltpu.make_async_copy(sums.at[:, pl.ds(a, w)], dst, out_sem) for a, w, dst in parts]
    for cp in ins:
        cp.start()
    for cp, tos in zip(ins, outs):
        cp.wait()
        for to in tos:
            to.start()
    for tos in outs:
        for to in tos:
            to.wait()


def solution(mesh):
    tok_spec = P(('dp', 'depth', 'row'), 'col')
    vec_spec = P('col')
    mat_spec = P('row', 'col')
    grad_vec = P(('dp', 'col'))
    grad_mat = P(('dp', 'row'), 'col')
    swap = ((0, 1), (1, 0))

    def local_pass(x, gamma, beta, w_up, b_up, w_down, b_down, dy):
        rows, hw = x.shape
        half_f = b_up.shape[0]
        full_f, full, hq = 2 * half_f, 2 * hw, hw // 2
        chunks = rows // M
        late = LATE * M
        hbm = pl.BlockSpec(memory_space=pltpu.HBM)
        sds = jax.ShapeDtypeStruct
        V, D = pltpu.VMEM, pltpu.SemaphoreType.DMA
        D2, D3, D4, D2S = D((2,)), D((3,)), D((4,)), D((2, SUBS))
        tiles, own_tiles = full_f // FT, half_f // FT
        outs = [
            sds((rows, hw), BF16), sds((rows, hw), BF16), sds((late, hw), BF16), sds((1, full_f), F32), sds((hw, half_f), BF16),
            sds((half_f // 2, hw), BF16),
            sds((rows // 2, hw), BF16), sds((tiles, 2, hq, FT), F32), sds((tiles, hq, FT), F32), sds((own_tiles, hq, FT), F32),
            sds((2, hw, half_f // 2), F32), sds((hw // LANES, LANES, half_f // 2), F32),
            sds((rows // 2, hw), BF16), sds((rows // 2, hw), BF16), sds((chunks // 2, 2, hq, full), F32), sds((chunks // 2, 2, hq, LANES), F32),
        ]
        scratch = [
            V((full, full_f), BF16), V((full_f, full), BF16), V((2, 2, hw, half_f // 2), F32), V((2, 2, hq, full_f), F32),
            V((2, M, hw), BF16), V((RING, M, hw), BF16), V((2, M, hw), BF16), V((M, full), BF16), V((full, M), BF16), V((hw, M), BF16),
            V((2, hq, LANES), F32), V((2, M, FT), BF16), V((2, 2, hq, FT), F32), V((2, M, FT), BF16), V((2, M, FT), BF16),
            V((M, hw), F32), V((2, hq, full), F32), V((M, hw), BF16), V((M, hw), BF16), V((M, hw), BF16),
            V((8, full_f), F32), V((8, 2 * full + hw), F32), V((2, 1, full_f), F32), V((2, half_f // LANES, LANES), BF16), V((hw // LANES, LANES), BF16),
            V((1, full_f), F32), V((2, 1, full_f), F32), V((3, 1, full_f), F32),
            D2, D2, D2, D2S, D2, D2S, D2, D2S, D2, D2S, D3, D3,
            D((RING,)), D((RING,)), D((6, 2)), D4, D4, D((2, 2)), D(()), D((tiles,)), D(()), D((tiles,)), D(()), D((own_tiles,)),
            D(()), D(()), D(()), D(()), D(()), D((hw // LANES,)), D(()), D(()), D3, D3, pltpu.SemaphoreType.REGULAR,
        ]
        res = pl.pallas_call(
            kernel,
            out_shape=outs,
            in_specs=[hbm] * 8,
            out_specs=[hbm] * len(outs),
            scratch_shapes=scratch,
            compiler_params=pltpu.CompilerParams(
                collective_id=0, has_side_effects=True, vmem_limit_bytes=67043328),
            cost_estimate=pl.CostEstimate(flops=14 * rows * full * full_f, bytes_accessed=2 ** 27, transcendentals=rows * full_f),
            name='mlp_block',
        )(x, dy, w_up, w_down, b_up.reshape(-1, LANES), gamma.reshape(1, -1), beta.reshape(1, -1), b_down.reshape(-1, LANES))
        y, dx, dxl, gs, gwu, gd = res[:6]
        gd_far = lax.ppermute(gd, 'depth', swap)
        dx_far = lax.ppermute(dxl, 'col', swap)
        moves = 2 * COPIES + 3
        y, dx, gwu, gwd, gbup, ggam, gbet, gbdn = pl.pallas_call(
            finish_kernel,
            out_shape=[sds((rows, hw), BF16), sds((rows, hw), BF16), sds((hw, half_f), BF16), sds((half_f, hw), BF16),
                       sds((1, half_f), F32), sds((1, hw), F32), sds((1, hw), F32), sds((1, hw), F32)],
            in_specs=[hbm] * 5,
            out_specs=[hbm] * 8,
            scratch_shapes=[V((3, rows, hw), BF16), V((hw, half_f), BF16), V((1, full_f), F32), D((moves,)), D(())],
            compiler_params=pltpu.CompilerParams(vmem_limit_bytes=62000000),
            cost_estimate=pl.CostEstimate(flops=2 ** 33, bytes_accessed=42 * 2 ** 20, transcendentals=0),
            name='finish',
        )(y, dx, gwu, gd, gs)
        gwd = lax.dynamic_update_slice(gwd, gd_far, ((1 - lax.axis_index('depth')) * (half_f // 2), 0))
        dx = lax.dynamic_update_slice(dx, dx_far, ((1 - lax.axis_index('col')) * (rows // 2) + rows // 2 - late, 0))
        return y, dx, ggam.reshape(-1), gbet.reshape(-1), gwu, gbup.reshape(-1), gwd, gbdn.reshape(-1)

    return jax.shard_map(
        local_pass,
        mesh=mesh,
        in_specs=(tok_spec, vec_spec, vec_spec, mat_spec, vec_spec, mat_spec, vec_spec, tok_spec),
        out_specs=(tok_spec, tok_spec, grad_vec, grad_vec, grad_mat, grad_vec, grad_mat, grad_vec),
        check_vma=False,
    )
```

```python
import jax
import jax.numpy as jnp
from jax import lax
from jax.experimental import pallas as pl
from jax.experimental.pallas import tpu as pltpu
from jax.sharding import PartitionSpec as P

LN_EPS = 1e-5
C0 = 0.7978845608
C1 = C0 * 0.044715
M = 512
FT = 512
SUBS = 4
RING = 6
LATE = 2
PROMPT = 2
COPIES = 4
LANES = 128
BF16, F32 = jnp.bfloat16, jnp.float32
MESH = pl.DeviceIdType.MESH


def dot(lhs, rhs, rhs_dim=0):
    return lax.dot_general(lhs, rhs, (((1,), (rhs_dim,)), ((), ())), preferred_element_type=F32)


def dot_t(lhs, rhs):
    return dot(lhs, rhs, 1)


def odd(n):
    return lax.rem(n, 2)


def cat(*parts):
    return jnp.concatenate(parts, axis=1)


def row_sum(v):
    return jnp.sum(v, axis=1, keepdims=True)


def col_sum(v):
    return jnp.sum(v, axis=0, keepdims=True)


def head(n):
    return pl.ds(0, n)


def tile(i, n):
    return slice(i * n, (i + 1) * n)


def gelu(v):
    t = jnp.tanh(v * (C1 * (v * v) + C0))
    h = 0.5 * v
    return h * t + h


def gelu_and_slope(v):
    v2 = v * v
    t = jnp.tanh(v * (C1 * v2 + C0))
    h = 0.5 * v
    slope = (v * (1.0 - t * t)) * (1.5 * C1 * v2 + 0.5 * C0) + (0.5 * t + 0.5)
    return h * t + h, slope


def fold8(v):
    return jnp.sum(v.reshape(v.shape[0] // 8, 8, v.shape[1]), axis=0)


def kernel(x_h, dy_h, wu_h, wd_h, bup_h, gam_h, bet_h, bdn_h,
           y_h, dx_h, dxl_h, gs_h, gu_h, gd_h, dxo_h, rrow_h, ryu_h, rx_h, rdn_h, ydn_h, xo_h, dyo_h, dxn_h, st_h,
           wu, wd, acc_d, acc_u, own, land, aux, xn, trx, trd, st, us, da_s, act, du_s, yacc, dxn, yo, dxa, dxb,
           bup8, gb8, smv, bup_s, bdn_s, gso, gsp, gsl,
           wrow_s, wrow_r, wx_s, wx_r, wy_s, wy_r, wa_s, wa_r, wb_s, wb_r, sm_s, sm_r,
           land_s, land_r, ld_sem, out_sem, sv_sem, t_sem, ru_s, ru_r, yu_s, yu_r, rx_s, rx_r, ag_s, ag_r, rdn_s, rdn_r,
           ydn_s, ydn_r, dx_s, dx_r, gs_s, gs_r, credit):
    chunks = x_h.shape[0] // M
    half_n = chunks // 2
    half_f = wu_h.shape[1]
    hw = x_h.shape[1]
    full = 2 * hw
    hq = hw // 2
    half_d = half_f // 2
    tiles = 2 * half_f // FT
    own_tiles = tiles // 2
    c, r, d = lax.axis_index('col'), lax.axis_index('row'), lax.axis_index('depth')
    b = lax.rem(r + c, 2)
    peer = {'col': 1 - c, 'row': 1 - r, 'depth': 1 - d}
    mine0, theirs0 = c * half_n, (1 - c) * half_n

    def send(src, dst, s_sem, r_sem, axis):
        return pltpu.make_async_remote_copy(src_ref=src, dst_ref=dst, send_sem=s_sem, recv_sem=r_sem,
                                            device_id={axis: peer[axis]}, device_id_type=MESH)

    def local(src, dst, sem):
        return pltpu.make_async_copy(src, dst, sem)

    def all_of(ref, sem):
        return pltpu.make_async_copy(ref, ref, sem)

    def rows_of(k):
        return pl.ds(pl.multiple_of(k * M, M), M)

    def chunk_at(n):
        return lax.rem(mine0 + n, chunks)

    bar = pltpu.get_barrier_semaphore()
    for axis in ('col', 'row', 'depth'):
        pl.semaphore_signal(bar, inc=1, device_id={axis: peer[axis]}, device_id_type=MESH)
    pl.semaphore_wait(bar, 3)

    half_rows = (hq, half_d)
    w_srcs = (wu_h, wd_h)

    def w_cols(kind, blk, dep, s):
        n = half_rows[kind] // SUBS
        if kind == 0:
            return wu.at[pl.ds(pl.multiple_of(blk * hw + dep * hq + s * n, n), n), pl.ds(half_f, half_f)]
        return wd.at[pl.ds(pl.multiple_of(blk * half_f + dep * half_d + s * n, n), n), pl.ds(hw, hw)]

    def w_half(kind):
        return wu.at[head(hq), head(half_f)] if kind == 0 else wd.at[head(half_d), head(hw)]

    def w_own(kind):
        if kind == 0:
            return wu.at[pl.ds(pl.multiple_of(b * hw, hw), hw), head(half_f)]
        return wd.at[pl.ds(pl.multiple_of(b * half_f, half_f), half_f), head(hw)]

    def w_x(kind, s):
        n = half_rows[kind] // SUBS
        src = w_srcs[kind].at[pl.ds(pl.multiple_of(d * half_rows[kind] + s * n, n), n), :]
        return send(src, w_cols(kind, 1 - b, d, s), wx_s.at[kind], wx_r.at[kind, s], 'col')

    def w_y(kind, s):
        return send(w_cols(kind, b, d, s), w_cols(kind, b, d, s), wy_s.at[kind], wy_r.at[kind, s], 'depth')

    def w_a(kind, s):
        return send(w_cols(kind, b, d, s), w_cols(kind, b, d, s), wa_s.at[kind], wa_r.at[kind, s], 'row')

    def w_b(kind, s):
        return send(w_cols(kind, b, 1 - d, s), w_cols(kind, b, 1 - d, s), wb_s.at[kind], wb_r.at[kind, s], 'row')

    def w_row(kind):
        return send(w_srcs[kind], w_own(kind), wrow_s.at[kind], wrow_r.at[kind], 'row')

    def w_load(kind):
        return local(w_srcs[kind], w_own(kind), out_sem.at[kind])

    def w_cross(kind):
        for s in range(SUBS):
            w_x(kind, s).start()

    def w_forward_x(kind):
        for s in range(SUBS):
            w_x(kind, s).wait_recv()
            w_y(kind, s).start()
            w_a(kind, s).start()

    def w_forward_y(kind):
        for s in range(SUBS):
            w_y(kind, s).wait_recv()
            w_b(kind, s).start()

    def w_arrive(kind):
        for s in range(SUBS):
            w_a(kind, s).wait_recv()
            w_b(kind, s).wait_recv()

    def stream(src, k, q):
        slot = lax.rem(q, RING)
        return send(src.at[rows_of(k), :], land.at[slot], land_s.at[slot], land_r.at[slot], 'col')

    def stream_next(src, k, q):
        @pl.when(q >= RING)
        def _():
            stream(src, k, q).wait_send()
            pl.semaphore_wait(credit, 1)
        stream(src, k, q).start()

    def give(n):
        for _ in range(n):
            pl.semaphore_signal(credit, inc=1, device_id={'col': peer['col']}, device_id_type=MESH)

    gam_at, bet_at = pl.ds(half_f, hw), pl.ds(half_f + hw, hw)
    sm_own = [local(bup_h, bup_s.at[0], ld_sem.at[0, 0]), local(gam_h, smv.at[0, :, gam_at], ld_sem.at[0, 1]),
              local(bet_h, smv.at[0, :, bet_at], ld_sem.at[1, 0]), local(bdn_h, bdn_s, ld_sem.at[1, 1])]
    sm_out = [send(bup_h, bup_s.at[1], sm_s.at[0], sm_r.at[0], 'col'),
              send(gam_h, smv.at[1, :, gam_at], sm_s.at[1], sm_r.at[1], 'col'),
              send(bet_h, smv.at[1, :, bet_at], sm_s.at[2], sm_r.at[2], 'col')]
    for cp in sm_own + sm_out:
        cp.start()
    @pl.when(b == 1)
    def _():
        w_cross(1)

    for kind in range(2):
        w_load(kind).start()
        w_row(kind).start()
    stream(x_h, theirs0, 0).start()
    stream(dy_h, theirs0, 1).start()
    w_cross(0)

    @pl.when(b == 0)
    def _():
        w_cross(1)

    stream(x_h, theirs0 + 1, 2).start()
    stream(dy_h, theirs0 + 1, 3).start()

    acc_d[...] = jnp.zeros_like(acc_d)
    acc_u[...] = jnp.zeros_like(acc_u)
    bup8[...] = jnp.zeros_like(bup8)
    gb8[...] = jnp.zeros_like(gb8)
    for cp in sm_own:
        cp.wait()

    def load(n):
        s = odd(n)
        rs = rows_of(chunk_at(n))
        return (local(x_h.at[rs, :], own.at[s], ld_sem.at[0, s]), local(dy_h.at[rs, :], aux.at[s], ld_sem.at[1, s]))

    for cp in load(0):
        cp.start()
    for kind in range(2):
        w_load(kind).wait()
        w_row(kind).wait()

    @pl.when(b == 0)
    def _():
        w_forward_x(1)
        w_forward_y(1)

    @pl.when(b == 1)
    def _():
        w_arrive(1)

    def w_rest():
        w_forward_x(0)

        @pl.when(b == 1)
        def _():
            w_forward_x(1)

        w_forward_y(0)

        @pl.when(b == 1)
        def _():
            w_forward_y(1)

        @pl.when(b == 0)
        def _():
            w_arrive(1)

        w_arrive(0)
        for kind in range(2):
            for sems in (wx_s, wy_s, wa_s, wb_s):
                all_of(w_half(kind), sems.at[kind]).wait()

    for cp in sm_out:
        cp.wait()
    for i in range(half_f // LANES):
        for side in range(2):
            smv[side, :, tile(i, LANES)] = bup_s[side, i:i + 1, :].astype(F32)
    for i in range(hw // LANES):
        smv[0, :, half_f + full + i * LANES:half_f + full + (i + 1) * LANES] = bdn_s[i:i + 1, :].astype(F32)

    def wide(at):
        return cat(smv[0, :, half_f + at:half_f + at + hw], smv[1, :, half_f + at:half_f + at + hw])

    def norm(s, slot, keep):
        gam, bet = wide(0), wide(hw)
        step = 32
        for i in range(M // step):
            rs = tile(i, step)
            xv = cat(own[s, rs, :], land[slot, rs, :]).astype(F32)
            mean = row_sum(xv) * (1.0 / full)
            cen = xv - mean
            istd = lax.rsqrt(row_sum(cen * cen) * (1.0 / full) + LN_EPS)
            xn[rs, :] = (cen * istd * gam + bet).astype(BF16)
            if keep:
                st[i * step // hq, i * step % hq:i * step % hq + step, :] = cat(jnp.broadcast_to(mean, (step, 64)), jnp.broadcast_to(istd, (step, 64)))
        dyv = aux[s]
        trd[...] = dyv.T
        gb8[:, 2 * full:2 * full + hw] += fold8(dyv.astype(F32))

    def write_y(s):
        bdn = smv[0, :, half_f + full:half_f + full + hw]
        yo[...] = (own[s].astype(F32) + yacc[...] + bdn).astype(BF16)

    def y_out(n):
        return local(yo, y_h.at[rows_of(chunk_at(n)), :], out_sem.at[0])

    def dx_out(n):
        return local(dxa, dx_h.at[rows_of(chunk_at(n)), :], out_sem.at[1])

    def dxo_out(n):
        return local(dxb, dxo_h.at[rows_of(n), :], out_sem.at[2])

    def dxl_out(n):
        return local(dxb, dxl_h.at[rows_of(n - (half_n - LATE)), :], out_sem.at[2])

    def saves(n, slot_x, slot_d):
        rs = rows_of(n)
        return (local(land.at[slot_x], xo_h.at[rs, :], sv_sem.at[0]), local(land.at[slot_d], dyo_h.at[rs, :], sv_sem.at[1]),
                local(dxn, dxn_h.at[n], sv_sem.at[2]), local(st, st_h.at[n], sv_sem.at[3]))

    def finish_dx(grads, xs, dys, stats):
        gam = wide(0)
        step = 32
        for i in range(M // step):
            rs = tile(i, step)
            h, hs = i * step // hq, slice(i * step % hq, i * step % hq + step)
            istd = stats[h, hs, 64:65]
            xh = (xs(rs).astype(F32) - stats[h, hs, 0:1]) * istd
            dv = grads(h, hs)
            px = dv * xh
            gb8[:, :full] += fold8(px)
            gb8[:, full:2 * full] += fold8(dv)
            m1 = row_sum(dv * gam) * (1.0 / full)
            m2 = row_sum(px * gam) * (1.0 / full)
            dxv = (dys(rs).astype(F32) + istd * (dv * gam - m1 - xh * m2)).astype(BF16)
            dxa[rs, :] = dxv[:, :hw]
            dxb[rs, :] = dxv[:, hw:]

    def dx_far(m):
        return send(dxo_h.at[rows_of(m), :], dx_h.at[rows_of(mine0 + m), :], dx_s, dx_r, 'col')

    def chunk_mine(n, carry):
        s = odd(n)
        slot_x, slot_d = lax.rem(2 * n, RING), lax.rem(2 * n + 1, RING)

        for cp in load(n):
            cp.wait()
        for cp in load(n + 1):
            cp.start()

        stream(x_h, n, 2 * n).wait_recv()
        stream(dy_h, n, 2 * n + 1).wait_recv()
        save = saves(n, slot_x, slot_d)
        save[0].start()
        save[1].start()

        @pl.when(n > 0)
        def _():
            save[3].wait()

        norm(s, slot_x, True)
        save[3].start()
        trx[...] = xn[...].T

        @pl.when(n > 0)
        def _():
            save[2].wait()

        @pl.when((n > 0) & (n <= PROMPT))
        def _():
            dx_out(n).wait()
            dxo_out(n).wait()

        yacc[...] = jnp.zeros_like(yacc)
        dxn[...] = jnp.zeros_like(dxn)

        def quad(jj, inner):
            @pl.when((n == 0) & (jj == 1))
            def _():
                w_rest()

            @pl.when((n < half_n - 2) & (jj == 1))
            def _():
                stream_next(x_h, theirs0 + n + 2, 2 * n + 4)
                stream_next(dy_h, theirs0 + n + 2, 2 * n + 5)

            @pl.when((n >= half_n - 2) & (jj == 1))
            def _():
                k = 2 * (n - (half_n - 2))
                stream_next(x_h, mine0 + k, chunks + k)
                stream_next(x_h, mine0 + k + 1, chunks + k + 1)

            cols = [pl.ds(pl.multiple_of((own_tiles * jj + t) * FT, FT), FT) for t in range(own_tiles)]

            def first(t):
                bias = smv[jj, :, tile(t, FT)]
                us[t % 2] = (dot(xn[...], wu[:, cols[t]]) + bias).astype(BF16)
                dyv = cat(aux[s], land[slot_d])
                da_s[t % 2] = dot_t(dyv, wd[cols[t], :]).reshape(2, hq, FT)

            def mid(t):
                a, slope = gelu_and_slope(us[t % 2].astype(F32))
                act[t % 2] = a.astype(BF16)
                du = (da_s[t % 2].reshape(M, FT) * slope).astype(BF16)
                du_s[t % 2] = du
                bup8[:, cols[t]] += fold8(du.astype(F32))

            def last(t):
                yacc[...] += dot(act[t % 2], wd[cols[t], :hw])
                at = t * FT % half_d
                acc_d[jj, t * FT // half_d, :, at:at + FT] += dot(trd[...], act[t % 2])
                dxn[...] += dot_t(du_s[t % 2], wu[:, cols[t]]).reshape(2, hq, full)
                part = dot(trx[...], du_s[t % 2])
                for i in range(4):
                    acc_u[i // 2, i % 2, :, cols[t]] += part[tile(i, hq)]

            first(0)
            first(1)
            mid(0)
            for t in range(own_tiles):
                last(t)
                if t + 2 < own_tiles:
                    first(t + 2)
                if t + 1 < own_tiles:
                    mid(t + 1)
            return inner

        lax.fori_loop(0, 2, quad, 0)

        @pl.when(n > 0)
        def _():
            y_out(n).wait()

        write_y(s)
        y_out(n).start()
        save[2].start()

        @pl.when(n < PROMPT)
        def _():
            finish_dx(lambda h, rs: dxn[h, rs, :],
                      lambda rs: cat(own[s, rs, :], land[slot_x, rs, :]),
                      lambda rs: cat(aux[s, rs, :], land[slot_d, rs, :]), st)
            dx_out(n).start()
            dxo_out(n).start()

        save[0].wait()
        save[1].wait()
        give(2)
        return carry

    lax.fori_loop(0, half_n, chunk_mine, 0)

    order = [*range(own_tiles, tiles), *range(own_tiles)]

    def ru(p):
        return send(acc_u.at[1 - b, :, :, pl.ds(p * FT, FT)], rrow_h.at[p], ru_s, ru_r.at[p], 'row')

    def yu(p):
        return send(acc_u.at[b, 1 - d, :, pl.ds(p * FT, FT)], ryu_h.at[p], yu_s, yu_r.at[p], 'depth')

    def rx(k):
        return send(acc_u.at[b, d, :, pl.ds((own_tiles + k) * FT, FT)], rx_h.at[k], rx_s, rx_r.at[k], 'col')

    gu_rows = pl.ds(pl.multiple_of(d * hq, hq), hq)

    def ag(k):
        ps = pl.ds(k * FT, FT)
        return send(trx.at[pl.ds(k * hq, hq), :], gu_h.at[gu_rows, ps], ag_s, ag_r, 'depth')

    def gu_out(k):
        return local(trx.at[pl.ds(k * hq, hq), :], gu_h.at[gu_rows, pl.ds(k * FT, FT)], out_sem.at[3])

    def row_load(i, p):
        return local(rrow_h.at[p], da_s.at[i % 2], t_sem.at[i % 2, 0])

    for p in order:
        ru(p).start()
    y_out(0).wait()
    for cp in saves(half_n - 1, 0, 0)[2:]:
        cp.wait()
    ru(order[0]).wait_recv()
    row_load(0, order[0]).start()
    for i, p in enumerate(order):
        if i + 1 < tiles:
            ru(order[i + 1]).wait_recv()
            row_load(i + 1, order[i + 1]).start()
        row_load(i, p).wait()
        for h in range(2):
            acc_u[b, h, :, tile(p, FT)] += da_s[i % 2, h]
        yu(p).start()

    def oth_load(k):
        yu(own_tiles + k).wait_recv()
        local(ryu_h.at[own_tiles + k], da_s.at[k % 2, 0], t_sem.at[k % 2, 0]).start()

    def oth_send(k):
        p = own_tiles + k
        local(ryu_h.at[p], da_s.at[k % 2, 0], t_sem.at[k % 2, 0]).wait()
        acc_u[b, d, :, tile(p, FT)] += da_s[k % 2, 0]
        rx(k).start()

    def own_loads(k):
        return (local(ryu_h.at[k], da_s.at[k % 2, 0], t_sem.at[k % 2, 0]),
                local(rx_h.at[k], da_s.at[k % 2, 1], t_sem.at[k % 2, 1]))

    def own_load(k):
        yu(k).wait_recv()
        rx(k).wait_recv()
        for cp in own_loads(k):
            cp.start()

    def own_send(k):
        for cp in own_loads(k):
            cp.wait()
        trx[tile(k, hq), :] = (acc_u[b, d, :, tile(k, FT)] + da_s[k % 2, 0] + da_s[k % 2, 1]).astype(BF16)
        ag(k).start()

    def background(n):
        for k in range(own_tiles):
            @pl.when(n == half_n + 2 + k)
            def _():
                oth_send(k)

            @pl.when(n == half_n + 1 + k)
            def _():
                oth_load(k)

        for k in range(own_tiles - 1):
            @pl.when(n == half_n + 6 + k)
            def _():
                own_send(k)

            @pl.when(n == half_n + 5 + k)
            def _():
                if k >= 1:
                    pass
                own_load(k)

        for m in range(PROMPT):
            @pl.when(n == half_n + 5 + m)
            def _():
                dx_far(m).start()

    def chunk_theirs(n, carry):
        s = odd(n)
        q = n + half_n
        slot = lax.rem(q, RING)

        @pl.when(n == half_n)
        def _():
            stream_next(x_h, mine0 + 4, chunks + 4)

        @pl.when(n <= half_n + 2)
        def _():
            stream_next(x_h, mine0 + 5 + (n - half_n), chunks + 5 + (n - half_n))

        background(n)
        for cp in load(n):
            cp.wait()

        @pl.when(n < chunks - 1)
        def _():
            for cp in load(n + 1):
                cp.start()

        stream(x_h, n, q).wait_recv()
        norm(s, slot, False)

        def up(j):
            side, at = divmod(j * FT, half_f)
            us[j % 2] = (dot(xn[...], wu[:, tile(j, FT)]) + smv[side, :, at:at + FT]).astype(BF16)

        def mid(j):
            act[j % 2] = gelu(us[j % 2].astype(F32)).astype(BF16)

        def down(j):
            part = dot(act[j % 2], wd[tile(j, FT), :hw])
            yacc[...] = part if j == 0 else yacc[...] + part
            blk, rest = divmod(j * FT, half_f)
            qt, at = divmod(rest, half_d)
            acc_d[blk, qt, :, at:at + FT] += dot(trd[...], act[j % 2])

        up(0)
        up(1)
        mid(0)
        for j in range(tiles):
            if j + 2 < tiles:
                up(j + 2)
            down(j)
            if j + 1 < tiles:
                mid(j + 1)

        @pl.when(n > half_n)
        def _():
            y_out(n).wait()

        write_y(s)
        y_out(n).start()

        @pl.when(n < half_n + 2)
        def _():
            give(1)
        return carry

    lax.fori_loop(half_n, chunks, chunk_theirs, 0)

    rdn = send(acc_d.at[1 - b], rdn_h, rdn_s, rdn_r, 'row')
    rdn.start()
    k = own_tiles - 1
    own_send(k - 1)
    own_load(k)
    own_send(k)
    for k in range(own_tiles):
        gu_out(k).start()
    all_of(acc_u.at[1 - b], ru_s).wait()

    def load_dx(n):
        s = odd(n)
        rs, ks = rows_of(n), rows_of(mine0 + n)
        return (local(x_h.at[ks, :], own.at[s], ld_sem.at[0, s]), local(dy_h.at[ks, :], aux.at[s], ld_sem.at[1, s]),
                local(xo_h.at[rs, :], land.at[2 * s], ld_sem.at[2, s]), local(dyo_h.at[rs, :], land.at[2 * s + 1], ld_sem.at[3, s]),
                local(dxn_h.at[n], acc_u.at[1 - b, :, :, pl.ds(pl.multiple_of(s * full, full), full)], ld_sem.at[4, s]),
                local(st_h.at[n], da_s.at[s, :, :, head(LANES)], ld_sem.at[5, s]))

    held = 2

    def chunk_dx(n, carry):
        s = odd(n)
        for cp in load_dx(n):
            cp.wait()

        @pl.when(n < half_n - 1)
        def _():
            for cp in load_dx(n + 1):
                cp.start()

        @pl.when(n > PROMPT)
        def _():
            dx_out(n).wait()
            dxo_out(n).wait()

        @pl.when((n > PROMPT) & (n <= half_n - LATE - held))
        def _():
            dx_far(n - 1).start()

        finish_dx(lambda h, rs: acc_u[1 - b, h, rs, pl.ds(pl.multiple_of(s * full, full), full)],
                  lambda rs: cat(own[s, rs, :], land[2 * s, rs, :]),
                  lambda rs: cat(aux[s, rs, :], land[2 * s + 1, rs, :]), da_s.at[s, :, :, head(LANES)])
        dx_out(n).start()

        @pl.when(n < half_n - LATE)
        def _():
            dxo_out(n).start()

        @pl.when(n >= half_n - LATE)
        def _():
            dxl_out(n).start()
        return carry

    for cp in load_dx(PROMPT):
        cp.start()
    lax.fori_loop(PROMPT, 2 * PROMPT, chunk_dx, 0)
    rdn.wait()
    rd_load = local(rdn_h, acc_d.at[1 - b], t_sem.at[0, 0])
    rd_load.start()
    rd_load.wait()
    steps = hw // LANES

    def ydn(i):
        return send(acc_d.at[b, 1 - d, pl.ds(i * LANES, LANES), :], ydn_h.at[i], ydn_s, ydn_r.at[i], 'depth')

    for i in range(steps):
        rs = tile(i, LANES)
        for qt in range(2):
            acc_d[b, qt, rs, :] += acc_d[1 - b, qt, rs, :]
        ydn(i).start()
    lax.fori_loop(2 * PROMPT, half_n, chunk_dx, 0)
    y_out(chunks - 1).wait()
    oth = lambda at, n: [col_sum(ref[:, a:a + n]) for ref, a in at]
    gso[...] = jnp.concatenate(oth(((bup8, half_f),), half_f) + oth(((gb8, hw), (gb8, full + hw)), hw)
                               + [jnp.zeros((1, half_f - full), F32)], axis=1)
    gs_col = send(gso, gsl.at[0], gs_s.at[0], gs_r.at[0], 'col')
    gs_col.start()
    for m in range(half_n - LATE - held, half_n - LATE):
        dx_far(m).start()
    dx_out(half_n - 1).wait()
    dxl_out(half_n - 1).wait()
    gs_col.wait()
    gsp[0] = jnp.concatenate(oth(((bup8, 0),), half_f) + oth(((gb8, 0), (gb8, full), (gb8, 2 * full)), hw)
                             + [jnp.zeros((1, half_f - 3 * hw), F32)], axis=1) + gsl[0]
    gs_row = send(gsp.at[0], gsl.at[1], gs_s.at[1], gs_r.at[1], 'row')
    gs_row.start()
    gs_row.wait()
    gsp[1] = gsp[0] + gsl[1]
    gs_dep = send(gsp.at[1], gsl.at[2], gs_s.at[2], gs_r.at[2], 'depth')
    gs_dep.start()
    for q in range(3 * half_n - RING, 3 * half_n):
        stream(x_h, 0, q).wait_send()
    all_of(acc_u.at[b, 1 - d], yu_s).wait()
    all_of(acc_u.at[b, d, :, pl.ds(half_f, half_f)], rx_s).wait()
    all_of(trx, out_sem.at[3]).wait()
    for i in range(steps):
        ydn(i).wait_recv()
        dn_load = local(ydn_h.at[i], acc_d.at[1 - b, 0, pl.ds(i * LANES, LANES), :], t_sem.at[1, 0])
        dn_load.start()
        dn_load.wait()
        rs = tile(i, LANES)
        for j in range(half_d // LANES):
            cs = tile(j, LANES)
            total = acc_d[b, d, rs, cs] + acc_d[1 - b, 0, rs, cs]
            us[j * LANES // M, j * LANES % M:j * LANES % M + LANES, rs] = total.T.astype(BF16)
    gd_out = [local(us.at[i], gd_h.at[pl.ds(i * M, M), :], t_sem.at[i, 1]) for i in range(2)]
    for cp in gd_out:
        cp.start()
    gs_dep.wait()
    gsp[0] = gsp[1] + gsl[2]
    gs_out = local(gsp.at[0], gs_h, out_sem.at[0])
    gs_out.start()
    all_of(acc_d.at[b, 1 - d], ydn_s).wait()
    for sem in (ag_s, ag_r):
        all_of(trx, sem).wait()
    sent = dxo_h.at[head((half_n - LATE) * M), :]
    for sem in (dx_s, dx_r):
        all_of(sent, sem).wait()
    for cp in gd_out:
        cp.wait()
    gs_out.wait()


def finish_kernel(y_in, dx_in, gwu_in, gd, gs, y, dx, gwu, gwd, gbup, ggam, gbet, gbdn, big, small, sums, in_sem, out_sem):
    rows, hw = y.shape
    half_f = gwd.shape[0]
    d = lax.axis_index('depth')
    n = rows // COPIES
    ins, outs = [], []

    def move(src, buf, *dst):
        ins.append(pltpu.make_async_copy(src, buf, in_sem.at[len(ins)]))
        outs.append([pltpu.make_async_copy(buf, to, out_sem) for to in dst])

    for i in range(COPIES):
        rs = pl.ds(i * n, n)
        move(y_in.at[rs], big.at[0, rs], y.at[rs])
        move(dx_in.at[rs], big.at[1, rs], dx.at[rs])
    move(gwu_in, small.at[:, head(half_f)], gwu)
    move(gd, big.at[2, head(half_f // 2)], gwd.at[pl.ds(pl.multiple_of(d * (half_f // 2), half_f // 2), half_f // 2)])
    parts = [(0, half_f, gbup), (half_f, hw, ggam), (half_f + hw, hw, gbet), (half_f + 2 * hw, hw, gbdn)]
    move(gs, sums)
    outs[-1] = [pltpu.make_async_copy(sums.at[:, pl.ds(a, w)], dst, out_sem) for a, w, dst in parts]
    for cp in ins:
        cp.start()
    for cp, tos in zip(ins, outs):
        cp.wait()
        for to in tos:
            to.start()
    for tos in outs:
        for to in tos:
            to.wait()


def solution(mesh):
    tok_spec = P(('dp', 'depth', 'row'), 'col')
    vec_spec = P('col')
    mat_spec = P('row', 'col')
    grad_vec = P(('dp', 'col'))
    grad_mat = P(('dp', 'row'), 'col')
    swap = ((0, 1), (1, 0))

    def local_pass(x, gamma, beta, w_up, b_up, w_down, b_down, dy):
        rows, hw = x.shape
        half_f = b_up.shape[0]
        full_f, full, hq = 2 * half_f, 2 * hw, hw // 2
        chunks = rows // M
        late = LATE * M
        hbm = pl.BlockSpec(memory_space=pltpu.HBM)
        sds = jax.ShapeDtypeStruct
        V, D = pltpu.VMEM, pltpu.SemaphoreType.DMA
        D2, D3, D4, D2S = D((2,)), D((3,)), D((4,)), D((2, SUBS))
        tiles, own_tiles = full_f // FT, half_f // FT
        outs = [
            sds((rows, hw), BF16), sds((rows, hw), BF16), sds((late, hw), BF16), sds((1, full_f), F32), sds((hw, half_f), BF16),
            sds((half_f // 2, hw), BF16),
            sds((rows // 2, hw), BF16), sds((tiles, 2, hq, FT), F32), sds((tiles, hq, FT), F32), sds((own_tiles, hq, FT), F32),
            sds((2, hw, half_f // 2), F32), sds((hw // LANES, LANES, half_f // 2), F32),
            sds((rows // 2, hw), BF16), sds((rows // 2, hw), BF16), sds((chunks // 2, 2, hq, full), F32), sds((chunks // 2, 2, hq, LANES), F32),
        ]
        scratch = [
            V((full, full_f), BF16), V((full_f, full), BF16), V((2, 2, hw, half_f // 2), F32), V((2, 2, hq, full_f), F32),
            V((2, M, hw), BF16), V((RING, M, hw), BF16), V((2, M, hw), BF16), V((M, full), BF16), V((full, M), BF16), V((hw, M), BF16),
            V((2, hq, LANES), F32), V((2, M, FT), BF16), V((2, 2, hq, FT), F32), V((2, M, FT), BF16), V((2, M, FT), BF16),
            V((M, hw), F32), V((2, hq, full), F32), V((M, hw), BF16), V((M, hw), BF16), V((M, hw), BF16),
            V((8, full_f), F32), V((8, 2 * full + hw), F32), V((2, 1, full_f), F32), V((2, half_f // LANES, LANES), BF16), V((hw // LANES, LANES), BF16),
            V((1, full_f), F32), V((2, 1, full_f), F32), V((3, 1, full_f), F32),
            D2, D2, D2, D2S, D2, D2S, D2, D2S, D2, D2S, D3, D3,
            D((RING,)), D((RING,)), D((6, 2)), D4, D4, D((2, 2)), D(()), D((tiles,)), D(()), D((tiles,)), D(()), D((own_tiles,)),
            D(()), D(()), D(()), D(()), D(()), D((hw // LANES,)), D(()), D(()), D3, D3, pltpu.SemaphoreType.REGULAR,
        ]
        res = pl.pallas_call(
            kernel,
            out_shape=outs,
            in_specs=[hbm] * 8,
            out_specs=[hbm] * len(outs),
            scratch_shapes=scratch,
            compiler_params=pltpu.CompilerParams(
                collective_id=0, has_side_effects=True, vmem_limit_bytes=67043328),
            cost_estimate=pl.CostEstimate(flops=14 * rows * full * full_f, bytes_accessed=2 ** 27, transcendentals=rows * full_f),
            name='mlp_block',
        )(x, dy, w_up, w_down, b_up.reshape(-1, LANES), gamma.reshape(1, -1), beta.reshape(1, -1), b_down.reshape(-1, LANES))
        y, dx, dxl, gs, gwu, gd = res[:6]
        gd_far = lax.ppermute(gd, 'depth', swap)
        dx_far = lax.ppermute(dxl, 'col', swap)
        moves = 2 * COPIES + 3
        y, dx, gwu, gwd, gbup, ggam, gbet, gbdn = pl.pallas_call(
            finish_kernel,
            out_shape=[sds((rows, hw), BF16), sds((rows, hw), BF16), sds((hw, half_f), BF16), sds((half_f, hw), BF16),
                       sds((1, half_f), F32), sds((1, hw), F32), sds((1, hw), F32), sds((1, hw), F32)],
            in_specs=[hbm] * 5,
            out_specs=[hbm] * 8,
            scratch_shapes=[V((3, rows, hw), BF16), V((hw, half_f), BF16), V((1, full_f), F32), D((moves,)), D(())],
            compiler_params=pltpu.CompilerParams(vmem_limit_bytes=62000000),
            cost_estimate=pl.CostEstimate(flops=2 ** 33, bytes_accessed=42 * 2 ** 20, transcendentals=0),
            name='finish',
        )(y, dx, gwu, gd, gs)
        gwd = lax.dynamic_update_slice(gwd, gd_far, ((1 - lax.axis_index('depth')) * (half_f // 2), 0))
        dx = lax.dynamic_update_slice(dx, dx_far, ((1 - lax.axis_index('col')) * (rows // 2) + rows // 2 - late, 0))
        return y, dx, ggam.reshape(-1), gbet.reshape(-1), gwu, gbup.reshape(-1), gwd, gbdn.reshape(-1)

    return jax.shard_map(
        local_pass,
        mesh=mesh,
        in_specs=(tok_spec, vec_spec, vec_spec, mat_spec, vec_spec, mat_spec, vec_spec, tok_spec),
        out_specs=(tok_spec, tok_spec, grad_vec, grad_vec, grad_mat, grad_vec, grad_mat, grad_vec),
        check_vma=False,
    )
```

```python
import jax
import jax.numpy as jnp
from jax import lax
from jax.experimental import pallas as pl
from jax.experimental.pallas import tpu as pltpu
from jax.sharding import PartitionSpec as P

LN_EPS = 1e-5
C0 = 0.7978845608
C1 = C0 * 0.044715
M = 512
FT = 512
SUBS = 4
RING = 6
LATE = 2
PROMPT = 2
COPIES = 4
LANES = 128
BF16, F32 = jnp.bfloat16, jnp.float32
MESH = pl.DeviceIdType.MESH


def dot(lhs, rhs, rhs_dim=0):
    return lax.dot_general(lhs, rhs, (((1,), (rhs_dim,)), ((), ())), preferred_element_type=F32)


def dot_t(lhs, rhs):
    return dot(lhs, rhs, 1)


def odd(n):
    return lax.rem(n, 2)


def cat(*parts):
    return jnp.concatenate(parts, axis=1)


def row_sum(v):
    return jnp.sum(v, axis=1, keepdims=True)


def col_sum(v):
    return jnp.sum(v, axis=0, keepdims=True)


def head(n):
    return pl.ds(0, n)


def tile(i, n):
    return slice(i * n, (i + 1) * n)


def gelu(v):
    t = jnp.tanh(v * (C1 * (v * v) + C0))
    h = 0.5 * v
    return h * t + h


def gelu_and_slope(v):
    v2 = v * v
    t = jnp.tanh(v * (C1 * v2 + C0))
    h = 0.5 * v
    slope = (v * (1.0 - t * t)) * (1.5 * C1 * v2 + 0.5 * C0) + (0.5 * t + 0.5)
    return h * t + h, slope


def fold8(v):
    return jnp.sum(v.reshape(v.shape[0] // 8, 8, v.shape[1]), axis=0)


def kernel(x_h, dy_h, wu_h, wd_h, bup_h, gam_h, bet_h, bdn_h,
           y_h, dx_h, dxl_h, gs_h, gu_h, gd_h, dxo_h, rrow_h, ryu_h, rx_h, rdn_h, ydn_h, xo_h, dyo_h, dxn_h, st_h,
           wu, wd, acc_d, acc_u, own, land, aux, xn, trx, trd, st, us, da_s, act, du_s, yacc, dxn, yo, dxa, dxb,
           bup8, gb8, smv, bup_s, bdn_s, gso, gsp, gsl,
           wrow_s, wrow_r, wx_s, wx_r, wy_s, wy_r, wa_s, wa_r, wb_s, wb_r, sm_s, sm_r,
           land_s, land_r, ld_sem, out_sem, sv_sem, t_sem, ru_s, ru_r, yu_s, yu_r, rx_s, rx_r, ag_s, ag_r, rdn_s, rdn_r,
           ydn_s, ydn_r, dx_s, dx_r, gs_s, gs_r, credit):
    chunks = x_h.shape[0] // M
    half_n = chunks // 2
    half_f = wu_h.shape[1]
    hw = x_h.shape[1]
    full = 2 * hw
    hq = hw // 2
    half_d = half_f // 2
    tiles = 2 * half_f // FT
    own_tiles = tiles // 2
    c, r, d = lax.axis_index('col'), lax.axis_index('row'), lax.axis_index('depth')
    b = lax.rem(r + c, 2)
    peer = {'col': 1 - c, 'row': 1 - r, 'depth': 1 - d}
    mine0, theirs0 = c * half_n, (1 - c) * half_n

    def send(src, dst, s_sem, r_sem, axis):
        return pltpu.make_async_remote_copy(src_ref=src, dst_ref=dst, send_sem=s_sem, recv_sem=r_sem,
                                            device_id={axis: peer[axis]}, device_id_type=MESH)

    def local(src, dst, sem):
        return pltpu.make_async_copy(src, dst, sem)

    def all_of(ref, sem):
        return pltpu.make_async_copy(ref, ref, sem)

    def rows_of(k):
        return pl.ds(pl.multiple_of(k * M, M), M)

    def chunk_at(n):
        return lax.rem(mine0 + n, chunks)

    bar = pltpu.get_barrier_semaphore()
    for axis in ('col', 'row', 'depth'):
        pl.semaphore_signal(bar, inc=1, device_id={axis: peer[axis]}, device_id_type=MESH)
    pl.semaphore_wait(bar, 3)

    half_rows = (hq, half_d)
    w_srcs = (wu_h, wd_h)

    def w_cols(kind, blk, dep, s):
        n = half_rows[kind] // SUBS
        if kind == 0:
            return wu.at[pl.ds(pl.multiple_of(blk * hw + dep * hq + s * n, n), n), pl.ds(half_f, half_f)]
        return wd.at[pl.ds(pl.multiple_of(blk * half_f + dep * half_d + s * n, n), n), pl.ds(hw, hw)]

    def w_half(kind):
        return wu.at[head(hq), head(half_f)] if kind == 0 else wd.at[head(half_d), head(hw)]

    def w_own(kind):
        if kind == 0:
            return wu.at[pl.ds(pl.multiple_of(b * hw, hw), hw), head(half_f)]
        return wd.at[pl.ds(pl.multiple_of(b * half_f, half_f), half_f), head(hw)]

    def w_x(kind, s):
        n = half_rows[kind] // SUBS
        src = w_srcs[kind].at[pl.ds(pl.multiple_of(d * half_rows[kind] + s * n, n), n), :]
        return send(src, w_cols(kind, 1 - b, d, s), wx_s.at[kind], wx_r.at[kind, s], 'col')

    def w_y(kind, s):
        return send(w_cols(kind, b, d, s), w_cols(kind, b, d, s), wy_s.at[kind], wy_r.at[kind, s], 'depth')

    def w_a(kind, s):
        return send(w_cols(kind, b, d, s), w_cols(kind, b, d, s), wa_s.at[kind], wa_r.at[kind, s], 'row')

    def w_b(kind, s):
        return send(w_cols(kind, b, 1 - d, s), w_cols(kind, b, 1 - d, s), wb_s.at[kind], wb_r.at[kind, s], 'row')

    def w_row(kind):
        return send(w_srcs[kind], w_own(kind), wrow_s.at[kind], wrow_r.at[kind], 'row')

    def w_load(kind):
        return local(w_srcs[kind], w_own(kind), out_sem.at[kind])

    def w_cross(kind):
        for s in range(SUBS):
            w_x(kind, s).start()

    def w_forward_x(kind):
        for s in range(SUBS):
            w_x(kind, s).wait_recv()
            w_y(kind, s).start()
            w_a(kind, s).start()

    def w_forward_y(kind):
        for s in range(SUBS):
            w_y(kind, s).wait_recv()
            w_b(kind, s).start()

    def w_arrive(kind):
        for s in range(SUBS):
            w_a(kind, s).wait_recv()
            w_b(kind, s).wait_recv()

    def stream(src, k, q):
        slot = lax.rem(q, RING)
        return send(src.at[rows_of(k), :], land.at[slot], land_s.at[slot], land_r.at[slot], 'col')

    def stream_next(src, k, q):
        @pl.when(q >= RING)
        def _():
            stream(src, k, q).wait_send()
            pl.semaphore_wait(credit, 1)
        stream(src, k, q).start()

    def give(n):
        for _ in range(n):
            pl.semaphore_signal(credit, inc=1, device_id={'col': peer['col']}, device_id_type=MESH)

    gam_at, bet_at = pl.ds(half_f, hw), pl.ds(half_f + hw, hw)
    sm_own = [local(bup_h, bup_s.at[0], ld_sem.at[0, 0]), local(gam_h, smv.at[0, :, gam_at], ld_sem.at[0, 1]),
              local(bet_h, smv.at[0, :, bet_at], ld_sem.at[1, 0]), local(bdn_h, bdn_s, ld_sem.at[1, 1])]
    sm_out = [send(bup_h, bup_s.at[1], sm_s.at[0], sm_r.at[0], 'col'),
              send(gam_h, smv.at[1, :, gam_at], sm_s.at[1], sm_r.at[1], 'col'),
              send(bet_h, smv.at[1, :, bet_at], sm_s.at[2], sm_r.at[2], 'col')]
    for cp in sm_own + sm_out:
        cp.start()
    @pl.when(b == 1)
    def _():
        w_cross(1)

    for kind in range(2):
        w_load(kind).start()
        w_row(kind).start()
    stream(x_h, theirs0, 0).start()
    stream(dy_h, theirs0, 1).start()
    w_cross(0)

    @pl.when(b == 0)
    def _():
        w_cross(1)

    stream(x_h, theirs0 + 1, 2).start()
    stream(dy_h, theirs0 + 1, 3).start()

    acc_d[...] = jnp.zeros_like(acc_d)
    acc_u[...] = jnp.zeros_like(acc_u)
    bup8[...] = jnp.zeros_like(bup8)
    gb8[...] = jnp.zeros_like(gb8)
    for cp in sm_own:
        cp.wait()

    def load(n):
        s = odd(n)
        rs = rows_of(chunk_at(n))
        return (local(x_h.at[rs, :], own.at[s], ld_sem.at[0, s]), local(dy_h.at[rs, :], aux.at[s], ld_sem.at[1, s]))

    for cp in load(0):
        cp.start()
    for kind in range(2):
        w_load(kind).wait()
        w_row(kind).wait()

    @pl.when(b == 0)
    def _():
        w_forward_x(1)
        w_forward_y(1)

    @pl.when(b == 1)
    def _():
        w_arrive(1)

    def w_rest():
        w_forward_x(0)

        @pl.when(b == 1)
        def _():
            w_forward_x(1)

        w_forward_y(0)

        @pl.when(b == 1)
        def _():
            w_forward_y(1)

        @pl.when(b == 0)
        def _():
            w_arrive(1)

        w_arrive(0)
        for kind in range(2):
            for sems in (wx_s, wy_s, wa_s, wb_s):
                all_of(w_half(kind), sems.at[kind]).wait()

    for cp in sm_out:
        cp.wait()
    for i in range(half_f // LANES):
        for side in range(2):
            smv[side, :, tile(i, LANES)] = bup_s[side, i:i + 1, :].astype(F32)
    for i in range(hw // LANES):
        smv[0, :, half_f + full + i * LANES:half_f + full + (i + 1) * LANES] = bdn_s[i:i + 1, :].astype(F32)

    def wide(at):
        return cat(smv[0, :, half_f + at:half_f + at + hw], smv[1, :, half_f + at:half_f + at + hw])

    def norm(s, slot, keep):
        gam, bet = wide(0), wide(hw)
        step = 32
        for i in range(M // step):
            rs = tile(i, step)
            xv = cat(own[s, rs, :], land[slot, rs, :]).astype(F32)
            mean = row_sum(xv) * (1.0 / full)
            cen = xv - mean
            istd = lax.rsqrt(row_sum(cen * cen) * (1.0 / full) + LN_EPS)
            xn[rs, :] = (cen * istd * gam + bet).astype(BF16)
            if keep:
                st[i * step // hq, i * step % hq:i * step % hq + step, :] = cat(jnp.broadcast_to(mean, (step, 64)), jnp.broadcast_to(istd, (step, 64)))
        dyv = aux[s]
        trd[...] = dyv.T
        gb8[:, 2 * full:2 * full + hw] += fold8(dyv.astype(F32))

    def write_y(s):
        bdn = smv[0, :, half_f + full:half_f + full + hw]
        yo[...] = (own[s].astype(F32) + yacc[...] + bdn).astype(BF16)

    def y_out(n):
        return local(yo, y_h.at[rows_of(chunk_at(n)), :], out_sem.at[0])

    def dx_out(n):
        return local(dxa, dx_h.at[rows_of(chunk_at(n)), :], out_sem.at[1])

    def dxo_out(n):
        return local(dxb, dxo_h.at[rows_of(n), :], out_sem.at[2])

    def dxl_out(n):
        return local(dxb, dxl_h.at[rows_of(n - (half_n - LATE)), :], out_sem.at[2])

    def saves(n, slot_x, slot_d):
        rs = rows_of(n)
        return (local(land.at[slot_x], xo_h.at[rs, :], sv_sem.at[0]), local(land.at[slot_d], dyo_h.at[rs, :], sv_sem.at[1]),
                local(dxn, dxn_h.at[n], sv_sem.at[2]), local(st, st_h.at[n], sv_sem.at[3]))

    def finish_dx(grads, xs, dys, stats):
        gam = wide(0)
        step = 32
        for i in range(M // step):
            rs = tile(i, step)
            h, hs = i * step // hq, slice(i * step % hq, i * step % hq + step)
            istd = stats[h, hs, 64:65]
            xh = (xs(rs).astype(F32) - stats[h, hs, 0:1]) * istd
            dv = grads(h, hs)
            px = dv * xh
            gb8[:, :full] += fold8(px)
            gb8[:, full:2 * full] += fold8(dv)
            m1 = row_sum(dv * gam) * (1.0 / full)
            m2 = row_sum(px * gam) * (1.0 / full)
            dxv = (dys(rs).astype(F32) + istd * (dv * gam - m1 - xh * m2)).astype(BF16)
            dxa[rs, :] = dxv[:, :hw]
            dxb[rs, :] = dxv[:, hw:]

    def dx_far(m):
        return send(dxo_h.at[rows_of(m), :], dx_h.at[rows_of(mine0 + m), :], dx_s, dx_r, 'col')

    def chunk_mine(n, carry):
        s = odd(n)
        slot_x, slot_d = lax.rem(2 * n, RING), lax.rem(2 * n + 1, RING)

        for cp in load(n):
            cp.wait()
        for cp in load(n + 1):
            cp.start()

        @pl.when(n == PROMPT + 1)
        def _():
            dx_far(0).start()

        stream(x_h, n, 2 * n).wait_recv()
        stream(dy_h, n, 2 * n + 1).wait_recv()
        save = saves(n, slot_x, slot_d)
        save[0].start()
        save[1].start()

        @pl.when(n > 0)
        def _():
            save[3].wait()

        norm(s, slot_x, True)
        save[3].start()
        trx[...] = xn[...].T

        @pl.when(n > 0)
        def _():
            save[2].wait()

        @pl.when((n > 0) & (n <= PROMPT))
        def _():
            dx_out(n).wait()
            dxo_out(n).wait()

        yacc[...] = jnp.zeros_like(yacc)
        dxn[...] = jnp.zeros_like(dxn)

        def quad(jj, inner):
            @pl.when((n == 0) & (jj == 1))
            def _():
                w_rest()

            @pl.when((n < half_n - 2) & (jj == 1))
            def _():
                stream_next(x_h, theirs0 + n + 2, 2 * n + 4)
                stream_next(dy_h, theirs0 + n + 2, 2 * n + 5)

            @pl.when((n >= half_n - 2) & (jj == 1))
            def _():
                k = 2 * (n - (half_n - 2))
                stream_next(x_h, mine0 + k, chunks + k)
                stream_next(x_h, mine0 + k + 1, chunks + k + 1)

            cols = [pl.ds(pl.multiple_of((own_tiles * jj + t) * FT, FT), FT) for t in range(own_tiles)]

            def first(t):
                bias = smv[jj, :, tile(t, FT)]
                us[t % 2] = (dot(xn[...], wu[:, cols[t]]) + bias).astype(BF16)
                dyv = cat(aux[s], land[slot_d])
                da_s[t % 2] = dot_t(dyv, wd[cols[t], :]).reshape(2, hq, FT)

            def mid(t):
                a, slope = gelu_and_slope(us[t % 2].astype(F32))
                act[t % 2] = a.astype(BF16)
                du = (da_s[t % 2].reshape(M, FT) * slope).astype(BF16)
                du_s[t % 2] = du
                bup8[:, cols[t]] += fold8(du.astype(F32))

            def last(t):
                yacc[...] += dot(act[t % 2], wd[cols[t], :hw])
                at = t * FT % half_d
                acc_d[jj, t * FT // half_d, :, at:at + FT] += dot(trd[...], act[t % 2])
                dxn[...] += dot_t(du_s[t % 2], wu[:, cols[t]]).reshape(2, hq, full)
                part = dot(trx[...], du_s[t % 2])
                for i in range(4):
                    acc_u[i // 2, i % 2, :, cols[t]] += part[tile(i, hq)]

            first(0)
            first(1)
            mid(0)
            for t in range(own_tiles):
                last(t)
                if t + 2 < own_tiles:
                    first(t + 2)
                if t + 1 < own_tiles:
                    mid(t + 1)
            return inner

        lax.fori_loop(0, 2, quad, 0)

        @pl.when(n > 0)
        def _():
            y_out(n).wait()

        write_y(s)
        y_out(n).start()
        save[2].start()

        @pl.when(n < PROMPT)
        def _():
            finish_dx(lambda h, rs: dxn[h, rs, :],
                      lambda rs: cat(own[s, rs, :], land[slot_x, rs, :]),
                      lambda rs: cat(aux[s, rs, :], land[slot_d, rs, :]), st)
            dx_out(n).start()
            dxo_out(n).start()

        save[0].wait()
        save[1].wait()
        give(2)
        return carry

    lax.fori_loop(0, half_n, chunk_mine, 0)

    order = [*range(own_tiles, tiles), *range(own_tiles)]

    def ru(p):
        return send(acc_u.at[1 - b, :, :, pl.ds(p * FT, FT)], rrow_h.at[p], ru_s, ru_r.at[p], 'row')

    def yu(p):
        return send(acc_u.at[b, 1 - d, :, pl.ds(p * FT, FT)], ryu_h.at[p], yu_s, yu_r.at[p], 'depth')

    def rx(k):
        return send(acc_u.at[b, d, :, pl.ds((own_tiles + k) * FT, FT)], rx_h.at[k], rx_s, rx_r.at[k], 'col')

    gu_rows = pl.ds(pl.multiple_of(d * hq, hq), hq)

    def ag(k):
        ps = pl.ds(k * FT, FT)
        return send(trx.at[pl.ds(k * hq, hq), :], gu_h.at[gu_rows, ps], ag_s, ag_r, 'depth')

    def gu_out(k):
        return local(trx.at[pl.ds(k * hq, hq), :], gu_h.at[gu_rows, pl.ds(k * FT, FT)], out_sem.at[3])

    def row_load(i, p):
        return local(rrow_h.at[p], da_s.at[i % 2], t_sem.at[i % 2, 0])

    for p in order:
        ru(p).start()
    y_out(0).wait()
    for cp in saves(half_n - 1, 0, 0)[2:]:
        cp.wait()
    ru(order[0]).wait_recv()
    row_load(0, order[0]).start()
    for i, p in enumerate(order):
        if i + 1 < tiles:
            ru(order[i + 1]).wait_recv()
            row_load(i + 1, order[i + 1]).start()
        row_load(i, p).wait()
        for h in range(2):
            acc_u[b, h, :, tile(p, FT)] += da_s[i % 2, h]
        yu(p).start()

    def oth_load(k):
        yu(own_tiles + k).wait_recv()
        local(ryu_h.at[own_tiles + k], da_s.at[k % 2, 0], t_sem.at[k % 2, 0]).start()

    def oth_send(k):
        p = own_tiles + k
        local(ryu_h.at[p], da_s.at[k % 2, 0], t_sem.at[k % 2, 0]).wait()
        acc_u[b, d, :, tile(p, FT)] += da_s[k % 2, 0]
        rx(k).start()

    def own_loads(k):
        return (local(ryu_h.at[k], da_s.at[k % 2, 0], t_sem.at[k % 2, 0]),
                local(rx_h.at[k], da_s.at[k % 2, 1], t_sem.at[k % 2, 1]))

    def own_load(k):
        yu(k).wait_recv()
        rx(k).wait_recv()
        for cp in own_loads(k):
            cp.start()

    def own_send(k):
        for cp in own_loads(k):
            cp.wait()
        trx[tile(k, hq), :] = (acc_u[b, d, :, tile(k, FT)] + da_s[k % 2, 0] + da_s[k % 2, 1]).astype(BF16)
        ag(k).start()

    def background(n):
        for k in range(own_tiles):
            @pl.when(n == half_n + 2 + k)
            def _():
                oth_send(k)

            @pl.when(n == half_n + 1 + k)
            def _():
                oth_load(k)

        for k in range(own_tiles - 1):
            @pl.when(n == half_n + 6 + k)
            def _():
                own_send(k)

            @pl.when(n == half_n + 5 + k)
            def _():
                if k >= 1:
                    pass
                own_load(k)

        for m in range(1, PROMPT):
            @pl.when(n == half_n + 4 + m)
            def _():
                dx_far(m).start()

    def chunk_theirs(n, carry):
        s = odd(n)
        q = n + half_n
        slot = lax.rem(q, RING)

        @pl.when(n == half_n)
        def _():
            stream_next(x_h, mine0 + 4, chunks + 4)

        @pl.when(n <= half_n + 2)
        def _():
            stream_next(x_h, mine0 + 5 + (n - half_n), chunks + 5 + (n - half_n))

        background(n)
        for cp in load(n):
            cp.wait()

        @pl.when(n < chunks - 1)
        def _():
            for cp in load(n + 1):
                cp.start()

        stream(x_h, n, q).wait_recv()
        norm(s, slot, False)

        def up(j):
            side, at = divmod(j * FT, half_f)
            us[j % 2] = (dot(xn[...], wu[:, tile(j, FT)]) + smv[side, :, at:at + FT]).astype(BF16)

        def mid(j):
            act[j % 2] = gelu(us[j % 2].astype(F32)).astype(BF16)

        def down(j):
            part = dot(act[j % 2], wd[tile(j, FT), :hw])
            yacc[...] = part if j == 0 else yacc[...] + part
            blk, rest = divmod(j * FT, half_f)
            qt, at = divmod(rest, half_d)
            acc_d[blk, qt, :, at:at + FT] += dot(trd[...], act[j % 2])

        up(0)
        up(1)
        mid(0)
        for j in range(tiles):
            if j + 2 < tiles:
                up(j + 2)
            down(j)
            if j + 1 < tiles:
                mid(j + 1)

        @pl.when(n > half_n)
        def _():
            y_out(n).wait()

        write_y(s)
        y_out(n).start()

        @pl.when(n < half_n + 2)
        def _():
            give(1)
        return carry

    lax.fori_loop(half_n, chunks, chunk_theirs, 0)

    rdn = send(acc_d.at[1 - b], rdn_h, rdn_s, rdn_r, 'row')
    rdn.start()
    k = own_tiles - 1
    own_send(k - 1)
    own_load(k)
    own_send(k)
    for k in range(own_tiles):
        gu_out(k).start()
    all_of(acc_u.at[1 - b], ru_s).wait()

    def load_dx(n):
        s = odd(n)
        rs, ks = rows_of(n), rows_of(mine0 + n)
        return (local(x_h.at[ks, :], own.at[s], ld_sem.at[0, s]), local(dy_h.at[ks, :], aux.at[s], ld_sem.at[1, s]),
                local(xo_h.at[rs, :], land.at[2 * s], ld_sem.at[2, s]), local(dyo_h.at[rs, :], land.at[2 * s + 1], ld_sem.at[3, s]),
                local(dxn_h.at[n], acc_u.at[1 - b, :, :, pl.ds(pl.multiple_of(s * full, full), full)], ld_sem.at[4, s]),
                local(st_h.at[n], da_s.at[s, :, :, head(LANES)], ld_sem.at[5, s]))

    held = 2

    def chunk_dx(n, carry):
        s = odd(n)
        for cp in load_dx(n):
            cp.wait()

        @pl.when(n < half_n - 1)
        def _():
            for cp in load_dx(n + 1):
                cp.start()

        @pl.when(n > PROMPT)
        def _():
            dx_out(n).wait()
            dxo_out(n).wait()

        @pl.when((n > PROMPT) & (n <= half_n - LATE - held))
        def _():
            dx_far(n - 1).start()

        finish_dx(lambda h, rs: acc_u[1 - b, h, rs, pl.ds(pl.multiple_of(s * full, full), full)],
                  lambda rs: cat(own[s, rs, :], land[2 * s, rs, :]),
                  lambda rs: cat(aux[s, rs, :], land[2 * s + 1, rs, :]), da_s.at[s, :, :, head(LANES)])
        dx_out(n).start()

        @pl.when(n < half_n - LATE)
        def _():
            dxo_out(n).start()

        @pl.when(n >= half_n - LATE)
        def _():
            dxl_out(n).start()
        return carry

    for cp in load_dx(PROMPT):
        cp.start()
    lax.fori_loop(PROMPT, 2 * PROMPT, chunk_dx, 0)
    rdn.wait()
    rd_load = local(rdn_h, acc_d.at[1 - b], t_sem.at[0, 0])
    rd_load.start()
    rd_load.wait()
    steps = hw // LANES

    def ydn(i):
        return send(acc_d.at[b, 1 - d, pl.ds(i * LANES, LANES), :], ydn_h.at[i], ydn_s, ydn_r.at[i], 'depth')

    for i in range(steps):
        rs = tile(i, LANES)
        for qt in range(2):
            acc_d[b, qt, rs, :] += acc_d[1 - b, qt, rs, :]
        ydn(i).start()
    lax.fori_loop(2 * PROMPT, half_n, chunk_dx, 0)
    y_out(chunks - 1).wait()
    oth = lambda at, n: [col_sum(ref[:, a:a + n]) for ref, a in at]
    gso[...] = jnp.concatenate(oth(((bup8, half_f),), half_f) + oth(((gb8, hw), (gb8, full + hw)), hw)
                               + [jnp.zeros((1, half_f - full), F32)], axis=1)
    gs_col = send(gso, gsl.at[0], gs_s.at[0], gs_r.at[0], 'col')
    gs_col.start()
    for m in range(half_n - LATE - held, half_n - LATE):
        dx_far(m).start()
    dx_out(half_n - 1).wait()
    dxl_out(half_n - 1).wait()
    gs_col.wait()
    gsp[0] = jnp.concatenate(oth(((bup8, 0),), half_f) + oth(((gb8, 0), (gb8, full), (gb8, 2 * full)), hw)
                             + [jnp.zeros((1, half_f - 3 * hw), F32)], axis=1) + gsl[0]
    gs_row = send(gsp.at[0], gsl.at[1], gs_s.at[1], gs_r.at[1], 'row')
    gs_row.start()
    gs_row.wait()
    gsp[1] = gsp[0] + gsl[1]
    gs_dep = send(gsp.at[1], gsl.at[2], gs_s.at[2], gs_r.at[2], 'depth')
    gs_dep.start()
    for q in range(3 * half_n - RING, 3 * half_n):
        stream(x_h, 0, q).wait_send()
    all_of(acc_u.at[b, 1 - d], yu_s).wait()
    all_of(acc_u.at[b, d, :, pl.ds(half_f, half_f)], rx_s).wait()
    all_of(trx, out_sem.at[3]).wait()
    for i in range(steps):
        ydn(i).wait_recv()
        dn_load = local(ydn_h.at[i], acc_d.at[1 - b, 0, pl.ds(i * LANES, LANES), :], t_sem.at[1, 0])
        dn_load.start()
        dn_load.wait()
        rs = tile(i, LANES)
        for j in range(half_d // LANES):
            cs = tile(j, LANES)
            total = acc_d[b, d, rs, cs] + acc_d[1 - b, 0, rs, cs]
            us[j * LANES // M, j * LANES % M:j * LANES % M + LANES, rs] = total.T.astype(BF16)
    gd_out = [local(us.at[i], gd_h.at[pl.ds(i * M, M), :], t_sem.at[i, 1]) for i in range(2)]
    for cp in gd_out:
        cp.start()
    gs_dep.wait()
    gsp[0] = gsp[1] + gsl[2]
    gs_out = local(gsp.at[0], gs_h, out_sem.at[0])
    gs_out.start()
    all_of(acc_d.at[b, 1 - d], ydn_s).wait()
    for sem in (ag_s, ag_r):
        all_of(trx, sem).wait()
    sent = dxo_h.at[head((half_n - LATE) * M), :]
    for sem in (dx_s, dx_r):
        all_of(sent, sem).wait()
    for cp in gd_out:
        cp.wait()
    gs_out.wait()


def finish_kernel(y_in, dx_in, gwu_in, gd, gs, y, dx, gwu, gwd, gbup, ggam, gbet, gbdn, big, small, sums, in_sem, out_sem):
    rows, hw = y.shape
    half_f = gwd.shape[0]
    d = lax.axis_index('depth')
    n = rows // COPIES
    ins, outs = [], []

    def move(src, buf, *dst):
        ins.append(pltpu.make_async_copy(src, buf, in_sem.at[len(ins)]))
        outs.append([pltpu.make_async_copy(buf, to, out_sem) for to in dst])

    for i in range(COPIES):
        rs = pl.ds(i * n, n)
        move(y_in.at[rs], big.at[0, rs], y.at[rs])
        move(dx_in.at[rs], big.at[1, rs], dx.at[rs])
    move(gwu_in, small.at[:, head(half_f)], gwu)
    move(gd, big.at[2, head(half_f // 2)], gwd.at[pl.ds(pl.multiple_of(d * (half_f // 2), half_f // 2), half_f // 2)])
    parts = [(0, half_f, gbup), (half_f, hw, ggam), (half_f + hw, hw, gbet), (half_f + 2 * hw, hw, gbdn)]
    move(gs, sums)
    outs[-1] = [pltpu.make_async_copy(sums.at[:, pl.ds(a, w)], dst, out_sem) for a, w, dst in parts]
    for cp in ins:
        cp.start()
    for cp, tos in zip(ins, outs):
        cp.wait()
        for to in tos:
            to.start()
    for tos in outs:
        for to in tos:
            to.wait()


def solution(mesh):
    tok_spec = P(('dp', 'depth', 'row'), 'col')
    vec_spec = P('col')
    mat_spec = P('row', 'col')
    grad_vec = P(('dp', 'col'))
    grad_mat = P(('dp', 'row'), 'col')
    swap = ((0, 1), (1, 0))

    def local_pass(x, gamma, beta, w_up, b_up, w_down, b_down, dy):
        rows, hw = x.shape
        half_f = b_up.shape[0]
        full_f, full, hq = 2 * half_f, 2 * hw, hw // 2
        chunks = rows // M
        late = LATE * M
        hbm = pl.BlockSpec(memory_space=pltpu.HBM)
        sds = jax.ShapeDtypeStruct
        V, D = pltpu.VMEM, pltpu.SemaphoreType.DMA
        D2, D3, D4, D2S = D((2,)), D((3,)), D((4,)), D((2, SUBS))
        tiles, own_tiles = full_f // FT, half_f // FT
        outs = [
            sds((rows, hw), BF16), sds((rows, hw), BF16), sds((late, hw), BF16), sds((1, full_f), F32), sds((hw, half_f), BF16),
            sds((half_f // 2, hw), BF16),
            sds((rows // 2, hw), BF16), sds((tiles, 2, hq, FT), F32), sds((tiles, hq, FT), F32), sds((own_tiles, hq, FT), F32),
            sds((2, hw, half_f // 2), F32), sds((hw // LANES, LANES, half_f // 2), F32),
            sds((rows // 2, hw), BF16), sds((rows // 2, hw), BF16), sds((chunks // 2, 2, hq, full), F32), sds((chunks // 2, 2, hq, LANES), F32),
        ]
        scratch = [
            V((full, full_f), BF16), V((full_f, full), BF16), V((2, 2, hw, half_f // 2), F32), V((2, 2, hq, full_f), F32),
            V((2, M, hw), BF16), V((RING, M, hw), BF16), V((2, M, hw), BF16), V((M, full), BF16), V((full, M), BF16), V((hw, M), BF16),
            V((2, hq, LANES), F32), V((2, M, FT), BF16), V((2, 2, hq, FT), F32), V((2, M, FT), BF16), V((2, M, FT), BF16),
            V((M, hw), F32), V((2, hq, full), F32), V((M, hw), BF16), V((M, hw), BF16), V((M, hw), BF16),
            V((8, full_f), F32), V((8, 2 * full + hw), F32), V((2, 1, full_f), F32), V((2, half_f // LANES, LANES), BF16), V((hw // LANES, LANES), BF16),
            V((1, full_f), F32), V((2, 1, full_f), F32), V((3, 1, full_f), F32),
            D2, D2, D2, D2S, D2, D2S, D2, D2S, D2, D2S, D3, D3,
            D((RING,)), D((RING,)), D((6, 2)), D4, D4, D((2, 2)), D(()), D((tiles,)), D(()), D((tiles,)), D(()), D((own_tiles,)),
            D(()), D(()), D(()), D(()), D(()), D((hw // LANES,)), D(()), D(()), D3, D3, pltpu.SemaphoreType.REGULAR,
        ]
        res = pl.pallas_call(
            kernel,
            out_shape=outs,
            in_specs=[hbm] * 8,
            out_specs=[hbm] * len(outs),
            scratch_shapes=scratch,
            compiler_params=pltpu.CompilerParams(
                collective_id=0, has_side_effects=True, vmem_limit_bytes=67043328),
            cost_estimate=pl.CostEstimate(flops=14 * rows * full * full_f, bytes_accessed=2 ** 27, transcendentals=rows * full_f),
            name='mlp_block',
        )(x, dy, w_up, w_down, b_up.reshape(-1, LANES), gamma.reshape(1, -1), beta.reshape(1, -1), b_down.reshape(-1, LANES))
        y, dx, dxl, gs, gwu, gd = res[:6]
        gd_far = lax.ppermute(gd, 'depth', swap)
        dx_far = lax.ppermute(dxl, 'col', swap)
        moves = 2 * COPIES + 3
        y, dx, gwu, gwd, gbup, ggam, gbet, gbdn = pl.pallas_call(
            finish_kernel,
            out_shape=[sds((rows, hw), BF16), sds((rows, hw), BF16), sds((hw, half_f), BF16), sds((half_f, hw), BF16),
                       sds((1, half_f), F32), sds((1, hw), F32), sds((1, hw), F32), sds((1, hw), F32)],
            in_specs=[hbm] * 5,
            out_specs=[hbm] * 8,
            scratch_shapes=[V((3, rows, hw), BF16), V((hw, half_f), BF16), V((1, full_f), F32), D((moves,)), D(())],
            compiler_params=pltpu.CompilerParams(vmem_limit_bytes=62000000),
            cost_estimate=pl.CostEstimate(flops=2 ** 33, bytes_accessed=42 * 2 ** 20, transcendentals=0),
            name='finish',
        )(y, dx, gwu, gd, gs)
        gwd = lax.dynamic_update_slice(gwd, gd_far, ((1 - lax.axis_index('depth')) * (half_f // 2), 0))
        dx = lax.dynamic_update_slice(dx, dx_far, ((1 - lax.axis_index('col')) * (rows // 2) + rows // 2 - late, 0))
        return y, dx, ggam.reshape(-1), gbet.reshape(-1), gwu, gbup.reshape(-1), gwd, gbdn.reshape(-1)

    return jax.shard_map(
        local_pass,
        mesh=mesh,
        in_specs=(tok_spec, vec_spec, vec_spec, mat_spec, vec_spec, mat_spec, vec_spec, tok_spec),
        out_specs=(tok_spec, tok_spec, grad_vec, grad_vec, grad_mat, grad_vec, grad_mat, grad_vec),
        check_vma=False,
    )
```

```python
import jax
import jax.numpy as jnp
from jax import lax
from jax.experimental import pallas as pl
from jax.experimental.pallas import tpu as pltpu
from jax.sharding import PartitionSpec as P

LN_EPS = 1e-5
C0 = 0.7978845608
C1 = C0 * 0.044715
M = 512
FT = 512
SUBS = 4
RING = 6
LATE = 2
PROMPT = 2
COPIES = 4
LANES = 128
BF16, F32 = jnp.bfloat16, jnp.float32
MESH = pl.DeviceIdType.MESH


def dot(lhs, rhs, rhs_dim=0):
    return lax.dot_general(lhs, rhs, (((1,), (rhs_dim,)), ((), ())), preferred_element_type=F32)


def dot_t(lhs, rhs):
    return dot(lhs, rhs, 1)


def odd(n):
    return lax.rem(n, 2)


def cat(*parts):
    return jnp.concatenate(parts, axis=1)


def row_sum(v):
    return jnp.sum(v, axis=1, keepdims=True)


def col_sum(v):
    return jnp.sum(v, axis=0, keepdims=True)


def head(n):
    return pl.ds(0, n)


def tile(i, n):
    return slice(i * n, (i + 1) * n)


def gelu(v):
    t = jnp.tanh(v * (C1 * (v * v) + C0))
    h = 0.5 * v
    return h * t + h


def gelu_and_slope(v):
    v2 = v * v
    t = jnp.tanh(v * (C1 * v2 + C0))
    h = 0.5 * v
    slope = (v * (1.0 - t * t)) * (1.5 * C1 * v2 + 0.5 * C0) + (0.5 * t + 0.5)
    return h * t + h, slope


def fold8(v):
    return jnp.sum(v.reshape(v.shape[0] // 8, 8, v.shape[1]), axis=0)


def kernel(x_h, dy_h, wu_h, wd_h, bup_h, gam_h, bet_h, bdn_h,
           y_h, dx_h, dxl_h, gs_h, gu_h, gd_h, dxo_h, rrow_h, ryu_h, rx_h, rdn_h, ydn_h, xo_h, dyo_h, dxn_h, st_h,
           wu, wd, acc_d, acc_u, own, land, aux, xn, trx, trd, st, us, da_s, act, du_s, yacc, dxn, yo, dxa, dxb,
           bup8, gb8, smv, bup_s, bdn_s, gso, gsp, gsl,
           wrow_s, wrow_r, wx_s, wx_r, wy_s, wy_r, wa_s, wa_r, wb_s, wb_r, sm_s, sm_r,
           land_s, land_r, ld_sem, out_sem, sv_sem, t_sem, ru_s, ru_r, yu_s, yu_r, rx_s, rx_r, ag_s, ag_r, rdn_s, rdn_r,
           ydn_s, ydn_r, dx_s, dx_r, gs_s, gs_r, credit):
    chunks = x_h.shape[0] // M
    half_n = chunks // 2
    half_f = wu_h.shape[1]
    hw = x_h.shape[1]
    full = 2 * hw
    hq = hw // 2
    half_d = half_f // 2
    tiles = 2 * half_f // FT
    own_tiles = tiles // 2
    c, r, d = lax.axis_index('col'), lax.axis_index('row'), lax.axis_index('depth')
    b = lax.rem(r + c, 2)
    peer = {'col': 1 - c, 'row': 1 - r, 'depth': 1 - d}
    mine0, theirs0 = c * half_n, (1 - c) * half_n

    def send(src, dst, s_sem, r_sem, axis):
        return pltpu.make_async_remote_copy(src_ref=src, dst_ref=dst, send_sem=s_sem, recv_sem=r_sem,
                                            device_id={axis: peer[axis]}, device_id_type=MESH)

    def local(src, dst, sem):
        return pltpu.make_async_copy(src, dst, sem)

    def all_of(ref, sem):
        return pltpu.make_async_copy(ref, ref, sem)

    def rows_of(k):
        return pl.ds(pl.multiple_of(k * M, M), M)

    def chunk_at(n):
        return lax.rem(mine0 + n, chunks)

    bar = pltpu.get_barrier_semaphore()
    for axis in ('col', 'row', 'depth'):
        pl.semaphore_signal(bar, inc=1, device_id={axis: peer[axis]}, device_id_type=MESH)
    pl.semaphore_wait(bar, 3)

    half_rows = (hq, half_d)
    w_srcs = (wu_h, wd_h)

    def w_cols(kind, blk, dep, s):
        n = half_rows[kind] // SUBS
        if kind == 0:
            return wu.at[pl.ds(pl.multiple_of(blk * hw + dep * hq + s * n, n), n), pl.ds(half_f, half_f)]
        return wd.at[pl.ds(pl.multiple_of(blk * half_f + dep * half_d + s * n, n), n), pl.ds(hw, hw)]

    def w_half(kind):
        return wu.at[head(hq), head(half_f)] if kind == 0 else wd.at[head(half_d), head(hw)]

    def w_own(kind):
        if kind == 0:
            return wu.at[pl.ds(pl.multiple_of(b * hw, hw), hw), head(half_f)]
        return wd.at[pl.ds(pl.multiple_of(b * half_f, half_f), half_f), head(hw)]

    def w_x(kind, s):
        n = half_rows[kind] // SUBS
        src = w_srcs[kind].at[pl.ds(pl.multiple_of(d * half_rows[kind] + s * n, n), n), :]
        return send(src, w_cols(kind, 1 - b, d, s), wx_s.at[kind], wx_r.at[kind, s], 'col')

    def w_y(kind, s):
        return send(w_cols(kind, b, d, s), w_cols(kind, b, d, s), wy_s.at[kind], wy_r.at[kind, s], 'depth')

    def w_a(kind, s):
        return send(w_cols(kind, b, d, s), w_cols(kind, b, d, s), wa_s.at[kind], wa_r.at[kind, s], 'row')

    def w_b(kind, s):
        return send(w_cols(kind, b, 1 - d, s), w_cols(kind, b, 1 - d, s), wb_s.at[kind], wb_r.at[kind, s], 'row')

    def w_row(kind):
        return send(w_srcs[kind], w_own(kind), wrow_s.at[kind], wrow_r.at[kind], 'row')

    def w_load(kind):
        return local(w_srcs[kind], w_own(kind), out_sem.at[kind])

    def w_cross(kind):
        for s in range(SUBS):
            w_x(kind, s).start()

    def w_forward_x(kind):
        for s in range(SUBS):
            w_x(kind, s).wait_recv()
            w_y(kind, s).start()
            w_a(kind, s).start()

    def w_forward_y(kind):
        for s in range(SUBS):
            w_y(kind, s).wait_recv()
            w_b(kind, s).start()

    def w_arrive(kind):
        for s in range(SUBS):
            w_a(kind, s).wait_recv()
            w_b(kind, s).wait_recv()

    def stream(src, k, q):
        slot = lax.rem(q, RING)
        return send(src.at[rows_of(k), :], land.at[slot], land_s.at[slot], land_r.at[slot], 'col')

    def stream_next(src, k, q):
        @pl.when(q >= RING)
        def _():
            stream(src, k, q).wait_send()
            pl.semaphore_wait(credit, 1)
        stream(src, k, q).start()

    def give(n):
        for _ in range(n):
            pl.semaphore_signal(credit, inc=1, device_id={'col': peer['col']}, device_id_type=MESH)

    gam_at, bet_at = pl.ds(half_f, hw), pl.ds(half_f + hw, hw)
    sm_own = [local(bup_h, bup_s.at[0], ld_sem.at[0, 0]), local(gam_h, smv.at[0, :, gam_at], ld_sem.at[0, 1]),
              local(bet_h, smv.at[0, :, bet_at], ld_sem.at[1, 0]), local(bdn_h, bdn_s, ld_sem.at[1, 1])]
    sm_out = [send(bup_h, bup_s.at[1], sm_s.at[0], sm_r.at[0], 'col'),
              send(gam_h, smv.at[1, :, gam_at], sm_s.at[1], sm_r.at[1], 'col'),
              send(bet_h, smv.at[1, :, bet_at], sm_s.at[2], sm_r.at[2], 'col')]
    for cp in sm_own + sm_out:
        cp.start()
    @pl.when(b == 1)
    def _():
        w_cross(1)

    for kind in range(2):
        w_load(kind).start()
        w_row(kind).start()
    stream(x_h, theirs0, 0).start()
    stream(dy_h, theirs0, 1).start()
    w_cross(0)

    @pl.when(b == 0)
    def _():
        w_cross(1)

    stream(x_h, theirs0 + 1, 2).start()
    stream(dy_h, theirs0 + 1, 3).start()

    acc_d[...] = jnp.zeros_like(acc_d)
    acc_u[...] = jnp.zeros_like(acc_u)
    bup8[...] = jnp.zeros_like(bup8)
    gb8[...] = jnp.zeros_like(gb8)
    for cp in sm_own:
        cp.wait()

    def load(n):
        s = odd(n)
        rs = rows_of(chunk_at(n))
        return (local(x_h.at[rs, :], own.at[s], ld_sem.at[0, s]), local(dy_h.at[rs, :], aux.at[s], ld_sem.at[1, s]))

    for cp in load(0):
        cp.start()
    for kind in range(2):
        w_load(kind).wait()
        w_row(kind).wait()

    @pl.when(b == 0)
    def _():
        w_forward_x(1)
        w_forward_y(1)

    @pl.when(b == 1)
    def _():
        w_arrive(1)

    def w_rest():
        w_forward_x(0)

        @pl.when(b == 1)
        def _():
            w_forward_x(1)

        w_forward_y(0)

        @pl.when(b == 1)
        def _():
            w_forward_y(1)

        @pl.when(b == 0)
        def _():
            w_arrive(1)

        w_arrive(0)
        for kind in range(2):
            for sems in (wx_s, wy_s, wa_s, wb_s):
                all_of(w_half(kind), sems.at[kind]).wait()

    for cp in sm_out:
        cp.wait()
    for i in range(half_f // LANES):
        for side in range(2):
            smv[side, :, tile(i, LANES)] = bup_s[side, i:i + 1, :].astype(F32)
    for i in range(hw // LANES):
        smv[0, :, half_f + full + i * LANES:half_f + full + (i + 1) * LANES] = bdn_s[i:i + 1, :].astype(F32)

    def wide(at):
        return cat(smv[0, :, half_f + at:half_f + at + hw], smv[1, :, half_f + at:half_f + at + hw])

    def norm(s, slot, keep):
        gam, bet = wide(0), wide(hw)
        step = 32
        for i in range(M // step):
            rs = tile(i, step)
            xv = cat(own[s, rs, :], land[slot, rs, :]).astype(F32)
            mean = row_sum(xv) * (1.0 / full)
            cen = xv - mean
            istd = lax.rsqrt(row_sum(cen * cen) * (1.0 / full) + LN_EPS)
            xn[rs, :] = (cen * istd * gam + bet).astype(BF16)
            if keep:
                st[i * step // hq, i * step % hq:i * step % hq + step, :] = cat(jnp.broadcast_to(mean, (step, 64)), jnp.broadcast_to(istd, (step, 64)))
        dyv = aux[s]
        trd[...] = dyv.T
        gb8[:, 2 * full:2 * full + hw] += fold8(dyv.astype(F32))

    def write_y(s):
        bdn = smv[0, :, half_f + full:half_f + full + hw]
        yo[...] = (own[s].astype(F32) + yacc[...] + bdn).astype(BF16)

    def y_out(n):
        return local(yo, y_h.at[rows_of(chunk_at(n)), :], out_sem.at[0])

    def dx_out(n):
        return local(dxa, dx_h.at[rows_of(chunk_at(n)), :], out_sem.at[1])

    def dxo_out(n):
        return local(dxb, dxo_h.at[rows_of(n), :], out_sem.at[2])

    def dxl_out(n):
        return local(dxb, dxl_h.at[rows_of(n - (half_n - LATE)), :], out_sem.at[2])

    def saves(n, slot_x, slot_d):
        rs = rows_of(n)
        return (local(land.at[slot_x], xo_h.at[rs, :], sv_sem.at[0]), local(land.at[slot_d], dyo_h.at[rs, :], sv_sem.at[1]),
                local(dxn, dxn_h.at[n], sv_sem.at[2]), local(st, st_h.at[n], sv_sem.at[3]))

    def finish_dx(grads, xs, dys, stats):
        gam = wide(0)
        step = 32
        for i in range(M // step):
            rs = tile(i, step)
            h, hs = i * step // hq, slice(i * step % hq, i * step % hq + step)
            istd = stats[h, hs, 64:65]
            xh = (xs(rs).astype(F32) - stats[h, hs, 0:1]) * istd
            dv = grads(h, hs)
            px = dv * xh
            gb8[:, :full] += fold8(px)
            gb8[:, full:2 * full] += fold8(dv)
            m1 = row_sum(dv * gam) * (1.0 / full)
            m2 = row_sum(px * gam) * (1.0 / full)
            dxv = (dys(rs).astype(F32) + istd * (dv * gam - m1 - xh * m2)).astype(BF16)
            dxa[rs, :] = dxv[:, :hw]
            dxb[rs, :] = dxv[:, hw:]

    def dx_far(m):
        return send(dxo_h.at[rows_of(m), :], dx_h.at[rows_of(mine0 + m), :], dx_s, dx_r, 'col')

    def dx_part(m, h):
        n = M // 2
        src, dst = (pl.ds(pl.multiple_of(k * M + h * n, n), n) for k in (m, mine0 + m))
        return send(dxo_h.at[src, :], dx_h.at[dst, :], dx_s, dx_r, 'col')

    def ru(p):
        return send(acc_u.at[1 - b, :, :, pl.ds(p * FT, FT)], rrow_h.at[p], ru_s, ru_r.at[p], 'row')

    def yu(p):
        return send(acc_u.at[b, 1 - d, :, pl.ds(p * FT, FT)], ryu_h.at[p], yu_s, yu_r.at[p], 'depth')

    def row_load(i, p):
        return local(rrow_h.at[p], da_s.at[i % 2], t_sem.at[i % 2, 0])

    def row_add(i, p):
        row_load(i, p).wait()
        for h in range(2):
            acc_u[b, h, :, tile(p, FT)] += da_s[i % 2, h]
        yu(p).start()

    def chunk_mine(n, carry):
        s = odd(n)
        slot_x, slot_d = lax.rem(2 * n, RING), lax.rem(2 * n + 1, RING)

        for cp in load(n):
            cp.wait()
        for cp in load(n + 1):
            cp.start()

        @pl.when(n == PROMPT + 1)
        def _():
            dx_far(0).start()

        @pl.when(n == 2 * PROMPT + 1)
        def _():
            dx_part(1, 0).start()

        stream(x_h, n, 2 * n).wait_recv()
        stream(dy_h, n, 2 * n + 1).wait_recv()
        save = saves(n, slot_x, slot_d)
        save[0].start()
        save[1].start()

        @pl.when(n > 0)
        def _():
            save[3].wait()

        norm(s, slot_x, True)
        save[3].start()
        trx[...] = xn[...].T

        @pl.when(n > 0)
        def _():
            save[2].wait()

        @pl.when((n > 0) & (n <= PROMPT))
        def _():
            dx_out(n).wait()
            dxo_out(n).wait()

        yacc[...] = jnp.zeros_like(yacc)
        dxn[...] = jnp.zeros_like(dxn)

        def quad(jj, inner):
            @pl.when((n == 0) & (jj == 1))
            def _():
                w_rest()

            @pl.when((n == half_n - 1) & (jj == 1))
            def _():
                for p in range(own_tiles):
                    ru(p).start()
                ru(0).wait_recv()
                row_load(0, 0).start()
                row_add(0, 0)

            @pl.when((n < half_n - 2) & (jj == 1))
            def _():
                stream_next(x_h, theirs0 + n + 2, 2 * n + 4)
                stream_next(dy_h, theirs0 + n + 2, 2 * n + 5)

            @pl.when((n >= half_n - 2) & (jj == 1))
            def _():
                k = 2 * (n - (half_n - 2))
                stream_next(x_h, mine0 + k, chunks + k)
                stream_next(x_h, mine0 + k + 1, chunks + k + 1)

            cols = [pl.ds(pl.multiple_of((own_tiles * jj + t) * FT, FT), FT) for t in range(own_tiles)]

            def first(t):
                bias = smv[jj, :, tile(t, FT)]
                us[t % 2] = (dot(xn[...], wu[:, cols[t]]) + bias).astype(BF16)
                dyv = cat(aux[s], land[slot_d])
                da_s[t % 2] = dot_t(dyv, wd[cols[t], :]).reshape(2, hq, FT)

            def mid(t):
                a, slope = gelu_and_slope(us[t % 2].astype(F32))
                act[t % 2] = a.astype(BF16)
                du = (da_s[t % 2].reshape(M, FT) * slope).astype(BF16)
                du_s[t % 2] = du
                bup8[:, cols[t]] += fold8(du.astype(F32))

            def last(t):
                yacc[...] += dot(act[t % 2], wd[cols[t], :hw])
                at = t * FT % half_d
                acc_d[jj, t * FT // half_d, :, at:at + FT] += dot(trd[...], act[t % 2])
                dxn[...] += dot_t(du_s[t % 2], wu[:, cols[t]]).reshape(2, hq, full)
                part = dot(trx[...], du_s[t % 2])
                for i in range(4):
                    acc_u[i // 2, i % 2, :, cols[t]] += part[tile(i, hq)]

            first(0)
            first(1)
            mid(0)
            for t in range(own_tiles):
                last(t)
                if t + 2 < own_tiles:
                    first(t + 2)
                if t + 1 < own_tiles:
                    mid(t + 1)
            return inner

        lax.fori_loop(0, 2, quad, 0)

        @pl.when(n > 0)
        def _():
            y_out(n).wait()

        write_y(s)
        y_out(n).start()
        save[2].start()

        @pl.when(n < PROMPT)
        def _():
            finish_dx(lambda h, rs: dxn[h, rs, :],
                      lambda rs: cat(own[s, rs, :], land[slot_x, rs, :]),
                      lambda rs: cat(aux[s, rs, :], land[slot_d, rs, :]), st)
            dx_out(n).start()
            dxo_out(n).start()

        save[0].wait()
        save[1].wait()
        give(2)
        return carry

    lax.fori_loop(0, half_n, chunk_mine, 0)

    order = [*range(own_tiles, tiles), *range(1, own_tiles)]

    def rx(k):
        return send(acc_u.at[b, d, :, pl.ds((own_tiles + k) * FT, FT)], rx_h.at[k], rx_s, rx_r.at[k], 'col')

    gu_rows = pl.ds(pl.multiple_of(d * hq, hq), hq)

    def ag(k):
        ps = pl.ds(k * FT, FT)
        return send(trx.at[pl.ds(k * hq, hq), :], gu_h.at[gu_rows, ps], ag_s, ag_r, 'depth')

    def gu_out(k):
        return local(trx.at[pl.ds(k * hq, hq), :], gu_h.at[gu_rows, pl.ds(k * FT, FT)], out_sem.at[3])

    for p in order[:own_tiles]:
        ru(p).start()
    y_out(0).wait()
    for cp in saves(half_n - 1, 0, 0)[2:]:
        cp.wait()
    ru(order[0]).wait_recv()
    row_load(0, order[0]).start()
    for i, p in enumerate(order):
        if i + 1 < len(order):
            ru(order[i + 1]).wait_recv()
            row_load(i + 1, order[i + 1]).start()
        row_add(i, p)

    def oth_load(k):
        yu(own_tiles + k).wait_recv()
        local(ryu_h.at[own_tiles + k], da_s.at[k % 2, 0], t_sem.at[k % 2, 0]).start()

    def oth_send(k):
        p = own_tiles + k
        local(ryu_h.at[p], da_s.at[k % 2, 0], t_sem.at[k % 2, 0]).wait()
        acc_u[b, d, :, tile(p, FT)] += da_s[k % 2, 0]
        rx(k).start()

    def own_loads(k):
        return (local(ryu_h.at[k], da_s.at[k % 2, 0], t_sem.at[k % 2, 0]),
                local(rx_h.at[k], da_s.at[k % 2, 1], t_sem.at[k % 2, 1]))

    def own_load(k):
        yu(k).wait_recv()
        rx(k).wait_recv()
        for cp in own_loads(k):
            cp.start()

    def own_send(k):
        for cp in own_loads(k):
            cp.wait()
        trx[tile(k, hq), :] = (acc_u[b, d, :, tile(k, FT)] + da_s[k % 2, 0] + da_s[k % 2, 1]).astype(BF16)
        ag(k).start()

    def background(n):
        for k in range(own_tiles):
            @pl.when(n == half_n + 2 + k)
            def _():
                oth_send(k)

            @pl.when(n == half_n + 1 + k)
            def _():
                oth_load(k)

        for k in range(own_tiles - 1):
            @pl.when(n == half_n + 6 + k)
            def _():
                own_send(k)

            @pl.when(n == half_n + 5 + k)
            def _():
                own_load(k)

        @pl.when(n == half_n + own_tiles + 1)
        def _():
            dx_part(1, 1).start()

    def chunk_theirs(n, carry):
        s = odd(n)
        q = n + half_n
        slot = lax.rem(q, RING)

        @pl.when(n == half_n)
        def _():
            stream_next(x_h, mine0 + 4, chunks + 4)

        @pl.when(n <= half_n + 2)
        def _():
            stream_next(x_h, mine0 + 5 + (n - half_n), chunks + 5 + (n - half_n))

        background(n)
        for cp in load(n):
            cp.wait()

        @pl.when(n < chunks - 1)
        def _():
            for cp in load(n + 1):
                cp.start()

        stream(x_h, n, q).wait_recv()
        norm(s, slot, False)

        def up(j):
            side, at = divmod(j * FT, half_f)
            us[j % 2] = (dot(xn[...], wu[:, tile(j, FT)]) + smv[side, :, at:at + FT]).astype(BF16)

        def mid(j):
            act[j % 2] = gelu(us[j % 2].astype(F32)).astype(BF16)

        def down(j):
            part = dot(act[j % 2], wd[tile(j, FT), :hw])
            yacc[...] = part if j == 0 else yacc[...] + part
            blk, rest = divmod(j * FT, half_f)
            qt, at = divmod(rest, half_d)
            acc_d[blk, qt, :, at:at + FT] += dot(trd[...], act[j % 2])

        up(0)
        up(1)
        mid(0)
        for j in range(tiles):
            if j + 2 < tiles:
                up(j + 2)
            down(j)
            if j + 1 < tiles:
                mid(j + 1)

        @pl.when(n > half_n)
        def _():
            y_out(n).wait()

        write_y(s)
        y_out(n).start()

        @pl.when(n < half_n + 2)
        def _():
            give(1)
        return carry

    lax.fori_loop(half_n, chunks, chunk_theirs, 0)

    rdn = send(acc_d.at[1 - b], rdn_h, rdn_s, rdn_r, 'row')
    rdn.start()
    k = own_tiles - 1
    own_send(k - 1)
    own_load(k)
    own_send(k)
    for k in range(own_tiles):
        gu_out(k).start()
    all_of(acc_u.at[1 - b], ru_s).wait()

    def load_dx(n):
        s = odd(n)
        rs, ks = rows_of(n), rows_of(mine0 + n)
        return (local(x_h.at[ks, :], own.at[s], ld_sem.at[0, s]), local(dy_h.at[ks, :], aux.at[s], ld_sem.at[1, s]),
                local(xo_h.at[rs, :], land.at[2 * s], ld_sem.at[2, s]), local(dyo_h.at[rs, :], land.at[2 * s + 1], ld_sem.at[3, s]),
                local(dxn_h.at[n], acc_u.at[1 - b, :, :, pl.ds(pl.multiple_of(s * full, full), full)], ld_sem.at[4, s]),
                local(st_h.at[n], da_s.at[s, :, :, head(LANES)], ld_sem.at[5, s]))

    held = 2

    def chunk_dx(n, carry):
        s = odd(n)
        for cp in load_dx(n):
            cp.wait()

        @pl.when(n < half_n - 1)
        def _():
            for cp in load_dx(n + 1):
                cp.start()

        @pl.when(n > PROMPT)
        def _():
            dx_out(n).wait()
            dxo_out(n).wait()

        @pl.when((n > PROMPT) & (n <= half_n - LATE - held))
        def _():
            dx_far(n - 1).start()

        finish_dx(lambda h, rs: acc_u[1 - b, h, rs, pl.ds(pl.multiple_of(s * full, full), full)],
                  lambda rs: cat(own[s, rs, :], land[2 * s, rs, :]),
                  lambda rs: cat(aux[s, rs, :], land[2 * s + 1, rs, :]), da_s.at[s, :, :, head(LANES)])
        dx_out(n).start()

        @pl.when(n < half_n - LATE)
        def _():
            dxo_out(n).start()

        @pl.when(n >= half_n - LATE)
        def _():
            dxl_out(n).start()
        return carry

    for cp in load_dx(PROMPT):
        cp.start()
    lax.fori_loop(PROMPT, 2 * PROMPT, chunk_dx, 0)
    rdn.wait()
    rd_load = local(rdn_h, acc_d.at[1 - b], t_sem.at[0, 0])
    rd_load.start()
    rd_load.wait()
    steps = hw // LANES

    def ydn(i):
        return send(acc_d.at[b, 1 - d, pl.ds(i * LANES, LANES), :], ydn_h.at[i], ydn_s, ydn_r.at[i], 'depth')

    for i in range(steps):
        rs = tile(i, LANES)
        for qt in range(2):
            acc_d[b, qt, rs, :] += acc_d[1 - b, qt, rs, :]
        ydn(i).start()
    lax.fori_loop(2 * PROMPT, half_n, chunk_dx, 0)
    y_out(chunks - 1).wait()
    oth = lambda at, n: [col_sum(ref[:, a:a + n]) for ref, a in at]
    gso[...] = jnp.concatenate(oth(((bup8, half_f),), half_f) + oth(((gb8, hw), (gb8, full + hw)), hw)
                               + [jnp.zeros((1, half_f - full), F32)], axis=1)
    gs_col = send(gso, gsl.at[0], gs_s.at[0], gs_r.at[0], 'col')
    gs_col.start()
    for m in range(half_n - LATE - held, half_n - LATE):
        dx_far(m).start()
    dx_out(half_n - 1).wait()
    dxl_out(half_n - 1).wait()
    gs_col.wait()
    gsp[0] = jnp.concatenate(oth(((bup8, 0),), half_f) + oth(((gb8, 0), (gb8, full), (gb8, 2 * full)), hw)
                             + [jnp.zeros((1, half_f - 3 * hw), F32)], axis=1) + gsl[0]
    gs_row = send(gsp.at[0], gsl.at[1], gs_s.at[1], gs_r.at[1], 'row')
    gs_row.start()
    gs_row.wait()
    gsp[1] = gsp[0] + gsl[1]
    gs_dep = send(gsp.at[1], gsl.at[2], gs_s.at[2], gs_r.at[2], 'depth')
    gs_dep.start()
    for q in range(3 * half_n - RING, 3 * half_n):
        stream(x_h, 0, q).wait_send()
    all_of(acc_u.at[b, 1 - d], yu_s).wait()
    all_of(acc_u.at[b, d, :, pl.ds(half_f, half_f)], rx_s).wait()
    all_of(trx, out_sem.at[3]).wait()
    for i in range(steps):
        ydn(i).wait_recv()
        dn_load = local(ydn_h.at[i], acc_d.at[1 - b, 0, pl.ds(i * LANES, LANES), :], t_sem.at[1, 0])
        dn_load.start()
        dn_load.wait()
        rs = tile(i, LANES)
        for j in range(half_d // LANES):
            cs = tile(j, LANES)
            total = acc_d[b, d, rs, cs] + acc_d[1 - b, 0, rs, cs]
            us[j * LANES // M, j * LANES % M:j * LANES % M + LANES, rs] = total.T.astype(BF16)
    gd_out = [local(us.at[i], gd_h.at[pl.ds(i * M, M), :], t_sem.at[i, 1]) for i in range(2)]
    for cp in gd_out:
        cp.start()
    gs_dep.wait()
    gsp[0] = gsp[1] + gsl[2]
    gs_out = local(gsp.at[0], gs_h, out_sem.at[0])
    gs_out.start()
    all_of(acc_d.at[b, 1 - d], ydn_s).wait()
    for sem in (ag_s, ag_r):
        all_of(trx, sem).wait()
    sent = dxo_h.at[head((half_n - LATE) * M), :]
    for sem in (dx_s, dx_r):
        all_of(sent, sem).wait()
    for cp in gd_out:
        cp.wait()
    gs_out.wait()


def finish_kernel(y_in, dx_in, gwu_in, gd, gs, y, dx, gwu, gwd, gbup, ggam, gbet, gbdn, big, small, sums, in_sem, out_sem):
    rows, hw = y.shape
    half_f = gwd.shape[0]
    d = lax.axis_index('depth')
    n = rows // COPIES
    ins, outs = [], []

    def move(src, buf, *dst):
        ins.append(pltpu.make_async_copy(src, buf, in_sem.at[len(ins)]))
        outs.append([pltpu.make_async_copy(buf, to, out_sem) for to in dst])

    for i in range(COPIES):
        rs = pl.ds(i * n, n)
        move(y_in.at[rs], big.at[0, rs], y.at[rs])
        move(dx_in.at[rs], big.at[1, rs], dx.at[rs])
    move(gwu_in, small.at[:, head(half_f)], gwu)
    move(gd, big.at[2, head(half_f // 2)], gwd.at[pl.ds(pl.multiple_of(d * (half_f // 2), half_f // 2), half_f // 2)])
    parts = [(0, half_f, gbup), (half_f, hw, ggam), (half_f + hw, hw, gbet), (half_f + 2 * hw, hw, gbdn)]
    move(gs, sums)
    outs[-1] = [pltpu.make_async_copy(sums.at[:, pl.ds(a, w)], dst, out_sem) for a, w, dst in parts]
    for cp in ins:
        cp.start()
    for cp, tos in zip(ins, outs):
        cp.wait()
        for to in tos:
            to.start()
    for tos in outs:
        for to in tos:
            to.wait()


def solution(mesh):
    tok_spec = P(('dp', 'depth', 'row'), 'col')
    vec_spec = P('col')
    mat_spec = P('row', 'col')
    grad_vec = P(('dp', 'col'))
    grad_mat = P(('dp', 'row'), 'col')
    swap = ((0, 1), (1, 0))

    def local_pass(x, gamma, beta, w_up, b_up, w_down, b_down, dy):
        rows, hw = x.shape
        half_f = b_up.shape[0]
        full_f, full, hq = 2 * half_f, 2 * hw, hw // 2
        chunks = rows // M
        late = LATE * M
        hbm = pl.BlockSpec(memory_space=pltpu.HBM)
        sds = jax.ShapeDtypeStruct
        V, D = pltpu.VMEM, pltpu.SemaphoreType.DMA
        D2, D3, D4, D2S = D((2,)), D((3,)), D((4,)), D((2, SUBS))
        tiles, own_tiles = full_f // FT, half_f // FT
        outs = [
            sds((rows, hw), BF16), sds((rows, hw), BF16), sds((late, hw), BF16), sds((1, full_f), F32), sds((hw, half_f), BF16),
            sds((half_f // 2, hw), BF16),
            sds((rows // 2, hw), BF16), sds((tiles, 2, hq, FT), F32), sds((tiles, hq, FT), F32), sds((own_tiles, hq, FT), F32),
            sds((2, hw, half_f // 2), F32), sds((hw // LANES, LANES, half_f // 2), F32),
            sds((rows // 2, hw), BF16), sds((rows // 2, hw), BF16), sds((chunks // 2, 2, hq, full), F32), sds((chunks // 2, 2, hq, LANES), F32),
        ]
        scratch = [
            V((full, full_f), BF16), V((full_f, full), BF16), V((2, 2, hw, half_f // 2), F32), V((2, 2, hq, full_f), F32),
            V((2, M, hw), BF16), V((RING, M, hw), BF16), V((2, M, hw), BF16), V((M, full), BF16), V((full, M), BF16), V((hw, M), BF16),
            V((2, hq, LANES), F32), V((2, M, FT), BF16), V((2, 2, hq, FT), F32), V((2, M, FT), BF16), V((2, M, FT), BF16),
            V((M, hw), F32), V((2, hq, full), F32), V((M, hw), BF16), V((M, hw), BF16), V((M, hw), BF16),
            V((8, full_f), F32), V((8, 2 * full + hw), F32), V((2, 1, full_f), F32), V((2, half_f // LANES, LANES), BF16), V((hw // LANES, LANES), BF16),
            V((1, full_f), F32), V((2, 1, full_f), F32), V((3, 1, full_f), F32),
            D2, D2, D2, D2S, D2, D2S, D2, D2S, D2, D2S, D3, D3,
            D((RING,)), D((RING,)), D((6, 2)), D4, D4, D((2, 2)), D(()), D((tiles,)), D(()), D((tiles,)), D(()), D((own_tiles,)),
            D(()), D(()), D(()), D(()), D(()), D((hw // LANES,)), D(()), D(()), D3, D3, pltpu.SemaphoreType.REGULAR,
        ]
        res = pl.pallas_call(
            kernel,
            out_shape=outs,
            in_specs=[hbm] * 8,
            out_specs=[hbm] * len(outs),
            scratch_shapes=scratch,
            compiler_params=pltpu.CompilerParams(
                collective_id=0, has_side_effects=True, vmem_limit_bytes=67043328),
            cost_estimate=pl.CostEstimate(flops=14 * rows * full * full_f, bytes_accessed=2 ** 27, transcendentals=rows * full_f),
            name='mlp_block',
        )(x, dy, w_up, w_down, b_up.reshape(-1, LANES), gamma.reshape(1, -1), beta.reshape(1, -1), b_down.reshape(-1, LANES))
        y, dx, dxl, gs, gwu, gd = res[:6]
        gd_far = lax.ppermute(gd, 'depth', swap)
        dx_far = lax.ppermute(dxl, 'col', swap)
        moves = 2 * COPIES + 3
        y, dx, gwu, gwd, gbup, ggam, gbet, gbdn = pl.pallas_call(
            finish_kernel,
            out_shape=[sds((rows, hw), BF16), sds((rows, hw), BF16), sds((hw, half_f), BF16), sds((half_f, hw), BF16),
                       sds((1, half_f), F32), sds((1, hw), F32), sds((1, hw), F32), sds((1, hw), F32)],
            in_specs=[hbm] * 5,
            out_specs=[hbm] * 8,
            scratch_shapes=[V((3, rows, hw), BF16), V((hw, half_f), BF16), V((1, full_f), F32), D((moves,)), D(())],
            compiler_params=pltpu.CompilerParams(vmem_limit_bytes=62000000),
            cost_estimate=pl.CostEstimate(flops=2 ** 33, bytes_accessed=42 * 2 ** 20, transcendentals=0),
            name='finish',
        )(y, dx, gwu, gd, gs)
        gwd = lax.dynamic_update_slice(gwd, gd_far, ((1 - lax.axis_index('depth')) * (half_f // 2), 0))
        dx = lax.dynamic_update_slice(dx, dx_far, ((1 - lax.axis_index('col')) * (rows // 2) + rows // 2 - late, 0))
        return y, dx, ggam.reshape(-1), gbet.reshape(-1), gwu, gbup.reshape(-1), gwd, gbdn.reshape(-1)

    return jax.shard_map(
        local_pass,
        mesh=mesh,
        in_specs=(tok_spec, vec_spec, vec_spec, mat_spec, vec_spec, mat_spec, vec_spec, tok_spec),
        out_specs=(tok_spec, tok_spec, grad_vec, grad_vec, grad_mat, grad_vec, grad_mat, grad_vec),
        check_vma=False,
    )
```

```python
import jax
import jax.numpy as jnp
from jax import lax
from jax.experimental import pallas as pl
from jax.experimental.pallas import tpu as pltpu
from jax.sharding import PartitionSpec as P

LN_EPS = 1e-5
C0 = 0.7978845608
C1 = C0 * 0.044715
M = 512
FT = 512
SUBS = 4
RING = 6
LATE = 2
PROMPT = 2
COPIES = 4
LANES = 128
BF16, F32 = jnp.bfloat16, jnp.float32
MESH = pl.DeviceIdType.MESH


def dot(lhs, rhs, rhs_dim=0):
    return lax.dot_general(lhs, rhs, (((1,), (rhs_dim,)), ((), ())), preferred_element_type=F32)


def dot_t(lhs, rhs):
    return dot(lhs, rhs, 1)


def odd(n):
    return lax.rem(n, 2)


def cat(*parts):
    return jnp.concatenate(parts, axis=1)


def row_sum(v):
    return jnp.sum(v, axis=1, keepdims=True)


def col_sum(v):
    return jnp.sum(v, axis=0, keepdims=True)


def head(n):
    return pl.ds(0, n)


def tile(i, n):
    return slice(i * n, (i + 1) * n)


def gelu(v):
    t = jnp.tanh(v * (C1 * (v * v) + C0))
    h = 0.5 * v
    return h * t + h


def gelu_and_slope(v):
    v2 = v * v
    t = jnp.tanh(v * (C1 * v2 + C0))
    h = 0.5 * v
    slope = (v * (1.0 - t * t)) * (1.5 * C1 * v2 + 0.5 * C0) + (0.5 * t + 0.5)
    return h * t + h, slope


def fold8(v):
    return jnp.sum(v.reshape(v.shape[0] // 8, 8, v.shape[1]), axis=0)


def kernel(x_h, dy_h, wu_h, wd_h, bup_h, gam_h, bet_h, bdn_h,
           y_h, dx_h, dxl_h, gs_h, gu_h, gd_h, dxo_h, rrow_h, ryu_h, rx_h, rdn_h, ydn_h, xo_h, dyo_h, dxn_h, st_h,
           wu, wd, acc_d, acc_u, own, land, aux, xn, trx, trd, st, us, da_s, act, du_s, yacc, dxn, yo, dxa, dxb,
           bup8, gb8, smv, bup_s, bdn_s, gso, gsp, gsl,
           wrow_s, wrow_r, wx_s, wx_r, wy_s, wy_r, wa_s, wa_r, wb_s, wb_r, sm_s, sm_r,
           land_s, land_r, ld_sem, out_sem, sv_sem, t_sem, ru_s, ru_r, yu_s, yu_r, rx_s, rx_r, ag_s, ag_r, rdn_s, rdn_r,
           ydn_s, ydn_r, dx_s, dx_r, gs_s, gs_r, credit):
    chunks = x_h.shape[0] // M
    half_n = chunks // 2
    half_f = wu_h.shape[1]
    hw = x_h.shape[1]
    full = 2 * hw
    hq = hw // 2
    half_d = half_f // 2
    tiles = 2 * half_f // FT
    own_tiles = tiles // 2
    c, r, d = lax.axis_index('col'), lax.axis_index('row'), lax.axis_index('depth')
    b = lax.rem(r + c, 2)
    peer = {'col': 1 - c, 'row': 1 - r, 'depth': 1 - d}
    mine0, theirs0 = c * half_n, (1 - c) * half_n

    def send(src, dst, s_sem, r_sem, axis):
        return pltpu.make_async_remote_copy(src_ref=src, dst_ref=dst, send_sem=s_sem, recv_sem=r_sem,
                                            device_id={axis: peer[axis]}, device_id_type=MESH)

    def local(src, dst, sem):
        return pltpu.make_async_copy(src, dst, sem)

    def all_of(ref, sem):
        return pltpu.make_async_copy(ref, ref, sem)

    def rows_of(k):
        return pl.ds(pl.multiple_of(k * M, M), M)

    def chunk_at(n):
        return lax.rem(mine0 + n, chunks)

    bar = pltpu.get_barrier_semaphore()
    for axis in ('col', 'row', 'depth'):
        pl.semaphore_signal(bar, inc=1, device_id={axis: peer[axis]}, device_id_type=MESH)
    pl.semaphore_wait(bar, 3)

    half_rows = (hq, half_d)
    w_srcs = (wu_h, wd_h)

    def w_cols(kind, blk, dep, s):
        n = half_rows[kind] // SUBS
        if kind == 0:
            return wu.at[pl.ds(pl.multiple_of(blk * hw + dep * hq + s * n, n), n), pl.ds(half_f, half_f)]
        return wd.at[pl.ds(pl.multiple_of(blk * half_f + dep * half_d + s * n, n), n), pl.ds(hw, hw)]

    def w_half(kind):
        return wu.at[head(hq), head(half_f)] if kind == 0 else wd.at[head(half_d), head(hw)]

    def w_own(kind):
        if kind == 0:
            return wu.at[pl.ds(pl.multiple_of(b * hw, hw), hw), head(half_f)]
        return wd.at[pl.ds(pl.multiple_of(b * half_f, half_f), half_f), head(hw)]

    def w_x(kind, s):
        n = half_rows[kind] // SUBS
        src = w_srcs[kind].at[pl.ds(pl.multiple_of(d * half_rows[kind] + s * n, n), n), :]
        return send(src, w_cols(kind, 1 - b, d, s), wx_s.at[kind], wx_r.at[kind, s], 'col')

    def w_y(kind, s):
        return send(w_cols(kind, b, d, s), w_cols(kind, b, d, s), wy_s.at[kind], wy_r.at[kind, s], 'depth')

    def w_a(kind, s):
        return send(w_cols(kind, b, d, s), w_cols(kind, b, d, s), wa_s.at[kind], wa_r.at[kind, s], 'row')

    def w_b(kind, s):
        return send(w_cols(kind, b, 1 - d, s), w_cols(kind, b, 1 - d, s), wb_s.at[kind], wb_r.at[kind, s], 'row')

    def w_row(kind):
        return send(w_srcs[kind], w_own(kind), wrow_s.at[kind], wrow_r.at[kind], 'row')

    def w_load(kind):
        return local(w_srcs[kind], w_own(kind), out_sem.at[kind])

    def w_cross(kind):
        for s in range(SUBS):
            w_x(kind, s).start()

    def w_forward_x(kind):
        for s in range(SUBS):
            w_x(kind, s).wait_recv()
            w_y(kind, s).start()
            w_a(kind, s).start()

    def w_forward_y(kind):
        for s in range(SUBS):
            w_y(kind, s).wait_recv()
            w_b(kind, s).start()

    def w_arrive(kind):
        for s in range(SUBS):
            w_a(kind, s).wait_recv()
            w_b(kind, s).wait_recv()

    def stream(src, k, q):
        slot = lax.rem(q, RING)
        return send(src.at[rows_of(k), :], land.at[slot], land_s.at[slot], land_r.at[slot], 'col')

    def stream_next(src, k, q):
        @pl.when(q >= RING)
        def _():
            stream(src, k, q).wait_send()
            pl.semaphore_wait(credit, 1)
        stream(src, k, q).start()

    def give(n):
        for _ in range(n):
            pl.semaphore_signal(credit, inc=1, device_id={'col': peer['col']}, device_id_type=MESH)

    gam_at, bet_at = pl.ds(half_f, hw), pl.ds(half_f + hw, hw)
    sm_own = [local(bup_h, bup_s.at[0], ld_sem.at[0, 0]), local(gam_h, smv.at[0, :, gam_at], ld_sem.at[0, 1]),
              local(bet_h, smv.at[0, :, bet_at], ld_sem.at[1, 0]), local(bdn_h, bdn_s, ld_sem.at[1, 1])]
    sm_out = [send(bup_h, bup_s.at[1], sm_s.at[0], sm_r.at[0], 'col'),
              send(gam_h, smv.at[1, :, gam_at], sm_s.at[1], sm_r.at[1], 'col'),
              send(bet_h, smv.at[1, :, bet_at], sm_s.at[2], sm_r.at[2], 'col')]
    for cp in sm_own + sm_out:
        cp.start()
    @pl.when(b == 1)
    def _():
        w_cross(1)

    for kind in range(2):
        w_load(kind).start()
        w_row(kind).start()
    stream(x_h, theirs0, 0).start()
    stream(dy_h, theirs0, 1).start()
    w_cross(0)

    @pl.when(b == 0)
    def _():
        w_cross(1)

    stream(x_h, theirs0 + 1, 2).start()
    stream(dy_h, theirs0 + 1, 3).start()

    acc_d[...] = jnp.zeros_like(acc_d)
    acc_u[...] = jnp.zeros_like(acc_u)
    bup8[...] = jnp.zeros_like(bup8)
    gb8[...] = jnp.zeros_like(gb8)
    for cp in sm_own:
        cp.wait()

    def load(n):
        s = odd(n)
        rs = rows_of(chunk_at(n))
        return (local(x_h.at[rs, :], own.at[s], ld_sem.at[0, s]), local(dy_h.at[rs, :], aux.at[s], ld_sem.at[1, s]))

    for cp in load(0):
        cp.start()
    for kind in range(2):
        w_load(kind).wait()
        w_row(kind).wait()

    @pl.when(b == 0)
    def _():
        w_forward_x(1)
        w_forward_y(1)

    @pl.when(b == 1)
    def _():
        w_arrive(1)

    def w_rest():
        w_forward_x(0)

        @pl.when(b == 1)
        def _():
            w_forward_x(1)

        w_forward_y(0)

        @pl.when(b == 1)
        def _():
            w_forward_y(1)

        @pl.when(b == 0)
        def _():
            w_arrive(1)

        w_arrive(0)
        for kind in range(2):
            for sems in (wx_s, wy_s, wa_s, wb_s):
                all_of(w_half(kind), sems.at[kind]).wait()

    for cp in sm_out:
        cp.wait()
    for i in range(half_f // LANES):
        for side in range(2):
            smv[side, :, tile(i, LANES)] = bup_s[side, i:i + 1, :].astype(F32)
    for i in range(hw // LANES):
        smv[0, :, half_f + full + i * LANES:half_f + full + (i + 1) * LANES] = bdn_s[i:i + 1, :].astype(F32)

    def wide(at):
        return cat(smv[0, :, half_f + at:half_f + at + hw], smv[1, :, half_f + at:half_f + at + hw])

    def norm(s, slot, keep):
        gam, bet = wide(0), wide(hw)
        step = 32
        for i in range(M // step):
            rs = tile(i, step)
            xv = cat(own[s, rs, :], land[slot, rs, :]).astype(F32)
            mean = row_sum(xv) * (1.0 / full)
            cen = xv - mean
            istd = lax.rsqrt(row_sum(cen * cen) * (1.0 / full) + LN_EPS)
            xn[rs, :] = (cen * istd * gam + bet).astype(BF16)
            if keep:
                st[i * step // hq, i * step % hq:i * step % hq + step, :] = cat(jnp.broadcast_to(mean, (step, 64)), jnp.broadcast_to(istd, (step, 64)))
        dyv = aux[s]
        trd[...] = dyv.T
        gb8[:, 2 * full:2 * full + hw] += fold8(dyv.astype(F32))

    def write_y(s):
        bdn = smv[0, :, half_f + full:half_f + full + hw]
        yo[...] = (own[s].astype(F32) + yacc[...] + bdn).astype(BF16)

    def y_out(n):
        return local(yo, y_h.at[rows_of(chunk_at(n)), :], out_sem.at[0])

    def dx_out(n):
        return local(dxa, dx_h.at[rows_of(chunk_at(n)), :], out_sem.at[1])

    def dxo_out(n):
        return local(dxb, dxo_h.at[rows_of(n), :], out_sem.at[2])

    def dxl_out(n):
        return local(dxb, dxl_h.at[rows_of(n - (half_n - LATE)), :], out_sem.at[2])

    def saves(n, slot_x, slot_d):
        rs = rows_of(n)
        return (local(land.at[slot_x], xo_h.at[rs, :], sv_sem.at[0]), local(land.at[slot_d], dyo_h.at[rs, :], sv_sem.at[1]),
                local(dxn, dxn_h.at[n], sv_sem.at[2]), local(st, st_h.at[n], sv_sem.at[3]))

    def finish_dx(grads, xs, dys, stats):
        gam = wide(0)
        step = 32
        for i in range(M // step):
            rs = tile(i, step)
            h, hs = i * step // hq, slice(i * step % hq, i * step % hq + step)
            istd = stats[h, hs, 64:65]
            xh = (xs(rs).astype(F32) - stats[h, hs, 0:1]) * istd
            dv = grads(h, hs)
            px = dv * xh
            gb8[:, :full] += fold8(px)
            gb8[:, full:2 * full] += fold8(dv)
            m1 = row_sum(dv * gam) * (1.0 / full)
            m2 = row_sum(px * gam) * (1.0 / full)
            dxv = (dys(rs).astype(F32) + istd * (dv * gam - m1 - xh * m2)).astype(BF16)
            dxa[rs, :] = dxv[:, :hw]
            dxb[rs, :] = dxv[:, hw:]

    def dx_far(m):
        return send(dxo_h.at[rows_of(m), :], dx_h.at[rows_of(mine0 + m), :], dx_s, dx_r, 'col')

    def ru(p):
        return send(acc_u.at[1 - b, :, :, pl.ds(p * FT, FT)], rrow_h.at[p], ru_s, ru_r.at[p], 'row')

    def yu(p):
        return send(acc_u.at[b, 1 - d, :, pl.ds(p * FT, FT)], ryu_h.at[p], yu_s, yu_r.at[p], 'depth')

    def row_load(i, p):
        return local(rrow_h.at[p], da_s.at[i % 2], t_sem.at[i % 2, 0])

    def row_add(i, p):
        row_load(i, p).wait()
        for h in range(2):
            acc_u[b, h, :, tile(p, FT)] += da_s[i % 2, h]
        yu(p).start()

    def chunk_mine(n, carry):
        s = odd(n)
        slot_x, slot_d = lax.rem(2 * n, RING), lax.rem(2 * n + 1, RING)

        for cp in load(n):
            cp.wait()
        for cp in load(n + 1):
            cp.start()

        @pl.when(n == PROMPT + 1)
        def _():
            dx_far(0).start()

        stream(x_h, n, 2 * n).wait_recv()
        stream(dy_h, n, 2 * n + 1).wait_recv()
        save = saves(n, slot_x, slot_d)
        save[0].start()
        save[1].start()

        @pl.when(n > 0)
        def _():
            save[3].wait()

        norm(s, slot_x, True)
        save[3].start()
        trx[...] = xn[...].T

        @pl.when(n > 0)
        def _():
            save[2].wait()

        @pl.when((n > 0) & (n <= PROMPT))
        def _():
            dx_out(n).wait()
            dxo_out(n).wait()

        yacc[...] = jnp.zeros_like(yacc)
        dxn[...] = jnp.zeros_like(dxn)

        def quad(jj, inner):
            @pl.when((n == 0) & (jj == 1))
            def _():
                w_rest()

            @pl.when((n == half_n - 1) & (jj == 1))
            def _():
                for p in range(own_tiles):
                    ru(p).start()
                ru(0).wait_recv()
                row_load(0, 0).start()
                row_add(0, 0)

            @pl.when((n < half_n - 2) & (jj == 1))
            def _():
                stream_next(x_h, theirs0 + n + 2, 2 * n + 4)
                stream_next(dy_h, theirs0 + n + 2, 2 * n + 5)

            @pl.when((n >= half_n - 2) & (jj == 1))
            def _():
                k = 2 * (n - (half_n - 2))
                stream_next(x_h, mine0 + k, chunks + k)
                stream_next(x_h, mine0 + k + 1, chunks + k + 1)

            cols = [pl.ds(pl.multiple_of((own_tiles * jj + t) * FT, FT), FT) for t in range(own_tiles)]

            def first(t):
                bias = smv[jj, :, tile(t, FT)]
                us[t % 2] = (dot(xn[...], wu[:, cols[t]]) + bias).astype(BF16)
                dyv = cat(aux[s], land[slot_d])
                da_s[t % 2] = dot_t(dyv, wd[cols[t], :]).reshape(2, hq, FT)

            def mid(t):
                a, slope = gelu_and_slope(us[t % 2].astype(F32))
                act[t % 2] = a.astype(BF16)
                du = (da_s[t % 2].reshape(M, FT) * slope).astype(BF16)
                du_s[t % 2] = du
                bup8[:, cols[t]] += fold8(du.astype(F32))

            def last(t):
                yacc[...] += dot(act[t % 2], wd[cols[t], :hw])
                at = t * FT % half_d
                acc_d[jj, t * FT // half_d, :, at:at + FT] += dot(trd[...], act[t % 2])
                dxn[...] += dot_t(du_s[t % 2], wu[:, cols[t]]).reshape(2, hq, full)
                part = dot(trx[...], du_s[t % 2])
                for i in range(4):
                    acc_u[i // 2, i % 2, :, cols[t]] += part[tile(i, hq)]

            first(0)
            first(1)
            mid(0)
            for t in range(own_tiles):
                last(t)
                if t + 2 < own_tiles:
                    first(t + 2)
                if t + 1 < own_tiles:
                    mid(t + 1)
            return inner

        lax.fori_loop(0, 2, quad, 0)

        @pl.when(n > 0)
        def _():
            y_out(n).wait()

        write_y(s)
        y_out(n).start()
        save[2].start()

        @pl.when(n < PROMPT)
        def _():
            finish_dx(lambda h, rs: dxn[h, rs, :],
                      lambda rs: cat(own[s, rs, :], land[slot_x, rs, :]),
                      lambda rs: cat(aux[s, rs, :], land[slot_d, rs, :]), st)
            dx_out(n).start()
            dxo_out(n).start()

        save[0].wait()
        save[1].wait()
        give(2)
        return carry

    lax.fori_loop(0, half_n, chunk_mine, 0)

    order = [*range(own_tiles, tiles), *range(1, own_tiles)]

    def rx(k):
        return send(acc_u.at[b, d, :, pl.ds((own_tiles + k) * FT, FT)], rx_h.at[k], rx_s, rx_r.at[k], 'col')

    gu_rows = pl.ds(pl.multiple_of(d * hq, hq), hq)

    def ag(k):
        ps = pl.ds(k * FT, FT)
        return send(trx.at[pl.ds(k * hq, hq), :], gu_h.at[gu_rows, ps], ag_s, ag_r, 'depth')

    def gu_out(k):
        return local(trx.at[pl.ds(k * hq, hq), :], gu_h.at[gu_rows, pl.ds(k * FT, FT)], out_sem.at[3])

    for p in order[:own_tiles]:
        ru(p).start()
    y_out(0).wait()
    for cp in saves(half_n - 1, 0, 0)[2:]:
        cp.wait()
    ru(order[0]).wait_recv()
    row_load(0, order[0]).start()
    for i, p in enumerate(order):
        if i + 1 < len(order):
            ru(order[i + 1]).wait_recv()
            row_load(i + 1, order[i + 1]).start()
        row_add(i, p)

    def oth_load(k):
        yu(own_tiles + k).wait_recv()
        local(ryu_h.at[own_tiles + k], da_s.at[k % 2, 0], t_sem.at[k % 2, 0]).start()

    def oth_send(k):
        p = own_tiles + k
        local(ryu_h.at[p], da_s.at[k % 2, 0], t_sem.at[k % 2, 0]).wait()
        acc_u[b, d, :, tile(p, FT)] += da_s[k % 2, 0]
        rx(k).start()

    def own_loads(k):
        return (local(ryu_h.at[k], da_s.at[k % 2, 0], t_sem.at[k % 2, 0]),
                local(rx_h.at[k], da_s.at[k % 2, 1], t_sem.at[k % 2, 1]))

    def own_load(k):
        yu(k).wait_recv()
        rx(k).wait_recv()
        for cp in own_loads(k):
            cp.start()

    def own_send(k):
        for cp in own_loads(k):
            cp.wait()
        trx[tile(k, hq), :] = (acc_u[b, d, :, tile(k, FT)] + da_s[k % 2, 0] + da_s[k % 2, 1]).astype(BF16)
        ag(k).start()

    def background(n):
        for k in range(own_tiles):
            @pl.when(n == half_n + 2 + k)
            def _():
                oth_send(k)

            @pl.when(n == half_n + 1 + k)
            def _():
                oth_load(k)

        for k in range(own_tiles - 1):
            @pl.when(n == half_n + 6 + k)
            def _():
                own_send(k)

            @pl.when(n == half_n + 5 + k)
            def _():
                own_load(k)

        @pl.when(n == half_n + own_tiles + 1)
        def _():
            dx_far(1).start()

    def chunk_theirs(n, carry):
        s = odd(n)
        q = n + half_n
        slot = lax.rem(q, RING)

        @pl.when(n == half_n)
        def _():
            stream_next(x_h, mine0 + 4, chunks + 4)

        @pl.when(n <= half_n + 2)
        def _():
            stream_next(x_h, mine0 + 5 + (n - half_n), chunks + 5 + (n - half_n))

        background(n)
        for cp in load(n):
            cp.wait()

        @pl.when(n < chunks - 1)
        def _():
            for cp in load(n + 1):
                cp.start()

        stream(x_h, n, q).wait_recv()
        norm(s, slot, False)

        def up(j):
            side, at = divmod(j * FT, half_f)
            us[j % 2] = (dot(xn[...], wu[:, tile(j, FT)]) + smv[side, :, at:at + FT]).astype(BF16)

        def mid(j):
            act[j % 2] = gelu(us[j % 2].astype(F32)).astype(BF16)

        def down(j):
            part = dot(act[j % 2], wd[tile(j, FT), :hw])
            yacc[...] = part if j == 0 else yacc[...] + part
            blk, rest = divmod(j * FT, half_f)
            qt, at = divmod(rest, half_d)
            acc_d[blk, qt, :, at:at + FT] += dot(trd[...], act[j % 2])

        up(0)
        up(1)
        mid(0)
        for j in range(tiles):
            if j + 2 < tiles:
                up(j + 2)
            down(j)
            if j + 1 < tiles:
                mid(j + 1)

        @pl.when(n > half_n)
        def _():
            y_out(n).wait()

        write_y(s)
        y_out(n).start()

        @pl.when(n < half_n + 2)
        def _():
            give(1)
        return carry

    lax.fori_loop(half_n, chunks, chunk_theirs, 0)

    rdn = send(acc_d.at[1 - b], rdn_h, rdn_s, rdn_r, 'row')
    rdn.start()
    k = own_tiles - 1
    own_send(k - 1)
    own_load(k)
    own_send(k)
    for k in range(own_tiles):
        gu_out(k).start()
    all_of(acc_u.at[1 - b], ru_s).wait()

    def load_dx(n):
        s = odd(n)
        rs, ks = rows_of(n), rows_of(mine0 + n)
        return (local(x_h.at[ks, :], own.at[s], ld_sem.at[0, s]), local(dy_h.at[ks, :], aux.at[s], ld_sem.at[1, s]),
                local(xo_h.at[rs, :], land.at[2 * s], ld_sem.at[2, s]), local(dyo_h.at[rs, :], land.at[2 * s + 1], ld_sem.at[3, s]),
                local(dxn_h.at[n], acc_u.at[1 - b, :, :, pl.ds(pl.multiple_of(s * full, full), full)], ld_sem.at[4, s]),
                local(st_h.at[n], da_s.at[s, :, :, head(LANES)], ld_sem.at[5, s]))

    held = 2

    def chunk_dx(n, carry):
        s = odd(n)
        for cp in load_dx(n):
            cp.wait()

        @pl.when(n < half_n - 1)
        def _():
            for cp in load_dx(n + 1):
                cp.start()

        @pl.when(n > PROMPT)
        def _():
            dx_out(n).wait()
            dxo_out(n).wait()

        @pl.when((n > PROMPT) & (n <= half_n - LATE - held))
        def _():
            dx_far(n - 1).start()

        finish_dx(lambda h, rs: acc_u[1 - b, h, rs, pl.ds(pl.multiple_of(s * full, full), full)],
                  lambda rs: cat(own[s, rs, :], land[2 * s, rs, :]),
                  lambda rs: cat(aux[s, rs, :], land[2 * s + 1, rs, :]), da_s.at[s, :, :, head(LANES)])
        dx_out(n).start()

        @pl.when(n < half_n - LATE)
        def _():
            dxo_out(n).start()

        @pl.when(n >= half_n - LATE)
        def _():
            dxl_out(n).start()
        return carry

    for cp in load_dx(PROMPT):
        cp.start()
    lax.fori_loop(PROMPT, 2 * PROMPT, chunk_dx, 0)
    rdn.wait()
    rd_load = local(rdn_h, acc_d.at[1 - b], t_sem.at[0, 0])
    rd_load.start()
    rd_load.wait()
    steps = hw // LANES

    def ydn(i):
        return send(acc_d.at[b, 1 - d, pl.ds(i * LANES, LANES), :], ydn_h.at[i], ydn_s, ydn_r.at[i], 'depth')

    for i in range(steps):
        rs = tile(i, LANES)
        for qt in range(2):
            acc_d[b, qt, rs, :] += acc_d[1 - b, qt, rs, :]
        ydn(i).start()
    lax.fori_loop(2 * PROMPT, half_n, chunk_dx, 0)
    y_out(chunks - 1).wait()
    oth = lambda at, n: [col_sum(ref[:, a:a + n]) for ref, a in at]
    gso[...] = jnp.concatenate(oth(((bup8, half_f),), half_f) + oth(((gb8, hw), (gb8, full + hw)), hw)
                               + [jnp.zeros((1, half_f - full), F32)], axis=1)
    gs_col = send(gso, gsl.at[0], gs_s.at[0], gs_r.at[0], 'col')
    gs_col.start()
    for m in range(half_n - LATE - held, half_n - LATE):
        dx_far(m).start()
    dx_out(half_n - 1).wait()
    dxl_out(half_n - 1).wait()
    gs_col.wait()
    gsp[0] = jnp.concatenate(oth(((bup8, 0),), half_f) + oth(((gb8, 0), (gb8, full), (gb8, 2 * full)), hw)
                             + [jnp.zeros((1, half_f - 3 * hw), F32)], axis=1) + gsl[0]
    gs_row = send(gsp.at[0], gsl.at[1], gs_s.at[1], gs_r.at[1], 'row')
    gs_row.start()
    gs_row.wait()
    gsp[1] = gsp[0] + gsl[1]
    gs_dep = send(gsp.at[1], gsl.at[2], gs_s.at[2], gs_r.at[2], 'depth')
    gs_dep.start()
    for q in range(3 * half_n - RING, 3 * half_n):
        stream(x_h, 0, q).wait_send()
    all_of(acc_u.at[b, 1 - d], yu_s).wait()
    all_of(acc_u.at[b, d, :, pl.ds(half_f, half_f)], rx_s).wait()
    all_of(trx, out_sem.at[3]).wait()
    for i in range(steps):
        ydn(i).wait_recv()
        dn_load = local(ydn_h.at[i], acc_d.at[1 - b, 0, pl.ds(i * LANES, LANES), :], t_sem.at[1, 0])
        dn_load.start()
        dn_load.wait()
        rs = tile(i, LANES)
        for j in range(half_d // LANES):
            cs = tile(j, LANES)
            total = acc_d[b, d, rs, cs] + acc_d[1 - b, 0, rs, cs]
            us[j * LANES // M, j * LANES % M:j * LANES % M + LANES, rs] = total.T.astype(BF16)
    gd_out = [local(us.at[i], gd_h.at[pl.ds(i * M, M), :], t_sem.at[i, 1]) for i in range(2)]
    for cp in gd_out:
        cp.start()
    gs_dep.wait()
    gsp[0] = gsp[1] + gsl[2]
    gs_out = local(gsp.at[0], gs_h, out_sem.at[0])
    gs_out.start()
    all_of(acc_d.at[b, 1 - d], ydn_s).wait()
    for sem in (ag_s, ag_r):
        all_of(trx, sem).wait()
    sent = dxo_h.at[head((half_n - LATE) * M), :]
    for sem in (dx_s, dx_r):
        all_of(sent, sem).wait()
    for cp in gd_out:
        cp.wait()
    gs_out.wait()


def finish_kernel(y_in, dx_in, gwu_in, gd, gs, y, dx, gwu, gwd, gbup, ggam, gbet, gbdn, big, small, sums, in_sem, out_sem):
    rows, hw = y.shape
    half_f = gwd.shape[0]
    d = lax.axis_index('depth')
    n = rows // COPIES
    ins, outs = [], []

    def move(src, buf, *dst):
        ins.append(pltpu.make_async_copy(src, buf, in_sem.at[len(ins)]))
        outs.append([pltpu.make_async_copy(buf, to, out_sem) for to in dst])

    for i in range(COPIES):
        rs = pl.ds(i * n, n)
        move(y_in.at[rs], big.at[0, rs], y.at[rs])
        move(dx_in.at[rs], big.at[1, rs], dx.at[rs])
    move(gwu_in, small.at[:, head(half_f)], gwu)
    move(gd, big.at[2, head(half_f // 2)], gwd.at[pl.ds(pl.multiple_of(d * (half_f // 2), half_f // 2), half_f // 2)])
    parts = [(0, half_f, gbup), (half_f, hw, ggam), (half_f + hw, hw, gbet), (half_f + 2 * hw, hw, gbdn)]
    move(gs, sums)
    outs[-1] = [pltpu.make_async_copy(sums.at[:, pl.ds(a, w)], dst, out_sem) for a, w, dst in parts]
    for cp in ins:
        cp.start()
    for cp, tos in zip(ins, outs):
        cp.wait()
        for to in tos:
            to.start()
    for tos in outs:
        for to in tos:
            to.wait()


def solution(mesh):
    tok_spec = P(('dp', 'depth', 'row'), 'col')
    vec_spec = P('col')
    mat_spec = P('row', 'col')
    grad_vec = P(('dp', 'col'))
    grad_mat = P(('dp', 'row'), 'col')
    swap = ((0, 1), (1, 0))

    def local_pass(x, gamma, beta, w_up, b_up, w_down, b_down, dy):
        rows, hw = x.shape
        half_f = b_up.shape[0]
        full_f, full, hq = 2 * half_f, 2 * hw, hw // 2
        chunks = rows // M
        late = LATE * M
        hbm = pl.BlockSpec(memory_space=pltpu.HBM)
        sds = jax.ShapeDtypeStruct
        V, D = pltpu.VMEM, pltpu.SemaphoreType.DMA
        D2, D3, D4, D2S = D((2,)), D((3,)), D((4,)), D((2, SUBS))
        tiles, own_tiles = full_f // FT, half_f // FT
        outs = [
            sds((rows, hw), BF16), sds((rows, hw), BF16), sds((late, hw), BF16), sds((1, full_f), F32), sds((hw, half_f), BF16),
            sds((half_f // 2, hw), BF16),
            sds((rows // 2, hw), BF16), sds((tiles, 2, hq, FT), F32), sds((tiles, hq, FT), F32), sds((own_tiles, hq, FT), F32),
            sds((2, hw, half_f // 2), F32), sds((hw // LANES, LANES, half_f // 2), F32),
            sds((rows // 2, hw), BF16), sds((rows // 2, hw), BF16), sds((chunks // 2, 2, hq, full), F32), sds((chunks // 2, 2, hq, LANES), F32),
        ]
        scratch = [
            V((full, full_f), BF16), V((full_f, full), BF16), V((2, 2, hw, half_f // 2), F32), V((2, 2, hq, full_f), F32),
            V((2, M, hw), BF16), V((RING, M, hw), BF16), V((2, M, hw), BF16), V((M, full), BF16), V((full, M), BF16), V((hw, M), BF16),
            V((2, hq, LANES), F32), V((2, M, FT), BF16), V((2, 2, hq, FT), F32), V((2, M, FT), BF16), V((2, M, FT), BF16),
            V((M, hw), F32), V((2, hq, full), F32), V((M, hw), BF16), V((M, hw), BF16), V((M, hw), BF16),
            V((8, full_f), F32), V((8, 2 * full + hw), F32), V((2, 1, full_f), F32), V((2, half_f // LANES, LANES), BF16), V((hw // LANES, LANES), BF16),
            V((1, full_f), F32), V((2, 1, full_f), F32), V((3, 1, full_f), F32),
            D2, D2, D2, D2S, D2, D2S, D2, D2S, D2, D2S, D3, D3,
            D((RING,)), D((RING,)), D((6, 2)), D4, D4, D((2, 2)), D(()), D((tiles,)), D(()), D((tiles,)), D(()), D((own_tiles,)),
            D(()), D(()), D(()), D(()), D(()), D((hw // LANES,)), D(()), D(()), D3, D3, pltpu.SemaphoreType.REGULAR,
        ]
        res = pl.pallas_call(
            kernel,
            out_shape=outs,
            in_specs=[hbm] * 8,
            out_specs=[hbm] * len(outs),
            scratch_shapes=scratch,
            compiler_params=pltpu.CompilerParams(
                collective_id=0, has_side_effects=True, vmem_limit_bytes=67043328),
            cost_estimate=pl.CostEstimate(flops=14 * rows * full * full_f, bytes_accessed=2 ** 27, transcendentals=rows * full_f),
            name='mlp_block',
        )(x, dy, w_up, w_down, b_up.reshape(-1, LANES), gamma.reshape(1, -1), beta.reshape(1, -1), b_down.reshape(-1, LANES))
        y, dx, dxl, gs, gwu, gd = res[:6]
        gd_far = lax.ppermute(gd, 'depth', swap)
        dx_far = lax.ppermute(dxl, 'col', swap)
        moves = 2 * COPIES + 3
        y, dx, gwu, gwd, gbup, ggam, gbet, gbdn = pl.pallas_call(
            finish_kernel,
            out_shape=[sds((rows, hw), BF16), sds((rows, hw), BF16), sds((hw, half_f), BF16), sds((half_f, hw), BF16),
                       sds((1, half_f), F32), sds((1, hw), F32), sds((1, hw), F32), sds((1, hw), F32)],
            in_specs=[hbm] * 5,
            out_specs=[hbm] * 8,
            scratch_shapes=[V((3, rows, hw), BF16), V((hw, half_f), BF16), V((1, full_f), F32), D((moves,)), D(())],
            compiler_params=pltpu.CompilerParams(vmem_limit_bytes=62000000),
            cost_estimate=pl.CostEstimate(flops=2 ** 33, bytes_accessed=42 * 2 ** 20, transcendentals=0),
            name='finish',
        )(y, dx, gwu, gd, gs)
        gwd = lax.dynamic_update_slice(gwd, gd_far, ((1 - lax.axis_index('depth')) * (half_f // 2), 0))
        dx = lax.dynamic_update_slice(dx, dx_far, ((1 - lax.axis_index('col')) * (rows // 2) + rows // 2 - late, 0))
        return y, dx, ggam.reshape(-1), gbet.reshape(-1), gwu, gbup.reshape(-1), gwd, gbdn.reshape(-1)

    return jax.shard_map(
        local_pass,
        mesh=mesh,
        in_specs=(tok_spec, vec_spec, vec_spec, mat_spec, vec_spec, mat_spec, vec_spec, tok_spec),
        out_specs=(tok_spec, tok_spec, grad_vec, grad_vec, grad_mat, grad_vec, grad_mat, grad_vec),
        check_vma=False,
    )
```
